32 devices in a mesh: seq: 8 (over z, x), head: 4 (over y, core).
Axes of the slice: x: 2, y: 2, z: 4, core: 2. Of those that a mesh axis runs over, the one named last changes fastest.
Arguments:
- queries: bfloat16 [8192, 4096], P('seq', 'head'), may hold values from -150 to 150
- keys: bfloat16 [8192, 4096], P('seq', 'head'), may hold values from -7 to 7
- values: bfloat16 [8192, 4096], P('seq', 'head'), may hold values from -6 to 6
- random_holder: int32 [32, 64, 3], P('head', 'seq'), may hold values from 0 to 7, all different within a row; in each aligned block of 8 rows (0 to 7, 8 to 15, ..., all dimensions but the last counted through in order) at most 3 rows name the same one
- random_offset: int32 [32, 64, 3], P('head', 'seq'), may hold values from 0 to 7
- keep: int32 [64], P('seq'), may hold values from 0 to 1, as said below
Outputs:
- packed: bfloat16 [8192, 4096], P('seq', 'head')
The draws below stay inside these ranges and needn't reach their ends.
Inputs may be any that keep to these rules, and one draw needn't show every extreme that they name: `random_holder`: for each head, the 8 query blocks of one index of seq name no index of seq more than 3 times over all their random entries; the 3 entries of one query block and head differ. `keep`: block j is kept where j % 8 == 0 or j % 8 == 7, and not kept where j % 8 == 1.
All inputs are finite; a program needn't handle non-finite values.
Results may differ from the reference program's by a relative error of at most 0.007.
Values may be sent and summed in bfloat16 or wider, within the bound.
A program may use at most 128 MiB of HBM per device.

```python
import math
import jax
import jax.numpy as jnp
import numpy as np
from jax import lax

H = 32
DH = 128
B = 128
G = 2
R = 3
BD = 8
NB = 64
L = 8192
MOST = 3
N_SEQ = 8


def paired_rows(key):
    base = jax.random.fold_in(key, 71)
    key_rows = jnp.clip(jax.random.normal(jax.random.fold_in(base, 1), (L, H * DH), jnp.float32), -6.0, 6.0)
    query_rows = jnp.clip(jax.random.normal(jax.random.fold_in(base, 2), (L, H * DH), jnp.float32), -6.0, 6.0)
    return (query_rows, key_rows)


def draw_queries(key, part):
    query_rows, key_rows = paired_rows(key)
    return query_rows.astype(jnp.bfloat16)


def draw_keys(key, part):
    query_rows, key_rows = paired_rows(key)
    return key_rows.astype(jnp.bfloat16)


def draw_keep(key, part):
    count = L // B
    rolled = jax.random.randint(jax.random.fold_in(key, 113), (count,), 0, 3)
    kept = (rolled == 0).astype(jnp.int32)
    position = jnp.arange(count, dtype=jnp.int32) % BD
    kept = jnp.where(position == 0, 1, kept)
    kept = jnp.where(position == BD - 1, 1, kept)
    kept = jnp.where(position == 1, 0, kept)
    return kept.astype(jnp.int32)


def plant(array, key, smallest, largest):
    extent = array.shape
    spot = [jax.random.randint(jax.random.fold_in(key, axis), (), 0, extent[axis]) for axis in range(len(extent))]
    array = array.at[tuple(spot)].set(smallest)
    longest = extent.index(max(extent))
    spot[longest] = (spot[longest] + 1) % extent[longest]
    return array.at[tuple(spot)].set(largest)


def levels(rng, shape, split, low, high):
    gain = 1.0
    for dim, shards_of in split:
        heights = jax.random.uniform(jax.random.fold_in(jax.random.fold_in(rng, 6), dim), (shards_of,), jnp.float32, low / len(split), high / len(split))
        gain = gain * jnp.repeat(jnp.exp(heights), shape[dim] // shards_of).reshape((-1,) + (1,) * (len(shape) - 1 - dim))
    return gain


def shared_out(rng, own, number, rows, number_of, top, limit, slope):
    sequence = jax.random.permutation(rng, number_of)
    heavy_load, usual = shares(number_of, rows * top, limit, slope, True), shares(number_of, rows * top, limit, slope, False)
    places = jnp.arange(number_of)

    def named(sizes, offset_by):
        used = int((sizes > 0).sum())
        fixed = max(1, used // 4)
        shifted = fixed + (places - fixed + offset_by * (used - fixed)) % max(1, number_of - fixed)
        return jnp.zeros((number_of,), jnp.int32).at[sequence[jnp.where(places < fixed, places, shifted)]].set(jnp.asarray(sizes, jnp.int32))

    sizes = jnp.where(number % 4 == 0, named(heavy_load, number // 4), named(usual, number - number // 4 - 1))
    mixed = jax.random.permutation(jax.random.fold_in(own, 3), number_of)
    source_of, sink = mixed[0:number_of // 2 * 2:2], mixed[1:number_of // 2 * 2:2]
    slack = jnp.minimum(sizes[source_of] - 1, limit - sizes[sink]) // 2
    slack = jnp.where((source_of == sequence[0]) | (sink == sequence[0]) | (sizes[sink] == 0), 0, jnp.maximum(slack, 0))
    shifted = jax.random.randint(jax.random.fold_in(own, 4), (number_of // 2,), 0, 1 << 20) % (slack + 1)
    sizes = sizes.at[source_of].add(-shifted).at[sink].add(shifted)
    labels = jnp.searchsorted(jnp.cumsum(sizes), jnp.arange(rows * top), side="right").astype(jnp.int32)
    table = labels.reshape(top, rows).T
    table = table[jax.random.permutation(jax.random.fold_in(own, 1), rows)]
    offset_by = jax.random.randint(jax.random.fold_in(own, 2), (rows, 1), 0, top)
    return jnp.take_along_axis(table, (jnp.arange(top)[None, :] + offset_by) % top, axis=1)


def shares(amount, total, limit, skew, full):
    weights = [(1 << 20) // math.isqrt(standing ** skew) + 1 for standing in range(1, amount + 1)]
    largest = limit if full else min(limit, max(-(-total // amount), total * weights[0] // sum(weights)))
    least = 1 if total - largest >= amount - 1 else 0
    counts, spare = [largest] + [least] * (amount - 1), total - largest - least * (amount - 1)
    while spare > 0:
        movable = [i for i in range(1, amount) if counts[i] < largest] or [i for i in range(1, amount) if counts[i] < limit]
        whole, left = sum([weights[i] for i in movable]), spare
        for i in movable:
            more = min(limit - counts[i], max(1, left * weights[i] // whole), spare)
            counts[i] = counts[i] + more
            spare = spare - more
    return np.array(counts)


def bell_draw(rng, dims, deviation, bound, split=(), kind=jnp.bfloat16):
    drawn = jax.random.normal(rng, dims, jnp.float32) * deviation
    if len(split) > 0:
        drawn = levels(rng, dims, split, -0.22, 0.18) * drawn
    return jnp.clip(drawn, min=-bound, max=bound).astype(kind)


def setup_inputs(seed: int = 0) -> dict:
    key_of = jax.random.split(jax.random.key(seed), 7)
    queries = draw_queries(jax.random.fold_in(key_of[6], 71), 0)
    keys = draw_keys(jax.random.fold_in(key_of[6], 71), 0)
    values = bell_draw(key_of[2], (L, H * DH), 1.0, 6.0, ((0, 8), (1, 4)))
    random_holder_keys = jax.random.split(jax.random.fold_in(key_of[3], 1), H * NB // BD)
    random_holder_turns = jax.random.permutation(jax.random.fold_in(key_of[3], 3), H * NB // BD)
    random_holder = jax.vmap(lambda own, number: shared_out(jax.random.fold_in(key_of[3], 2), own, number, BD, N_SEQ, R, MOST, 2))(random_holder_keys, random_holder_turns).reshape((H, NB, R))
    random_offset = plant(jax.random.randint(key_of[4], (H, NB, R), 0, BD), jax.random.fold_in(key_of[4], 1), 0, BD - 1).astype(jnp.int32)
    keep = draw_keep(jax.random.fold_in(key_of[6], 71), 0)
    return {"queries": queries, "keys": keys, "values": values, "random_holder": random_holder, "random_offset": random_offset, "keep": keep}


neg_big = -1.0e30


def reference(queries, keys, values, random_holder, random_offset, keep):
    score_scale = 1.0 / (DH ** 0.5)
    query_blocks = queries.reshape(NB, B, H, DH)
    key_blocks = keys.reshape(NB, B, H, DH)
    value_blocks = values.reshape(NB, B, H, DH)
    head_idx = jnp.arange(H, dtype=jnp.int32)[:, None]

    def one_block(block_idx):
        left = jnp.maximum(block_idx - 1, 0)
        right = jnp.minimum(block_idx + 1, NB - 1)
        common = jnp.concatenate((jnp.stack((left, block_idx, right)).astype(jnp.int32), jnp.arange(G, dtype=jnp.int32)))
        common_keys = jnp.transpose(key_blocks[common], (0, 2, 1, 3))
        common_values = jnp.transpose(value_blocks[common], (0, 2, 1, 3))
        chosen = (random_holder[:, block_idx] * BD + random_offset[:, block_idx]).astype(jnp.int32)
        rand_keys = jnp.transpose(key_blocks[chosen, :, head_idx, :], (1, 0, 2, 3))
        rand_values = jnp.transpose(value_blocks[chosen, :, head_idx, :], (1, 0, 2, 3))
        tile_keys = jnp.concatenate((common_keys, rand_keys), axis=0).astype(jnp.float32)
        tile_values = jnp.concatenate((common_values, rand_values), axis=0).astype(jnp.float32)
        live = jnp.concatenate((jnp.stack((block_idx > 0, block_idx >= 0, block_idx < NB - 1)), jnp.ones((G + R,), dtype=bool)))
        query_tile = jnp.transpose(query_blocks[block_idx], (1, 0, 2)).astype(jnp.float32)
        scores = jnp.einsum('hqd,thkd->thqk', query_tile, tile_keys) * score_scale
        row_max = jnp.max(scores, axis=-1)
        weights = jnp.exp(scores - row_max[..., None]).astype(jnp.bfloat16).astype(jnp.float32)
        row_sum = jnp.sum(weights, axis=-1)
        summed = jnp.einsum('thqk,thkd->thqd', weights, tile_values)
        live_b = live[:, None, None]
        overall = jnp.max(jnp.where(live_b, row_max, neg_big), axis=0)
        factor = jnp.where(live_b, jnp.exp(row_max - overall[None]), 0.0)
        numer = jnp.sum(factor[..., None] * summed, axis=0)
        denom = jnp.sum(factor * row_sum, axis=0)
        result = numer / denom[..., None]
        return jnp.transpose(result, (1, 0, 2)).reshape(B, H * DH).astype(jnp.bfloat16)

    attended = lax.map(one_block, jnp.arange(NB, dtype=jnp.int32))
    keep_i = keep.astype(jnp.int32)
    local_rank = (jnp.cumsum(keep_i) - keep_i).astype(jnp.int32)
    place = jnp.where(keep_i > 0, local_rank, NB).astype(jnp.int32)
    packed = jnp.zeros((NB + 1, B, H * DH), jnp.bfloat16).at[place].set(attended)
    return packed[:NB].reshape(L, H * DH)
```

```python
import functools
import math

import jax
import jax.numpy as jnp
from jax import lax
from jax.experimental import pallas as pl
from jax.experimental.pallas import tpu as pltpu
from jax.sharding import PartitionSpec as P

DH = 128
B = 128
G = 2
R = 3

neg_big = -1e30
ANYWHERE = pltpu.CompilerParams(
    dimension_semantics=("arbitrary",), vmem_limit_bytes=60 * 1024 * 1024
)


def halo(block, axis, width):
    count = lax.axis_size(axis)
    forward = [(i, i + 1) for i in range(count - 1)]
    backward = [(target, source) for source, target in forward]
    low = lax.ppermute(block[-width:], axis, forward)
    high = lax.ppermute(block[:width], axis, backward)
    return jnp.concatenate([low, high], axis=0)


def broadcast(block, axis, source):
    block = jnp.where(lax.axis_index(axis) == source, block, jnp.zeros_like(block))
    return lax.psum(block, axis)


def pick_kernel(cap, head_ref, block_ref, k_ref, v_ref, out_ref):
    dest = pl.program_id(0)

    @pl.loop(0, cap)
    def _(j):
        rows = pl.ds(pl.multiple_of(block_ref[dest, j] * B, B), B)
        cols = pl.ds(pl.multiple_of(head_ref[dest, j] * DH, DH), DH)
        out_ref[j, 0] = k_ref[rows, cols]
        out_ref[j, 1] = v_ref[rows, cols]


def pick(keys, values, heads, blocks, seq_count, cap):
    whole = pl.BlockSpec(keys.shape, lambda d, *_: (0, 0))
    return pl.pallas_call(
        functools.partial(pick_kernel, cap),
        out_shape=jax.ShapeDtypeStruct((seq_count * cap, 2, B, DH), keys.dtype),
        grid_spec=pltpu.PrefetchScalarGridSpec(
            num_scalar_prefetch=2,
            grid=(seq_count,),
            in_specs=[whole, whole],
            out_specs=pl.BlockSpec((cap, 2, B, DH), lambda d, *_: (d, 0, 0, 0)),
        ),
        compiler_params=ANYWHERE,
    )(heads, blocks, keys, values)


def attend_kernel(
    blk_dev,
    keep_ref,
    slot_ref,
    live_ref,
    where_ref,
    q_ref,
    k_ref,
    v_ref,
    hk_ref,
    hv_ref,
    gk_ref,
    gv_ref,
    rand_ref,
    out_ref,
):
    scale = 1.0 / math.sqrt(DH)
    head = pl.program_id(0)
    out_ref[...] = jnp.zeros_like(out_ref)

    def tile(ref, halo_ref, i):
        if i < 0:
            return halo_ref[:B]
        if i >= blk_dev:
            return halo_ref[B:]
        return ref[i * B : (i + 1) * B]

    def one(i):
        q = q_ref[i * B : (i + 1) * B]
        near = range(i - 1, i + 2)
        picks = [where_ref[(head * blk_dev + i) * R + r] for r in range(R)]
        k_parts = [
            jnp.concatenate([tile(k_ref, hk_ref, n) for n in near], axis=0),
            gk_ref[...],
            jnp.concatenate([rand_ref[p, 0] for p in picks], axis=0),
        ]
        v_parts = [
            jnp.concatenate([tile(v_ref, hv_ref, n) for n in near], axis=0),
            gv_ref[...],
            jnp.concatenate([rand_ref[p, 1] for p in picks], axis=0),
        ]
        scores = [
            lax.dot_general(
                q, k, (((1,), (1,)), ((), ())), preferred_element_type=jnp.float32
            )
            * scale
            for k in k_parts
        ]
        lanes = lax.broadcasted_iota(jnp.int32, scores[0].shape, 1)
        if i == 0:
            dead = jnp.logical_and(lanes < B, live_ref[0] == 0)
            scores[0] = jnp.where(dead, neg_big, scores[0])
        if i == blk_dev - 1:
            dead = jnp.logical_and(lanes >= 2 * B, live_ref[1] == 0)
            scores[0] = jnp.where(dead, neg_big, scores[0])
        peak = functools.reduce(
            jnp.maximum, [jnp.max(s, axis=-1, keepdims=True) for s in scores]
        )
        numer = jnp.zeros((B, DH), jnp.float32)
        denom = jnp.zeros((B, 1), jnp.float32)
        for s, v in zip(scores, v_parts):
            w = jnp.exp(s - peak).astype(jnp.bfloat16)
            denom = denom + jnp.sum(w.astype(jnp.float32), axis=-1, keepdims=True)
            numer = numer + jnp.dot(w, v, preferred_element_type=jnp.float32)
        rows = pl.ds(pl.multiple_of(slot_ref[i] * B, B), B)
        out_ref[rows, :] = (numer / denom).astype(out_ref.dtype)

    for i in range(blk_dev):
        pl.when(keep_ref[i] > 0)(functools.partial(one, i))


def attend(keep, slot, live, where, q, k, v, hk, hv, gk, gv, rand):
    tok_dev, width_dev = q.shape
    blk_dev, head_dev = tok_dev // B, width_dev // DH

    def column(rows):
        return pl.BlockSpec((rows, DH), lambda h, *_: (0, h))

    return pl.pallas_call(
        functools.partial(attend_kernel, blk_dev),
        out_shape=jax.ShapeDtypeStruct(q.shape, q.dtype),
        grid_spec=pltpu.PrefetchScalarGridSpec(
            num_scalar_prefetch=4,
            grid=(head_dev,),
            in_specs=[column(tok_dev)] * 3
            + [column(2 * B)] * 2
            + [column(G * B)] * 2
            + [pl.BlockSpec(rand.shape, lambda h, *_: (0, 0, 0, 0))],
            out_specs=column(tok_dev),
        ),
        compiler_params=ANYWHERE,
    )(keep, slot, live, where, q, k, v, hk, hv, gk, gv, rand)


def copy_kernel(order_ref, in_ref, out_ref):
    out_ref[...] = in_ref[...]


def take_blocks(blocks, order, cap):
    width = blocks.shape[1]
    return pl.pallas_call(
        copy_kernel,
        out_shape=jax.ShapeDtypeStruct((cap * B, width), blocks.dtype),
        grid_spec=pltpu.PrefetchScalarGridSpec(
            num_scalar_prefetch=1,
            grid=(cap,),
            in_specs=[pl.BlockSpec((B, width), lambda j, order: (order[j], 0))],
            out_specs=pl.BlockSpec((B, width), lambda j, order: (j, 0)),
        ),
        compiler_params=ANYWHERE,
    )(order, blocks)


def merge_kernel(kind_ref, from_ref, old_ref, new_ref, out_ref):
    kind = kind_ref[pl.program_id(0)]

    @pl.when(kind == 0)
    def _():
        out_ref[...] = old_ref[...]

    @pl.when(kind == 1)
    def _():
        out_ref[...] = jnp.zeros_like(out_ref)

    @pl.when(kind == 2)
    def _():
        out_ref[...] = new_ref[...]


def merge_blocks(old, new, kind, place):
    tok_dev, width = old.shape
    return pl.pallas_call(
        merge_kernel,
        out_shape=jax.ShapeDtypeStruct(old.shape, old.dtype),
        grid_spec=pltpu.PrefetchScalarGridSpec(
            num_scalar_prefetch=2,
            grid=(tok_dev // B,),
            in_specs=[
                pl.BlockSpec((B, width), lambda j, kind, place: (j, 0)),
                pl.BlockSpec((B, width), lambda j, kind, place: (place[j], 0)),
            ],
            out_specs=pl.BlockSpec((B, width), lambda j, kind, place: (j, 0)),
        ),
        compiler_params=ANYWHERE,
    )(kind, place, old, new)


def exclusive(flags, axis):
    return jnp.cumsum(flags, axis=axis) - flags


def first_at_least(caps, amount):
    return jnp.sum((amount > jnp.asarray(caps, jnp.int32)).astype(jnp.int32))


def settle(blocks, keep_all, slot, source, distance, me, count, blk_dev):
    i32 = jnp.int32
    devices = jnp.arange(count, dtype=i32)
    slots = jnp.arange(blk_dev, dtype=i32)
    sizes = sorted({0, *range(blk_dev // 2, blk_dev - 1), blk_dev})
    for bit_pos in range((count - 1).bit_length()):
        stride = 2**bit_pos
        at = source - distance % stride
        moving = (keep_all > 0) & (distance // stride % 2 > 0)
        on_slot = ((slot[:, None] == slots) & moving[:, None]).astype(i32)
        on_device = (at[:, None] == devices).astype(i32)
        leaving = jnp.sum(on_device[:, :, None] * on_slot[:, None, :], axis=0)
        needed = jnp.max(jnp.sum(leaving, axis=1))
        nth = exclusive(leaving, 1)
        mine_out, mine_nth = leaving[me], nth[me]
        send = jnp.sum(
            mine_out[:, None] * (mine_nth[:, None] == slots).astype(i32) * slots[:, None], axis=0
        )
        far = jnp.minimum(me + stride, count - 1)
        comes = jnp.where(me + stride < count, leaving[far], 0)
        kind = jnp.where(comes > 0, 2, jnp.where(mine_out > 0, 1, 0)).astype(i32)
        place = jnp.where(comes > 0, nth[far], 0)
        all_pairs = [(i, i - stride) for i in range(stride, count)]
        split = count - stride // 2
        upper = [pair for pair in all_pairs if pair[0] >= split]
        halves = 2 * stride >= count and 0 < len(upper) < len(all_pairs)

        def shifting(cap, pairs, send=send, kind=kind, place=place):
            def run(blocks):
                if cap == 0:
                    return blocks
                moved = lax.ppermute(take_blocks(blocks, send, cap), "seq", pairs)
                return merge_blocks(blocks, moved, kind, jnp.minimum(place, cap - 1))

            return run

        which = first_at_least(sizes[:-1], needed)
        runs = [shifting(cap, all_pairs) for cap in sizes]
        if halves:
            runs += [shifting(cap, upper) for cap in sizes]
            lower = jnp.sum(leaving * (devices < split)[:, None].astype(i32))
            which = which + jnp.where(lower > 0, 0, len(sizes))
        blocks = lax.switch(which, runs, blocks)
    return blocks


def plain_body(queries, keys, values, random_holder, random_offset, keep):
    tok_dev, width_dev = queries.shape
    blk_dev = tok_dev // B
    head_dev = width_dev // DH
    seq_count = lax.axis_size("seq")
    head_count = lax.axis_size("head")
    me = lax.axis_index("seq")
    count_req = blk_dev * R
    total = head_dev * count_req
    i32 = jnp.int32

    code = random_holder * blk_dev + random_offset
    code = jnp.where((keep > 0)[None, :, None], code, -1).reshape(total)
    note = jnp.concatenate([code, keep])
    note = jnp.broadcast_to(note, (seq_count * head_count,) + note.shape)
    table = lax.all_to_all(note, ("seq", "head"), split_axis=0, concat_axis=0, tiled=True)
    table = table.reshape(seq_count, head_count, total + blk_dev)
    keep_all = table[:, 0, total:].reshape(seq_count * blk_dev)
    codes = table[:, :, :total]
    devices = jnp.arange(seq_count, dtype=i32)

    halo_k, halo_v = halo(keys, "seq", B), halo(values, "seq", B)

    named = jnp.where(codes >= 0, codes // blk_dev, -1)
    counts = jnp.sum((named[..., None] == devices).astype(i32), axis=2)
    most = jnp.max(counts)
    onehot = (named[me, lax.axis_index("head")][:, None] == devices).astype(i32)
    mine = exclusive(onehot, 0)
    my_slot = jnp.sum(mine * onehot, axis=1)
    my_holder = jnp.sum(onehot * devices, axis=1)

    group = codes[:, lax.axis_index("head")]
    asks = (named[:, lax.axis_index("head")] == me).astype(i32)
    order = exclusive(asks, 1)
    full = min(total, head_dev * max(2, (count_req + seq_count - 1) // seq_count))
    chosen = asks[..., None] * (order[..., None] == jnp.arange(full, dtype=i32)).astype(i32)
    ask_head = jnp.arange(total, dtype=i32) // count_req
    ask = jnp.where(group >= 0, group % blk_dev, 0) + ask_head[None] * blk_dev
    ask = jnp.sum(chosen * ask[..., None], axis=1)
    pick_head, pick_block = ask // blk_dev, ask % blk_dev

    rank = exclusive(keep_all, 0)
    slot = rank % blk_dev
    source = jnp.arange(seq_count * blk_dev, dtype=i32) // blk_dev
    distance = jnp.where(keep_all > 0, source - rank // blk_dev, 0)
    my_slots = lax.dynamic_slice_in_dim(slot, me * blk_dev, blk_dev)
    live = jnp.stack([me > 0, me < seq_count - 1]).astype(i32)

    caps = sorted({max(1, full * part // 12) for part in range(8, 13)})

    def gathered(cap):
        def run(q, k, v, hk, hv):
            gk, gv = broadcast(jnp.stack((k[: G * B], v[: G * B])), "seq", 0)
            picked = pick(k, v, pick_head, pick_block, seq_count, cap)
            replies = lax.all_to_all(picked, "seq", split_axis=0, concat_axis=0, tiled=True)
            where = jnp.minimum(my_holder * cap + my_slot, seq_count * cap - 1)
            return attend(keep, my_slots, live, where, q, k, v, hk, hv, gk, gv, replies)

        return run

    blocks = lax.switch(
        first_at_least(caps[:-1], most),
        [gathered(cap) for cap in caps],
        queries, keys, values, halo_k, halo_v,
    )

    return settle(blocks, keep_all, slot, source, distance, me, seq_count, blk_dev)


TILE = (2 * B, DH)
SMALL = pltpu.CompilerParams(vmem_limit_bytes=60 * 1024 * 1024)


def fits(planes, tiles, most):
    slots = 2 * (planes - 1) * tiles + 2 * planes * most + most
    return slots * 2 * B * DH * 2 <= 44 * 1024 * 1024


def exchange_kernel(
    count, cz, cx, blk_dev, ztab, xtab, k_ref, v_ref,
    rand_ref, halo_ref, glob_ref, home, zs, zr, xs, own,
    z_send, z_recv, x_send, x_recv, h_send, h_recv, g_send, g_recv, l_sem,
):
    planes = count // 2
    me = lax.axis_index("seq")
    plane, side = me // 2, me % 2
    mate = plane * 2 + 1 - side
    tok = k_ref.shape[0]
    head_dev = k_ref.shape[1] // DH
    barrier = pltpu.get_barrier_semaphore()
    for step in range(1, count):
        peer = lax.rem(me + step, count)
        pl.semaphore_signal(
            barrier, inc=1, device_id={"seq": peer}, device_id_type=pl.DeviceIdType.MESH
        )
    pl.semaphore_wait(barrier, count - 1)

    def remote(src, dst, send, recv, peer):
        return pltpu.make_async_remote_copy(
            src_ref=src, dst_ref=dst, send_sem=send, recv_sem=recv,
            device_id={"seq": peer}, device_id_type=pl.DeviceIdType.MESH,
        )

    tables = (k_ref, v_ref)
    low, high = pl.ds(0, B), pl.ds(B, B)
    first, last = pl.ds(0, B), pl.ds(tok - B, B)
    after = jnp.minimum(me + 1, count - 1)
    before = jnp.maximum(me - 1, 0)
    ups = [
        remote(tables[i].at[last], halo_ref.at[i, low], h_send.at[i], h_recv.at[i], after)
        for i in range(2)
    ]
    downs = [
        remote(tables[i].at[first], halo_ref.at[i, high], h_send.at[2 + i], h_recv.at[2 + i], before)
        for i in range(2)
    ]
    local = [
        pltpu.make_async_copy(tables[i].at[pl.ds(0, G * B)], glob_ref.at[i], l_sem.at[i])
        for i in range(2)
    ]
    to_mate = [
        remote(glob_ref.at[i], glob_ref.at[i], g_send.at[i], g_recv.at[i], mate)
        for i in range(2)
    ]
    onward = [
        remote(
            glob_ref.at[i], glob_ref.at[i], g_send.at[2 + i], g_recv.at[i],
            jnp.minimum(me + 2, count - 1),
        )
        for i in range(2)
    ]

    @pl.when(me == 0)
    def _():
        for c in local:
            c.start()
        for c in local:
            c.wait()
        for c in onward:
            c.start()
        for c in to_mate:
            c.start()

    @pl.when(me < count - 1)
    def _():
        for c in ups:
            c.start()

    @pl.when(me > 0)
    def _():
        for c in downs:
            c.start()

    @pl.when(me == 0)
    def _():
        halo_ref[:, low, :] = jnp.zeros((2, B, k_ref.shape[1]), k_ref.dtype)

    @pl.when(me == count - 1)
    def _():
        halo_ref[:, high, :] = jnp.zeros((2, B, k_ref.shape[1]), k_ref.dtype)

    def load_home(block, carry):
        rows = pl.ds(pl.multiple_of(block * B, B), B)
        for h in range(head_dev):
            cols = slice(h * DH, (h + 1) * DH)
            home[h * blk_dev + block, low, :] = k_ref[rows, cols]
            home[h * blk_dev + block, high, :] = v_ref[rows, cols]
        return carry

    lax.fori_loop(0, blk_dev, load_home, 0)

    def from_slots(dst, src, table, row, cap):
        def one(j, carry):
            dst[j] = src[table[row, j]]
            return carry

        lax.fori_loop(0, cap, one, 0)

    steps = list(range(1, planes))
    steps.sort(key=lambda d: abs(d - planes / 2))
    x_base = (planes - 1) * cz
    z_copies = {
        d: remote(
            zs[d - 1], zr[d - 1], z_send.at[d - 1], z_recv.at[d - 1],
            lax.rem(plane + d, planes) * 2 + side,
        )
        for d in steps
    }
    x_copies = [
        remote(
            xs[d], rand_ref.at[pl.ds(x_base + d * cx, cx)],
            x_send.at[d], x_recv.at[d], mate,
        )
        for d in range(planes)
    ]
    for d in steps:
        from_slots(zs[d - 1], home, ztab, d - 1, cz)
        if d == steps[0]:
            continue
        z_copies[steps[steps.index(d) - 1]].start()
    from_slots(xs[0], home, xtab, 0, cx)
    z_copies[steps[-1]].start()
    from_slots(own, home, xtab, planes, cx)
    x_copies[0].start()

    @pl.when(jnp.logical_and(side == 0, plane > 0))
    def _():
        for c in to_mate:
            c.wait_recv()
        for c in to_mate:
            c.start()

        @pl.when(plane < planes - 1)
        def _():
            for c in onward:
                c.start()

    keep_own = pltpu.make_async_copy(
        own, rand_ref.at[pl.ds(x_base + planes * cx, cx)], l_sem.at[2]
    )
    keep_own.start()
    kept = []
    for d in steps:
        z_copies[d].wait_recv()
        out = pltpu.make_async_copy(
            zr[d - 1], rand_ref.at[pl.ds((d - 1) * cz, cz)], l_sem.at[2 + d]
        )
        out.start()
        kept.append(out)
        from_slots(xs[d], zr[d - 1], xtab, d, cx)
        x_copies[d].start()

    @pl.when(side == 1)
    def _():
        for c in to_mate:
            c.wait_recv()

    @pl.when(side == 0)
    def _():
        for c in to_mate:
            c.wait_send()

        @pl.when(plane < planes - 1)
        def _():
            for c in onward:
                c.wait_send()

    @pl.when(me < count - 1)
    def _():
        for c in ups:
            c.wait_send()
        for c in downs:
            c.wait_recv()

    @pl.when(me > 0)
    def _():
        for c in downs:
            c.wait_send()
        for c in ups:
            c.wait_recv()

    keep_own.wait()
    for c in kept:
        c.wait()
    for d in steps:
        z_copies[d].wait_send()
    for c in x_copies:
        c.wait()


def exchange(count, level, cz, cx, slots, blk_dev, ztab, xtab, keys, values):
    planes = count // 2
    tok, width = keys.shape
    smem = pl.BlockSpec(memory_space=pltpu.SMEM)
    vmem = pl.BlockSpec(memory_space=pltpu.VMEM)
    dtype = keys.dtype
    dma = pltpu.SemaphoreType.DMA
    return pl.pallas_call(
        functools.partial(exchange_kernel, count, cz, cx, blk_dev),
        out_shape=(
            jax.ShapeDtypeStruct((slots, *TILE), dtype),
            jax.ShapeDtypeStruct((2, 2 * B, width), dtype),
            jax.ShapeDtypeStruct((2, G * B, width), dtype),
        ),
        in_specs=[smem, smem, vmem, vmem],
        out_specs=(pl.BlockSpec(memory_space=pl.ANY), vmem, vmem),
        scratch_shapes=[
            pltpu.VMEM((tok // B * (width // DH), *TILE), dtype),
            [pltpu.VMEM((cz, *TILE), dtype) for _ in range(planes - 1)],
            [pltpu.VMEM((cz, *TILE), dtype) for _ in range(planes - 1)],
            [pltpu.VMEM((cx, *TILE), dtype) for _ in range(planes)],
            pltpu.VMEM((cx, *TILE), dtype),
            dma((planes - 1,)), dma((planes - 1,)),
            dma((planes,)), dma((planes,)),
            dma((4,)), dma((4,)), dma((4,)), dma((2,)), dma((2 + planes,)),
        ],
        compiler_params=pltpu.CompilerParams(
            collective_id=level, has_side_effects=True,
            vmem_limit_bytes=60 * 1024 * 1024,
        ),
    )(ztab, xtab, keys, values)


CHUNK = 8


def near_far_kernel(
    blk_dev, keep_ref, slot_ref, live_ref, where_ref, used_ref,
    q_ref, k_ref, v_ref, hk_ref, hv_ref, gk_ref, gv_ref, rand_hbm, out_ref, rand_ref, sems,
):
    scale = 1.0 / math.sqrt(DH)
    head = pl.program_id(0)
    chunks = rand_hbm.shape[0] // CHUNK

    @pl.when(head == 0)
    def _():
        def copy(c):
            rows = pl.ds(c * CHUNK, CHUNK)
            return pltpu.make_async_copy(rand_hbm.at[rows], rand_ref.at[rows], sems.at[c])

        for c in range(chunks):
            pl.when(c * CHUNK < used_ref[0])(lambda c=c: copy(c).start())
        for c in range(chunks):
            pl.when(c * CHUNK < used_ref[0])(lambda c=c: copy(c).wait())

    out_ref[...] = jnp.zeros_like(out_ref)

    def tile(ref, halo_ref, i):
        if i < 0:
            return halo_ref[0, :B]
        if i >= blk_dev:
            return halo_ref[0, B:]
        return ref[i * B : (i + 1) * B]

    def one(i):
        q = q_ref[i * B : (i + 1) * B]
        near = range(i - 1, i + 2)
        picks = [where_ref[(head * blk_dev + i) * R + r] for r in range(R)]
        k_parts = [
            jnp.concatenate([tile(k_ref, hk_ref, n) for n in near], axis=0),
            gk_ref[0],
            jnp.concatenate([rand_ref[p, :B] for p in picks], axis=0),
        ]
        v_parts = [
            jnp.concatenate([tile(v_ref, hv_ref, n) for n in near], axis=0),
            gv_ref[0],
            jnp.concatenate([rand_ref[p, B:] for p in picks], axis=0),
        ]
        scores = [
            lax.dot_general(
                q, k, (((1,), (1,)), ((), ())), preferred_element_type=jnp.float32
            )
            * scale
            for k in k_parts
        ]
        lanes = lax.broadcasted_iota(jnp.int32, scores[0].shape, 1)
        if i == 0:
            dead = jnp.logical_and(lanes < B, live_ref[0] == 0)
            scores[0] = jnp.where(dead, neg_big, scores[0])
        if i == blk_dev - 1:
            dead = jnp.logical_and(lanes >= 2 * B, live_ref[1] == 0)
            scores[0] = jnp.where(dead, neg_big, scores[0])
        peak = functools.reduce(
            jnp.maximum, [jnp.max(s, axis=-1, keepdims=True) for s in scores]
        )
        numer = jnp.zeros((B, DH), jnp.float32)
        denom = jnp.zeros((B, 1), jnp.float32)
        for s, v in zip(scores, v_parts):
            w = jnp.exp(s - peak).astype(jnp.bfloat16)
            denom = denom + jnp.sum(w.astype(jnp.float32), axis=-1, keepdims=True)
            numer = numer + jnp.dot(w, v, preferred_element_type=jnp.float32)
        rows = pl.ds(pl.multiple_of(slot_ref[i] * B, B), B)
        out_ref[rows, :] = (numer / denom).astype(out_ref.dtype)

    for i in range(blk_dev):
        pl.when(keep_ref[i] > 0)(functools.partial(one, i))


def near_far(keep, slot, live, where, used, q, k, v, halo_kv, glob, rand):
    tok_dev, width_dev = q.shape
    blk_dev, head_dev = tok_dev // B, width_dev // DH

    def column(rows):
        return pl.BlockSpec((rows, DH), lambda h, *_: (0, h))

    def part(rows, which):
        return pl.BlockSpec((1, rows, DH), lambda h, *_: (which, 0, h))

    return pl.pallas_call(
        functools.partial(near_far_kernel, blk_dev),
        out_shape=jax.ShapeDtypeStruct(q.shape, q.dtype),
        grid_spec=pltpu.PrefetchScalarGridSpec(
            num_scalar_prefetch=5,
            grid=(head_dev,),
            in_specs=[column(tok_dev)] * 3
            + [part(2 * B, 0), part(2 * B, 1), part(G * B, 0), part(G * B, 1)]
            + [pl.BlockSpec(memory_space=pl.ANY)],
            out_specs=column(tok_dev),
            scratch_shapes=[
                pltpu.VMEM(rand.shape, rand.dtype),
                pltpu.SemaphoreType.DMA((rand.shape[0] // CHUNK,)),
            ],
        ),
        compiler_params=ANYWHERE,
    )(keep, slot, live, where, used, q, k, v, halo_kv, halo_kv, glob, glob, rand)


def levels(tiles, most):
    caps = []
    for part in (22, 24, 26, 28, 30, 32, 36):
        cz = min(tiles, tiles * part // 64)
        caps.append((cz, min(most, max(1, most * (part // 2 + 4) // 24))))
    caps.append((tiles, most))
    return sorted(set(caps))


def body(queries, keys, values, random_holder, random_offset, keep):
    tok_dev, width_dev = queries.shape
    blk_dev = tok_dev // B
    head_dev = width_dev // DH
    count = lax.axis_size("seq")
    head_count = lax.axis_size("head")
    count_req = blk_dev * R
    total = head_dev * count_req
    tiles = head_dev * blk_dev
    most = min(tiles, head_dev * max(2, (count_req + count - 1) // count))
    planes = count // 2
    if count % 2 or planes < 2 or not fits(planes, tiles, most):
        return plain_body(queries, keys, values, random_holder, random_offset, keep)
    me = lax.axis_index("seq")
    plane, side = me // 2, me % 2
    mate = me + 1 - 2 * side
    i32, f32 = jnp.int32, jnp.float32

    code = random_holder * blk_dev + random_offset
    code = jnp.where((keep > 0)[None, :, None], code, -1).reshape(total)
    note = jnp.concatenate([code, keep])
    note = jnp.broadcast_to(note, (count * head_count,) + note.shape)
    table = lax.all_to_all(note, ("seq", "head"), split_axis=0, concat_axis=0, tiled=True)
    table = table.reshape(count, head_count, total + blk_dev)
    keep_all = table[:, 0, total:].reshape(count * blk_dev)
    codes = table[:, :, :total].reshape(count, head_count, head_dev, 1, count_req)

    blocks = jnp.arange(count * blk_dev, dtype=i32)[:, None]
    need = jnp.max((codes == blocks).astype(i32), axis=-1)
    need = need.reshape(count, head_count, head_dev, count, blk_dev)
    both = jnp.max(need.reshape(planes, 2, *need.shape[1:]), axis=1)
    devices = jnp.arange(count, dtype=i32)
    away = (devices[None] // 2 != jnp.arange(planes, dtype=i32)[:, None]).astype(i32)
    most_z = jnp.max(jnp.sum(both, axis=(2, 4)) * away[:, None])
    most_x = jnp.max(jnp.sum(need, axis=(2, 4)))

    group = lax.axis_index("head")

    def flat(array):
        array = lax.dynamic_index_in_dim(array, group, 1, keepdims=False)
        return jnp.transpose(array, (0, 2, 1, 3)).reshape(array.shape[0], count, tiles)

    want, want_z = flat(need), flat(both)
    order = jnp.arange(tiles, dtype=i32)
    before = (order[:, None] < order[None]).astype(f32)

    def places(flags):
        got = jnp.dot(flags.astype(jnp.bfloat16), before.astype(jnp.bfloat16), preferred_element_type=f32)
        return got.astype(i32)

    slot_x, slot_z = places(want), places(want_z)

    def listed(flags, slots, worth, cap):
        hit = flags[:, None] * (slots[:, None] == jnp.arange(cap, dtype=i32)[:, None]).astype(i32)
        return jnp.sum(hit * worth[:, None], axis=2)

    def at(array, i):
        return lax.dynamic_index_in_dim(array, i, 0, keepdims=False)

    steps = jnp.arange(planes, dtype=i32)
    goal = (plane + steps[1:]) % planes
    mine_z, mine_slot_z = jnp.take(want_z[:, me], goal, axis=0), jnp.take(slot_z[:, me], goal, axis=0)
    plain = jnp.broadcast_to(order, (planes + 1, tiles))
    ztab = listed(mine_z, mine_slot_z, plain[: planes - 1], tiles)
    here = at(slot_z, plane)
    source = ((plane - steps) % planes) * 2 + side
    worth = jnp.where((steps == 0)[:, None], order, jnp.take(here, source, axis=0))
    asked = jnp.concatenate([jnp.take(at(want, mate), source, axis=0), at(want, me)[me][None]])
    asked_slot = jnp.concatenate([jnp.take(at(slot_x, mate), source, axis=0), at(slot_x, me)[me][None]])
    xtab = listed(asked, asked_slot, jnp.concatenate([worth, order[None]]), most)

    caps = levels(tiles, most)
    cz_of = jnp.asarray([c[0] for c in caps], i32)
    cx_of = jnp.asarray([c[1] for c in caps], i32)
    level = jnp.sum(((most_z > cz_of) | (most_x > cx_of))[:-1].astype(i32))
    cz, cx = cz_of[level], cx_of[level]
    gap = (plane - devices // 2) % planes
    x_base = (planes - 1) * cz
    straight = jnp.where(devices == me, x_base + planes * cx, (gap - 1) * cz)
    start = jnp.where(devices % 2 == side, straight, x_base + gap * cx)
    by_z = ((devices % 2 == side) & (devices != me))[:, None]
    spot = start[:, None] + jnp.where(by_z, here, at(slot_x, me))
    spot = jnp.transpose(spot.reshape(count, head_dev, blk_dev), (1, 0, 2)).reshape(head_dev, 1, count * blk_dev)
    picks = (random_holder * blk_dev + random_offset).reshape(head_dev, count_req, 1)
    hits = (picks == jnp.arange(count * blk_dev, dtype=i32)).astype(i32)
    where = jnp.sum(hits * spot, axis=2).reshape(total)
    used = x_base + (planes + 1) * cx

    slots_all = -(-max((planes - 1) * c[0] + (planes + 1) * c[1] for c in caps) // CHUNK) * CHUNK
    where = jnp.minimum(where, slots_all - 1)

    def exchanged(number, caps):
        def run(ztab, xtab, k, v):
            return exchange(count, number, *caps, slots_all, blk_dev, ztab, xtab, k, v)

        return run

    rand, halo_kv, glob = lax.switch(
        level, [exchanged(n, c) for n, c in enumerate(caps)], ztab, xtab, keys, values
    )

    rank = exclusive(keep_all, 0)
    slot = rank % blk_dev
    source = jnp.arange(count * blk_dev, dtype=i32) // blk_dev
    distance = jnp.where(keep_all > 0, source - rank // blk_dev, 0)
    my_slots = lax.dynamic_slice_in_dim(slot, me * blk_dev, blk_dev)
    live = jnp.stack([me > 0, me < count - 1]).astype(i32)
    blocks = near_far(
        keep, my_slots, live, where, used[None], queries, keys, values, halo_kv, glob, rand
    )
    return settle(blocks, keep_all, slot, source, distance, me, count, blk_dev)


def solution(mesh):
    in_specs = (
        P("seq", "head"),
        P("seq", "head"),
        P("seq", "head"),
        P("head", "seq", None),
        P("head", "seq", None),
        P("seq"),
    )
    out_specs = P("seq", "head")
    return jax.shard_map(body, mesh=mesh, in_specs=in_specs, out_specs=out_specs, check_vma=False)
```

```python
import functools
import math

import jax
import jax.numpy as jnp
from jax import lax
from jax.experimental import pallas as pl
from jax.experimental.pallas import tpu as pltpu
from jax.sharding import PartitionSpec as P

DH = 128
B = 128
G = 2
R = 3

neg_big = -1e30
ANYWHERE = pltpu.CompilerParams(
    dimension_semantics=("arbitrary",), vmem_limit_bytes=60 * 1024 * 1024
)


def halo(block, axis, width):
    count = lax.axis_size(axis)
    forward = [(i, i + 1) for i in range(count - 1)]
    backward = [(target, source) for source, target in forward]
    low = lax.ppermute(block[-width:], axis, forward)
    high = lax.ppermute(block[:width], axis, backward)
    return jnp.concatenate([low, high], axis=0)


def broadcast(block, axis, source):
    block = jnp.where(lax.axis_index(axis) == source, block, jnp.zeros_like(block))
    return lax.psum(block, axis)


def pick_kernel(cap, head_ref, block_ref, k_ref, v_ref, out_ref):
    dest = pl.program_id(0)

    @pl.loop(0, cap)
    def _(j):
        rows = pl.ds(pl.multiple_of(block_ref[dest, j] * B, B), B)
        cols = pl.ds(pl.multiple_of(head_ref[dest, j] * DH, DH), DH)
        out_ref[j, 0] = k_ref[rows, cols]
        out_ref[j, 1] = v_ref[rows, cols]


def pick(keys, values, heads, blocks, seq_count, cap):
    whole = pl.BlockSpec(keys.shape, lambda d, *_: (0, 0))
    return pl.pallas_call(
        functools.partial(pick_kernel, cap),
        out_shape=jax.ShapeDtypeStruct((seq_count * cap, 2, B, DH), keys.dtype),
        grid_spec=pltpu.PrefetchScalarGridSpec(
            num_scalar_prefetch=2,
            grid=(seq_count,),
            in_specs=[whole, whole],
            out_specs=pl.BlockSpec((cap, 2, B, DH), lambda d, *_: (d, 0, 0, 0)),
        ),
        compiler_params=ANYWHERE,
    )(heads, blocks, keys, values)


def attend_kernel(
    blk_dev,
    keep_ref,
    slot_ref,
    live_ref,
    where_ref,
    q_ref,
    k_ref,
    v_ref,
    hk_ref,
    hv_ref,
    gk_ref,
    gv_ref,
    rand_ref,
    out_ref,
):
    scale = 1.0 / math.sqrt(DH)
    head = pl.program_id(0)
    out_ref[...] = jnp.zeros_like(out_ref)

    def tile(ref, halo_ref, i):
        if i < 0:
            return halo_ref[:B]
        if i >= blk_dev:
            return halo_ref[B:]
        return ref[i * B : (i + 1) * B]

    def one(i):
        q = q_ref[i * B : (i + 1) * B]
        near = range(i - 1, i + 2)
        picks = [where_ref[(head * blk_dev + i) * R + r] for r in range(R)]
        k_parts = [
            jnp.concatenate([tile(k_ref, hk_ref, n) for n in near], axis=0),
            gk_ref[...],
            jnp.concatenate([rand_ref[p, 0] for p in picks], axis=0),
        ]
        v_parts = [
            jnp.concatenate([tile(v_ref, hv_ref, n) for n in near], axis=0),
            gv_ref[...],
            jnp.concatenate([rand_ref[p, 1] for p in picks], axis=0),
        ]
        scores = [
            lax.dot_general(
                q, k, (((1,), (1,)), ((), ())), preferred_element_type=jnp.float32
            )
            * scale
            for k in k_parts
        ]
        lanes = lax.broadcasted_iota(jnp.int32, scores[0].shape, 1)
        if i == 0:
            dead = jnp.logical_and(lanes < B, live_ref[0] == 0)
            scores[0] = jnp.where(dead, neg_big, scores[0])
        if i == blk_dev - 1:
            dead = jnp.logical_and(lanes >= 2 * B, live_ref[1] == 0)
            scores[0] = jnp.where(dead, neg_big, scores[0])
        peak = functools.reduce(
            jnp.maximum, [jnp.max(s, axis=-1, keepdims=True) for s in scores]
        )
        numer = jnp.zeros((B, DH), jnp.float32)
        denom = jnp.zeros((B, 1), jnp.float32)
        for s, v in zip(scores, v_parts):
            w = jnp.exp(s - peak).astype(jnp.bfloat16)
            denom = denom + jnp.sum(w.astype(jnp.float32), axis=-1, keepdims=True)
            numer = numer + jnp.dot(w, v, preferred_element_type=jnp.float32)
        rows = pl.ds(pl.multiple_of(slot_ref[i] * B, B), B)
        out_ref[rows, :] = (numer / denom).astype(out_ref.dtype)

    for i in range(blk_dev):
        pl.when(keep_ref[i] > 0)(functools.partial(one, i))


def attend(keep, slot, live, where, q, k, v, hk, hv, gk, gv, rand):
    tok_dev, width_dev = q.shape
    blk_dev, head_dev = tok_dev // B, width_dev // DH

    def column(rows):
        return pl.BlockSpec((rows, DH), lambda h, *_: (0, h))

    return pl.pallas_call(
        functools.partial(attend_kernel, blk_dev),
        out_shape=jax.ShapeDtypeStruct(q.shape, q.dtype),
        grid_spec=pltpu.PrefetchScalarGridSpec(
            num_scalar_prefetch=4,
            grid=(head_dev,),
            in_specs=[column(tok_dev)] * 3
            + [column(2 * B)] * 2
            + [column(G * B)] * 2
            + [pl.BlockSpec(rand.shape, lambda h, *_: (0, 0, 0, 0))],
            out_specs=column(tok_dev),
        ),
        compiler_params=ANYWHERE,
    )(keep, slot, live, where, q, k, v, hk, hv, gk, gv, rand)


def copy_kernel(order_ref, in_ref, out_ref):
    out_ref[...] = in_ref[...]


def take_blocks(blocks, order, cap):
    width = blocks.shape[1]
    return pl.pallas_call(
        copy_kernel,
        out_shape=jax.ShapeDtypeStruct((cap * B, width), blocks.dtype),
        grid_spec=pltpu.PrefetchScalarGridSpec(
            num_scalar_prefetch=1,
            grid=(cap,),
            in_specs=[pl.BlockSpec((B, width), lambda j, order: (order[j], 0))],
            out_specs=pl.BlockSpec((B, width), lambda j, order: (j, 0)),
        ),
        compiler_params=ANYWHERE,
    )(order, blocks)


def merge_kernel(kind_ref, from_ref, old_ref, new_ref, out_ref):
    kind = kind_ref[pl.program_id(0)]

    @pl.when(kind == 0)
    def _():
        out_ref[...] = old_ref[...]

    @pl.when(kind == 1)
    def _():
        out_ref[...] = jnp.zeros_like(out_ref)

    @pl.when(kind == 2)
    def _():
        out_ref[...] = new_ref[...]


def merge_blocks(old, new, kind, place):
    tok_dev, width = old.shape
    return pl.pallas_call(
        merge_kernel,
        out_shape=jax.ShapeDtypeStruct(old.shape, old.dtype),
        grid_spec=pltpu.PrefetchScalarGridSpec(
            num_scalar_prefetch=2,
            grid=(tok_dev // B,),
            in_specs=[
                pl.BlockSpec((B, width), lambda j, kind, place: (j, 0)),
                pl.BlockSpec((B, width), lambda j, kind, place: (place[j], 0)),
            ],
            out_specs=pl.BlockSpec((B, width), lambda j, kind, place: (j, 0)),
        ),
        compiler_params=ANYWHERE,
    )(kind, place, old, new)


def exclusive(flags, axis):
    return jnp.cumsum(flags, axis=axis) - flags


def first_at_least(caps, amount):
    return jnp.sum((amount > jnp.asarray(caps, jnp.int32)).astype(jnp.int32))


def settle(blocks, keep_all, slot, source, distance, me, count, blk_dev):
    i32 = jnp.int32
    devices = jnp.arange(count, dtype=i32)
    slots = jnp.arange(blk_dev, dtype=i32)
    sizes = sorted({0, *range(blk_dev // 2, blk_dev - 1), blk_dev})
    for bit_pos in range((count - 1).bit_length()):
        stride = 2**bit_pos
        at = source - distance % stride
        moving = (keep_all > 0) & (distance // stride % 2 > 0)
        on_slot = ((slot[:, None] == slots) & moving[:, None]).astype(i32)
        on_device = (at[:, None] == devices).astype(i32)
        leaving = jnp.sum(on_device[:, :, None] * on_slot[:, None, :], axis=0)
        needed = jnp.max(jnp.sum(leaving, axis=1))
        nth = exclusive(leaving, 1)
        mine_out, mine_nth = leaving[me], nth[me]
        send = jnp.sum(
            mine_out[:, None] * (mine_nth[:, None] == slots).astype(i32) * slots[:, None], axis=0
        )
        far = jnp.minimum(me + stride, count - 1)
        comes = jnp.where(me + stride < count, leaving[far], 0)
        kind = jnp.where(comes > 0, 2, jnp.where(mine_out > 0, 1, 0)).astype(i32)
        place = jnp.where(comes > 0, nth[far], 0)
        all_pairs = [(i, i - stride) for i in range(stride, count)]
        split = count - stride // 2
        upper = [pair for pair in all_pairs if pair[0] >= split]
        halves = 2 * stride >= count and 0 < len(upper) < len(all_pairs)

        def shifting(cap, pairs, send=send, kind=kind, place=place):
            def run(blocks):
                if cap == 0:
                    return blocks
                moved = lax.ppermute(take_blocks(blocks, send, cap), "seq", pairs)
                return merge_blocks(blocks, moved, kind, jnp.minimum(place, cap - 1))

            return run

        which = first_at_least(sizes[:-1], needed)
        runs = [shifting(cap, all_pairs) for cap in sizes]
        if halves:
            runs += [shifting(cap, upper) for cap in sizes]
            lower = jnp.sum(leaving * (devices < split)[:, None].astype(i32))
            which = which + jnp.where(lower > 0, 0, len(sizes))
        blocks = lax.switch(which, runs, blocks)
    return blocks


def plain_body(queries, keys, values, random_holder, random_offset, keep):
    tok_dev, width_dev = queries.shape
    blk_dev = tok_dev // B
    head_dev = width_dev // DH
    seq_count = lax.axis_size("seq")
    head_count = lax.axis_size("head")
    me = lax.axis_index("seq")
    count_req = blk_dev * R
    total = head_dev * count_req
    i32 = jnp.int32

    code = random_holder * blk_dev + random_offset
    code = jnp.where((keep > 0)[None, :, None], code, -1).reshape(total)
    note = jnp.concatenate([code, keep])
    note = jnp.broadcast_to(note, (seq_count * head_count,) + note.shape)
    table = lax.all_to_all(note, ("seq", "head"), split_axis=0, concat_axis=0, tiled=True)
    table = table.reshape(seq_count, head_count, total + blk_dev)
    keep_all = table[:, 0, total:].reshape(seq_count * blk_dev)
    codes = table[:, :, :total]
    devices = jnp.arange(seq_count, dtype=i32)

    halo_k, halo_v = halo(keys, "seq", B), halo(values, "seq", B)

    named = jnp.where(codes >= 0, codes // blk_dev, -1)
    counts = jnp.sum((named[..., None] == devices).astype(i32), axis=2)
    most = jnp.max(counts)
    onehot = (named[me, lax.axis_index("head")][:, None] == devices).astype(i32)
    mine = exclusive(onehot, 0)
    my_slot = jnp.sum(mine * onehot, axis=1)
    my_holder = jnp.sum(onehot * devices, axis=1)

    group = codes[:, lax.axis_index("head")]
    asks = (named[:, lax.axis_index("head")] == me).astype(i32)
    order = exclusive(asks, 1)
    full = min(total, head_dev * max(2, (count_req + seq_count - 1) // seq_count))
    chosen = asks[..., None] * (order[..., None] == jnp.arange(full, dtype=i32)).astype(i32)
    ask_head = jnp.arange(total, dtype=i32) // count_req
    ask = jnp.where(group >= 0, group % blk_dev, 0) + ask_head[None] * blk_dev
    ask = jnp.sum(chosen * ask[..., None], axis=1)
    pick_head, pick_block = ask // blk_dev, ask % blk_dev

    rank = exclusive(keep_all, 0)
    slot = rank % blk_dev
    source = jnp.arange(seq_count * blk_dev, dtype=i32) // blk_dev
    distance = jnp.where(keep_all > 0, source - rank // blk_dev, 0)
    my_slots = lax.dynamic_slice_in_dim(slot, me * blk_dev, blk_dev)
    live = jnp.stack([me > 0, me < seq_count - 1]).astype(i32)

    caps = sorted({max(1, full * part // 12) for part in range(8, 13)})

    def gathered(cap):
        def run(q, k, v, hk, hv):
            gk, gv = broadcast(jnp.stack((k[: G * B], v[: G * B])), "seq", 0)
            picked = pick(k, v, pick_head, pick_block, seq_count, cap)
            replies = lax.all_to_all(picked, "seq", split_axis=0, concat_axis=0, tiled=True)
            where = jnp.minimum(my_holder * cap + my_slot, seq_count * cap - 1)
            return attend(keep, my_slots, live, where, q, k, v, hk, hv, gk, gv, replies)

        return run

    blocks = lax.switch(
        first_at_least(caps[:-1], most),
        [gathered(cap) for cap in caps],
        queries, keys, values, halo_k, halo_v,
    )

    return settle(blocks, keep_all, slot, source, distance, me, seq_count, blk_dev)


TILE = (2 * B, DH)
SMALL = pltpu.CompilerParams(vmem_limit_bytes=60 * 1024 * 1024)


def fits(planes, tiles, most):
    slots = 2 * (planes - 1) * tiles + 2 * planes * most + most
    return slots * 2 * B * DH * 2 <= 44 * 1024 * 1024


def exchange_kernel(
    count, cz, cx, blk_dev, ztab, xtab, k_ref, v_ref,
    rand_ref, halo_ref, glob_ref, home, zs, zr, xs, own,
    z_send, z_recv, x_send, x_recv, h_send, h_recv, g_send, g_recv, l_sem,
):
    planes = count // 2
    me = lax.axis_index("seq")
    plane, side = me // 2, me % 2
    mate = plane * 2 + 1 - side
    tok = k_ref.shape[0]
    head_dev = k_ref.shape[1] // DH
    barrier = pltpu.get_barrier_semaphore()
    for step in range(1, count):
        peer = lax.rem(me + step, count)
        pl.semaphore_signal(
            barrier, inc=1, device_id={"seq": peer}, device_id_type=pl.DeviceIdType.MESH
        )
    pl.semaphore_wait(barrier, count - 1)

    def remote(src, dst, send, recv, peer):
        return pltpu.make_async_remote_copy(
            src_ref=src, dst_ref=dst, send_sem=send, recv_sem=recv,
            device_id={"seq": peer}, device_id_type=pl.DeviceIdType.MESH,
        )

    tables = (k_ref, v_ref)
    low, high = pl.ds(0, B), pl.ds(B, B)
    first, last = pl.ds(0, B), pl.ds(tok - B, B)
    after = jnp.minimum(me + 1, count - 1)
    before = jnp.maximum(me - 1, 0)
    ups = [
        remote(tables[i].at[last], halo_ref.at[i, low], h_send.at[i], h_recv.at[i], after)
        for i in range(2)
    ]
    downs = [
        remote(tables[i].at[first], halo_ref.at[i, high], h_send.at[2 + i], h_recv.at[2 + i], before)
        for i in range(2)
    ]
    local = [
        pltpu.make_async_copy(tables[i].at[pl.ds(0, G * B)], glob_ref.at[i], l_sem.at[i])
        for i in range(2)
    ]
    item = glob_ref.at[side]
    chain = remote(item, item, g_send.at[0], g_recv.at[0], jnp.minimum(me + 2, count - 1))
    swap = remote(item, item, g_send.at[1], g_recv.at[1], mate)
    extra = remote(glob_ref.at[1], glob_ref.at[1], g_send.at[2], g_recv.at[0], mate)

    @pl.when(me == 0)
    def _():
        for c in local:
            c.start()
        for c in local:
            c.wait()
        chain.start()
        extra.start()
        swap.start()

    def pass_on():
        @pl.when(me > 0)
        def _():
            chain.wait_recv()

            @pl.when(plane < planes - 1)
            def _():
                chain.start()

            @pl.when(me > 1)
            def _():
                swap.start()

    @pl.when(me < count - 1)
    def _():
        for c in ups:
            c.start()

    @pl.when(me > 0)
    def _():
        for c in downs:
            c.start()

    @pl.when(me == 0)
    def _():
        halo_ref[:, low, :] = jnp.zeros((2, B, k_ref.shape[1]), k_ref.dtype)

    @pl.when(me == count - 1)
    def _():
        halo_ref[:, high, :] = jnp.zeros((2, B, k_ref.shape[1]), k_ref.dtype)

    def load_home(block, carry):
        rows = pl.ds(pl.multiple_of(block * B, B), B)
        for h in range(head_dev):
            cols = slice(h * DH, (h + 1) * DH)
            home[h * blk_dev + block, low, :] = k_ref[rows, cols]
            home[h * blk_dev + block, high, :] = v_ref[rows, cols]
        return carry

    lax.fori_loop(0, blk_dev, load_home, 0)

    def from_slots(dst, src, table, row, cap):
        def one(j, carry):
            dst[j] = src[table[row, j]]
            return carry

        lax.fori_loop(0, cap, one, 0)

    half = planes // 2
    lower = plane < half
    rest = [d for d in range(1, planes) if d != half]
    rising, falling = [half, *rest], [half, *reversed(rest)]
    x_base = (planes - 1) * cz
    z_copies = {
        d: remote(
            zs[d - 1], zr[d - 1], z_send.at[d - 1], z_recv.at[d - 1],
            lax.rem(plane + d, planes) * 2 + side,
        )
        for d in rising
    }
    x_copies = [
        remote(
            xs[d], rand_ref.at[pl.ds(x_base + d * cx, cx)],
            x_send.at[d], x_recv.at[d], mate,
        )
        for d in range(planes)
    ]
    from_slots(zs[half - 1], home, ztab, half - 1, cz)
    from_slots(xs[0], home, xtab, 0, cx)
    z_copies[half].start()
    for d in rest:
        from_slots(zs[d - 1], home, ztab, d - 1, cz)
    x_copies[0].start()

    @pl.when(lower)
    def _():
        pass_on()
        for d in falling[1:]:
            z_copies[d].start()

    @pl.when(jnp.logical_not(lower))
    def _():
        for d in rising[1:]:
            z_copies[d].start()
        pass_on()

    from_slots(own, home, xtab, planes, cx)
    keep_own = pltpu.make_async_copy(
        own, rand_ref.at[pl.ds(x_base + planes * cx, cx)], l_sem.at[2]
    )
    keep_own.start()
    outs = {
        d: pltpu.make_async_copy(
            zr[d - 1], rand_ref.at[pl.ds((d - 1) * cz, cz)], l_sem.at[2 + d]
        )
        for d in rising
    }

    def forward(d):
        z_copies[d].wait_recv()
        outs[d].start()
        from_slots(xs[d], zr[d - 1], xtab, d, cx)
        x_copies[d].start()

    @pl.when(lower)
    def _():
        for d in falling:
            forward(d)

    @pl.when(jnp.logical_not(lower))
    def _():
        for d in rising:
            forward(d)

    @pl.when(me > 0)
    def _():
        swap.wait_recv()

    @pl.when(plane < planes - 1)
    def _():
        chain.wait_send()

    @pl.when(me == 0)
    def _():
        extra.wait_send()

    @pl.when(me != 1)
    def _():
        swap.wait_send()

    @pl.when(me < count - 1)
    def _():
        for c in ups:
            c.wait_send()
        for c in downs:
            c.wait_recv()

    @pl.when(me > 0)
    def _():
        for c in downs:
            c.wait_send()
        for c in ups:
            c.wait_recv()

    keep_own.wait()
    for d in rising:
        outs[d].wait()
        z_copies[d].wait_send()
    for c in x_copies:
        c.wait()


def exchange(count, level, cz, cx, slots, blk_dev, ztab, xtab, keys, values):
    planes = count // 2
    tok, width = keys.shape
    smem = pl.BlockSpec(memory_space=pltpu.SMEM)
    vmem = pl.BlockSpec(memory_space=pltpu.VMEM)
    dtype = keys.dtype
    dma = pltpu.SemaphoreType.DMA
    return pl.pallas_call(
        functools.partial(exchange_kernel, count, cz, cx, blk_dev),
        out_shape=(
            jax.ShapeDtypeStruct((slots, *TILE), dtype),
            jax.ShapeDtypeStruct((2, 2 * B, width), dtype),
            jax.ShapeDtypeStruct((2, G * B, width), dtype),
        ),
        in_specs=[smem, smem, vmem, vmem],
        out_specs=(pl.BlockSpec(memory_space=pl.ANY), vmem, vmem),
        scratch_shapes=[
            pltpu.VMEM((tok // B * (width // DH), *TILE), dtype),
            [pltpu.VMEM((cz, *TILE), dtype) for _ in range(planes - 1)],
            [pltpu.VMEM((cz, *TILE), dtype) for _ in range(planes - 1)],
            [pltpu.VMEM((cx, *TILE), dtype) for _ in range(planes)],
            pltpu.VMEM((cx, *TILE), dtype),
            dma((planes - 1,)), dma((planes - 1,)),
            dma((planes,)), dma((planes,)),
            dma((4,)), dma((4,)), dma((3,)), dma((2,)), dma((2 + planes,)),
        ],
        compiler_params=pltpu.CompilerParams(
            collective_id=level, has_side_effects=True,
            vmem_limit_bytes=60 * 1024 * 1024,
        ),
    )(ztab, xtab, keys, values)


PIECES = 4


def settle_kernel(
    count, caps, cx, blk_dev, ztab, xtab, otab, in_ref, out_ref,
    mine, zs, pool, xs, xr, z_send, z_recv, x_send, x_recv,
):
    planes = count // 2
    me = lax.axis_index("seq")
    plane, side = me // 2, me % 2
    mate = plane * 2 + 1 - side
    wide = in_ref.shape[1] // PIECES
    barrier = pltpu.get_barrier_semaphore()
    for step in range(1, count):
        peer = lax.rem(me + step, count)
        pl.semaphore_signal(
            barrier, inc=1, device_id={"seq": peer}, device_id_type=pl.DeviceIdType.MESH
        )
    pl.semaphore_wait(barrier, count - 1)

    def remote(src, dst, send, recv, peer):
        return pltpu.make_async_remote_copy(
            src_ref=src, dst_ref=dst, send_sem=send, recv_sem=recv,
            device_id={"seq": peer}, device_id_type=pl.DeviceIdType.MESH,
        )

    used = [d for d in range(1, planes) if caps[d - 1] > 0]
    used.sort(reverse=True)
    base = {d: blk_dev + sum(caps[: d - 1]) for d in used}

    def fill(dst, src, table, row, cap):
        def one(j, carry):
            dst[j] = src[table[row, j]]
            return carry

        lax.fori_loop(0, cap, one, 0)

    def own_part(piece):
        def one(j, carry):
            rows = pl.ds(pl.multiple_of(j * B, B), B)
            block = in_ref[rows, piece * wide : (piece + 1) * wide]
            mine[piece][j] = block
            pool[piece][j] = block
            return carry

        lax.fori_loop(0, blk_dev, one, 0)

    z_copies, x_copies = {}, []
    for piece in range(PIECES):
        for n, d in enumerate(used):
            z_copies[piece, d] = remote(
                zs[piece][n], pool[piece].at[pl.ds(base[d], caps[d - 1])],
                z_send.at[piece, n], z_recv.at[piece, n],
                jnp.maximum(me - 2 * d, 0),
            )
        x_copies.append(remote(xs[piece], xr[piece], x_send.at[piece], x_recv.at[piece], mate))
    def start_z(piece):
        for d in used:
            @pl.when(plane >= d)
            def _(d=d):
                z_copies[piece, d].start()

    for piece in range(PIECES):
        own_part(piece)
        for n, d in enumerate(used):
            fill(zs[piece][n], mine[piece], ztab, d - 1, caps[d - 1])
        if piece > 0:
            start_z(piece - 1)
    start_z(PIECES - 1)

    def finish(piece):
        x_copies[piece].wait_recv()

        def one(j, carry):
            rows = pl.ds(pl.multiple_of(j * B, B), B)
            kind = otab[0, j]
            near, far = pool[piece][otab[1, j]], xr[piece][otab[2, j]]
            block = jnp.where(kind == 1, near, jnp.where(kind == 2, far, jnp.zeros_like(far)))
            out_ref[rows, piece * wide : (piece + 1) * wide] = block
            return carry

        lax.fori_loop(0, blk_dev, one, 0)

    for piece in range(PIECES):
        for d in used:
            @pl.when(plane + d < planes)
            def _(d=d, piece=piece):
                z_copies[piece, d].wait_recv()
        fill(xs[piece], pool[piece], xtab, 0, cx)
        x_copies[piece].start()
        if piece > 0:
            finish(piece - 1)
    finish(PIECES - 1)
    for piece in range(PIECES):
        x_copies[piece].wait_send()
        for d in used:
            @pl.when(plane >= d)
            def _(d=d, piece=piece):
                z_copies[piece, d].wait_send()


def settled(count, number, caps, cx, blk_dev, ztab, xtab, otab, blocks):
    tok, width = blocks.shape
    planes, wide = count // 2, width // PIECES
    smem = pl.BlockSpec(memory_space=pltpu.SMEM)
    vmem = pl.BlockSpec(memory_space=pltpu.VMEM)
    dma, dtype = pltpu.SemaphoreType.DMA, blocks.dtype
    sent = [caps[d - 1] for d in range(planes - 1, 0, -1) if caps[d - 1] > 0]

    def each(rows):
        return [pltpu.VMEM((rows, B, wide), dtype) for _ in range(PIECES)]

    return pl.pallas_call(
        functools.partial(settle_kernel, count, caps, cx, blk_dev),
        out_shape=jax.ShapeDtypeStruct(blocks.shape, dtype),
        in_specs=[smem, smem, smem, vmem],
        out_specs=vmem,
        scratch_shapes=[
            each(blk_dev),
            [[pltpu.VMEM((c, B, wide), dtype) for c in sent] for _ in range(PIECES)],
            each(blk_dev + sum(caps)),
            each(cx),
            each(cx),
            dma((PIECES, len(sent))), dma((PIECES, len(sent))), dma((PIECES,)), dma((PIECES,)),
        ],
        compiler_params=pltpu.CompilerParams(
            collective_id=number, has_side_effects=True,
            vmem_limit_bytes=60 * 1024 * 1024,
        ),
    )(ztab, xtab, otab, blocks)


def settle_levels(planes, blk_dev):
    def pad(first, second):
        return ((first, second) + (0,) * planes)[: planes - 1]

    few = blk_dev * 3 // 4
    pairs = [(f, s) for f in range(blk_dev // 2, few + 1) for s in range(blk_dev // 2, few + 1)]
    pairs = sorted((f + 2 * s, pad(f, s), few) for f, s in pairs if abs(f - s) < 2 or s < f or f == s)
    return [(c, cx) for _, c, cx in pairs] + [((blk_dev,) * (planes - 1), blk_dev)]


def pack(blocks, keep_all, me, count, blk_dev, first_id):
    i32 = jnp.int32
    planes = count // 2
    plane, side = me // 2, me % 2
    index = jnp.arange(count * blk_dev, dtype=i32)
    kept = keep_all > 0
    rank = exclusive(keep_all, 0)
    source, goal = index // blk_dev, rank // blk_dev
    far = source // 2 - goal // 2
    earlier = index[None] < index[:, None]
    same_z = (source[:, None] == source[None]) & (far[:, None] == far[None])
    by_z = jnp.sum((earlier & same_z & kept[None]).astype(i32), axis=1)
    crosses = kept & (source % 2 != goal % 2)
    same_x = (goal[:, None] // 2 == goal[None] // 2) & (source[:, None] % 2 == source[None] % 2)
    by_x = jnp.sum((earlier & same_x & crosses[None]).astype(i32), axis=1)
    deltas = jnp.arange(1, planes, dtype=i32)
    of_delta = kept[None] & (far[None] == deltas[:, None])
    most_z = jnp.max(of_delta * (by_z + 1)[None], axis=1)
    most_x = jnp.max(crosses * (by_x + 1))
    choices = settle_levels(planes, blk_dev)
    caps = jnp.asarray([c for c, _ in choices], i32)
    caps_x = jnp.asarray([c for _, c in choices], i32)
    enough = jnp.all(most_z[None] <= caps, axis=1) & (most_x <= caps_x)
    level = jnp.argmax(enough).astype(i32)
    own_caps = caps[level]
    base = blk_dev + exclusive(own_caps, 0)
    base = jnp.sum((far[:, None] == deltas[None]).astype(i32) * base[None], axis=1)
    held = jnp.where(far == 0, index % blk_dev, base + by_z)

    def listed(flags, places, worth, cap):
        hit = (flags[..., None, :] & (places == jnp.arange(cap, dtype=i32)[:, None])).astype(i32)
        return jnp.sum(hit * worth, axis=-1)

    ztab = listed(of_delta & (source == me)[None], by_z, index % blk_dev, blk_dev)
    comes = crosses & (goal // 2 == plane) & (source % 2 == side)
    xtab = listed(comes, by_x, held, blk_dev)[None]
    lands = kept & (goal == me)
    straight = source % 2 == side
    kind = jnp.where(straight, 1, 2)
    worth = jnp.stack([kind, jnp.where(straight, held, 0), jnp.where(straight, 0, by_x)])
    hit = (lands & (rank % blk_dev == jnp.arange(blk_dev, dtype=i32)[:, None])).astype(i32)
    otab = jnp.sum(hit[None] * worth[:, None], axis=-1)

    def run(number, caps, cx):
        return lambda *args: settled(count, first_id + number, caps, cx, blk_dev, *args)

    runs = [run(n, c, cx) for n, (c, cx) in enumerate(choices)]
    return lax.switch(level, runs, ztab, xtab, otab, blocks)


CHUNK = 8


def near_far_kernel(
    blk_dev, keep_ref, live_ref, where_ref, used_ref,
    q_ref, k_ref, v_ref, hk_ref, hv_ref, gk_ref, gv_ref, rand_hbm, out_ref, rand_ref, sems,
):
    scale = 1.0 / math.sqrt(DH)
    head = pl.program_id(0)
    chunks = rand_hbm.shape[0] // CHUNK

    @pl.when(head == 0)
    def _():
        def copy(c):
            rows = pl.ds(c * CHUNK, CHUNK)
            return pltpu.make_async_copy(rand_hbm.at[rows], rand_ref.at[rows], sems.at[c])

        for c in range(chunks):
            pl.when(c * CHUNK < used_ref[0])(lambda c=c: copy(c).start())
        for c in range(chunks):
            pl.when(c * CHUNK < used_ref[0])(lambda c=c: copy(c).wait())

    def tile(ref, halo_ref, i):
        if i < 0:
            return halo_ref[0, :B]
        if i >= blk_dev:
            return halo_ref[0, B:]
        return ref[i * B : (i + 1) * B]

    def one(i):
        q = q_ref[i * B : (i + 1) * B]
        near = range(i - 1, i + 2)
        picks = [where_ref[(head * blk_dev + i) * R + r] for r in range(R)]
        k_parts = [
            jnp.concatenate([tile(k_ref, hk_ref, n) for n in near], axis=0),
            gk_ref[0],
            jnp.concatenate([rand_ref[p, :B] for p in picks], axis=0),
        ]
        v_parts = [
            jnp.concatenate([tile(v_ref, hv_ref, n) for n in near], axis=0),
            gv_ref[0],
            jnp.concatenate([rand_ref[p, B:] for p in picks], axis=0),
        ]
        scores = [
            lax.dot_general(
                q, k, (((1,), (1,)), ((), ())), preferred_element_type=jnp.float32
            )
            * scale
            for k in k_parts
        ]
        lanes = lax.broadcasted_iota(jnp.int32, scores[0].shape, 1)
        if i == 0:
            dead = jnp.logical_and(lanes < B, live_ref[0] == 0)
            scores[0] = jnp.where(dead, neg_big, scores[0])
        if i == blk_dev - 1:
            dead = jnp.logical_and(lanes >= 2 * B, live_ref[1] == 0)
            scores[0] = jnp.where(dead, neg_big, scores[0])
        peak = functools.reduce(
            jnp.maximum, [jnp.max(s, axis=-1, keepdims=True) for s in scores]
        )
        numer = jnp.zeros((B, DH), jnp.float32)
        denom = jnp.zeros((B, 1), jnp.float32)
        for s, v in zip(scores, v_parts):
            w = jnp.exp(s - peak).astype(jnp.bfloat16)
            denom = denom + jnp.sum(w.astype(jnp.float32), axis=-1, keepdims=True)
            numer = numer + jnp.dot(w, v, preferred_element_type=jnp.float32)
        out_ref[i * B : (i + 1) * B, :] = (numer / denom).astype(out_ref.dtype)

    for i in range(blk_dev):
        pl.when(keep_ref[i] > 0)(functools.partial(one, i))


def near_far(keep, live, where, used, q, k, v, halo_kv, glob, rand):
    tok_dev, width_dev = q.shape
    blk_dev, head_dev = tok_dev // B, width_dev // DH

    def column(rows):
        return pl.BlockSpec((rows, DH), lambda h, *_: (0, h))

    def part(rows, which):
        return pl.BlockSpec((1, rows, DH), lambda h, *_: (which, 0, h))

    return pl.pallas_call(
        functools.partial(near_far_kernel, blk_dev),
        out_shape=jax.ShapeDtypeStruct(q.shape, q.dtype),
        grid_spec=pltpu.PrefetchScalarGridSpec(
            num_scalar_prefetch=4,
            grid=(head_dev,),
            in_specs=[column(tok_dev)] * 3
            + [part(2 * B, 0), part(2 * B, 1), part(G * B, 0), part(G * B, 1)]
            + [pl.BlockSpec(memory_space=pl.ANY)],
            out_specs=column(tok_dev),
            scratch_shapes=[
                pltpu.VMEM(rand.shape, rand.dtype),
                pltpu.SemaphoreType.DMA((rand.shape[0] // CHUNK,)),
            ],
        ),
        compiler_params=ANYWHERE,
    )(keep, live, where, used, q, k, v, halo_kv, halo_kv, glob, glob, rand)


def levels(tiles, most):
    caps = []
    for part in (22, 24, 26, 28, 30, 32, 36):
        cz = min(tiles, tiles * part // 64)
        caps.append((cz, min(most, max(1, most * (part // 2 + 4) // 24))))
    caps.append((tiles, most))
    return sorted(set(caps))


def body(queries, keys, values, random_holder, random_offset, keep):
    tok_dev, width_dev = queries.shape
    blk_dev = tok_dev // B
    head_dev = width_dev // DH
    count = lax.axis_size("seq")
    head_count = lax.axis_size("head")
    count_req = blk_dev * R
    total = head_dev * count_req
    tiles = head_dev * blk_dev
    most = min(tiles, head_dev * max(2, (count_req + count - 1) // count))
    planes = count // 2
    if count % 2 or planes % 2 or not fits(planes, tiles, most):
        return plain_body(queries, keys, values, random_holder, random_offset, keep)
    me = lax.axis_index("seq")
    plane, side = me // 2, me % 2
    mate = me + 1 - 2 * side
    i32, f32 = jnp.int32, jnp.float32

    code = random_holder * blk_dev + random_offset
    code = jnp.where((keep > 0)[None, :, None], code, -1).reshape(total)
    note = jnp.concatenate([code, keep])
    note = jnp.broadcast_to(note, (count * head_count,) + note.shape)
    table = lax.all_to_all(note, ("seq", "head"), split_axis=0, concat_axis=0, tiled=True)
    table = table.reshape(count, head_count, total + blk_dev)
    keep_all = table[:, 0, total:].reshape(count * blk_dev)
    codes = table[:, :, :total].reshape(count, head_count, head_dev, 1, count_req)

    blocks = jnp.arange(count * blk_dev, dtype=i32)[:, None]
    need = jnp.max((codes == blocks).astype(i32), axis=-1)
    need = need.reshape(count, head_count, head_dev, count, blk_dev)
    both = jnp.max(need.reshape(planes, 2, *need.shape[1:]), axis=1)
    devices = jnp.arange(count, dtype=i32)
    away = (devices[None] // 2 != jnp.arange(planes, dtype=i32)[:, None]).astype(i32)
    most_z = jnp.max(jnp.sum(both, axis=(2, 4)) * away[:, None])
    most_x = jnp.max(jnp.sum(need, axis=(2, 4)))

    group = lax.axis_index("head")

    def flat(array):
        array = lax.dynamic_index_in_dim(array, group, 1, keepdims=False)
        return jnp.transpose(array, (0, 2, 1, 3)).reshape(array.shape[0], count, tiles)

    want, want_z = flat(need), flat(both)
    order = jnp.arange(tiles, dtype=i32)
    before = (order[:, None] < order[None]).astype(f32)

    def places(flags):
        got = jnp.dot(flags.astype(jnp.bfloat16), before.astype(jnp.bfloat16), preferred_element_type=f32)
        return got.astype(i32)

    slot_x, slot_z = places(want), places(want_z)

    def listed(flags, slots, worth, cap):
        hit = flags[:, None] * (slots[:, None] == jnp.arange(cap, dtype=i32)[:, None]).astype(i32)
        return jnp.sum(hit * worth[:, None], axis=2)

    def at(array, i):
        return lax.dynamic_index_in_dim(array, i, 0, keepdims=False)

    steps = jnp.arange(planes, dtype=i32)
    goal = (plane + steps[1:]) % planes
    mine_z, mine_slot_z = jnp.take(want_z[:, me], goal, axis=0), jnp.take(slot_z[:, me], goal, axis=0)
    plain = jnp.broadcast_to(order, (planes + 1, tiles))
    ztab = listed(mine_z, mine_slot_z, plain[: planes - 1], tiles)
    here = at(slot_z, plane)
    source = ((plane - steps) % planes) * 2 + side
    worth = jnp.where((steps == 0)[:, None], order, jnp.take(here, source, axis=0))
    asked = jnp.concatenate([jnp.take(at(want, mate), source, axis=0), at(want, me)[me][None]])
    asked_slot = jnp.concatenate([jnp.take(at(slot_x, mate), source, axis=0), at(slot_x, me)[me][None]])
    xtab = listed(asked, asked_slot, jnp.concatenate([worth, order[None]]), most)

    caps = levels(tiles, most)
    cz_of = jnp.asarray([c[0] for c in caps], i32)
    cx_of = jnp.asarray([c[1] for c in caps], i32)
    level = jnp.sum(((most_z > cz_of) | (most_x > cx_of))[:-1].astype(i32))
    cz, cx = cz_of[level], cx_of[level]
    gap = (plane - devices // 2) % planes
    x_base = (planes - 1) * cz
    straight = jnp.where(devices == me, x_base + planes * cx, (gap - 1) * cz)
    start = jnp.where(devices % 2 == side, straight, x_base + gap * cx)
    by_z = ((devices % 2 == side) & (devices != me))[:, None]
    spot = start[:, None] + jnp.where(by_z, here, at(slot_x, me))
    spot = jnp.transpose(spot.reshape(count, head_dev, blk_dev), (1, 0, 2)).reshape(head_dev, 1, count * blk_dev)
    picks = (random_holder * blk_dev + random_offset).reshape(head_dev, count_req, 1)
    hits = (picks == jnp.arange(count * blk_dev, dtype=i32)).astype(i32)
    where = jnp.sum(hits * spot, axis=2).reshape(total)
    used = x_base + (planes + 1) * cx

    slots_all = -(-max((planes - 1) * c[0] + (planes + 1) * c[1] for c in caps) // CHUNK) * CHUNK
    where = jnp.minimum(where, slots_all - 1)

    def exchanged(number, caps):
        def run(ztab, xtab, k, v):
            return exchange(count, number, *caps, slots_all, blk_dev, ztab, xtab, k, v)

        return run

    rand, halo_kv, glob = lax.switch(
        level, [exchanged(n, c) for n, c in enumerate(caps)], ztab, xtab, keys, values
    )

    live = jnp.stack([me > 0, me < count - 1]).astype(i32)
    blocks = near_far(
        keep, live, where, used[None], queries, keys, values, halo_kv, glob, rand
    )
    return pack(blocks, keep_all, me, count, blk_dev, len(caps))


def solution(mesh):
    in_specs = (
        P("seq", "head"),
        P("seq", "head"),
        P("seq", "head"),
        P("head", "seq", None),
        P("head", "seq", None),
        P("seq"),
    )
    out_specs = P("seq", "head")
    return jax.shard_map(body, mesh=mesh, in_specs=in_specs, out_specs=out_specs, check_vma=False)
```

```python
import functools
import math

import jax
import jax.numpy as jnp
from jax import lax
from jax.experimental import pallas as pl
from jax.experimental.pallas import tpu as pltpu
from jax.sharding import PartitionSpec as P

DH = 128
B = 128
G = 2
R = 3

neg_big = -1e30
ANYWHERE = pltpu.CompilerParams(
    dimension_semantics=("arbitrary",), vmem_limit_bytes=60 * 1024 * 1024
)


def halo(block, axis, width):
    count = lax.axis_size(axis)
    forward = [(i, i + 1) for i in range(count - 1)]
    backward = [(target, source) for source, target in forward]
    low = lax.ppermute(block[-width:], axis, forward)
    high = lax.ppermute(block[:width], axis, backward)
    return jnp.concatenate([low, high], axis=0)


def broadcast(block, axis, source):
    block = jnp.where(lax.axis_index(axis) == source, block, jnp.zeros_like(block))
    return lax.psum(block, axis)


def pick_kernel(cap, head_ref, block_ref, k_ref, v_ref, out_ref):
    dest = pl.program_id(0)

    @pl.loop(0, cap)
    def _(j):
        rows = pl.ds(pl.multiple_of(block_ref[dest, j] * B, B), B)
        cols = pl.ds(pl.multiple_of(head_ref[dest, j] * DH, DH), DH)
        out_ref[j, 0] = k_ref[rows, cols]
        out_ref[j, 1] = v_ref[rows, cols]


def pick(keys, values, heads, blocks, seq_count, cap):
    whole = pl.BlockSpec(keys.shape, lambda d, *_: (0, 0))
    return pl.pallas_call(
        functools.partial(pick_kernel, cap),
        out_shape=jax.ShapeDtypeStruct((seq_count * cap, 2, B, DH), keys.dtype),
        grid_spec=pltpu.PrefetchScalarGridSpec(
            num_scalar_prefetch=2,
            grid=(seq_count,),
            in_specs=[whole, whole],
            out_specs=pl.BlockSpec((cap, 2, B, DH), lambda d, *_: (d, 0, 0, 0)),
        ),
        compiler_params=ANYWHERE,
    )(heads, blocks, keys, values)


def attend_kernel(
    blk_dev,
    keep_ref,
    slot_ref,
    live_ref,
    where_ref,
    q_ref,
    k_ref,
    v_ref,
    hk_ref,
    hv_ref,
    gk_ref,
    gv_ref,
    rand_ref,
    out_ref,
):
    scale = 1.0 / math.sqrt(DH)
    head = pl.program_id(0)
    out_ref[...] = jnp.zeros_like(out_ref)

    def tile(ref, halo_ref, i):
        if i < 0:
            return halo_ref[:B]
        if i >= blk_dev:
            return halo_ref[B:]
        return ref[i * B : (i + 1) * B]

    def one(i):
        q = q_ref[i * B : (i + 1) * B]
        near = range(i - 1, i + 2)
        picks = [where_ref[(head * blk_dev + i) * R + r] for r in range(R)]
        k_parts = [
            jnp.concatenate([tile(k_ref, hk_ref, n) for n in near], axis=0),
            gk_ref[...],
            jnp.concatenate([rand_ref[p, 0] for p in picks], axis=0),
        ]
        v_parts = [
            jnp.concatenate([tile(v_ref, hv_ref, n) for n in near], axis=0),
            gv_ref[...],
            jnp.concatenate([rand_ref[p, 1] for p in picks], axis=0),
        ]
        scores = [
            lax.dot_general(
                q, k, (((1,), (1,)), ((), ())), preferred_element_type=jnp.float32
            )
            * scale
            for k in k_parts
        ]
        lanes = lax.broadcasted_iota(jnp.int32, scores[0].shape, 1)
        if i == 0:
            dead = jnp.logical_and(lanes < B, live_ref[0] == 0)
            scores[0] = jnp.where(dead, neg_big, scores[0])
        if i == blk_dev - 1:
            dead = jnp.logical_and(lanes >= 2 * B, live_ref[1] == 0)
            scores[0] = jnp.where(dead, neg_big, scores[0])
        peak = functools.reduce(
            jnp.maximum, [jnp.max(s, axis=-1, keepdims=True) for s in scores]
        )
        numer = jnp.zeros((B, DH), jnp.float32)
        denom = jnp.zeros((B, 1), jnp.float32)
        for s, v in zip(scores, v_parts):
            w = jnp.exp(s - peak).astype(jnp.bfloat16)
            denom = denom + jnp.sum(w.astype(jnp.float32), axis=-1, keepdims=True)
            numer = numer + jnp.dot(w, v, preferred_element_type=jnp.float32)
        rows = pl.ds(pl.multiple_of(slot_ref[i] * B, B), B)
        out_ref[rows, :] = (numer / denom).astype(out_ref.dtype)

    for i in range(blk_dev):
        pl.when(keep_ref[i] > 0)(functools.partial(one, i))


def attend(keep, slot, live, where, q, k, v, hk, hv, gk, gv, rand):
    tok_dev, width_dev = q.shape
    blk_dev, head_dev = tok_dev // B, width_dev // DH

    def column(rows):
        return pl.BlockSpec((rows, DH), lambda h, *_: (0, h))

    return pl.pallas_call(
        functools.partial(attend_kernel, blk_dev),
        out_shape=jax.ShapeDtypeStruct(q.shape, q.dtype),
        grid_spec=pltpu.PrefetchScalarGridSpec(
            num_scalar_prefetch=4,
            grid=(head_dev,),
            in_specs=[column(tok_dev)] * 3
            + [column(2 * B)] * 2
            + [column(G * B)] * 2
            + [pl.BlockSpec(rand.shape, lambda h, *_: (0, 0, 0, 0))],
            out_specs=column(tok_dev),
        ),
        compiler_params=ANYWHERE,
    )(keep, slot, live, where, q, k, v, hk, hv, gk, gv, rand)


def copy_kernel(order_ref, in_ref, out_ref):
    out_ref[...] = in_ref[...]


def take_blocks(blocks, order, cap):
    width = blocks.shape[1]
    return pl.pallas_call(
        copy_kernel,
        out_shape=jax.ShapeDtypeStruct((cap * B, width), blocks.dtype),
        grid_spec=pltpu.PrefetchScalarGridSpec(
            num_scalar_prefetch=1,
            grid=(cap,),
            in_specs=[pl.BlockSpec((B, width), lambda j, order: (order[j], 0))],
            out_specs=pl.BlockSpec((B, width), lambda j, order: (j, 0)),
        ),
        compiler_params=ANYWHERE,
    )(order, blocks)


def merge_kernel(kind_ref, from_ref, old_ref, new_ref, out_ref):
    kind = kind_ref[pl.program_id(0)]

    @pl.when(kind == 0)
    def _():
        out_ref[...] = old_ref[...]

    @pl.when(kind == 1)
    def _():
        out_ref[...] = jnp.zeros_like(out_ref)

    @pl.when(kind == 2)
    def _():
        out_ref[...] = new_ref[...]


def merge_blocks(old, new, kind, place):
    tok_dev, width = old.shape
    return pl.pallas_call(
        merge_kernel,
        out_shape=jax.ShapeDtypeStruct(old.shape, old.dtype),
        grid_spec=pltpu.PrefetchScalarGridSpec(
            num_scalar_prefetch=2,
            grid=(tok_dev // B,),
            in_specs=[
                pl.BlockSpec((B, width), lambda j, kind, place: (j, 0)),
                pl.BlockSpec((B, width), lambda j, kind, place: (place[j], 0)),
            ],
            out_specs=pl.BlockSpec((B, width), lambda j, kind, place: (j, 0)),
        ),
        compiler_params=ANYWHERE,
    )(kind, place, old, new)


def exclusive(flags, axis):
    return jnp.cumsum(flags, axis=axis) - flags


def first_at_least(caps, amount):
    return jnp.sum((amount > jnp.asarray(caps, jnp.int32)).astype(jnp.int32))


def settle(blocks, keep_all, slot, source, distance, me, count, blk_dev):
    i32 = jnp.int32
    devices = jnp.arange(count, dtype=i32)
    slots = jnp.arange(blk_dev, dtype=i32)
    sizes = sorted({0, *range(blk_dev // 2, blk_dev - 1), blk_dev})
    for bit_pos in range((count - 1).bit_length()):
        stride = 2**bit_pos
        at = source - distance % stride
        moving = (keep_all > 0) & (distance // stride % 2 > 0)
        on_slot = ((slot[:, None] == slots) & moving[:, None]).astype(i32)
        on_device = (at[:, None] == devices).astype(i32)
        leaving = jnp.sum(on_device[:, :, None] * on_slot[:, None, :], axis=0)
        needed = jnp.max(jnp.sum(leaving, axis=1))
        nth = exclusive(leaving, 1)
        mine_out, mine_nth = leaving[me], nth[me]
        send = jnp.sum(
            mine_out[:, None] * (mine_nth[:, None] == slots).astype(i32) * slots[:, None], axis=0
        )
        far = jnp.minimum(me + stride, count - 1)
        comes = jnp.where(me + stride < count, leaving[far], 0)
        kind = jnp.where(comes > 0, 2, jnp.where(mine_out > 0, 1, 0)).astype(i32)
        place = jnp.where(comes > 0, nth[far], 0)
        all_pairs = [(i, i - stride) for i in range(stride, count)]
        split = count - stride // 2
        upper = [pair for pair in all_pairs if pair[0] >= split]
        halves = 2 * stride >= count and 0 < len(upper) < len(all_pairs)

        def shifting(cap, pairs, send=send, kind=kind, place=place):
            def run(blocks):
                if cap == 0:
                    return blocks
                moved = lax.ppermute(take_blocks(blocks, send, cap), "seq", pairs)
                return merge_blocks(blocks, moved, kind, jnp.minimum(place, cap - 1))

            return run

        which = first_at_least(sizes[:-1], needed)
        runs = [shifting(cap, all_pairs) for cap in sizes]
        if halves:
            runs += [shifting(cap, upper) for cap in sizes]
            lower = jnp.sum(leaving * (devices < split)[:, None].astype(i32))
            which = which + jnp.where(lower > 0, 0, len(sizes))
        blocks = lax.switch(which, runs, blocks)
    return blocks


def plain_body(queries, keys, values, random_holder, random_offset, keep):
    tok_dev, width_dev = queries.shape
    blk_dev = tok_dev // B
    head_dev = width_dev // DH
    seq_count = lax.axis_size("seq")
    head_count = lax.axis_size("head")
    me = lax.axis_index("seq")
    count_req = blk_dev * R
    total = head_dev * count_req
    i32 = jnp.int32

    code = random_holder * blk_dev + random_offset
    code = jnp.where((keep > 0)[None, :, None], code, -1).reshape(total)
    note = jnp.concatenate([code, keep])
    note = jnp.broadcast_to(note, (seq_count * head_count,) + note.shape)
    table = lax.all_to_all(note, ("seq", "head"), split_axis=0, concat_axis=0, tiled=True)
    table = table.reshape(seq_count, head_count, total + blk_dev)
    keep_all = table[:, 0, total:].reshape(seq_count * blk_dev)
    codes = table[:, :, :total]
    devices = jnp.arange(seq_count, dtype=i32)

    halo_k, halo_v = halo(keys, "seq", B), halo(values, "seq", B)

    named = jnp.where(codes >= 0, codes // blk_dev, -1)
    counts = jnp.sum((named[..., None] == devices).astype(i32), axis=2)
    most = jnp.max(counts)
    onehot = (named[me, lax.axis_index("head")][:, None] == devices).astype(i32)
    mine = exclusive(onehot, 0)
    my_slot = jnp.sum(mine * onehot, axis=1)
    my_holder = jnp.sum(onehot * devices, axis=1)

    group = codes[:, lax.axis_index("head")]
    asks = (named[:, lax.axis_index("head")] == me).astype(i32)
    order = exclusive(asks, 1)
    full = min(total, head_dev * max(2, (count_req + seq_count - 1) // seq_count))
    chosen = asks[..., None] * (order[..., None] == jnp.arange(full, dtype=i32)).astype(i32)
    ask_head = jnp.arange(total, dtype=i32) // count_req
    ask = jnp.where(group >= 0, group % blk_dev, 0) + ask_head[None] * blk_dev
    ask = jnp.sum(chosen * ask[..., None], axis=1)
    pick_head, pick_block = ask // blk_dev, ask % blk_dev

    rank = exclusive(keep_all, 0)
    slot = rank % blk_dev
    source = jnp.arange(seq_count * blk_dev, dtype=i32) // blk_dev
    distance = jnp.where(keep_all > 0, source - rank // blk_dev, 0)
    my_slots = lax.dynamic_slice_in_dim(slot, me * blk_dev, blk_dev)
    live = jnp.stack([me > 0, me < seq_count - 1]).astype(i32)

    caps = sorted({max(1, full * part // 12) for part in range(8, 13)})

    def gathered(cap):
        def run(q, k, v, hk, hv):
            gk, gv = broadcast(jnp.stack((k[: G * B], v[: G * B])), "seq", 0)
            picked = pick(k, v, pick_head, pick_block, seq_count, cap)
            replies = lax.all_to_all(picked, "seq", split_axis=0, concat_axis=0, tiled=True)
            where = jnp.minimum(my_holder * cap + my_slot, seq_count * cap - 1)
            return attend(keep, my_slots, live, where, q, k, v, hk, hv, gk, gv, replies)

        return run

    blocks = lax.switch(
        first_at_least(caps[:-1], most),
        [gathered(cap) for cap in caps],
        queries, keys, values, halo_k, halo_v,
    )

    return settle(blocks, keep_all, slot, source, distance, me, seq_count, blk_dev)


TILE = (2 * B, DH)
SMALL = pltpu.CompilerParams(vmem_limit_bytes=60 * 1024 * 1024)


def fits(planes, tiles, most):
    slots = 2 * (planes - 1) * tiles + 2 * planes * most + most
    return slots * 2 * B * DH * 2 <= 44 * 1024 * 1024


def exchange_kernel(
    count, cz, cx, blk_dev, ztab, xtab, k_ref, v_ref,
    rand_ref, halo_ref, glob_ref, home, zs, zr, xs, own,
    z_send, z_recv, x_send, x_recv, h_send, h_recv, g_send, g_recv, l_sem,
):
    planes = count // 2
    me = lax.axis_index("seq")
    plane, side = me // 2, me % 2
    mate = plane * 2 + 1 - side
    tok = k_ref.shape[0]
    head_dev = k_ref.shape[1] // DH
    barrier = pltpu.get_barrier_semaphore()
    for step in range(1, count):
        peer = lax.rem(me + step, count)
        pl.semaphore_signal(
            barrier, inc=1, device_id={"seq": peer}, device_id_type=pl.DeviceIdType.MESH
        )
    pl.semaphore_wait(barrier, count - 1)

    def remote(src, dst, send, recv, peer):
        return pltpu.make_async_remote_copy(
            src_ref=src, dst_ref=dst, send_sem=send, recv_sem=recv,
            device_id={"seq": peer}, device_id_type=pl.DeviceIdType.MESH,
        )

    tables = (k_ref, v_ref)
    low, high = pl.ds(0, B), pl.ds(B, B)
    first, last = pl.ds(0, B), pl.ds(tok - B, B)
    after = jnp.minimum(me + 1, count - 1)
    before = jnp.maximum(me - 1, 0)
    ups = [
        remote(tables[i].at[last], halo_ref.at[i, low], h_send.at[i], h_recv.at[i], after)
        for i in range(2)
    ]
    downs = [
        remote(tables[i].at[first], halo_ref.at[i, high], h_send.at[2 + i], h_recv.at[2 + i], before)
        for i in range(2)
    ]
    local = [
        pltpu.make_async_copy(tables[i].at[pl.ds(0, G * B)], glob_ref.at[i], l_sem.at[i])
        for i in range(2)
    ]
    item = glob_ref.at[side]
    chain = remote(item, item, g_send.at[0], g_recv.at[0], jnp.minimum(me + 2, count - 1))
    swap = remote(item, item, g_send.at[1], g_recv.at[1], mate)
    extra = remote(glob_ref.at[1], glob_ref.at[1], g_send.at[2], g_recv.at[0], mate)

    @pl.when(me == 0)
    def _():
        for c in local:
            c.start()
        for c in local:
            c.wait()
        chain.start()
        extra.start()
        swap.start()

    def pass_on():
        @pl.when(me > 0)
        def _():
            chain.wait_recv()

            @pl.when(plane < planes - 1)
            def _():
                chain.start()

            @pl.when(me > 1)
            def _():
                swap.start()

    @pl.when(me < count - 1)
    def _():
        for c in ups:
            c.start()

    @pl.when(me > 0)
    def _():
        for c in downs:
            c.start()

    @pl.when(me == 0)
    def _():
        halo_ref[:, low, :] = jnp.zeros((2, B, k_ref.shape[1]), k_ref.dtype)

    @pl.when(me == count - 1)
    def _():
        halo_ref[:, high, :] = jnp.zeros((2, B, k_ref.shape[1]), k_ref.dtype)

    def load_home(block, carry):
        rows = pl.ds(pl.multiple_of(block * B, B), B)
        for h in range(head_dev):
            cols = slice(h * DH, (h + 1) * DH)
            home[h * blk_dev + block, low, :] = k_ref[rows, cols]
            home[h * blk_dev + block, high, :] = v_ref[rows, cols]
        return carry

    lax.fori_loop(0, blk_dev, load_home, 0)

    def from_slots(dst, src, table, row, cap):
        def one(j, carry):
            dst[j] = src[table[row, j]]
            return carry

        lax.fori_loop(0, cap, one, 0)

    half = planes // 2
    lower = plane < half
    rest = [d for d in range(1, planes) if d != half]
    rising, falling = [half, *rest], [half, *reversed(rest)]
    x_base = (planes - 1) * cz
    z_copies = {
        d: remote(
            zs[d - 1], zr[d - 1], z_send.at[d - 1], z_recv.at[d - 1],
            lax.rem(plane + d, planes) * 2 + side,
        )
        for d in rising
    }
    x_copies = [
        remote(
            xs[d], rand_ref.at[pl.ds(x_base + d * cx, cx)],
            x_send.at[d], x_recv.at[d], mate,
        )
        for d in range(planes)
    ]
    from_slots(zs[half - 1], home, ztab, half - 1, cz)
    from_slots(xs[0], home, xtab, 0, cx)
    z_copies[half].start()
    for d in rest:
        from_slots(zs[d - 1], home, ztab, d - 1, cz)
    x_copies[0].start()

    @pl.when(lower)
    def _():
        pass_on()
        for d in falling[1:]:
            z_copies[d].start()

    @pl.when(jnp.logical_not(lower))
    def _():
        for d in rising[1:]:
            z_copies[d].start()
        pass_on()

    from_slots(own, home, xtab, planes, cx)
    keep_own = pltpu.make_async_copy(
        own, rand_ref.at[pl.ds(x_base + planes * cx, cx)], l_sem.at[2]
    )
    keep_own.start()
    outs = {
        d: pltpu.make_async_copy(
            zr[d - 1], rand_ref.at[pl.ds((d - 1) * cz, cz)], l_sem.at[2 + d]
        )
        for d in rising
    }

    def forward(d):
        z_copies[d].wait_recv()
        outs[d].start()
        from_slots(xs[d], zr[d - 1], xtab, d, cx)
        x_copies[d].start()

    @pl.when(lower)
    def _():
        for d in falling:
            forward(d)

    @pl.when(jnp.logical_not(lower))
    def _():
        for d in rising:
            forward(d)

    @pl.when(me > 0)
    def _():
        swap.wait_recv()

    @pl.when(plane < planes - 1)
    def _():
        chain.wait_send()

    @pl.when(me == 0)
    def _():
        extra.wait_send()

    @pl.when(me != 1)
    def _():
        swap.wait_send()

    @pl.when(me < count - 1)
    def _():
        for c in ups:
            c.wait_send()
        for c in downs:
            c.wait_recv()

    @pl.when(me > 0)
    def _():
        for c in downs:
            c.wait_send()
        for c in ups:
            c.wait_recv()

    keep_own.wait()
    for d in rising:
        outs[d].wait()
        z_copies[d].wait_send()
    for c in x_copies:
        c.wait()


def exchange(count, level, cz, cx, slots, blk_dev, ztab, xtab, keys, values):
    planes = count // 2
    tok, width = keys.shape
    smem = pl.BlockSpec(memory_space=pltpu.SMEM)
    vmem = pl.BlockSpec(memory_space=pltpu.VMEM)
    dtype = keys.dtype
    dma = pltpu.SemaphoreType.DMA
    return pl.pallas_call(
        functools.partial(exchange_kernel, count, cz, cx, blk_dev),
        out_shape=(
            jax.ShapeDtypeStruct((slots, *TILE), dtype),
            jax.ShapeDtypeStruct((2, 2 * B, width), dtype),
            jax.ShapeDtypeStruct((2, G * B, width), dtype),
        ),
        in_specs=[smem, smem, vmem, vmem],
        out_specs=(pl.BlockSpec(memory_space=pl.ANY), vmem, vmem),
        scratch_shapes=[
            pltpu.VMEM((tok // B * (width // DH), *TILE), dtype),
            [pltpu.VMEM((cz, *TILE), dtype) for _ in range(planes - 1)],
            [pltpu.VMEM((cz, *TILE), dtype) for _ in range(planes - 1)],
            [pltpu.VMEM((cx, *TILE), dtype) for _ in range(planes)],
            pltpu.VMEM((cx, *TILE), dtype),
            dma((planes - 1,)), dma((planes - 1,)),
            dma((planes,)), dma((planes,)),
            dma((4,)), dma((4,)), dma((3,)), dma((2,)), dma((2 + planes,)),
        ],
        compiler_params=pltpu.CompilerParams(
            collective_id=level, has_side_effects=True,
            vmem_limit_bytes=60 * 1024 * 1024,
        ),
    )(ztab, xtab, keys, values)


PIECES = 4


def settle_kernel(
    count, caps, cr, cx, blk_dev, ztab, rtab, xtab, otab, in_ref, out_ref,
    mine, zs, pool, rs, xs, xr, z_send, z_recv, r_send, r_recv, x_send, x_recv,
):
    planes = count // 2
    me = lax.axis_index("seq")
    plane, side = me // 2, me % 2
    mate = plane * 2 + 1 - side
    wide = in_ref.shape[1] // PIECES
    barrier = pltpu.get_barrier_semaphore()
    for step in range(1, count):
        peer = lax.rem(me + step, count)
        pl.semaphore_signal(
            barrier, inc=1, device_id={"seq": peer}, device_id_type=pl.DeviceIdType.MESH
        )
    pl.semaphore_wait(barrier, count - 1)

    def remote(src, dst, send, recv, peer):
        return pltpu.make_async_remote_copy(
            src_ref=src, dst_ref=dst, send_sem=send, recv_sem=recv,
            device_id={"seq": peer}, device_id_type=pl.DeviceIdType.MESH,
        )

    used = [d for d in range(1, planes) if caps[d - 1] > 0]
    used.sort(reverse=True)
    base = {d: blk_dev + sum(caps[: d - 1]) for d in used}
    gate = planes // 2 - 1
    beyond = range(1, gate + 1)
    r_base = blk_dev + sum(caps)

    def fill(dst, src, table, row, cap):
        def one(j, carry):
            dst[j] = src[table[row, j]]
            return carry

        lax.fori_loop(0, cap, one, 0)

    def own_part(piece):
        def one(j, carry):
            rows = pl.ds(pl.multiple_of(j * B, B), B)
            block = in_ref[rows, piece * wide : (piece + 1) * wide]
            mine[piece][j] = block
            pool[piece][j] = block
            return carry

        lax.fori_loop(0, blk_dev, one, 0)

    z_copies, x_copies = {}, []
    for piece in range(PIECES):
        for n, d in enumerate(used):
            z_copies[piece, d] = remote(
                zs[piece][n], pool[piece].at[pl.ds(base[d], caps[d - 1])],
                z_send.at[piece, n], z_recv.at[piece, n],
                jnp.maximum(me - 2 * d, 0),
            )
        for d in beyond:
            z_copies[piece, -d] = remote(
                rs[piece][d - 1], pool[piece].at[pl.ds(r_base, cr)],
                r_send.at[piece, d - 1], r_recv.at[piece],
                jnp.maximum(me - 2 * d, 0),
            )
        x_copies.append(remote(xs[piece], xr[piece], x_send.at[piece], x_recv.at[piece], mate))
    def start_z(piece):
        for d in used:
            @pl.when(plane >= d)
            def _(d=d):
                z_copies[piece, d].start()

    for piece in range(PIECES):
        own_part(piece)
        for n, d in enumerate(used):
            fill(zs[piece][n], mine[piece], ztab, d - 1, caps[d - 1])
        if piece > 0:
            start_z(piece - 1)
    start_z(PIECES - 1)

    def finish(piece):
        x_copies[piece].wait_recv()

        def one(j, carry):
            rows = pl.ds(pl.multiple_of(j * B, B), B)
            kind = otab[0, j]
            near, far = pool[piece][otab[1, j]], xr[piece][otab[2, j]]
            block = jnp.where(kind == 1, near, jnp.where(kind == 2, far, jnp.zeros_like(far)))
            out_ref[rows, piece * wide : (piece + 1) * wide] = block
            return carry

        lax.fori_loop(0, blk_dev, one, 0)

    for piece in range(PIECES):
        for d in used:
            @pl.when(plane + d < planes)
            def _(d=d, piece=piece):
                z_copies[piece, d].wait_recv()

        @pl.when(plane == gate)
        def _(piece=piece):
            for d in beyond:
                fill(rs[piece][d - 1], pool[piece], rtab, d - 1, cr)
                z_copies[piece, -d].start()

        @pl.when(plane < gate)
        def _(piece=piece):
            if gate > 0:
                z_copies[piece, -1].wait_recv()

        fill(xs[piece], pool[piece], xtab, 0, cx)
        x_copies[piece].start()
        if piece > 0:
            finish(piece - 1)
    finish(PIECES - 1)
    for piece in range(PIECES):
        x_copies[piece].wait_send()
        for d in used:
            @pl.when(plane >= d)
            def _(d=d, piece=piece):
                z_copies[piece, d].wait_send()

        @pl.when(plane == gate)
        def _(piece=piece):
            for d in beyond:
                z_copies[piece, -d].wait_send()


def settled(count, number, caps, cr, cx, blk_dev, ztab, rtab, xtab, otab, blocks):
    tok, width = blocks.shape
    planes, wide = count // 2, width // PIECES
    smem = pl.BlockSpec(memory_space=pltpu.SMEM)
    vmem = pl.BlockSpec(memory_space=pltpu.VMEM)
    dma, dtype = pltpu.SemaphoreType.DMA, blocks.dtype
    sent = [caps[d - 1] for d in range(planes - 1, 0, -1) if caps[d - 1] > 0]

    def each(rows):
        return [pltpu.VMEM((rows, B, wide), dtype) for _ in range(PIECES)]

    return pl.pallas_call(
        functools.partial(settle_kernel, count, caps, cr, cx, blk_dev),
        out_shape=jax.ShapeDtypeStruct(blocks.shape, dtype),
        in_specs=[smem, smem, smem, smem, vmem],
        out_specs=vmem,
        scratch_shapes=[
            each(blk_dev),
            [[pltpu.VMEM((c, B, wide), dtype) for c in sent] for _ in range(PIECES)],
            each(blk_dev + sum(caps) + cr),
            [[pltpu.VMEM((cr, B, wide), dtype) for _ in range(planes // 2 - 1)] for _ in range(PIECES)],
            each(cx),
            each(cx),
            dma((PIECES, len(sent))), dma((PIECES, len(sent))),
            dma((PIECES, planes // 2)), dma((PIECES,)), dma((PIECES,)), dma((PIECES,)),
        ],
        compiler_params=pltpu.CompilerParams(
            collective_id=number, has_side_effects=True,
            vmem_limit_bytes=60 * 1024 * 1024,
        ),
    )(ztab, rtab, xtab, otab, blocks)


def settle_levels(planes, blk_dev):
    def pad(first, second):
        return ((first, second) + (0,) * planes)[: planes - 1]

    half, few = blk_dev // 2, blk_dev * 3 // 4
    choices = [
        (2 * max(f + t, f + r) + r, pad(f, t), r, few)
        for f in range(half, few + 1)
        for t in range(half, few + 1)
        for r in (half // 2, half)
        if abs(f - t) < 2 or t == half
    ]
    choices = sorted(choices) + [(0, (blk_dev,) * (planes - 1), blk_dev, blk_dev)]
    return [limits for _, *limits in choices]


def pack(blocks, keep_all, me, count, blk_dev, first_id):
    i32 = jnp.int32
    planes = count // 2
    plane, side = me // 2, me % 2
    index = jnp.arange(count * blk_dev, dtype=i32)
    kept = keep_all > 0
    rank = exclusive(keep_all, 0)
    source, goal = index // blk_dev, rank // blk_dev
    gate = planes // 2 - 1
    relayed = kept & (source // 2 == gate + 1) & (goal // 2 < gate)
    far = jnp.where(relayed, 1, source // 2 - goal // 2)
    earlier = index[None] < index[:, None]
    same_z = (source[:, None] == source[None]) & (far[:, None] == far[None])
    by_z = jnp.sum((earlier & same_z & kept[None]).astype(i32), axis=1)
    same_r = (goal[:, None] // 2 == goal[None] // 2) & (source[:, None] % 2 == source[None] % 2)
    by_r = jnp.sum((earlier & same_r & relayed[None]).astype(i32), axis=1)
    crosses = kept & (source % 2 != goal % 2)
    same_x = (goal[:, None] // 2 == goal[None] // 2) & (source[:, None] % 2 == source[None] % 2)
    by_x = jnp.sum((earlier & same_x & crosses[None]).astype(i32), axis=1)
    deltas = jnp.arange(1, planes, dtype=i32)
    of_delta = kept[None] & (far[None] == deltas[:, None])
    most_z = jnp.max(of_delta * (by_z + 1)[None], axis=1)
    most_x = jnp.max(crosses * (by_x + 1))
    most_r = jnp.max(relayed * (by_r + 1))
    choices = settle_levels(planes, blk_dev)
    caps = jnp.asarray([c for c, _, _ in choices], i32)
    caps_r = jnp.asarray([c for _, c, _ in choices], i32)
    caps_x = jnp.asarray([c for _, _, c in choices], i32)
    enough = jnp.all(most_z[None] <= caps, axis=1) & (most_x <= caps_x) & (most_r <= caps_r)
    level = jnp.argmax(enough).astype(i32)
    own_caps = caps[level]
    base = blk_dev + exclusive(own_caps, 0)
    base = jnp.sum((far[:, None] == deltas[None]).astype(i32) * base[None], axis=1)
    first = jnp.where(far == 0, index % blk_dev, base + by_z)
    held = jnp.where(relayed, blk_dev + jnp.sum(own_caps) + by_r, first)

    def listed(flags, places, worth, cap):
        hit = (flags[..., None, :] & (places == jnp.arange(cap, dtype=i32)[:, None])).astype(i32)
        return jnp.sum(hit * worth, axis=-1)

    ztab = listed(of_delta & (source == me)[None], by_z, index % blk_dev, blk_dev)
    hops = jnp.arange(1, max(gate, 1) + 1, dtype=i32)
    passes = relayed & (source % 2 == side) & (plane == gate)
    rtab = listed(passes[None] & (gate - goal // 2 == hops[:, None]), by_r, first, blk_dev)
    comes = crosses & (goal // 2 == plane) & (source % 2 == side)
    xtab = listed(comes, by_x, held, blk_dev)[None]
    lands = kept & (goal == me)
    straight = source % 2 == side
    kind = jnp.where(straight, 1, 2)
    worth = jnp.stack([kind, jnp.where(straight, held, 0), jnp.where(straight, 0, by_x)])
    hit = (lands & (rank % blk_dev == jnp.arange(blk_dev, dtype=i32)[:, None])).astype(i32)
    otab = jnp.sum(hit[None] * worth[:, None], axis=-1)

    def run(number, *limits):
        return lambda *args: settled(count, first_id + number, *limits, blk_dev, *args)

    runs = [run(n, *limits) for n, limits in enumerate(choices)]
    return lax.switch(level, runs, ztab, rtab, xtab, otab, blocks)


CHUNK = 8


def near_far_kernel(
    blk_dev, keep_ref, live_ref, where_ref, used_ref,
    q_ref, k_ref, v_ref, hk_ref, hv_ref, gk_ref, gv_ref, rand_hbm, out_ref, rand_ref, sems,
):
    scale = 1.0 / math.sqrt(DH)
    head = pl.program_id(0)
    chunks = rand_hbm.shape[0] // CHUNK

    @pl.when(head == 0)
    def _():
        def copy(c):
            rows = pl.ds(c * CHUNK, CHUNK)
            return pltpu.make_async_copy(rand_hbm.at[rows], rand_ref.at[rows], sems.at[c])

        for c in range(chunks):
            pl.when(c * CHUNK < used_ref[0])(lambda c=c: copy(c).start())
        for c in range(chunks):
            pl.when(c * CHUNK < used_ref[0])(lambda c=c: copy(c).wait())

    def tile(ref, halo_ref, i):
        if i < 0:
            return halo_ref[0, :B]
        if i >= blk_dev:
            return halo_ref[0, B:]
        return ref[i * B : (i + 1) * B]

    def one(i):
        q = q_ref[i * B : (i + 1) * B]
        near = range(i - 1, i + 2)
        picks = [where_ref[(head * blk_dev + i) * R + r] for r in range(R)]
        k_parts = [
            jnp.concatenate([tile(k_ref, hk_ref, n) for n in near], axis=0),
            gk_ref[0],
            jnp.concatenate([rand_ref[p, :B] for p in picks], axis=0),
        ]
        v_parts = [
            jnp.concatenate([tile(v_ref, hv_ref, n) for n in near], axis=0),
            gv_ref[0],
            jnp.concatenate([rand_ref[p, B:] for p in picks], axis=0),
        ]
        scores = [
            lax.dot_general(
                q, k, (((1,), (1,)), ((), ())), preferred_element_type=jnp.float32
            )
            * scale
            for k in k_parts
        ]
        lanes = lax.broadcasted_iota(jnp.int32, scores[0].shape, 1)
        if i == 0:
            dead = jnp.logical_and(lanes < B, live_ref[0] == 0)
            scores[0] = jnp.where(dead, neg_big, scores[0])
        if i == blk_dev - 1:
            dead = jnp.logical_and(lanes >= 2 * B, live_ref[1] == 0)
            scores[0] = jnp.where(dead, neg_big, scores[0])
        peak = functools.reduce(
            jnp.maximum, [jnp.max(s, axis=-1, keepdims=True) for s in scores]
        )
        numer = jnp.zeros((B, DH), jnp.float32)
        denom = jnp.zeros((B, 1), jnp.float32)
        for s, v in zip(scores, v_parts):
            w = jnp.exp(s - peak).astype(jnp.bfloat16)
            denom = denom + jnp.sum(w.astype(jnp.float32), axis=-1, keepdims=True)
            numer = numer + jnp.dot(w, v, preferred_element_type=jnp.float32)
        out_ref[i * B : (i + 1) * B, :] = (numer / denom).astype(out_ref.dtype)

    for i in range(blk_dev):
        pl.when(keep_ref[i] > 0)(functools.partial(one, i))


def near_far(keep, live, where, used, q, k, v, halo_kv, glob, rand):
    tok_dev, width_dev = q.shape
    blk_dev, head_dev = tok_dev // B, width_dev // DH

    def column(rows):
        return pl.BlockSpec((rows, DH), lambda h, *_: (0, h))

    def part(rows, which):
        return pl.BlockSpec((1, rows, DH), lambda h, *_: (which, 0, h))

    return pl.pallas_call(
        functools.partial(near_far_kernel, blk_dev),
        out_shape=jax.ShapeDtypeStruct(q.shape, q.dtype),
        grid_spec=pltpu.PrefetchScalarGridSpec(
            num_scalar_prefetch=4,
            grid=(head_dev,),
            in_specs=[column(tok_dev)] * 3
            + [part(2 * B, 0), part(2 * B, 1), part(G * B, 0), part(G * B, 1)]
            + [pl.BlockSpec(memory_space=pl.ANY)],
            out_specs=column(tok_dev),
            scratch_shapes=[
                pltpu.VMEM(rand.shape, rand.dtype),
                pltpu.SemaphoreType.DMA((rand.shape[0] // CHUNK,)),
            ],
        ),
        compiler_params=ANYWHERE,
    )(keep, live, where, used, q, k, v, halo_kv, halo_kv, glob, glob, rand)


def levels(tiles, most):
    caps = []
    for part in (22, 24, 26, 28, 30, 32, 36):
        cz = min(tiles, tiles * part // 64)
        caps.append((cz, min(most, max(1, most * (part // 2 + 4) // 24))))
    caps.append((tiles, most))
    return sorted(set(caps))


def body(queries, keys, values, random_holder, random_offset, keep):
    tok_dev, width_dev = queries.shape
    blk_dev = tok_dev // B
    head_dev = width_dev // DH
    count = lax.axis_size("seq")
    head_count = lax.axis_size("head")
    count_req = blk_dev * R
    total = head_dev * count_req
    tiles = head_dev * blk_dev
    most = min(tiles, head_dev * max(2, (count_req + count - 1) // count))
    planes = count // 2
    if count % 2 or planes % 2 or not fits(planes, tiles, most):
        return plain_body(queries, keys, values, random_holder, random_offset, keep)
    me = lax.axis_index("seq")
    plane, side = me // 2, me % 2
    mate = me + 1 - 2 * side
    i32, f32 = jnp.int32, jnp.float32

    code = random_holder * blk_dev + random_offset
    code = jnp.where((keep > 0)[None, :, None], code, -1).reshape(total)
    note = jnp.concatenate([code, keep])
    note = jnp.broadcast_to(note, (count * head_count,) + note.shape)
    table = lax.all_to_all(note, ("seq", "head"), split_axis=0, concat_axis=0, tiled=True)
    table = table.reshape(count, head_count, total + blk_dev)
    keep_all = table[:, 0, total:].reshape(count * blk_dev)
    codes = table[:, :, :total].reshape(count, head_count, head_dev, 1, count_req)

    blocks = jnp.arange(count * blk_dev, dtype=i32)[:, None]
    need = jnp.max((codes == blocks).astype(i32), axis=-1)
    need = need.reshape(count, head_count, head_dev, count, blk_dev)
    both = jnp.max(need.reshape(planes, 2, *need.shape[1:]), axis=1)
    devices = jnp.arange(count, dtype=i32)
    away = (devices[None] // 2 != jnp.arange(planes, dtype=i32)[:, None]).astype(i32)
    most_z = jnp.max(jnp.sum(both, axis=(2, 4)) * away[:, None])
    most_x = jnp.max(jnp.sum(need, axis=(2, 4)))

    group = lax.axis_index("head")

    def flat(array):
        array = lax.dynamic_index_in_dim(array, group, 1, keepdims=False)
        return jnp.transpose(array, (0, 2, 1, 3)).reshape(array.shape[0], count, tiles)

    want, want_z = flat(need), flat(both)
    order = jnp.arange(tiles, dtype=i32)
    before = (order[:, None] < order[None]).astype(f32)

    def places(flags):
        got = jnp.dot(flags.astype(jnp.bfloat16), before.astype(jnp.bfloat16), preferred_element_type=f32)
        return got.astype(i32)

    slot_x, slot_z = places(want), places(want_z)

    def listed(flags, slots, worth, cap):
        hit = flags[:, None] * (slots[:, None] == jnp.arange(cap, dtype=i32)[:, None]).astype(i32)
        return jnp.sum(hit * worth[:, None], axis=2)

    def at(array, i):
        return lax.dynamic_index_in_dim(array, i, 0, keepdims=False)

    steps = jnp.arange(planes, dtype=i32)
    goal = (plane + steps[1:]) % planes
    mine_z, mine_slot_z = jnp.take(want_z[:, me], goal, axis=0), jnp.take(slot_z[:, me], goal, axis=0)
    plain = jnp.broadcast_to(order, (planes + 1, tiles))
    ztab = listed(mine_z, mine_slot_z, plain[: planes - 1], tiles)
    here = at(slot_z, plane)
    source = ((plane - steps) % planes) * 2 + side
    worth = jnp.where((steps == 0)[:, None], order, jnp.take(here, source, axis=0))
    asked = jnp.concatenate([jnp.take(at(want, mate), source, axis=0), at(want, me)[me][None]])
    asked_slot = jnp.concatenate([jnp.take(at(slot_x, mate), source, axis=0), at(slot_x, me)[me][None]])
    xtab = listed(asked, asked_slot, jnp.concatenate([worth, order[None]]), most)

    caps = levels(tiles, most)
    cz_of = jnp.asarray([c[0] for c in caps], i32)
    cx_of = jnp.asarray([c[1] for c in caps], i32)
    level = jnp.sum(((most_z > cz_of) | (most_x > cx_of))[:-1].astype(i32))
    cz, cx = cz_of[level], cx_of[level]
    gap = (plane - devices // 2) % planes
    x_base = (planes - 1) * cz
    straight = jnp.where(devices == me, x_base + planes * cx, (gap - 1) * cz)
    start = jnp.where(devices % 2 == side, straight, x_base + gap * cx)
    by_z = ((devices % 2 == side) & (devices != me))[:, None]
    spot = start[:, None] + jnp.where(by_z, here, at(slot_x, me))
    spot = jnp.transpose(spot.reshape(count, head_dev, blk_dev), (1, 0, 2)).reshape(head_dev, 1, count * blk_dev)
    picks = (random_holder * blk_dev + random_offset).reshape(head_dev, count_req, 1)
    hits = (picks == jnp.arange(count * blk_dev, dtype=i32)).astype(i32)
    where = jnp.sum(hits * spot, axis=2).reshape(total)
    used = x_base + (planes + 1) * cx

    slots_all = -(-max((planes - 1) * c[0] + (planes + 1) * c[1] for c in caps) // CHUNK) * CHUNK
    where = jnp.minimum(where, slots_all - 1)

    def exchanged(number, caps):
        def run(ztab, xtab, k, v):
            return exchange(count, number, *caps, slots_all, blk_dev, ztab, xtab, k, v)

        return run

    rand, halo_kv, glob = lax.switch(
        level, [exchanged(n, c) for n, c in enumerate(caps)], ztab, xtab, keys, values
    )

    live = jnp.stack([me > 0, me < count - 1]).astype(i32)
    blocks = near_far(
        keep, live, where, used[None], queries, keys, values, halo_kv, glob, rand
    )
    return pack(blocks, keep_all, me, count, blk_dev, len(caps))


def solution(mesh):
    in_specs = (
        P("seq", "head"),
        P("seq", "head"),
        P("seq", "head"),
        P("head", "seq", None),
        P("head", "seq", None),
        P("seq"),
    )
    out_specs = P("seq", "head")
    return jax.shard_map(body, mesh=mesh, in_specs=in_specs, out_specs=out_specs, check_vma=False)
```

```python
import functools
import math

import jax
import jax.numpy as jnp
from jax import lax
from jax.experimental import pallas as pl
from jax.experimental.pallas import tpu as pltpu
from jax.sharding import PartitionSpec as P

DH = 128
B = 128
G = 2
R = 3

neg_big = -1e30
ANYWHERE = pltpu.CompilerParams(
    dimension_semantics=("arbitrary",), vmem_limit_bytes=60 * 1024 * 1024
)


def halo(block, axis, width):
    count = lax.axis_size(axis)
    forward = [(i, i + 1) for i in range(count - 1)]
    backward = [(target, source) for source, target in forward]
    low = lax.ppermute(block[-width:], axis, forward)
    high = lax.ppermute(block[:width], axis, backward)
    return jnp.concatenate([low, high], axis=0)


def broadcast(block, axis, source):
    block = jnp.where(lax.axis_index(axis) == source, block, jnp.zeros_like(block))
    return lax.psum(block, axis)


def pick_kernel(cap, head_ref, block_ref, k_ref, v_ref, out_ref):
    dest = pl.program_id(0)

    @pl.loop(0, cap)
    def _(j):
        rows = pl.ds(pl.multiple_of(block_ref[dest, j] * B, B), B)
        cols = pl.ds(pl.multiple_of(head_ref[dest, j] * DH, DH), DH)
        out_ref[j, 0] = k_ref[rows, cols]
        out_ref[j, 1] = v_ref[rows, cols]


def pick(keys, values, heads, blocks, seq_count, cap):
    whole = pl.BlockSpec(keys.shape, lambda d, *_: (0, 0))
    return pl.pallas_call(
        functools.partial(pick_kernel, cap),
        out_shape=jax.ShapeDtypeStruct((seq_count * cap, 2, B, DH), keys.dtype),
        grid_spec=pltpu.PrefetchScalarGridSpec(
            num_scalar_prefetch=2,
            grid=(seq_count,),
            in_specs=[whole, whole],
            out_specs=pl.BlockSpec((cap, 2, B, DH), lambda d, *_: (d, 0, 0, 0)),
        ),
        compiler_params=ANYWHERE,
    )(heads, blocks, keys, values)


def attend_kernel(
    blk_dev,
    keep_ref,
    slot_ref,
    live_ref,
    where_ref,
    q_ref,
    k_ref,
    v_ref,
    hk_ref,
    hv_ref,
    gk_ref,
    gv_ref,
    rand_ref,
    out_ref,
):
    scale = 1.0 / math.sqrt(DH)
    head = pl.program_id(0)
    out_ref[...] = jnp.zeros_like(out_ref)

    def tile(ref, halo_ref, i):
        if i < 0:
            return halo_ref[:B]
        if i >= blk_dev:
            return halo_ref[B:]
        return ref[i * B : (i + 1) * B]

    def one(i):
        q = q_ref[i * B : (i + 1) * B]
        near = range(i - 1, i + 2)
        picks = [where_ref[(head * blk_dev + i) * R + r] for r in range(R)]
        k_parts = [
            jnp.concatenate([tile(k_ref, hk_ref, n) for n in near], axis=0),
            gk_ref[...],
            jnp.concatenate([rand_ref[p, 0] for p in picks], axis=0),
        ]
        v_parts = [
            jnp.concatenate([tile(v_ref, hv_ref, n) for n in near], axis=0),
            gv_ref[...],
            jnp.concatenate([rand_ref[p, 1] for p in picks], axis=0),
        ]
        scores = [
            lax.dot_general(
                q, k, (((1,), (1,)), ((), ())), preferred_element_type=jnp.float32
            )
            * scale
            for k in k_parts
        ]
        lanes = lax.broadcasted_iota(jnp.int32, scores[0].shape, 1)
        if i == 0:
            dead = jnp.logical_and(lanes < B, live_ref[0] == 0)
            scores[0] = jnp.where(dead, neg_big, scores[0])
        if i == blk_dev - 1:
            dead = jnp.logical_and(lanes >= 2 * B, live_ref[1] == 0)
            scores[0] = jnp.where(dead, neg_big, scores[0])
        peak = functools.reduce(
            jnp.maximum, [jnp.max(s, axis=-1, keepdims=True) for s in scores]
        )
        numer = jnp.zeros((B, DH), jnp.float32)
        denom = jnp.zeros((B, 1), jnp.float32)
        for s, v in zip(scores, v_parts):
            w = jnp.exp(s - peak).astype(jnp.bfloat16)
            denom = denom + jnp.sum(w.astype(jnp.float32), axis=-1, keepdims=True)
            numer = numer + jnp.dot(w, v, preferred_element_type=jnp.float32)
        rows = pl.ds(pl.multiple_of(slot_ref[i] * B, B), B)
        out_ref[rows, :] = (numer / denom).astype(out_ref.dtype)

    for i in range(blk_dev):
        pl.when(keep_ref[i] > 0)(functools.partial(one, i))


def attend(keep, slot, live, where, q, k, v, hk, hv, gk, gv, rand):
    tok_dev, width_dev = q.shape
    blk_dev, head_dev = tok_dev // B, width_dev // DH

    def column(rows):
        return pl.BlockSpec((rows, DH), lambda h, *_: (0, h))

    return pl.pallas_call(
        functools.partial(attend_kernel, blk_dev),
        out_shape=jax.ShapeDtypeStruct(q.shape, q.dtype),
        grid_spec=pltpu.PrefetchScalarGridSpec(
            num_scalar_prefetch=4,
            grid=(head_dev,),
            in_specs=[column(tok_dev)] * 3
            + [column(2 * B)] * 2
            + [column(G * B)] * 2
            + [pl.BlockSpec(rand.shape, lambda h, *_: (0, 0, 0, 0))],
            out_specs=column(tok_dev),
        ),
        compiler_params=ANYWHERE,
    )(keep, slot, live, where, q, k, v, hk, hv, gk, gv, rand)


def copy_kernel(order_ref, in_ref, out_ref):
    out_ref[...] = in_ref[...]


def take_blocks(blocks, order, cap):
    width = blocks.shape[1]
    return pl.pallas_call(
        copy_kernel,
        out_shape=jax.ShapeDtypeStruct((cap * B, width), blocks.dtype),
        grid_spec=pltpu.PrefetchScalarGridSpec(
            num_scalar_prefetch=1,
            grid=(cap,),
            in_specs=[pl.BlockSpec((B, width), lambda j, order: (order[j], 0))],
            out_specs=pl.BlockSpec((B, width), lambda j, order: (j, 0)),
        ),
        compiler_params=ANYWHERE,
    )(order, blocks)


def merge_kernel(kind_ref, from_ref, old_ref, new_ref, out_ref):
    kind = kind_ref[pl.program_id(0)]

    @pl.when(kind == 0)
    def _():
        out_ref[...] = old_ref[...]

    @pl.when(kind == 1)
    def _():
        out_ref[...] = jnp.zeros_like(out_ref)

    @pl.when(kind == 2)
    def _():
        out_ref[...] = new_ref[...]


def merge_blocks(old, new, kind, place):
    tok_dev, width = old.shape
    return pl.pallas_call(
        merge_kernel,
        out_shape=jax.ShapeDtypeStruct(old.shape, old.dtype),
        grid_spec=pltpu.PrefetchScalarGridSpec(
            num_scalar_prefetch=2,
            grid=(tok_dev // B,),
            in_specs=[
                pl.BlockSpec((B, width), lambda j, kind, place: (j, 0)),
                pl.BlockSpec((B, width), lambda j, kind, place: (place[j], 0)),
            ],
            out_specs=pl.BlockSpec((B, width), lambda j, kind, place: (j, 0)),
        ),
        compiler_params=ANYWHERE,
    )(kind, place, old, new)


def exclusive(flags, axis):
    return jnp.cumsum(flags, axis=axis) - flags


def first_at_least(caps, amount):
    return jnp.sum((amount > jnp.asarray(caps, jnp.int32)).astype(jnp.int32))


def settle(blocks, keep_all, slot, source, distance, me, count, blk_dev):
    i32 = jnp.int32
    devices = jnp.arange(count, dtype=i32)
    slots = jnp.arange(blk_dev, dtype=i32)
    sizes = sorted({0, *range(blk_dev // 2, blk_dev - 1), blk_dev})
    for bit_pos in range((count - 1).bit_length()):
        stride = 2**bit_pos
        at = source - distance % stride
        moving = (keep_all > 0) & (distance // stride % 2 > 0)
        on_slot = ((slot[:, None] == slots) & moving[:, None]).astype(i32)
        on_device = (at[:, None] == devices).astype(i32)
        leaving = jnp.sum(on_device[:, :, None] * on_slot[:, None, :], axis=0)
        needed = jnp.max(jnp.sum(leaving, axis=1))
        nth = exclusive(leaving, 1)
        mine_out, mine_nth = leaving[me], nth[me]
        send = jnp.sum(
            mine_out[:, None] * (mine_nth[:, None] == slots).astype(i32) * slots[:, None], axis=0
        )
        far = jnp.minimum(me + stride, count - 1)
        comes = jnp.where(me + stride < count, leaving[far], 0)
        kind = jnp.where(comes > 0, 2, jnp.where(mine_out > 0, 1, 0)).astype(i32)
        place = jnp.where(comes > 0, nth[far], 0)
        all_pairs = [(i, i - stride) for i in range(stride, count)]
        split = count - stride // 2
        upper = [pair for pair in all_pairs if pair[0] >= split]
        halves = 2 * stride >= count and 0 < len(upper) < len(all_pairs)

        def shifting(cap, pairs, send=send, kind=kind, place=place):
            def run(blocks):
                if cap == 0:
                    return blocks
                moved = lax.ppermute(take_blocks(blocks, send, cap), "seq", pairs)
                return merge_blocks(blocks, moved, kind, jnp.minimum(place, cap - 1))

            return run

        which = first_at_least(sizes[:-1], needed)
        runs = [shifting(cap, all_pairs) for cap in sizes]
        if halves:
            runs += [shifting(cap, upper) for cap in sizes]
            lower = jnp.sum(leaving * (devices < split)[:, None].astype(i32))
            which = which + jnp.where(lower > 0, 0, len(sizes))
        blocks = lax.switch(which, runs, blocks)
    return blocks


def plain_body(queries, keys, values, random_holder, random_offset, keep):
    tok_dev, width_dev = queries.shape
    blk_dev = tok_dev // B
    head_dev = width_dev // DH
    seq_count = lax.axis_size("seq")
    head_count = lax.axis_size("head")
    me = lax.axis_index("seq")
    count_req = blk_dev * R
    total = head_dev * count_req
    i32 = jnp.int32

    code = random_holder * blk_dev + random_offset
    code = jnp.where((keep > 0)[None, :, None], code, -1).reshape(total)
    note = jnp.concatenate([code, keep])
    note = jnp.broadcast_to(note, (seq_count * head_count,) + note.shape)
    table = lax.all_to_all(note, ("seq", "head"), split_axis=0, concat_axis=0, tiled=True)
    table = table.reshape(seq_count, head_count, total + blk_dev)
    keep_all = table[:, 0, total:].reshape(seq_count * blk_dev)
    codes = table[:, :, :total]
    devices = jnp.arange(seq_count, dtype=i32)

    halo_k, halo_v = halo(keys, "seq", B), halo(values, "seq", B)

    named = jnp.where(codes >= 0, codes // blk_dev, -1)
    counts = jnp.sum((named[..., None] == devices).astype(i32), axis=2)
    most = jnp.max(counts)
    onehot = (named[me, lax.axis_index("head")][:, None] == devices).astype(i32)
    mine = exclusive(onehot, 0)
    my_slot = jnp.sum(mine * onehot, axis=1)
    my_holder = jnp.sum(onehot * devices, axis=1)

    group = codes[:, lax.axis_index("head")]
    asks = (named[:, lax.axis_index("head")] == me).astype(i32)
    order = exclusive(asks, 1)
    full = min(total, head_dev * max(2, (count_req + seq_count - 1) // seq_count))
    chosen = asks[..., None] * (order[..., None] == jnp.arange(full, dtype=i32)).astype(i32)
    ask_head = jnp.arange(total, dtype=i32) // count_req
    ask = jnp.where(group >= 0, group % blk_dev, 0) + ask_head[None] * blk_dev
    ask = jnp.sum(chosen * ask[..., None], axis=1)
    pick_head, pick_block = ask // blk_dev, ask % blk_dev

    rank = exclusive(keep_all, 0)
    slot = rank % blk_dev
    source = jnp.arange(seq_count * blk_dev, dtype=i32) // blk_dev
    distance = jnp.where(keep_all > 0, source - rank // blk_dev, 0)
    my_slots = lax.dynamic_slice_in_dim(slot, me * blk_dev, blk_dev)
    live = jnp.stack([me > 0, me < seq_count - 1]).astype(i32)

    caps = sorted({max(1, full * part // 12) for part in range(8, 13)})

    def gathered(cap):
        def run(q, k, v, hk, hv):
            gk, gv = broadcast(jnp.stack((k[: G * B], v[: G * B])), "seq", 0)
            picked = pick(k, v, pick_head, pick_block, seq_count, cap)
            replies = lax.all_to_all(picked, "seq", split_axis=0, concat_axis=0, tiled=True)
            where = jnp.minimum(my_holder * cap + my_slot, seq_count * cap - 1)
            return attend(keep, my_slots, live, where, q, k, v, hk, hv, gk, gv, replies)

        return run

    blocks = lax.switch(
        first_at_least(caps[:-1], most),
        [gathered(cap) for cap in caps],
        queries, keys, values, halo_k, halo_v,
    )

    return settle(blocks, keep_all, slot, source, distance, me, seq_count, blk_dev)


TILE = (2 * B, DH)
SMALL = pltpu.CompilerParams(vmem_limit_bytes=60 * 1024 * 1024)


def fits(planes, tiles, most):
    slots = 2 * (planes - 1) * tiles + 2 * planes * most + most
    return slots * 2 * B * DH * 2 <= 44 * 1024 * 1024


def exchange_kernel(
    count, cz, cx, blk_dev, ztab, xtab, k_ref, v_ref,
    rand_ref, halo_ref, glob_ref, home, zs, zr, xs, own,
    z_send, z_recv, x_send, x_recv, h_send, h_recv, g_send, g_recv, l_sem,
):
    planes = count // 2
    me = lax.axis_index("seq")
    plane, side = me // 2, me % 2
    mate = plane * 2 + 1 - side
    tok = k_ref.shape[0]
    head_dev = k_ref.shape[1] // DH
    barrier = pltpu.get_barrier_semaphore()
    for step in range(1, count):
        peer = lax.rem(me + step, count)
        pl.semaphore_signal(
            barrier, inc=1, device_id={"seq": peer}, device_id_type=pl.DeviceIdType.MESH
        )
    pl.semaphore_wait(barrier, count - 1)

    def remote(src, dst, send, recv, peer):
        return pltpu.make_async_remote_copy(
            src_ref=src, dst_ref=dst, send_sem=send, recv_sem=recv,
            device_id={"seq": peer}, device_id_type=pl.DeviceIdType.MESH,
        )

    tables = (k_ref, v_ref)
    low, high = pl.ds(0, B), pl.ds(B, B)
    first, last = pl.ds(0, B), pl.ds(tok - B, B)
    after = jnp.minimum(me + 1, count - 1)
    before = jnp.maximum(me - 1, 0)
    ups = [
        remote(tables[i].at[last], halo_ref.at[i, low], h_send.at[i], h_recv.at[i], after)
        for i in range(2)
    ]
    downs = [
        remote(tables[i].at[first], halo_ref.at[i, high], h_send.at[2 + i], h_recv.at[2 + i], before)
        for i in range(2)
    ]
    local = [
        pltpu.make_async_copy(tables[i].at[pl.ds(0, G * B)], glob_ref.at[i], l_sem.at[i])
        for i in range(2)
    ]
    item = glob_ref.at[side]
    chain = remote(item, item, g_send.at[0], g_recv.at[0], jnp.minimum(me + 2, count - 1))
    swap = remote(item, item, g_send.at[1], g_recv.at[1], mate)
    extra = remote(glob_ref.at[1], glob_ref.at[1], g_send.at[2], g_recv.at[0], mate)

    @pl.when(me == 0)
    def _():
        for c in local:
            c.start()
        for c in local:
            c.wait()
        chain.start()
        extra.start()
        swap.start()

    def pass_on():
        @pl.when(me > 0)
        def _():
            chain.wait_recv()

            @pl.when(plane < planes - 1)
            def _():
                chain.start()

            @pl.when(me > 1)
            def _():
                swap.start()

    @pl.when(me < count - 1)
    def _():
        for c in ups:
            c.start()

    @pl.when(me > 0)
    def _():
        for c in downs:
            c.start()

    @pl.when(me == 0)
    def _():
        halo_ref[:, low, :] = jnp.zeros((2, B, k_ref.shape[1]), k_ref.dtype)

    @pl.when(me == count - 1)
    def _():
        halo_ref[:, high, :] = jnp.zeros((2, B, k_ref.shape[1]), k_ref.dtype)

    def load_home(block, carry):
        rows = pl.ds(pl.multiple_of(block * B, B), B)
        for h in range(head_dev):
            cols = slice(h * DH, (h + 1) * DH)
            home[h * blk_dev + block, low, :] = k_ref[rows, cols]
            home[h * blk_dev + block, high, :] = v_ref[rows, cols]
        return carry

    lax.fori_loop(0, blk_dev, load_home, 0)

    def from_slots(dst, src, table, row, cap):
        def one(j, carry):
            dst[j] = src[table[row, j]]
            return carry

        lax.fori_loop(0, cap, one, 0)

    half = planes // 2
    lower = plane < half
    rest = [d for d in range(1, planes) if d != half]
    rising, falling = [half, *rest], [half, *reversed(rest)]
    x_base = (planes - 1) * cz
    z_copies = {
        d: remote(
            zs[d - 1], zr[d - 1], z_send.at[d - 1], z_recv.at[d - 1],
            lax.rem(plane + d, planes) * 2 + side,
        )
        for d in rising
    }
    x_copies = [
        remote(
            xs[d], rand_ref.at[pl.ds(x_base + d * cx, cx)],
            x_send.at[d], x_recv.at[d], mate,
        )
        for d in range(planes)
    ]
    from_slots(zs[half - 1], home, ztab, half - 1, cz)
    from_slots(xs[0], home, xtab, 0, cx)
    z_copies[half].start()
    for d in rest:
        from_slots(zs[d - 1], home, ztab, d - 1, cz)
    x_copies[0].start()

    @pl.when(lower)
    def _():
        pass_on()
        for d in falling[1:]:
            z_copies[d].start()

    @pl.when(jnp.logical_not(lower))
    def _():
        for d in rising[1:]:
            z_copies[d].start()
        pass_on()

    from_slots(own, home, xtab, planes, cx)
    keep_own = pltpu.make_async_copy(
        own, rand_ref.at[pl.ds(x_base + planes * cx, cx)], l_sem.at[2]
    )
    keep_own.start()
    outs = {
        d: pltpu.make_async_copy(
            zr[d - 1], rand_ref.at[pl.ds((d - 1) * cz, cz)], l_sem.at[2 + d]
        )
        for d in rising
    }

    def forward(d):
        z_copies[d].wait_recv()
        outs[d].start()
        from_slots(xs[d], zr[d - 1], xtab, d, cx)
        x_copies[d].start()

    @pl.when(lower)
    def _():
        for d in falling:
            forward(d)

    @pl.when(jnp.logical_not(lower))
    def _():
        for d in rising:
            forward(d)

    @pl.when(me > 0)
    def _():
        swap.wait_recv()

    @pl.when(plane < planes - 1)
    def _():
        chain.wait_send()

    @pl.when(me == 0)
    def _():
        extra.wait_send()

    @pl.when(me != 1)
    def _():
        swap.wait_send()

    @pl.when(me < count - 1)
    def _():
        for c in ups:
            c.wait_send()
        for c in downs:
            c.wait_recv()

    @pl.when(me > 0)
    def _():
        for c in downs:
            c.wait_send()
        for c in ups:
            c.wait_recv()

    keep_own.wait()
    for d in rising:
        outs[d].wait()
        z_copies[d].wait_send()
    for c in x_copies:
        c.wait()


def exchange(count, level, cz, cx, slots, blk_dev, ztab, xtab, keys, values):
    planes = count // 2
    tok, width = keys.shape
    smem = pl.BlockSpec(memory_space=pltpu.SMEM)
    vmem = pl.BlockSpec(memory_space=pltpu.VMEM)
    dtype = keys.dtype
    dma = pltpu.SemaphoreType.DMA
    return pl.pallas_call(
        functools.partial(exchange_kernel, count, cz, cx, blk_dev),
        out_shape=(
            jax.ShapeDtypeStruct((slots, *TILE), dtype),
            jax.ShapeDtypeStruct((2, 2 * B, width), dtype),
            jax.ShapeDtypeStruct((2, G * B, width), dtype),
        ),
        in_specs=[smem, smem, vmem, vmem],
        out_specs=(pl.BlockSpec(memory_space=pl.ANY), vmem, vmem),
        scratch_shapes=[
            pltpu.VMEM((tok // B * (width // DH), *TILE), dtype),
            [pltpu.VMEM((cz, *TILE), dtype) for _ in range(planes - 1)],
            [pltpu.VMEM((cz, *TILE), dtype) for _ in range(planes - 1)],
            [pltpu.VMEM((cx, *TILE), dtype) for _ in range(planes)],
            pltpu.VMEM((cx, *TILE), dtype),
            dma((planes - 1,)), dma((planes - 1,)),
            dma((planes,)), dma((planes,)),
            dma((4,)), dma((4,)), dma((3,)), dma((2,)), dma((2 + planes,)),
        ],
        compiler_params=pltpu.CompilerParams(
            collective_id=level, has_side_effects=True,
            vmem_limit_bytes=60 * 1024 * 1024,
        ),
    )(ztab, xtab, keys, values)


PIECES = 4


def settle_kernel(
    count, caps, cr, cx, blk_dev, ztab, rtab, xtab, otab, in_ref, out_ref,
    mine, zs, pool, rs, xs, xr, z_send, z_recv, r_send, r_recv, x_send, x_recv,
):
    planes = count // 2
    me = lax.axis_index("seq")
    plane, side = me // 2, me % 2
    mate = plane * 2 + 1 - side
    wide = in_ref.shape[1] // PIECES
    barrier = pltpu.get_barrier_semaphore()
    for step in range(1, count):
        peer = lax.rem(me + step, count)
        pl.semaphore_signal(
            barrier, inc=1, device_id={"seq": peer}, device_id_type=pl.DeviceIdType.MESH
        )
    pl.semaphore_wait(barrier, count - 1)

    def remote(src, dst, send, recv, peer):
        return pltpu.make_async_remote_copy(
            src_ref=src, dst_ref=dst, send_sem=send, recv_sem=recv,
            device_id={"seq": peer}, device_id_type=pl.DeviceIdType.MESH,
        )

    used = [d for d in range(1, planes) if caps[d - 1] > 0]
    used.sort(reverse=True)
    base = {d: blk_dev + sum(caps[: d - 1]) for d in used}
    gate = planes // 2 - 1
    beyond = range(1, gate + 1)
    r_base = blk_dev + sum(caps)

    def sends(d):
        return jnp.logical_and(plane >= d, jnp.logical_or(plane != gate + 1, d == 1))

    def gets(d):
        return jnp.logical_and(plane + d < planes, jnp.logical_or(plane + d != gate + 1, d == 1))

    def fill(dst, src, table, row, cap):
        def one(j, carry):
            dst[j] = src[table[row, j]]
            return carry

        lax.fori_loop(0, cap, one, 0)

    def own_part(piece):
        def one(j, carry):
            rows = pl.ds(pl.multiple_of(j * B, B), B)
            block = in_ref[rows, piece * wide : (piece + 1) * wide]
            mine[piece][j] = block
            pool[piece][j] = block
            return carry

        lax.fori_loop(0, blk_dev, one, 0)

    z_copies, x_copies = {}, []
    for piece in range(PIECES):
        for n, d in enumerate(used):
            z_copies[piece, d] = remote(
                zs[piece][n], pool[piece].at[pl.ds(base[d], caps[d - 1])],
                z_send.at[piece, n], z_recv.at[piece, n],
                jnp.maximum(me - 2 * d, 0),
            )
        for d in beyond:
            z_copies[piece, -d] = remote(
                rs[piece][d - 1], pool[piece].at[pl.ds(r_base, cr)],
                r_send.at[piece, d - 1], r_recv.at[piece],
                jnp.maximum(me - 2 * d, 0),
            )
        x_copies.append(remote(xs[piece], xr[piece], x_send.at[piece], x_recv.at[piece], mate))
    def start_z(piece):
        for d in used:
            @pl.when(sends(d))
            def _(d=d):
                z_copies[piece, d].start()

    for piece in range(PIECES):
        own_part(piece)
        for n, d in enumerate(used):
            fill(zs[piece][n], mine[piece], ztab, d - 1, caps[d - 1])
        if piece > 0:
            start_z(piece - 1)
    start_z(PIECES - 1)

    def finish(piece):
        x_copies[piece].wait_recv()

        def one(j, carry):
            rows = pl.ds(pl.multiple_of(j * B, B), B)
            kind = otab[0, j]
            near, far = pool[piece][otab[1, j]], xr[piece][otab[2, j]]
            block = jnp.where(kind == 1, near, jnp.where(kind == 2, far, jnp.zeros_like(far)))
            out_ref[rows, piece * wide : (piece + 1) * wide] = block
            return carry

        lax.fori_loop(0, blk_dev, one, 0)

    for piece in range(PIECES):
        for d in used:
            @pl.when(gets(d))
            def _(d=d, piece=piece):
                z_copies[piece, d].wait_recv()

        @pl.when(plane == gate)
        def _(piece=piece):
            for d in beyond:
                fill(rs[piece][d - 1], pool[piece], rtab, d - 1, cr)
                z_copies[piece, -d].start()

        @pl.when(plane < gate)
        def _(piece=piece):
            if gate > 0:
                z_copies[piece, -1].wait_recv()

        fill(xs[piece], pool[piece], xtab, 0, cx)
        x_copies[piece].start()
        if piece > 0:
            finish(piece - 1)
    finish(PIECES - 1)
    for piece in range(PIECES):
        x_copies[piece].wait_send()
        for d in used:
            @pl.when(sends(d))
            def _(d=d, piece=piece):
                z_copies[piece, d].wait_send()

        @pl.when(plane == gate)
        def _(piece=piece):
            for d in beyond:
                z_copies[piece, -d].wait_send()


def settled(count, number, caps, cr, cx, blk_dev, ztab, rtab, xtab, otab, blocks):
    tok, width = blocks.shape
    planes, wide = count // 2, width // PIECES
    smem = pl.BlockSpec(memory_space=pltpu.SMEM)
    vmem = pl.BlockSpec(memory_space=pltpu.VMEM)
    dma, dtype = pltpu.SemaphoreType.DMA, blocks.dtype
    sent = [caps[d - 1] for d in range(planes - 1, 0, -1) if caps[d - 1] > 0]

    def each(rows):
        return [pltpu.VMEM((rows, B, wide), dtype) for _ in range(PIECES)]

    return pl.pallas_call(
        functools.partial(settle_kernel, count, caps, cr, cx, blk_dev),
        out_shape=jax.ShapeDtypeStruct(blocks.shape, dtype),
        in_specs=[smem, smem, smem, smem, vmem],
        out_specs=vmem,
        scratch_shapes=[
            each(blk_dev),
            [[pltpu.VMEM((c, B, wide), dtype) for c in sent] for _ in range(PIECES)],
            each(blk_dev + sum(caps) + cr),
            [[pltpu.VMEM((cr, B, wide), dtype) for _ in range(planes // 2 - 1)] for _ in range(PIECES)],
            each(cx),
            each(cx),
            dma((PIECES, len(sent))), dma((PIECES, len(sent))),
            dma((PIECES, planes // 2)), dma((PIECES,)), dma((PIECES,)), dma((PIECES,)),
        ],
        compiler_params=pltpu.CompilerParams(
            collective_id=number, has_side_effects=True,
            vmem_limit_bytes=60 * 1024 * 1024,
        ),
    )(ztab, rtab, xtab, otab, blocks)


def settle_levels(planes, blk_dev):
    def pad(first, second):
        return ((first, second) + (0,) * planes)[: planes - 1]

    half, few = blk_dev // 2, blk_dev * 3 // 4
    choices = [
        (2 * max(f + t, f + r) + r, pad(f, t), r, few)
        for f in range(half, few + 1)
        for t in range(half, few + 1)
        for r in (half // 2, half)
        if abs(f - t) < 2 or t == half
    ]
    choices = sorted(choices) + [(0, (blk_dev,) * (planes - 1), blk_dev, blk_dev)]
    return [limits for _, *limits in choices]


def pack(blocks, keep_all, me, count, blk_dev, first_id):
    i32 = jnp.int32
    planes = count // 2
    plane, side = me // 2, me % 2
    index = jnp.arange(count * blk_dev, dtype=i32)
    kept = keep_all > 0
    rank = exclusive(keep_all, 0)
    source, goal = index // blk_dev, rank // blk_dev
    gate = planes // 2 - 1
    relayed = kept & (source // 2 == gate + 1) & (goal // 2 < gate)
    far = jnp.where(relayed, 1, source // 2 - goal // 2)
    earlier = index[None] < index[:, None]
    same_z = (source[:, None] == source[None]) & (far[:, None] == far[None])
    by_z = jnp.sum((earlier & same_z & kept[None]).astype(i32), axis=1)
    same_r = (goal[:, None] // 2 == goal[None] // 2) & (source[:, None] % 2 == source[None] % 2)
    by_r = jnp.sum((earlier & same_r & relayed[None]).astype(i32), axis=1)
    crosses = kept & (source % 2 != goal % 2)
    same_x = (goal[:, None] // 2 == goal[None] // 2) & (source[:, None] % 2 == source[None] % 2)
    by_x = jnp.sum((earlier & same_x & crosses[None]).astype(i32), axis=1)
    deltas = jnp.arange(1, planes, dtype=i32)
    of_delta = kept[None] & (far[None] == deltas[:, None])
    most_z = jnp.max(of_delta * (by_z + 1)[None], axis=1)
    most_x = jnp.max(crosses * (by_x + 1))
    most_r = jnp.max(relayed * (by_r + 1))
    choices = settle_levels(planes, blk_dev)
    caps = jnp.asarray([c for c, _, _ in choices], i32)
    caps_r = jnp.asarray([c for _, c, _ in choices], i32)
    caps_x = jnp.asarray([c for _, _, c in choices], i32)
    enough = jnp.all(most_z[None] <= caps, axis=1) & (most_x <= caps_x) & (most_r <= caps_r)
    level = jnp.argmax(enough).astype(i32)
    own_caps = caps[level]
    base = blk_dev + exclusive(own_caps, 0)
    base = jnp.sum((far[:, None] == deltas[None]).astype(i32) * base[None], axis=1)
    first = jnp.where(far == 0, index % blk_dev, base + by_z)
    held = jnp.where(relayed, blk_dev + jnp.sum(own_caps) + by_r, first)

    def listed(flags, places, worth, cap):
        hit = (flags[..., None, :] & (places == jnp.arange(cap, dtype=i32)[:, None])).astype(i32)
        return jnp.sum(hit * worth, axis=-1)

    ztab = listed(of_delta & (source == me)[None], by_z, index % blk_dev, blk_dev)
    hops = jnp.arange(1, max(gate, 1) + 1, dtype=i32)
    passes = relayed & (source % 2 == side) & (plane == gate)
    rtab = listed(passes[None] & (gate - goal // 2 == hops[:, None]), by_r, first, blk_dev)
    comes = crosses & (goal // 2 == plane) & (source % 2 == side)
    xtab = listed(comes, by_x, held, blk_dev)[None]
    lands = kept & (goal == me)
    straight = source % 2 == side
    kind = jnp.where(straight, 1, 2)
    worth = jnp.stack([kind, jnp.where(straight, held, 0), jnp.where(straight, 0, by_x)])
    hit = (lands & (rank % blk_dev == jnp.arange(blk_dev, dtype=i32)[:, None])).astype(i32)
    otab = jnp.sum(hit[None] * worth[:, None], axis=-1)

    def run(number, *limits):
        return lambda *args: settled(count, first_id + number, *limits, blk_dev, *args)

    runs = [run(n, *limits) for n, limits in enumerate(choices)]
    return lax.switch(level, runs, ztab, rtab, xtab, otab, blocks)


CHUNK = 8


def near_far_kernel(
    blk_dev, keep_ref, live_ref, where_ref, used_ref,
    q_ref, k_ref, v_ref, hk_ref, hv_ref, gk_ref, gv_ref, rand_hbm, out_ref, rand_ref, sems,
):
    scale = 1.0 / math.sqrt(DH)
    head = pl.program_id(0)
    chunks = rand_hbm.shape[0] // CHUNK

    @pl.when(head == 0)
    def _():
        def copy(c):
            rows = pl.ds(c * CHUNK, CHUNK)
            return pltpu.make_async_copy(rand_hbm.at[rows], rand_ref.at[rows], sems.at[c])

        for c in range(chunks):
            pl.when(c * CHUNK < used_ref[0])(lambda c=c: copy(c).start())
        for c in range(chunks):
            pl.when(c * CHUNK < used_ref[0])(lambda c=c: copy(c).wait())

    def tile(ref, halo_ref, i):
        if i < 0:
            return halo_ref[0, :B]
        if i >= blk_dev:
            return halo_ref[0, B:]
        return ref[i * B : (i + 1) * B]

    def one(i):
        q = q_ref[i * B : (i + 1) * B]
        near = range(i - 1, i + 2)
        picks = [where_ref[(head * blk_dev + i) * R + r] for r in range(R)]
        k_parts = [
            jnp.concatenate([tile(k_ref, hk_ref, n) for n in near], axis=0),
            gk_ref[0],
            jnp.concatenate([rand_ref[p, :B] for p in picks], axis=0),
        ]
        v_parts = [
            jnp.concatenate([tile(v_ref, hv_ref, n) for n in near], axis=0),
            gv_ref[0],
            jnp.concatenate([rand_ref[p, B:] for p in picks], axis=0),
        ]
        scores = [
            lax.dot_general(
                q, k, (((1,), (1,)), ((), ())), preferred_element_type=jnp.float32
            )
            * scale
            for k in k_parts
        ]
        lanes = lax.broadcasted_iota(jnp.int32, scores[0].shape, 1)
        if i == 0:
            dead = jnp.logical_and(lanes < B, live_ref[0] == 0)
            scores[0] = jnp.where(dead, neg_big, scores[0])
        if i == blk_dev - 1:
            dead = jnp.logical_and(lanes >= 2 * B, live_ref[1] == 0)
            scores[0] = jnp.where(dead, neg_big, scores[0])
        peak = functools.reduce(
            jnp.maximum, [jnp.max(s, axis=-1, keepdims=True) for s in scores]
        )
        numer = jnp.zeros((B, DH), jnp.float32)
        denom = jnp.zeros((B, 1), jnp.float32)
        for s, v in zip(scores, v_parts):
            w = jnp.exp(s - peak).astype(jnp.bfloat16)
            denom = denom + jnp.sum(w.astype(jnp.float32), axis=-1, keepdims=True)
            numer = numer + jnp.dot(w, v, preferred_element_type=jnp.float32)
        out_ref[i * B : (i + 1) * B, :] = (numer / denom).astype(out_ref.dtype)

    for i in range(blk_dev):
        pl.when(keep_ref[i] > 0)(functools.partial(one, i))


def near_far(keep, live, where, used, q, k, v, halo_kv, glob, rand):
    tok_dev, width_dev = q.shape
    blk_dev, head_dev = tok_dev // B, width_dev // DH

    def column(rows):
        return pl.BlockSpec((rows, DH), lambda h, *_: (0, h))

    def part(rows, which):
        return pl.BlockSpec((1, rows, DH), lambda h, *_: (which, 0, h))

    return pl.pallas_call(
        functools.partial(near_far_kernel, blk_dev),
        out_shape=jax.ShapeDtypeStruct(q.shape, q.dtype),
        grid_spec=pltpu.PrefetchScalarGridSpec(
            num_scalar_prefetch=4,
            grid=(head_dev,),
            in_specs=[column(tok_dev)] * 3
            + [part(2 * B, 0), part(2 * B, 1), part(G * B, 0), part(G * B, 1)]
            + [pl.BlockSpec(memory_space=pl.ANY)],
            out_specs=column(tok_dev),
            scratch_shapes=[
                pltpu.VMEM(rand.shape, rand.dtype),
                pltpu.SemaphoreType.DMA((rand.shape[0] // CHUNK,)),
            ],
        ),
        compiler_params=ANYWHERE,
    )(keep, live, where, used, q, k, v, halo_kv, halo_kv, glob, glob, rand)


def levels(tiles, most):
    caps = []
    for part in (22, 24, 26, 28, 30, 32, 36):
        cz = min(tiles, tiles * part // 64)
        caps.append((cz, min(most, max(1, most * (part // 2 + 4) // 24))))
    caps.append((tiles, most))
    return sorted(set(caps))


def body(queries, keys, values, random_holder, random_offset, keep):
    tok_dev, width_dev = queries.shape
    blk_dev = tok_dev // B
    head_dev = width_dev // DH
    count = lax.axis_size("seq")
    head_count = lax.axis_size("head")
    count_req = blk_dev * R
    total = head_dev * count_req
    tiles = head_dev * blk_dev
    most = min(tiles, head_dev * max(2, (count_req + count - 1) // count))
    planes = count // 2
    if count % 2 or planes % 2 or not fits(planes, tiles, most):
        return plain_body(queries, keys, values, random_holder, random_offset, keep)
    me = lax.axis_index("seq")
    plane, side = me // 2, me % 2
    mate = me + 1 - 2 * side
    i32, f32 = jnp.int32, jnp.float32

    code = random_holder * blk_dev + random_offset
    code = jnp.where((keep > 0)[None, :, None], code, -1).reshape(total)
    note = jnp.concatenate([code, keep])
    note = jnp.broadcast_to(note, (count * head_count,) + note.shape)
    table = lax.all_to_all(note, ("seq", "head"), split_axis=0, concat_axis=0, tiled=True)
    table = table.reshape(count, head_count, total + blk_dev)
    keep_all = table[:, 0, total:].reshape(count * blk_dev)
    codes = table[:, :, :total].reshape(count, head_count, head_dev, 1, count_req)

    blocks = jnp.arange(count * blk_dev, dtype=i32)[:, None]
    need = jnp.max((codes == blocks).astype(i32), axis=-1)
    need = need.reshape(count, head_count, head_dev, count, blk_dev)
    both = jnp.max(need.reshape(planes, 2, *need.shape[1:]), axis=1)
    devices = jnp.arange(count, dtype=i32)
    away = (devices[None] // 2 != jnp.arange(planes, dtype=i32)[:, None]).astype(i32)
    most_z = jnp.max(jnp.sum(both, axis=(2, 4)) * away[:, None])
    most_x = jnp.max(jnp.sum(need, axis=(2, 4)))

    group = lax.axis_index("head")

    def flat(array):
        array = lax.dynamic_index_in_dim(array, group, 1, keepdims=False)
        return jnp.transpose(array, (0, 2, 1, 3)).reshape(array.shape[0], count, tiles)

    want, want_z = flat(need), flat(both)
    order = jnp.arange(tiles, dtype=i32)
    before = (order[:, None] < order[None]).astype(f32)

    def places(flags):
        got = jnp.dot(flags.astype(jnp.bfloat16), before.astype(jnp.bfloat16), preferred_element_type=f32)
        return got.astype(i32)

    slot_x, slot_z = places(want), places(want_z)

    def listed(flags, slots, worth, cap):
        hit = flags[:, None] * (slots[:, None] == jnp.arange(cap, dtype=i32)[:, None]).astype(i32)
        return jnp.sum(hit * worth[:, None], axis=2)

    def at(array, i):
        return lax.dynamic_index_in_dim(array, i, 0, keepdims=False)

    steps = jnp.arange(planes, dtype=i32)
    goal = (plane + steps[1:]) % planes
    mine_z, mine_slot_z = jnp.take(want_z[:, me], goal, axis=0), jnp.take(slot_z[:, me], goal, axis=0)
    plain = jnp.broadcast_to(order, (planes + 1, tiles))
    ztab = listed(mine_z, mine_slot_z, plain[: planes - 1], tiles)
    here = at(slot_z, plane)
    source = ((plane - steps) % planes) * 2 + side
    worth = jnp.where((steps == 0)[:, None], order, jnp.take(here, source, axis=0))
    asked = jnp.concatenate([jnp.take(at(want, mate), source, axis=0), at(want, me)[me][None]])
    asked_slot = jnp.concatenate([jnp.take(at(slot_x, mate), source, axis=0), at(slot_x, me)[me][None]])
    xtab = listed(asked, asked_slot, jnp.concatenate([worth, order[None]]), most)

    caps = levels(tiles, most)
    cz_of = jnp.asarray([c[0] for c in caps], i32)
    cx_of = jnp.asarray([c[1] for c in caps], i32)
    level = jnp.sum(((most_z > cz_of) | (most_x > cx_of))[:-1].astype(i32))
    cz, cx = cz_of[level], cx_of[level]
    gap = (plane - devices // 2) % planes
    x_base = (planes - 1) * cz
    straight = jnp.where(devices == me, x_base + planes * cx, (gap - 1) * cz)
    start = jnp.where(devices % 2 == side, straight, x_base + gap * cx)
    by_z = ((devices % 2 == side) & (devices != me))[:, None]
    spot = start[:, None] + jnp.where(by_z, here, at(slot_x, me))
    spot = jnp.transpose(spot.reshape(count, head_dev, blk_dev), (1, 0, 2)).reshape(head_dev, 1, count * blk_dev)
    picks = (random_holder * blk_dev + random_offset).reshape(head_dev, count_req, 1)
    hits = (picks == jnp.arange(count * blk_dev, dtype=i32)).astype(i32)
    where = jnp.sum(hits * spot, axis=2).reshape(total)
    used = x_base + (planes + 1) * cx

    slots_all = -(-max((planes - 1) * c[0] + (planes + 1) * c[1] for c in caps) // CHUNK) * CHUNK
    where = jnp.minimum(where, slots_all - 1)

    def exchanged(number, caps):
        def run(ztab, xtab, k, v):
            return exchange(count, number, *caps, slots_all, blk_dev, ztab, xtab, k, v)

        return run

    rand, halo_kv, glob = lax.switch(
        level, [exchanged(n, c) for n, c in enumerate(caps)], ztab, xtab, keys, values
    )

    live = jnp.stack([me > 0, me < count - 1]).astype(i32)
    blocks = near_far(
        keep, live, where, used[None], queries, keys, values, halo_kv, glob, rand
    )
    return pack(blocks, keep_all, me, count, blk_dev, len(caps))


def solution(mesh):
    in_specs = (
        P("seq", "head"),
        P("seq", "head"),
        P("seq", "head"),
        P("head", "seq", None),
        P("head", "seq", None),
        P("seq"),
    )
    out_specs = P("seq", "head")
    return jax.shard_map(body, mesh=mesh, in_specs=in_specs, out_specs=out_specs, check_vma=False)
```

```python
import functools
import math

import jax
import jax.numpy as jnp
from jax import lax
from jax.experimental import pallas as pl
from jax.experimental.pallas import tpu as pltpu
from jax.sharding import PartitionSpec as P

DH = 128
B = 128
G = 2
R = 3

neg_big = -1e30
ANYWHERE = pltpu.CompilerParams(
    dimension_semantics=("arbitrary",), vmem_limit_bytes=60 * 1024 * 1024
)


def halo(block, axis, width):
    count = lax.axis_size(axis)
    forward = [(i, i + 1) for i in range(count - 1)]
    backward = [(target, source) for source, target in forward]
    low = lax.ppermute(block[-width:], axis, forward)
    high = lax.ppermute(block[:width], axis, backward)
    return jnp.concatenate([low, high], axis=0)


def broadcast(block, axis, source):
    block = jnp.where(lax.axis_index(axis) == source, block, jnp.zeros_like(block))
    return lax.psum(block, axis)


def pick_kernel(cap, head_ref, block_ref, k_ref, v_ref, out_ref):
    dest = pl.program_id(0)

    @pl.loop(0, cap)
    def _(j):
        rows = pl.ds(pl.multiple_of(block_ref[dest, j] * B, B), B)
        cols = pl.ds(pl.multiple_of(head_ref[dest, j] * DH, DH), DH)
        out_ref[j, 0] = k_ref[rows, cols]
        out_ref[j, 1] = v_ref[rows, cols]


def pick(keys, values, heads, blocks, seq_count, cap):
    whole = pl.BlockSpec(keys.shape, lambda d, *_: (0, 0))
    return pl.pallas_call(
        functools.partial(pick_kernel, cap),
        out_shape=jax.ShapeDtypeStruct((seq_count * cap, 2, B, DH), keys.dtype),
        grid_spec=pltpu.PrefetchScalarGridSpec(
            num_scalar_prefetch=2,
            grid=(seq_count,),
            in_specs=[whole, whole],
            out_specs=pl.BlockSpec((cap, 2, B, DH), lambda d, *_: (d, 0, 0, 0)),
        ),
        compiler_params=ANYWHERE,
    )(heads, blocks, keys, values)


def attend_kernel(
    blk_dev,
    keep_ref,
    slot_ref,
    live_ref,
    where_ref,
    q_ref,
    k_ref,
    v_ref,
    hk_ref,
    hv_ref,
    gk_ref,
    gv_ref,
    rand_ref,
    out_ref,
):
    scale = 1.0 / math.sqrt(DH)
    head = pl.program_id(0)
    out_ref[...] = jnp.zeros_like(out_ref)

    def tile(ref, halo_ref, i):
        if i < 0:
            return halo_ref[:B]
        if i >= blk_dev:
            return halo_ref[B:]
        return ref[i * B : (i + 1) * B]

    def one(i):
        q = q_ref[i * B : (i + 1) * B]
        near = range(i - 1, i + 2)
        picks = [where_ref[(head * blk_dev + i) * R + r] for r in range(R)]
        k_parts = [
            jnp.concatenate([tile(k_ref, hk_ref, n) for n in near], axis=0),
            gk_ref[...],
            jnp.concatenate([rand_ref[p, 0] for p in picks], axis=0),
        ]
        v_parts = [
            jnp.concatenate([tile(v_ref, hv_ref, n) for n in near], axis=0),
            gv_ref[...],
            jnp.concatenate([rand_ref[p, 1] for p in picks], axis=0),
        ]
        scores = [
            lax.dot_general(
                q, k, (((1,), (1,)), ((), ())), preferred_element_type=jnp.float32
            )
            * scale
            for k in k_parts
        ]
        lanes = lax.broadcasted_iota(jnp.int32, scores[0].shape, 1)
        if i == 0:
            dead = jnp.logical_and(lanes < B, live_ref[0] == 0)
            scores[0] = jnp.where(dead, neg_big, scores[0])
        if i == blk_dev - 1:
            dead = jnp.logical_and(lanes >= 2 * B, live_ref[1] == 0)
            scores[0] = jnp.where(dead, neg_big, scores[0])
        peak = functools.reduce(
            jnp.maximum, [jnp.max(s, axis=-1, keepdims=True) for s in scores]
        )
        numer = jnp.zeros((B, DH), jnp.float32)
        denom = jnp.zeros((B, 1), jnp.float32)
        for s, v in zip(scores, v_parts):
            w = jnp.exp(s - peak).astype(jnp.bfloat16)
            denom = denom + jnp.sum(w.astype(jnp.float32), axis=-1, keepdims=True)
            numer = numer + jnp.dot(w, v, preferred_element_type=jnp.float32)
        rows = pl.ds(pl.multiple_of(slot_ref[i] * B, B), B)
        out_ref[rows, :] = (numer / denom).astype(out_ref.dtype)

    for i in range(blk_dev):
        pl.when(keep_ref[i] > 0)(functools.partial(one, i))


def attend(keep, slot, live, where, q, k, v, hk, hv, gk, gv, rand):
    tok_dev, width_dev = q.shape
    blk_dev, head_dev = tok_dev // B, width_dev // DH

    def column(rows):
        return pl.BlockSpec((rows, DH), lambda h, *_: (0, h))

    return pl.pallas_call(
        functools.partial(attend_kernel, blk_dev),
        out_shape=jax.ShapeDtypeStruct(q.shape, q.dtype),
        grid_spec=pltpu.PrefetchScalarGridSpec(
            num_scalar_prefetch=4,
            grid=(head_dev,),
            in_specs=[column(tok_dev)] * 3
            + [column(2 * B)] * 2
            + [column(G * B)] * 2
            + [pl.BlockSpec(rand.shape, lambda h, *_: (0, 0, 0, 0))],
            out_specs=column(tok_dev),
        ),
        compiler_params=ANYWHERE,
    )(keep, slot, live, where, q, k, v, hk, hv, gk, gv, rand)


def copy_kernel(order_ref, in_ref, out_ref):
    out_ref[...] = in_ref[...]


def take_blocks(blocks, order, cap):
    width = blocks.shape[1]
    return pl.pallas_call(
        copy_kernel,
        out_shape=jax.ShapeDtypeStruct((cap * B, width), blocks.dtype),
        grid_spec=pltpu.PrefetchScalarGridSpec(
            num_scalar_prefetch=1,
            grid=(cap,),
            in_specs=[pl.BlockSpec((B, width), lambda j, order: (order[j], 0))],
            out_specs=pl.BlockSpec((B, width), lambda j, order: (j, 0)),
        ),
        compiler_params=ANYWHERE,
    )(order, blocks)


def merge_kernel(kind_ref, from_ref, old_ref, new_ref, out_ref):
    kind = kind_ref[pl.program_id(0)]

    @pl.when(kind == 0)
    def _():
        out_ref[...] = old_ref[...]

    @pl.when(kind == 1)
    def _():
        out_ref[...] = jnp.zeros_like(out_ref)

    @pl.when(kind == 2)
    def _():
        out_ref[...] = new_ref[...]


def merge_blocks(old, new, kind, place):
    tok_dev, width = old.shape
    return pl.pallas_call(
        merge_kernel,
        out_shape=jax.ShapeDtypeStruct(old.shape, old.dtype),
        grid_spec=pltpu.PrefetchScalarGridSpec(
            num_scalar_prefetch=2,
            grid=(tok_dev // B,),
            in_specs=[
                pl.BlockSpec((B, width), lambda j, kind, place: (j, 0)),
                pl.BlockSpec((B, width), lambda j, kind, place: (place[j], 0)),
            ],
            out_specs=pl.BlockSpec((B, width), lambda j, kind, place: (j, 0)),
        ),
        compiler_params=ANYWHERE,
    )(kind, place, old, new)


def exclusive(flags, axis):
    return jnp.cumsum(flags, axis=axis) - flags


def first_at_least(caps, amount):
    return jnp.sum((amount > jnp.asarray(caps, jnp.int32)).astype(jnp.int32))


def settle(blocks, keep_all, slot, source, distance, me, count, blk_dev):
    i32 = jnp.int32
    devices = jnp.arange(count, dtype=i32)
    slots = jnp.arange(blk_dev, dtype=i32)
    sizes = sorted({0, *range(blk_dev // 2, blk_dev - 1), blk_dev})
    for bit_pos in range((count - 1).bit_length()):
        stride = 2**bit_pos
        at = source - distance % stride
        moving = (keep_all > 0) & (distance // stride % 2 > 0)
        on_slot = ((slot[:, None] == slots) & moving[:, None]).astype(i32)
        on_device = (at[:, None] == devices).astype(i32)
        leaving = jnp.sum(on_device[:, :, None] * on_slot[:, None, :], axis=0)
        needed = jnp.max(jnp.sum(leaving, axis=1))
        nth = exclusive(leaving, 1)
        mine_out, mine_nth = leaving[me], nth[me]
        send = jnp.sum(
            mine_out[:, None] * (mine_nth[:, None] == slots).astype(i32) * slots[:, None], axis=0
        )
        far = jnp.minimum(me + stride, count - 1)
        comes = jnp.where(me + stride < count, leaving[far], 0)
        kind = jnp.where(comes > 0, 2, jnp.where(mine_out > 0, 1, 0)).astype(i32)
        place = jnp.where(comes > 0, nth[far], 0)
        all_pairs = [(i, i - stride) for i in range(stride, count)]
        split = count - stride // 2
        upper = [pair for pair in all_pairs if pair[0] >= split]
        halves = 2 * stride >= count and 0 < len(upper) < len(all_pairs)

        def shifting(cap, pairs, send=send, kind=kind, place=place):
            def run(blocks):
                if cap == 0:
                    return blocks
                moved = lax.ppermute(take_blocks(blocks, send, cap), "seq", pairs)
                return merge_blocks(blocks, moved, kind, jnp.minimum(place, cap - 1))

            return run

        which = first_at_least(sizes[:-1], needed)
        runs = [shifting(cap, all_pairs) for cap in sizes]
        if halves:
            runs += [shifting(cap, upper) for cap in sizes]
            lower = jnp.sum(leaving * (devices < split)[:, None].astype(i32))
            which = which + jnp.where(lower > 0, 0, len(sizes))
        blocks = lax.switch(which, runs, blocks)
    return blocks


def plain_body(queries, keys, values, random_holder, random_offset, keep):
    tok_dev, width_dev = queries.shape
    blk_dev = tok_dev // B
    head_dev = width_dev // DH
    seq_count = lax.axis_size("seq")
    head_count = lax.axis_size("head")
    me = lax.axis_index("seq")
    count_req = blk_dev * R
    total = head_dev * count_req
    i32 = jnp.int32

    code = random_holder * blk_dev + random_offset
    code = jnp.where((keep > 0)[None, :, None], code, -1).reshape(total)
    note = jnp.concatenate([code, keep])
    note = jnp.broadcast_to(note, (seq_count * head_count,) + note.shape)
    table = lax.all_to_all(note, ("seq", "head"), split_axis=0, concat_axis=0, tiled=True)
    table = table.reshape(seq_count, head_count, total + blk_dev)
    keep_all = table[:, 0, total:].reshape(seq_count * blk_dev)
    codes = table[:, :, :total]
    devices = jnp.arange(seq_count, dtype=i32)

    halo_k, halo_v = halo(keys, "seq", B), halo(values, "seq", B)

    named = jnp.where(codes >= 0, codes // blk_dev, -1)
    counts = jnp.sum((named[..., None] == devices).astype(i32), axis=2)
    most = jnp.max(counts)
    onehot = (named[me, lax.axis_index("head")][:, None] == devices).astype(i32)
    mine = exclusive(onehot, 0)
    my_slot = jnp.sum(mine * onehot, axis=1)
    my_holder = jnp.sum(onehot * devices, axis=1)

    group = codes[:, lax.axis_index("head")]
    asks = (named[:, lax.axis_index("head")] == me).astype(i32)
    order = exclusive(asks, 1)
    full = min(total, head_dev * max(2, (count_req + seq_count - 1) // seq_count))
    chosen = asks[..., None] * (order[..., None] == jnp.arange(full, dtype=i32)).astype(i32)
    ask_head = jnp.arange(total, dtype=i32) // count_req
    ask = jnp.where(group >= 0, group % blk_dev, 0) + ask_head[None] * blk_dev
    ask = jnp.sum(chosen * ask[..., None], axis=1)
    pick_head, pick_block = ask // blk_dev, ask % blk_dev

    rank = exclusive(keep_all, 0)
    slot = rank % blk_dev
    source = jnp.arange(seq_count * blk_dev, dtype=i32) // blk_dev
    distance = jnp.where(keep_all > 0, source - rank // blk_dev, 0)
    my_slots = lax.dynamic_slice_in_dim(slot, me * blk_dev, blk_dev)
    live = jnp.stack([me > 0, me < seq_count - 1]).astype(i32)

    caps = sorted({max(1, full * part // 12) for part in range(8, 13)})

    def gathered(cap):
        def run(q, k, v, hk, hv):
            gk, gv = broadcast(jnp.stack((k[: G * B], v[: G * B])), "seq", 0)
            picked = pick(k, v, pick_head, pick_block, seq_count, cap)
            replies = lax.all_to_all(picked, "seq", split_axis=0, concat_axis=0, tiled=True)
            where = jnp.minimum(my_holder * cap + my_slot, seq_count * cap - 1)
            return attend(keep, my_slots, live, where, q, k, v, hk, hv, gk, gv, replies)

        return run

    blocks = lax.switch(
        first_at_least(caps[:-1], most),
        [gathered(cap) for cap in caps],
        queries, keys, values, halo_k, halo_v,
    )

    return settle(blocks, keep_all, slot, source, distance, me, seq_count, blk_dev)


TILE = (2 * B, DH)
SMALL = pltpu.CompilerParams(vmem_limit_bytes=60 * 1024 * 1024)


def fits(planes, tiles, most):
    slots = 2 * (planes - 1) * tiles + 2 * planes * most + most
    return slots * 2 * B * DH * 2 <= 44 * 1024 * 1024


def exchange_kernel(
    count, cz, cx, blk_dev, tab, k_ref, v_ref,
    rand_ref, halo_ref, glob_ref, home, zs, zr, xs, own,
    z_send, z_recv, x_send, x_recv, h_send, h_recv, g_send, g_recv, l_sem,
):
    planes = count // 2
    me = lax.axis_index("seq")
    plane, side = me // 2, me % 2
    mate = plane * 2 + 1 - side
    tok = k_ref.shape[0]
    head_dev = k_ref.shape[1] // DH
    barrier = pltpu.get_barrier_semaphore()
    for step in range(1, count):
        peer = lax.rem(me + step, count)
        pl.semaphore_signal(
            barrier, inc=1, device_id={"seq": peer}, device_id_type=pl.DeviceIdType.MESH
        )
    pl.semaphore_wait(barrier, count - 1)

    def remote(src, dst, send, recv, peer):
        return pltpu.make_async_remote_copy(
            src_ref=src, dst_ref=dst, send_sem=send, recv_sem=recv,
            device_id={"seq": peer}, device_id_type=pl.DeviceIdType.MESH,
        )

    tables = (k_ref, v_ref)
    low, high = pl.ds(0, B), pl.ds(B, B)
    first, last = pl.ds(0, B), pl.ds(tok - B, B)
    after = jnp.minimum(me + 1, count - 1)
    before = jnp.maximum(me - 1, 0)
    ups = [
        remote(tables[i].at[last], halo_ref.at[i, low], h_send.at[i], h_recv.at[i], after)
        for i in range(2)
    ]
    downs = [
        remote(tables[i].at[first], halo_ref.at[i, high], h_send.at[2 + i], h_recv.at[2 + i], before)
        for i in range(2)
    ]
    local = [
        pltpu.make_async_copy(tables[i].at[pl.ds(0, G * B)], glob_ref.at[i], l_sem.at[i])
        for i in range(2)
    ]
    item = glob_ref.at[side]
    chain = remote(item, item, g_send.at[0], g_recv.at[0], jnp.minimum(me + 2, count - 1))
    swap = remote(item, item, g_send.at[1], g_recv.at[1], mate)
    extra = remote(glob_ref.at[1], glob_ref.at[1], g_send.at[2], g_recv.at[0], mate)

    @pl.when(me == 0)
    def _():
        for c in local:
            c.start()
        for c in local:
            c.wait()
        chain.start()
        extra.start()
        swap.start()

    def pass_on():
        @pl.when(me > 0)
        def _():
            chain.wait_recv()

            @pl.when(plane < planes - 1)
            def _():
                chain.start()

            @pl.when(me > 1)
            def _():
                swap.start()

    @pl.when(me < count - 1)
    def _():
        for c in ups:
            c.start()

    @pl.when(me > 0)
    def _():
        for c in downs:
            c.start()

    @pl.when(me == 0)
    def _():
        halo_ref[:, low, :] = jnp.zeros((2, B, k_ref.shape[1]), k_ref.dtype)

    @pl.when(me == count - 1)
    def _():
        halo_ref[:, high, :] = jnp.zeros((2, B, k_ref.shape[1]), k_ref.dtype)

    def load_home(block, carry):
        rows = pl.ds(pl.multiple_of(block * B, B), B)
        for h in range(head_dev):
            cols = slice(h * DH, (h + 1) * DH)
            home[h * blk_dev + block, low, :] = k_ref[rows, cols]
            home[h * blk_dev + block, high, :] = v_ref[rows, cols]
        return carry

    lax.fori_loop(0, blk_dev, load_home, 0)

    def from_slots(dst, src, table, row, cap):
        def one(j, carry):
            dst[j] = src[table[row, j]]
            return carry

        lax.fori_loop(0, cap, one, 0)

    half = planes // 2
    lower = plane < half
    rest = [d for d in range(1, planes) if d != half]
    rising, falling = [half, *rest], [half, *reversed(rest)]
    x_base = (planes - 1) * cz
    z_copies = {
        d: remote(
            zs[d - 1], zr[d - 1], z_send.at[d - 1], z_recv.at[d - 1],
            lax.rem(plane + d, planes) * 2 + side,
        )
        for d in rising
    }
    x_copies = [
        remote(
            xs[d], rand_ref.at[pl.ds(x_base + d * cx, cx)],
            x_send.at[d], x_recv.at[d], mate,
        )
        for d in range(planes)
    ]
    from_slots(zs[half - 1], home, tab, half - 1, cz)
    from_slots(xs[0], home, tab, planes - 1, cx)
    z_copies[half].start()
    for d in rest:
        from_slots(zs[d - 1], home, tab, d - 1, cz)
    x_copies[0].start()

    @pl.when(lower)
    def _():
        pass_on()
        for d in falling[1:]:
            z_copies[d].start()

    @pl.when(jnp.logical_not(lower))
    def _():
        for d in rising[1:]:
            z_copies[d].start()
        pass_on()

    from_slots(own, home, tab, 2 * planes - 1, cx)
    keep_own = pltpu.make_async_copy(
        own, rand_ref.at[pl.ds(x_base + planes * cx, cx)], l_sem.at[2]
    )
    keep_own.start()
    outs = {
        d: pltpu.make_async_copy(
            zr[d - 1], rand_ref.at[pl.ds((d - 1) * cz, cz)], l_sem.at[2 + d]
        )
        for d in rising
    }

    def forward(d):
        z_copies[d].wait_recv()
        outs[d].start()
        from_slots(xs[d], zr[d - 1], tab, planes - 1 + d, cx)
        x_copies[d].start()

    @pl.when(lower)
    def _():
        for d in falling:
            forward(d)

    @pl.when(jnp.logical_not(lower))
    def _():
        for d in rising:
            forward(d)

    @pl.when(me > 0)
    def _():
        swap.wait_recv()

    @pl.when(plane < planes - 1)
    def _():
        chain.wait_send()

    @pl.when(me == 0)
    def _():
        extra.wait_send()

    @pl.when(me != 1)
    def _():
        swap.wait_send()

    @pl.when(me < count - 1)
    def _():
        for c in ups:
            c.wait_send()
        for c in downs:
            c.wait_recv()

    @pl.when(me > 0)
    def _():
        for c in downs:
            c.wait_send()
        for c in ups:
            c.wait_recv()

    keep_own.wait()
    for d in rising:
        outs[d].wait()
        z_copies[d].wait_send()
    for c in x_copies:
        c.wait()


def exchange(count, level, cz, cx, slots, blk_dev, tab, keys, values):
    planes = count // 2
    tok, width = keys.shape
    smem = pl.BlockSpec(memory_space=pltpu.SMEM)
    vmem = pl.BlockSpec(memory_space=pltpu.VMEM)
    dtype = keys.dtype
    dma = pltpu.SemaphoreType.DMA
    return pl.pallas_call(
        functools.partial(exchange_kernel, count, cz, cx, blk_dev),
        out_shape=(
            jax.ShapeDtypeStruct((slots, *TILE), dtype),
            jax.ShapeDtypeStruct((2, 2 * B, width), dtype),
            jax.ShapeDtypeStruct((2, G * B, width), dtype),
        ),
        in_specs=[smem, vmem, vmem],
        out_specs=(pl.BlockSpec(memory_space=pl.ANY), vmem, vmem),
        scratch_shapes=[
            pltpu.VMEM((tok // B * (width // DH), *TILE), dtype),
            [pltpu.VMEM((cz, *TILE), dtype) for _ in range(planes - 1)],
            [pltpu.VMEM((cz, *TILE), dtype) for _ in range(planes - 1)],
            [pltpu.VMEM((cx, *TILE), dtype) for _ in range(planes)],
            pltpu.VMEM((cx, *TILE), dtype),
            dma((planes - 1,)), dma((planes - 1,)),
            dma((planes,)), dma((planes,)),
            dma((4,)), dma((4,)), dma((3,)), dma((2,)), dma((2 + planes,)),
        ],
        compiler_params=pltpu.CompilerParams(
            collective_id=level, has_side_effects=True,
            vmem_limit_bytes=60 * 1024 * 1024,
        ),
    )(tab, keys, values)


PIECES = 4


def settle_kernel(
    count, caps, cr, cx, blk_dev, table, in_ref, out_ref,
    mine, zs, pool, rs, xs, xr, z_send, z_recv, r_send, r_recv, x_send, x_recv,
):
    planes = count // 2
    me = lax.axis_index("seq")
    plane, side = me // 2, me % 2
    mate = plane * 2 + 1 - side
    wide = in_ref.shape[1] // PIECES
    barrier = pltpu.get_barrier_semaphore()
    for step in range(1, count):
        peer = lax.rem(me + step, count)
        pl.semaphore_signal(
            barrier, inc=1, device_id={"seq": peer}, device_id_type=pl.DeviceIdType.MESH
        )
    pl.semaphore_wait(barrier, count - 1)

    def remote(src, dst, send, recv, peer):
        return pltpu.make_async_remote_copy(
            src_ref=src, dst_ref=dst, send_sem=send, recv_sem=recv,
            device_id={"seq": peer}, device_id_type=pl.DeviceIdType.MESH,
        )

    used = [d for d in range(1, planes) if caps[d - 1] > 0]
    used.sort(reverse=True)
    base = {d: blk_dev + sum(caps[: d - 1]) for d in used}
    gate = planes // 2 - 1
    beyond = range(1, gate + 1)
    r_base = blk_dev + sum(caps)
    x_row = planes - 1 + max(gate, 1)

    def sends(d):
        return jnp.logical_and(plane >= d, jnp.logical_or(plane != gate + 1, d == 1))

    def gets(d):
        return jnp.logical_and(plane + d < planes, jnp.logical_or(plane + d != gate + 1, d == 1))

    def fill(dst, src, table, row, cap):
        def one(j, carry):
            dst[j] = src[table[row, j]]
            return carry

        lax.fori_loop(0, cap, one, 0)

    def own_part(piece):
        def one(j, carry):
            rows = pl.ds(pl.multiple_of(j * B, B), B)
            block = in_ref[rows, piece * wide : (piece + 1) * wide]
            mine[piece][j] = block
            pool[piece][j] = block
            return carry

        lax.fori_loop(0, blk_dev, one, 0)

    z_copies, x_copies = {}, []
    for piece in range(PIECES):
        for n, d in enumerate(used):
            z_copies[piece, d] = remote(
                zs[piece][n], pool[piece].at[pl.ds(base[d], caps[d - 1])],
                z_send.at[piece, n], z_recv.at[piece, n],
                jnp.maximum(me - 2 * d, 0),
            )
        for d in beyond:
            z_copies[piece, -d] = remote(
                rs[piece][d - 1], pool[piece].at[pl.ds(r_base, cr)],
                r_send.at[piece, d - 1], r_recv.at[piece],
                jnp.maximum(me - 2 * d, 0),
            )
        x_copies.append(remote(xs[piece], xr[piece], x_send.at[piece], x_recv.at[piece], mate))
    def start_z(piece):
        for d in used:
            @pl.when(sends(d))
            def _(d=d):
                z_copies[piece, d].start()

    for piece in range(PIECES):
        own_part(piece)
        for n, d in enumerate(used):
            fill(zs[piece][n], mine[piece], table, d - 1, caps[d - 1])
        if piece > 0:
            start_z(piece - 1)
    start_z(PIECES - 1)

    def finish(piece):
        x_copies[piece].wait_recv()

        def one(j, carry):
            rows = pl.ds(pl.multiple_of(j * B, B), B)
            kind = table[x_row + 1, j]
            near, far = pool[piece][table[x_row + 2, j]], xr[piece][table[x_row + 3, j]]
            block = jnp.where(kind == 1, near, jnp.where(kind == 2, far, jnp.zeros_like(far)))
            out_ref[rows, piece * wide : (piece + 1) * wide] = block
            return carry

        lax.fori_loop(0, blk_dev, one, 0)

    for piece in range(PIECES):
        for d in used:
            @pl.when(gets(d))
            def _(d=d, piece=piece):
                z_copies[piece, d].wait_recv()

        @pl.when(plane == gate)
        def _(piece=piece):
            for d in beyond:
                fill(rs[piece][d - 1], pool[piece], table, planes - 2 + d, cr)
                z_copies[piece, -d].start()

        @pl.when(plane < gate)
        def _(piece=piece):
            if gate > 0:
                z_copies[piece, -1].wait_recv()

        fill(xs[piece], pool[piece], table, x_row, cx)
        x_copies[piece].start()
        if piece > 0:
            finish(piece - 1)
    finish(PIECES - 1)
    for piece in range(PIECES):
        x_copies[piece].wait_send()
        for d in used:
            @pl.when(sends(d))
            def _(d=d, piece=piece):
                z_copies[piece, d].wait_send()

        @pl.when(plane == gate)
        def _(piece=piece):
            for d in beyond:
                z_copies[piece, -d].wait_send()


def settled(count, number, caps, cr, cx, blk_dev, packs, blocks):
    tok, width = blocks.shape
    planes, wide = count // 2, width // PIECES
    smem = pl.BlockSpec(memory_space=pltpu.SMEM)
    vmem = pl.BlockSpec(memory_space=pltpu.VMEM)
    dma, dtype = pltpu.SemaphoreType.DMA, blocks.dtype
    sent = [caps[d - 1] for d in range(planes - 1, 0, -1) if caps[d - 1] > 0]

    def each(rows):
        return [pltpu.VMEM((rows, B, wide), dtype) for _ in range(PIECES)]

    return pl.pallas_call(
        functools.partial(settle_kernel, count, caps, cr, cx, blk_dev),
        out_shape=jax.ShapeDtypeStruct(blocks.shape, dtype),
        in_specs=[smem, vmem],
        out_specs=vmem,
        scratch_shapes=[
            each(blk_dev),
            [[pltpu.VMEM((c, B, wide), dtype) for c in sent] for _ in range(PIECES)],
            each(blk_dev + sum(caps) + cr),
            [[pltpu.VMEM((cr, B, wide), dtype) for _ in range(planes // 2 - 1)] for _ in range(PIECES)],
            each(cx),
            each(cx),
            dma((PIECES, len(sent))), dma((PIECES, len(sent))),
            dma((PIECES, planes // 2)), dma((PIECES,)), dma((PIECES,)), dma((PIECES,)),
        ],
        compiler_params=pltpu.CompilerParams(
            collective_id=number, has_side_effects=True,
            vmem_limit_bytes=60 * 1024 * 1024,
        ),
    )(packs, blocks)


def settle_levels(planes, blk_dev):
    def pad(first, second):
        return ((first, second) + (0,) * planes)[: planes - 1]

    half, few = blk_dev // 2, blk_dev * 3 // 4
    choices = [
        (2 * max(f + t, f + r) + r, pad(f, t), r, few)
        for f in range(half, few + 1)
        for t in range(half, few + 1)
        for r in (half // 2, half)
        if abs(f - t) < 2 or t == half
    ]
    choices = sorted(choices) + [(0, (blk_dev,) * (planes - 1), blk_dev, blk_dev)]
    return [limits for _, *limits in choices]


def pack(blocks, packs, level, count, blk_dev, first_id, choices):
    def run(number, *limits):
        return lambda *args: settled(count, first_id + number, *limits, blk_dev, *args)

    runs = [run(n, *limits) for n, limits in enumerate(choices)]
    return lax.switch(level, runs, packs, blocks)


CHUNK = 8


def near_far_kernel(
    blk_dev, keep_ref, live_ref, where_ref, used_ref,
    q_ref, k_ref, v_ref, hk_ref, hv_ref, gk_ref, gv_ref, rand_hbm, out_ref, rand_ref, sems,
):
    scale = 1.0 / math.sqrt(DH)
    head = pl.program_id(0)
    chunks = rand_hbm.shape[0] // CHUNK

    @pl.when(head == 0)
    def _():
        def copy(c):
            rows = pl.ds(c * CHUNK, CHUNK)
            return pltpu.make_async_copy(rand_hbm.at[rows], rand_ref.at[rows], sems.at[c])

        for c in range(chunks):
            pl.when(c * CHUNK < used_ref[0, 1])(lambda c=c: copy(c).start())
        for c in range(chunks):
            pl.when(c * CHUNK < used_ref[0, 1])(lambda c=c: copy(c).wait())

    def tile(ref, halo_ref, i):
        if i < 0:
            return halo_ref[0, :B]
        if i >= blk_dev:
            return halo_ref[0, B:]
        return ref[i * B : (i + 1) * B]

    def one(i):
        q = q_ref[i * B : (i + 1) * B]
        near = range(i - 1, i + 2)
        picks = [where_ref[head, i * R + r] for r in range(R)]
        k_parts = [
            jnp.concatenate([tile(k_ref, hk_ref, n) for n in near], axis=0),
            gk_ref[0],
            jnp.concatenate([rand_ref[p, :B] for p in picks], axis=0),
        ]
        v_parts = [
            jnp.concatenate([tile(v_ref, hv_ref, n) for n in near], axis=0),
            gv_ref[0],
            jnp.concatenate([rand_ref[p, B:] for p in picks], axis=0),
        ]
        scores = [
            lax.dot_general(
                q, k, (((1,), (1,)), ((), ())), preferred_element_type=jnp.float32
            )
            * scale
            for k in k_parts
        ]
        lanes = lax.broadcasted_iota(jnp.int32, scores[0].shape, 1)
        if i == 0:
            dead = jnp.logical_and(lanes < B, live_ref[0] == 0)
            scores[0] = jnp.where(dead, neg_big, scores[0])
        if i == blk_dev - 1:
            dead = jnp.logical_and(lanes >= 2 * B, live_ref[1] == 0)
            scores[0] = jnp.where(dead, neg_big, scores[0])
        peak = functools.reduce(
            jnp.maximum, [jnp.max(s, axis=-1, keepdims=True) for s in scores]
        )
        numer = jnp.zeros((B, DH), jnp.float32)
        denom = jnp.zeros((B, 1), jnp.float32)
        for s, v in zip(scores, v_parts):
            w = jnp.exp(s - peak).astype(jnp.bfloat16)
            denom = denom + jnp.sum(w.astype(jnp.float32), axis=-1, keepdims=True)
            numer = numer + jnp.dot(w, v, preferred_element_type=jnp.float32)
        out_ref[i * B : (i + 1) * B, :] = (numer / denom).astype(out_ref.dtype)

    for i in range(blk_dev):
        pl.when(keep_ref[i] > 0)(functools.partial(one, i))


def near_far(keep, live, where, used, q, k, v, halo_kv, glob, rand):
    tok_dev, width_dev = q.shape
    blk_dev, head_dev = tok_dev // B, width_dev // DH

    def column(rows):
        return pl.BlockSpec((rows, DH), lambda h, *_: (0, h))

    def part(rows, which):
        return pl.BlockSpec((1, rows, DH), lambda h, *_: (which, 0, h))

    return pl.pallas_call(
        functools.partial(near_far_kernel, blk_dev),
        out_shape=jax.ShapeDtypeStruct(q.shape, q.dtype),
        grid_spec=pltpu.PrefetchScalarGridSpec(
            num_scalar_prefetch=4,
            grid=(head_dev,),
            in_specs=[column(tok_dev)] * 3
            + [part(2 * B, 0), part(2 * B, 1), part(G * B, 0), part(G * B, 1)]
            + [pl.BlockSpec(memory_space=pl.ANY)],
            out_specs=column(tok_dev),
            scratch_shapes=[
                pltpu.VMEM(rand.shape, rand.dtype),
                pltpu.SemaphoreType.DMA((rand.shape[0] // CHUNK,)),
            ],
        ),
        compiler_params=ANYWHERE,
    )(keep, live, where, used, q, k, v, halo_kv, halo_kv, glob, glob, rand)


def quotient(x, n):
    return jnp.floor((x.astype(jnp.float32) + 0.5) * (1.0 / n)).astype(jnp.int32)


def plan_kernel(
    count, head_count, blk_dev, most, caps, choices, note_ref, tab_ref, where_ref, misc_ref, pack_ref,
    need_ref, want_ref, slot_ref, both_ref, both_slot_ref,
):
    i32, f32, bf16 = jnp.int32, jnp.float32, jnp.bfloat16
    planes = count // 2
    me, group = lax.axis_index("seq"), lax.axis_index("head")
    plane, side = me // 2, me % 2
    mate = me + 1 - 2 * side
    rows, lanes = note_ref.shape[0], tab_ref.shape[1]
    head_dev = rows // (count * head_count)
    count_req = blk_dev * R
    blocks = count * blk_dev

    def iota(shape, axis):
        return lax.broadcasted_iota(i32, shape, axis)

    def dot(a, b):
        return jnp.dot(a.astype(bf16), b.astype(bf16), preferred_element_type=f32)

    def flag(x):
        return x.astype(f32)

    notes = note_ref[...]
    lane = iota((rows, lanes), 1)
    need = jnp.zeros((rows, lanes), f32)
    for e in range(count_req):
        need = jnp.where(notes[:, e : e + 1] == lane, 1.0, need)
    need_ref[...] = need

    wide_r, wide_c = iota((lanes, lanes), 0), iota((lanes, lanes), 1)
    own_r, own_c = quotient(wide_r, blk_dev), quotient(wide_c, blk_dev)
    same = flag(own_r == own_c)
    inside = flag((own_r == own_c) & (wide_r < wide_c))

    def by_head(x):
        return jnp.sum(x.reshape(-1, head_dev, lanes), axis=1)

    most_x = jnp.max(dot(by_head(need), same))
    span = head_count * head_dev
    pairs = need.reshape(planes, 2, span, lanes)
    union = jnp.maximum(pairs[:, 0], pairs[:, 1]).reshape(planes * span, lanes)
    union_count = dot(by_head(union), same)
    holder_plane = quotient(quotient(iota(union_count.shape, 1), blk_dev), 2)
    goal_plane = quotient(iota(union_count.shape, 0), head_count)
    most_z = jnp.max(jnp.where(holder_plane != goal_plane, union_count, 0.0))
    level = jnp.int32(0)
    cz, cx = jnp.int32(caps[0][0]), jnp.int32(caps[0][1])
    for n in range(1, len(caps)):
        over = (most_z > caps[n - 1][0]) | (most_x > caps[n - 1][1])
        level = jnp.where(over, n, level)
        cz = jnp.where(over, caps[n][0], cz)
        cx = jnp.where(over, caps[n][1], cx)

    for d in range(count):
        start = pl.multiple_of((d * head_count + group) * head_dev, head_dev)
        want_ref[d * head_dev : (d + 1) * head_dev, :] = need_ref[pl.ds(start, head_dev), :]
    want = want_ref[...]
    both = jnp.maximum(
        *[want.reshape(planes, 2, head_dev, lanes)[:, i] for i in range(2)]
    ).reshape(planes * head_dev, lanes)
    both_ref[...] = both

    def slots(x):
        tall = x.shape[0]
        r, c = iota((tall, tall), 0), iota((tall, tall), 1)
        above = flag((quotient(r, head_dev) == quotient(c, head_dev)) & (c < r))
        return dot(x, inside) + dot(above, dot(x, same))

    slot_ref[...] = slots(want)
    both_slot_ref[...] = slots(both)

    def head_rows(ref, i):
        return ref[pl.ds(pl.multiple_of(i * head_dev, head_dev), head_dev), :]

    def shifted(x, holder):
        return pltpu.roll(x, lax.rem(lanes - holder * blk_dev, lanes), 1)

    short = iota((head_dev, lanes), 1)
    first = iota((head_dev, 1), 0)

    def listed(flags, places, holder, worth):
        key = jnp.where(shifted(flags, holder) > 0, shifted(places, holder), -1.0).astype(i32)
        total = jnp.zeros((head_dev, lanes), f32)
        if worth is not None:
            worth = shifted(worth, holder)
        for b in range(blk_dev):
            value = (first * blk_dev + b).astype(f32) if worth is None else worth[:, b : b + 1]
            total = total + jnp.where(key[:, b : b + 1] == short, value, 0.0)
        return jnp.sum(total, axis=0, keepdims=True).astype(i32)

    tables = []
    for d in range(1, planes):
        goal = lax.rem(plane + d, planes)
        tables.append(listed(head_rows(both_ref, goal), head_rows(both_slot_ref, goal), me, None))
    here = head_rows(both_slot_ref, plane)
    for d in range(planes):
        source = lax.rem(plane - d + planes, planes) * 2 + side
        tables.append(
            listed(head_rows(want_ref, mate), head_rows(slot_ref, mate), source, here if d else None)
        )
    tables.append(listed(head_rows(want_ref, me), head_rows(slot_ref, me), me, None))
    tab_ref[...] = jnp.zeros(tab_ref.shape, i32)
    for n, row in enumerate(tables):
        tab_ref[n : n + 1, :] = row

    holder = quotient(short, blk_dev)
    h_plane = quotient(holder, 2)
    h_side = holder - 2 * h_plane
    gap = plane - h_plane
    gap = jnp.where(gap < 0, gap + planes, gap)
    x_base = (planes - 1) * cz
    by_z = (h_side == side) & (holder != me)
    start = jnp.where(
        by_z, (gap - 1) * cz, jnp.where(holder == me, x_base + planes * cx, x_base + gap * cx)
    )
    spot = start.astype(f32) + jnp.where(by_z, here, head_rows(slot_ref, me))
    mine = pl.multiple_of((me * head_count + group) * head_dev, head_dev)
    picks = note_ref[pl.ds(mine, head_dev), :]
    found = jnp.zeros((head_dev, lanes), f32)
    for e in range(count_req):
        value = jnp.sum(jnp.where(picks[:, e : e + 1] == short, spot, 0.0), axis=1, keepdims=True)
        found = jnp.where(short == e, value, found)
    where_ref[...] = found.astype(i32)

    grid_keep = note_ref[...].astype(f32)
    picked = jnp.zeros((count, grid_keep.shape[1]), f32)
    tall_r, tall_c = iota((count, rows), 0), iota((count, rows), 1)
    stride = head_count * head_dev
    picked = dot(flag(tall_c == tall_r * stride), jnp.clip(grid_keep, 0.0, 1.0))
    spread_r, spread_c = iota((picked.shape[1], lanes), 0), iota((picked.shape[1], lanes), 1)
    spread = flag(spread_r == count_req + spread_c - quotient(spread_c, blk_dev) * blk_dev)
    table = dot(picked, spread)
    row8, lane8 = iota((count, lanes), 0), iota((count, lanes), 1)
    kept_r = jnp.sum(jnp.where(quotient(lane8, blk_dev) == row8, table, 0.0), axis=0, keepdims=True)
    kept8 = jnp.broadcast_to(kept_r, (8, lanes))
    rank_r = dot(kept8, flag(wide_r < wide_c))[:1]

    sub, across = iota((blocks, lanes), 0), iota((blocks, lanes), 1)
    turn = sub == across

    def column(row):
        return jnp.sum(jnp.where(turn, row, 0.0), axis=1, keepdims=True)

    def facts(kept, rank, index):
        rank = rank.astype(i32)
        source, goal = quotient(index, blk_dev), quotient(rank, blk_dev)
        s_plane, g_plane = quotient(source, 2), quotient(goal, 2)
        gate = planes // 2 - 1
        relayed = (kept > 0) & (s_plane == gate + 1) & (g_plane < gate)
        far = jnp.where(relayed, 1, s_plane - g_plane)
        s_side, g_side = source - 2 * s_plane, goal - 2 * g_plane
        return kept > 0, rank, source, goal, g_plane, s_side, g_side, relayed, far

    index_r = iota((1, lanes), 1)
    index_c = iota((blocks, 1), 0)
    kr, _, sr, gr, pr, xr, yr, rr, fr = facts(kept_r, rank_r, index_r)
    kc, rank, sc, gc, pc, xc, yc, rc, fc = facts(column(kept_r), column(rank_r), index_c)
    earlier = across < sub

    def tally(hit):
        return jnp.sum(jnp.where(earlier & hit, 1.0, 0.0), axis=1, keepdims=True).astype(i32)

    by_z = tally((sc == sr) & (fc == fr) & kr)
    flow = (pc == pr) & (xc == xr)
    by_r = tally(flow & rr)
    by_x = tally(flow & kr & (xr != yr))
    crosses = kc & (xc != yc)
    gate = planes // 2 - 1

    def largest(hit, value):
        return jnp.max(jnp.where(hit, value + 1, 0).astype(f32))

    tops = [largest(kc & (fc == d), by_z) for d in range(1, planes)]
    top_r, top_x = largest(rc, by_r), largest(crosses, by_x)
    last = len(choices) - 1
    pick = jnp.int32(last)
    own = [jnp.int32(c) for c in choices[last][0]]
    for n in range(last - 1, -1, -1):
        limits, limit_r, limit_x = choices[n]
        ok = (top_r <= limit_r) & (top_x <= limit_x)
        for top, limit in zip(tops, limits):
            ok = ok & (top <= limit)
        pick = jnp.where(ok, n, pick)
        own = [jnp.where(ok, c, o) for c, o in zip(limits, own)]
    local = index_c - sc * blk_dev
    held = local
    base = jnp.int32(blk_dev)
    for d in range(1, planes):
        held = jnp.where(fc == d, base + by_z, held)
        base = base + own[d - 1]
    ahead = held
    held = jnp.where(rc, base + by_r, held)

    def rows_of(hit, places, worth):
        value = jnp.where(hit & (places == across), worth, 0).astype(f32)
        return jnp.sum(value, axis=0, keepdims=True).astype(i32)

    packs = [rows_of(kc & (fc == d) & (sc == me), by_z, local) for d in range(1, planes)]
    for d in range(1, max(gate, 1) + 1):
        packs.append(rows_of(rc & (xc == side) & (plane == gate) & (pc == gate - d), by_r, ahead))
    packs.append(rows_of(crosses & (pc == plane) & (xc == side), by_x, held))
    lands = kc & (gc == me)
    place = rank - gc * blk_dev
    straight = xc == side
    packs.append(rows_of(lands, place, jnp.where(straight, 1, 2)))
    packs.append(rows_of(lands & straight, place, held))
    packs.append(rows_of(lands & jnp.logical_not(straight), place, by_x))
    pack_ref[...] = jnp.zeros(pack_ref.shape, i32)
    for n, row in enumerate(packs):
        pack_ref[n : n + 1, :] = row

    used = x_base + (planes + 1) * cx
    spot8 = iota(misc_ref.shape, 1)
    misc_ref[...] = jnp.where(
        spot8 == 0, level, jnp.where(spot8 == 1, used, jnp.where(spot8 == 2, pick, 0))
    )


def plan(note, count, head_count, blk_dev, most, caps, choices):
    rows = note.shape[0]
    planes = count // 2
    head_dev = rows // (count * head_count)
    lanes = max(128, count * blk_dev)
    i32, f32 = jnp.int32, jnp.float32
    tabs = -(-2 * planes // 8) * 8
    packs = -(-(planes + max(planes // 2 - 1, 1) + 3) // 8) * 8
    shape = jax.ShapeDtypeStruct
    return pl.pallas_call(
        functools.partial(plan_kernel, count, head_count, blk_dev, most, caps, choices),
        out_shape=(
            shape((tabs, lanes), i32), shape((head_dev, lanes), i32),
            shape((8, lanes), i32), shape((packs, lanes), i32),
        ),
        scratch_shapes=[
            pltpu.VMEM((rows, lanes), f32),
            pltpu.VMEM((count * head_dev, lanes), f32), pltpu.VMEM((count * head_dev, lanes), f32),
            pltpu.VMEM((planes * head_dev, lanes), f32), pltpu.VMEM((planes * head_dev, lanes), f32),
        ],
        compiler_params=SMALL,
    )(note)


def levels(tiles, most):
    caps = []
    for part in (22, 24, 26, 28, 29, 30, 32, 36):
        cz = min(tiles, tiles * part // 64)
        caps.append((cz, min(most, max(1, most * min(24, part // 2 + 7) // 24))))
    caps.append((tiles, most))
    return sorted(set(caps))


def body(queries, keys, values, random_holder, random_offset, keep):
    tok_dev, width_dev = queries.shape
    blk_dev = tok_dev // B
    head_dev = width_dev // DH
    count = lax.axis_size("seq")
    head_count = lax.axis_size("head")
    count_req = blk_dev * R
    total = head_dev * count_req
    tiles = head_dev * blk_dev
    most = min(tiles, head_dev * max(2, (count_req + count - 1) // count))
    planes = count // 2
    if count % 2 or planes % 2 or not fits(planes, tiles, most):
        return plain_body(queries, keys, values, random_holder, random_offset, keep)
    me = lax.axis_index("seq")
    plane, side = me // 2, me % 2
    mate = me + 1 - 2 * side
    i32 = jnp.int32
    code = random_holder * blk_dev + random_offset
    code = jnp.where((keep > 0)[None, :, None], code, -1).reshape(head_dev, count_req)
    note = jnp.concatenate([code, jnp.broadcast_to(keep[None], (head_dev, blk_dev))], axis=1)
    note = jnp.broadcast_to(note, (count * head_count,) + note.shape)
    table = lax.all_to_all(note, ("seq", "head"), split_axis=0, concat_axis=0, tiled=True)
    table = table.reshape(count * head_count * head_dev, count_req + blk_dev)
    caps, choices = levels(tiles, most), settle_levels(planes, blk_dev)
    tab, where, misc, packs = plan(table, count, head_count, blk_dev, most, caps, choices)

    slots_all = -(-max((planes - 1) * c[0] + (planes + 1) * c[1] for c in caps) // CHUNK) * CHUNK
    def exchanged(number, caps):
        def run(tab, k, v):
            return exchange(count, number, *caps, slots_all, blk_dev, tab, k, v)

        return run

    rand, halo_kv, glob = lax.switch(
        misc[0, 0], [exchanged(n, c) for n, c in enumerate(caps)], tab, keys, values
    )

    live = jnp.stack([me > 0, me < count - 1]).astype(i32)
    blocks = near_far(
        keep, live, where, misc, queries, keys, values, halo_kv, glob, rand
    )
    return pack(blocks, packs, misc[0, 2], count, blk_dev, len(caps), choices)


def solution(mesh):
    in_specs = (
        P("seq", "head"),
        P("seq", "head"),
        P("seq", "head"),
        P("head", "seq", None),
        P("head", "seq", None),
        P("seq"),
    )
    out_specs = P("seq", "head")
    return jax.shard_map(body, mesh=mesh, in_specs=in_specs, out_specs=out_specs, check_vma=False)
```

```python
import functools
import math

import jax
import jax.numpy as jnp
from jax import lax
from jax.experimental import pallas as pl
from jax.experimental.pallas import tpu as pltpu
from jax.sharding import PartitionSpec as P

DH = 128
B = 128
G = 2
R = 3

neg_big = -1e30
ANYWHERE = pltpu.CompilerParams(
    dimension_semantics=("arbitrary",), vmem_limit_bytes=60 * 1024 * 1024
)


def halo(block, axis, width):
    count = lax.axis_size(axis)
    forward = [(i, i + 1) for i in range(count - 1)]
    backward = [(target, source) for source, target in forward]
    low = lax.ppermute(block[-width:], axis, forward)
    high = lax.ppermute(block[:width], axis, backward)
    return jnp.concatenate([low, high], axis=0)


def broadcast(block, axis, source):
    block = jnp.where(lax.axis_index(axis) == source, block, jnp.zeros_like(block))
    return lax.psum(block, axis)


def pick_kernel(cap, head_ref, block_ref, k_ref, v_ref, out_ref):
    dest = pl.program_id(0)

    @pl.loop(0, cap)
    def _(j):
        rows = pl.ds(pl.multiple_of(block_ref[dest, j] * B, B), B)
        cols = pl.ds(pl.multiple_of(head_ref[dest, j] * DH, DH), DH)
        out_ref[j, 0] = k_ref[rows, cols]
        out_ref[j, 1] = v_ref[rows, cols]


def pick(keys, values, heads, blocks, seq_count, cap):
    whole = pl.BlockSpec(keys.shape, lambda d, *_: (0, 0))
    return pl.pallas_call(
        functools.partial(pick_kernel, cap),
        out_shape=jax.ShapeDtypeStruct((seq_count * cap, 2, B, DH), keys.dtype),
        grid_spec=pltpu.PrefetchScalarGridSpec(
            num_scalar_prefetch=2,
            grid=(seq_count,),
            in_specs=[whole, whole],
            out_specs=pl.BlockSpec((cap, 2, B, DH), lambda d, *_: (d, 0, 0, 0)),
        ),
        compiler_params=ANYWHERE,
    )(heads, blocks, keys, values)


def attend_kernel(
    blk_dev,
    keep_ref,
    slot_ref,
    live_ref,
    where_ref,
    q_ref,
    k_ref,
    v_ref,
    hk_ref,
    hv_ref,
    gk_ref,
    gv_ref,
    rand_ref,
    out_ref,
):
    scale = 1.0 / math.sqrt(DH)
    head = pl.program_id(0)
    out_ref[...] = jnp.zeros_like(out_ref)

    def tile(ref, halo_ref, i):
        if i < 0:
            return halo_ref[:B]
        if i >= blk_dev:
            return halo_ref[B:]
        return ref[i * B : (i + 1) * B]

    def one(i):
        q = q_ref[i * B : (i + 1) * B]
        near = range(i - 1, i + 2)
        picks = [where_ref[(head * blk_dev + i) * R + r] for r in range(R)]
        k_parts = [
            jnp.concatenate([tile(k_ref, hk_ref, n) for n in near], axis=0),
            gk_ref[...],
            jnp.concatenate([rand_ref[p, 0] for p in picks], axis=0),
        ]
        v_parts = [
            jnp.concatenate([tile(v_ref, hv_ref, n) for n in near], axis=0),
            gv_ref[...],
            jnp.concatenate([rand_ref[p, 1] for p in picks], axis=0),
        ]
        scores = [
            lax.dot_general(
                q, k, (((1,), (1,)), ((), ())), preferred_element_type=jnp.float32
            )
            * scale
            for k in k_parts
        ]
        lanes = lax.broadcasted_iota(jnp.int32, scores[0].shape, 1)
        if i == 0:
            dead = jnp.logical_and(lanes < B, live_ref[0] == 0)
            scores[0] = jnp.where(dead, neg_big, scores[0])
        if i == blk_dev - 1:
            dead = jnp.logical_and(lanes >= 2 * B, live_ref[1] == 0)
            scores[0] = jnp.where(dead, neg_big, scores[0])
        peak = functools.reduce(
            jnp.maximum, [jnp.max(s, axis=-1, keepdims=True) for s in scores]
        )
        numer = jnp.zeros((B, DH), jnp.float32)
        denom = jnp.zeros((B, 1), jnp.float32)
        for s, v in zip(scores, v_parts):
            w = jnp.exp(s - peak).astype(jnp.bfloat16)
            denom = denom + jnp.sum(w.astype(jnp.float32), axis=-1, keepdims=True)
            numer = numer + jnp.dot(w, v, preferred_element_type=jnp.float32)
        rows = pl.ds(pl.multiple_of(slot_ref[i] * B, B), B)
        out_ref[rows, :] = (numer / denom).astype(out_ref.dtype)

    for i in range(blk_dev):
        pl.when(keep_ref[i] > 0)(functools.partial(one, i))


def attend(keep, slot, live, where, q, k, v, hk, hv, gk, gv, rand):
    tok_dev, width_dev = q.shape
    blk_dev, head_dev = tok_dev // B, width_dev // DH

    def column(rows):
        return pl.BlockSpec((rows, DH), lambda h, *_: (0, h))

    return pl.pallas_call(
        functools.partial(attend_kernel, blk_dev),
        out_shape=jax.ShapeDtypeStruct(q.shape, q.dtype),
        grid_spec=pltpu.PrefetchScalarGridSpec(
            num_scalar_prefetch=4,
            grid=(head_dev,),
            in_specs=[column(tok_dev)] * 3
            + [column(2 * B)] * 2
            + [column(G * B)] * 2
            + [pl.BlockSpec(rand.shape, lambda h, *_: (0, 0, 0, 0))],
            out_specs=column(tok_dev),
        ),
        compiler_params=ANYWHERE,
    )(keep, slot, live, where, q, k, v, hk, hv, gk, gv, rand)


def copy_kernel(order_ref, in_ref, out_ref):
    out_ref[...] = in_ref[...]


def take_blocks(blocks, order, cap):
    width = blocks.shape[1]
    return pl.pallas_call(
        copy_kernel,
        out_shape=jax.ShapeDtypeStruct((cap * B, width), blocks.dtype),
        grid_spec=pltpu.PrefetchScalarGridSpec(
            num_scalar_prefetch=1,
            grid=(cap,),
            in_specs=[pl.BlockSpec((B, width), lambda j, order: (order[j], 0))],
            out_specs=pl.BlockSpec((B, width), lambda j, order: (j, 0)),
        ),
        compiler_params=ANYWHERE,
    )(order, blocks)


def merge_kernel(kind_ref, from_ref, old_ref, new_ref, out_ref):
    kind = kind_ref[pl.program_id(0)]

    @pl.when(kind == 0)
    def _():
        out_ref[...] = old_ref[...]

    @pl.when(kind == 1)
    def _():
        out_ref[...] = jnp.zeros_like(out_ref)

    @pl.when(kind == 2)
    def _():
        out_ref[...] = new_ref[...]


def merge_blocks(old, new, kind, place):
    tok_dev, width = old.shape
    return pl.pallas_call(
        merge_kernel,
        out_shape=jax.ShapeDtypeStruct(old.shape, old.dtype),
        grid_spec=pltpu.PrefetchScalarGridSpec(
            num_scalar_prefetch=2,
            grid=(tok_dev // B,),
            in_specs=[
                pl.BlockSpec((B, width), lambda j, kind, place: (j, 0)),
                pl.BlockSpec((B, width), lambda j, kind, place: (place[j], 0)),
            ],
            out_specs=pl.BlockSpec((B, width), lambda j, kind, place: (j, 0)),
        ),
        compiler_params=ANYWHERE,
    )(kind, place, old, new)


def exclusive(flags, axis):
    return jnp.cumsum(flags, axis=axis) - flags


def first_at_least(caps, amount):
    return jnp.sum((amount > jnp.asarray(caps, jnp.int32)).astype(jnp.int32))


def settle(blocks, keep_all, slot, source, distance, me, count, blk_dev):
    i32 = jnp.int32
    devices = jnp.arange(count, dtype=i32)
    slots = jnp.arange(blk_dev, dtype=i32)
    sizes = sorted({0, *range(blk_dev // 2, blk_dev - 1), blk_dev})
    for bit_pos in range((count - 1).bit_length()):
        stride = 2**bit_pos
        at = source - distance % stride
        moving = (keep_all > 0) & (distance // stride % 2 > 0)
        on_slot = ((slot[:, None] == slots) & moving[:, None]).astype(i32)
        on_device = (at[:, None] == devices).astype(i32)
        leaving = jnp.sum(on_device[:, :, None] * on_slot[:, None, :], axis=0)
        needed = jnp.max(jnp.sum(leaving, axis=1))
        nth = exclusive(leaving, 1)
        mine_out, mine_nth = leaving[me], nth[me]
        send = jnp.sum(
            mine_out[:, None] * (mine_nth[:, None] == slots).astype(i32) * slots[:, None], axis=0
        )
        far = jnp.minimum(me + stride, count - 1)
        comes = jnp.where(me + stride < count, leaving[far], 0)
        kind = jnp.where(comes > 0, 2, jnp.where(mine_out > 0, 1, 0)).astype(i32)
        place = jnp.where(comes > 0, nth[far], 0)
        all_pairs = [(i, i - stride) for i in range(stride, count)]
        split = count - stride // 2
        upper = [pair for pair in all_pairs if pair[0] >= split]
        halves = 2 * stride >= count and 0 < len(upper) < len(all_pairs)

        def shifting(cap, pairs, send=send, kind=kind, place=place):
            def run(blocks):
                if cap == 0:
                    return blocks
                moved = lax.ppermute(take_blocks(blocks, send, cap), "seq", pairs)
                return merge_blocks(blocks, moved, kind, jnp.minimum(place, cap - 1))

            return run

        which = first_at_least(sizes[:-1], needed)
        runs = [shifting(cap, all_pairs) for cap in sizes]
        if halves:
            runs += [shifting(cap, upper) for cap in sizes]
            lower = jnp.sum(leaving * (devices < split)[:, None].astype(i32))
            which = which + jnp.where(lower > 0, 0, len(sizes))
        blocks = lax.switch(which, runs, blocks)
    return blocks


def plain_body(queries, keys, values, random_holder, random_offset, keep):
    tok_dev, width_dev = queries.shape
    blk_dev = tok_dev // B
    head_dev = width_dev // DH
    seq_count = lax.axis_size("seq")
    head_count = lax.axis_size("head")
    me = lax.axis_index("seq")
    count_req = blk_dev * R
    total = head_dev * count_req
    i32 = jnp.int32

    code = random_holder * blk_dev + random_offset
    code = jnp.where((keep > 0)[None, :, None], code, -1).reshape(total)
    note = jnp.concatenate([code, keep])
    note = jnp.broadcast_to(note, (seq_count * head_count,) + note.shape)
    table = lax.all_to_all(note, ("seq", "head"), split_axis=0, concat_axis=0, tiled=True)
    table = table.reshape(seq_count, head_count, total + blk_dev)
    keep_all = table[:, 0, total:].reshape(seq_count * blk_dev)
    codes = table[:, :, :total]
    devices = jnp.arange(seq_count, dtype=i32)

    halo_k, halo_v = halo(keys, "seq", B), halo(values, "seq", B)

    named = jnp.where(codes >= 0, codes // blk_dev, -1)
    counts = jnp.sum((named[..., None] == devices).astype(i32), axis=2)
    most = jnp.max(counts)
    onehot = (named[me, lax.axis_index("head")][:, None] == devices).astype(i32)
    mine = exclusive(onehot, 0)
    my_slot = jnp.sum(mine * onehot, axis=1)
    my_holder = jnp.sum(onehot * devices, axis=1)

    group = codes[:, lax.axis_index("head")]
    asks = (named[:, lax.axis_index("head")] == me).astype(i32)
    order = exclusive(asks, 1)
    full = min(total, head_dev * max(2, (count_req + seq_count - 1) // seq_count))
    chosen = asks[..., None] * (order[..., None] == jnp.arange(full, dtype=i32)).astype(i32)
    ask_head = jnp.arange(total, dtype=i32) // count_req
    ask = jnp.where(group >= 0, group % blk_dev, 0) + ask_head[None] * blk_dev
    ask = jnp.sum(chosen * ask[..., None], axis=1)
    pick_head, pick_block = ask // blk_dev, ask % blk_dev

    rank = exclusive(keep_all, 0)
    slot = rank % blk_dev
    source = jnp.arange(seq_count * blk_dev, dtype=i32) // blk_dev
    distance = jnp.where(keep_all > 0, source - rank // blk_dev, 0)
    my_slots = lax.dynamic_slice_in_dim(slot, me * blk_dev, blk_dev)
    live = jnp.stack([me > 0, me < seq_count - 1]).astype(i32)

    caps = sorted({max(1, full * part // 12) for part in range(8, 13)})

    def gathered(cap):
        def run(q, k, v, hk, hv):
            gk, gv = broadcast(jnp.stack((k[: G * B], v[: G * B])), "seq", 0)
            picked = pick(k, v, pick_head, pick_block, seq_count, cap)
            replies = lax.all_to_all(picked, "seq", split_axis=0, concat_axis=0, tiled=True)
            where = jnp.minimum(my_holder * cap + my_slot, seq_count * cap - 1)
            return attend(keep, my_slots, live, where, q, k, v, hk, hv, gk, gv, replies)

        return run

    blocks = lax.switch(
        first_at_least(caps[:-1], most),
        [gathered(cap) for cap in caps],
        queries, keys, values, halo_k, halo_v,
    )

    return settle(blocks, keep_all, slot, source, distance, me, seq_count, blk_dev)


TILE = (2 * B, DH)
SMALL = pltpu.CompilerParams(vmem_limit_bytes=60 * 1024 * 1024)


def fits(planes, tiles, most):
    slots = 2 * (planes - 1) * tiles + 2 * planes * most + most
    return slots * 2 * B * DH * 2 <= 44 * 1024 * 1024


def exchange_kernel(
    count, cz, cx, blk_dev, tab, k_ref, v_ref,
    rand_ref, halo_ref, glob_ref, home, zs, zr, xs, own,
    z_send, z_recv, x_send, x_recv, h_send, h_recv, g_send, g_recv, l_sem,
):
    planes = count // 2
    me = lax.axis_index("seq")
    plane, side = me // 2, me % 2
    mate = plane * 2 + 1 - side
    tok = k_ref.shape[0]
    head_dev = k_ref.shape[1] // DH
    barrier = pltpu.get_barrier_semaphore()
    for step in range(1, count):
        peer = lax.rem(me + step, count)
        pl.semaphore_signal(
            barrier, inc=1, device_id={"seq": peer}, device_id_type=pl.DeviceIdType.MESH
        )
    pl.semaphore_wait(barrier, count - 1)

    def remote(src, dst, send, recv, peer):
        return pltpu.make_async_remote_copy(
            src_ref=src, dst_ref=dst, send_sem=send, recv_sem=recv,
            device_id={"seq": peer}, device_id_type=pl.DeviceIdType.MESH,
        )

    tables = (k_ref, v_ref)
    low, high = pl.ds(0, B), pl.ds(B, B)
    first, last = pl.ds(0, B), pl.ds(tok - B, B)
    after = jnp.minimum(me + 1, count - 1)
    before = jnp.maximum(me - 1, 0)
    ups = [
        remote(tables[i].at[last], halo_ref.at[i, low], h_send.at[i], h_recv.at[i], after)
        for i in range(2)
    ]
    downs = [
        remote(tables[i].at[first], halo_ref.at[i, high], h_send.at[2 + i], h_recv.at[2 + i], before)
        for i in range(2)
    ]
    local = [
        pltpu.make_async_copy(tables[i].at[pl.ds(0, G * B)], glob_ref.at[i], l_sem.at[i])
        for i in range(2)
    ]
    item = glob_ref.at[side]
    chain = remote(item, item, g_send.at[0], g_recv.at[0], jnp.minimum(me + 2, count - 1))
    swap = remote(item, item, g_send.at[1], g_recv.at[1], mate)
    extra = remote(glob_ref.at[1], glob_ref.at[1], g_send.at[2], g_recv.at[0], mate)

    @pl.when(me == 0)
    def _():
        for c in local:
            c.start()
        for c in local:
            c.wait()
        chain.start()
        extra.start()
        swap.start()

    def pass_on():
        @pl.when(me > 0)
        def _():
            chain.wait_recv()

            @pl.when(plane < planes - 1)
            def _():
                chain.start()

            @pl.when(me > 1)
            def _():
                swap.start()

    @pl.when(me < count - 1)
    def _():
        for c in ups:
            c.start()

    @pl.when(me > 0)
    def _():
        for c in downs:
            c.start()

    @pl.when(me == 0)
    def _():
        halo_ref[:, low, :] = jnp.zeros((2, B, k_ref.shape[1]), k_ref.dtype)

    @pl.when(me == count - 1)
    def _():
        halo_ref[:, high, :] = jnp.zeros((2, B, k_ref.shape[1]), k_ref.dtype)

    def load_home(block, carry):
        rows = pl.ds(pl.multiple_of(block * B, B), B)
        for h in range(head_dev):
            cols = slice(h * DH, (h + 1) * DH)
            home[h * blk_dev + block, low, :] = k_ref[rows, cols]
            home[h * blk_dev + block, high, :] = v_ref[rows, cols]
        return carry

    lax.fori_loop(0, blk_dev, load_home, 0)

    def from_slots(dst, src, table, row, cap):
        def one(j, carry):
            dst[j] = src[table[row, j]]
            return carry

        lax.fori_loop(0, cap, one, 0)

    deltas = range(1, planes)

    def goals(q):
        return sorted(deltas, key=lambda d: (abs((q + d) % planes - q), d))

    def arrival(q, d):
        source, half = (q - d) % planes, planes // 2
        if (source < half) == (q < half):
            return (0, abs(source - q))
        edges = (half - 1, half)
        return (1 if source in edges and q in edges else 2 if source not in edges else 3, d)

    def sources(q):
        return sorted(deltas, key=lambda d: arrival(q, d))

    x_base = (planes - 1) * cz
    z_copies = {
        d: remote(
            zs[d - 1], zr[d - 1], z_send.at[d - 1], z_recv.at[d - 1],
            lax.rem(plane + d, planes) * 2 + side,
        )
        for d in deltas
    }
    x_copies = [
        remote(
            xs[d], rand_ref.at[pl.ds(x_base + d * cx, cx)],
            x_send.at[d], x_recv.at[d], mate,
        )
        for d in range(planes)
    ]
    for d in deltas:
        from_slots(zs[d - 1], home, tab, d - 1, cz)
    from_slots(xs[0], home, tab, planes - 1, cx)
    for q in range(planes):
        @pl.when(plane == q)
        def _(q=q):
            order = goals(q)
            for n, d in enumerate(order):
                z_copies[d].start()
                if n == 0 and q == 0:
                    pass_on()

    x_copies[0].start()
    from_slots(own, home, tab, 2 * planes - 1, cx)
    keep_own = pltpu.make_async_copy(
        own, rand_ref.at[pl.ds(x_base + planes * cx, cx)], l_sem.at[2]
    )
    keep_own.start()
    outs = {
        d: pltpu.make_async_copy(
            zr[d - 1], rand_ref.at[pl.ds((d - 1) * cz, cz)], l_sem.at[2 + d]
        )
        for d in deltas
    }

    def forward(d):
        z_copies[d].wait_recv()
        outs[d].start()
        from_slots(xs[d], zr[d - 1], tab, planes - 1 + d, cx)
        x_copies[d].start()

    for q in range(planes):
        @pl.when(plane == q)
        def _(q=q):
            for n, d in enumerate(sources(q)):
                forward(d)
                if n == 0 and 0 < q < planes // 2:
                    pass_on()
            if q >= planes // 2:
                pass_on()

    @pl.when(me > 0)
    def _():
        swap.wait_recv()

    @pl.when(plane < planes - 1)
    def _():
        chain.wait_send()

    @pl.when(me == 0)
    def _():
        extra.wait_send()

    @pl.when(me != 1)
    def _():
        swap.wait_send()

    @pl.when(me < count - 1)
    def _():
        for c in ups:
            c.wait_send()
        for c in downs:
            c.wait_recv()

    @pl.when(me > 0)
    def _():
        for c in downs:
            c.wait_send()
        for c in ups:
            c.wait_recv()

    keep_own.wait()
    for d in deltas:
        outs[d].wait()
        z_copies[d].wait_send()
    for c in x_copies:
        c.wait()


def exchange(count, level, cz, cx, slots, blk_dev, tab, keys, values):
    planes = count // 2
    tok, width = keys.shape
    smem = pl.BlockSpec(memory_space=pltpu.SMEM)
    vmem = pl.BlockSpec(memory_space=pltpu.VMEM)
    dtype = keys.dtype
    dma = pltpu.SemaphoreType.DMA
    return pl.pallas_call(
        functools.partial(exchange_kernel, count, cz, cx, blk_dev),
        out_shape=(
            jax.ShapeDtypeStruct((slots, *TILE), dtype),
            jax.ShapeDtypeStruct((2, 2 * B, width), dtype),
            jax.ShapeDtypeStruct((2, G * B, width), dtype),
        ),
        in_specs=[smem, vmem, vmem],
        out_specs=(pl.BlockSpec(memory_space=pl.ANY), vmem, vmem),
        scratch_shapes=[
            pltpu.VMEM((tok // B * (width // DH), *TILE), dtype),
            [pltpu.VMEM((cz, *TILE), dtype) for _ in range(planes - 1)],
            [pltpu.VMEM((cz, *TILE), dtype) for _ in range(planes - 1)],
            [pltpu.VMEM((cx, *TILE), dtype) for _ in range(planes)],
            pltpu.VMEM((cx, *TILE), dtype),
            dma((planes - 1,)), dma((planes - 1,)),
            dma((planes,)), dma((planes,)),
            dma((4,)), dma((4,)), dma((3,)), dma((2,)), dma((2 + planes,)),
        ],
        compiler_params=pltpu.CompilerParams(
            collective_id=level, has_side_effects=True,
            vmem_limit_bytes=60 * 1024 * 1024,
        ),
    )(tab, keys, values)


PIECES = 4


def settle_kernel(
    count, caps, cr, cx, blk_dev, table, in_ref, out_ref,
    mine, zs, pool, rs, xs, xr, z_send, z_recv, r_send, r_recv, x_send, x_recv,
):
    planes = count // 2
    me = lax.axis_index("seq")
    plane, side = me // 2, me % 2
    mate = plane * 2 + 1 - side
    wide = in_ref.shape[1] // PIECES
    barrier = pltpu.get_barrier_semaphore()
    for step in range(1, count):
        peer = lax.rem(me + step, count)
        pl.semaphore_signal(
            barrier, inc=1, device_id={"seq": peer}, device_id_type=pl.DeviceIdType.MESH
        )
    pl.semaphore_wait(barrier, count - 1)

    def remote(src, dst, send, recv, peer):
        return pltpu.make_async_remote_copy(
            src_ref=src, dst_ref=dst, send_sem=send, recv_sem=recv,
            device_id={"seq": peer}, device_id_type=pl.DeviceIdType.MESH,
        )

    used = [d for d in range(1, planes) if caps[d - 1] > 0]
    used.sort(reverse=True)
    base = {d: blk_dev + sum(caps[: d - 1]) for d in used}
    gate = planes // 2 - 1
    beyond = range(1, gate + 1)
    r_base = blk_dev + sum(caps)
    x_row = planes - 1 + max(gate, 1)

    def sends(d):
        return jnp.logical_and(plane >= d, jnp.logical_or(plane != gate + 1, d == 1))

    def gets(d):
        return jnp.logical_and(plane + d < planes, jnp.logical_or(plane + d != gate + 1, d == 1))

    def fill(dst, src, table, row, cap):
        def one(j, carry):
            dst[j] = src[table[row, j]]
            return carry

        lax.fori_loop(0, cap, one, 0)

    def own_part(piece):
        def one(j, carry):
            rows = pl.ds(pl.multiple_of(j * B, B), B)
            block = in_ref[rows, piece * wide : (piece + 1) * wide]
            mine[piece][j] = block
            pool[piece][j] = block
            return carry

        lax.fori_loop(0, blk_dev, one, 0)

    z_copies, x_copies = {}, []
    for piece in range(PIECES):
        for n, d in enumerate(used):
            z_copies[piece, d] = remote(
                zs[piece][n], pool[piece].at[pl.ds(base[d], caps[d - 1])],
                z_send.at[piece, n], z_recv.at[piece, n],
                jnp.maximum(me - 2 * d, 0),
            )
        for d in beyond:
            z_copies[piece, -d] = remote(
                rs[piece][d - 1], pool[piece].at[pl.ds(r_base, cr)],
                r_send.at[piece, d - 1], r_recv.at[piece],
                jnp.maximum(me - 2 * d, 0),
            )
        x_copies.append(remote(xs[piece], xr[piece], x_send.at[piece], x_recv.at[piece], mate))
    def start_z(piece):
        for d in used:
            @pl.when(sends(d))
            def _(d=d):
                z_copies[piece, d].start()

    for piece in range(PIECES):
        own_part(piece)
        for n, d in enumerate(used):
            fill(zs[piece][n], mine[piece], table, d - 1, caps[d - 1])
        if piece > 0:
            start_z(piece - 1)
    start_z(PIECES - 1)

    def finish(piece):
        x_copies[piece].wait_recv()

        def one(j, carry):
            rows = pl.ds(pl.multiple_of(j * B, B), B)
            kind = table[x_row + 1, j]
            near, far = pool[piece][table[x_row + 2, j]], xr[piece][table[x_row + 3, j]]
            block = jnp.where(kind == 1, near, jnp.where(kind == 2, far, jnp.zeros_like(far)))
            out_ref[rows, piece * wide : (piece + 1) * wide] = block
            return carry

        lax.fori_loop(0, blk_dev, one, 0)

    for piece in range(PIECES):
        for d in used:
            @pl.when(gets(d))
            def _(d=d, piece=piece):
                z_copies[piece, d].wait_recv()

        @pl.when(plane == gate)
        def _(piece=piece):
            for d in beyond:
                fill(rs[piece][d - 1], pool[piece], table, planes - 2 + d, cr)
                z_copies[piece, -d].start()

        @pl.when(plane < gate)
        def _(piece=piece):
            if gate > 0:
                z_copies[piece, -1].wait_recv()

        fill(xs[piece], pool[piece], table, x_row, cx)
        x_copies[piece].start()
        if piece > 0:
            finish(piece - 1)
    finish(PIECES - 1)
    for piece in range(PIECES):
        x_copies[piece].wait_send()
        for d in used:
            @pl.when(sends(d))
            def _(d=d, piece=piece):
                z_copies[piece, d].wait_send()

        @pl.when(plane == gate)
        def _(piece=piece):
            for d in beyond:
                z_copies[piece, -d].wait_send()


def settled(count, number, caps, cr, cx, blk_dev, packs, blocks):
    tok, width = blocks.shape
    planes, wide = count // 2, width // PIECES
    smem = pl.BlockSpec(memory_space=pltpu.SMEM)
    vmem = pl.BlockSpec(memory_space=pltpu.VMEM)
    dma, dtype = pltpu.SemaphoreType.DMA, blocks.dtype
    sent = [caps[d - 1] for d in range(planes - 1, 0, -1) if caps[d - 1] > 0]

    def each(rows):
        return [pltpu.VMEM((rows, B, wide), dtype) for _ in range(PIECES)]

    return pl.pallas_call(
        functools.partial(settle_kernel, count, caps, cr, cx, blk_dev),
        out_shape=jax.ShapeDtypeStruct(blocks.shape, dtype),
        in_specs=[smem, vmem],
        out_specs=vmem,
        scratch_shapes=[
            each(blk_dev),
            [[pltpu.VMEM((c, B, wide), dtype) for c in sent] for _ in range(PIECES)],
            each(blk_dev + sum(caps) + cr),
            [[pltpu.VMEM((cr, B, wide), dtype) for _ in range(planes // 2 - 1)] for _ in range(PIECES)],
            each(cx),
            each(cx),
            dma((PIECES, len(sent))), dma((PIECES, len(sent))),
            dma((PIECES, planes // 2)), dma((PIECES,)), dma((PIECES,)), dma((PIECES,)),
        ],
        compiler_params=pltpu.CompilerParams(
            collective_id=number, has_side_effects=True,
            vmem_limit_bytes=60 * 1024 * 1024,
        ),
    )(packs, blocks)


def settle_levels(planes, blk_dev):
    def pad(first, second):
        return ((first, second) + (0,) * planes)[: planes - 1]

    half, few = blk_dev // 2, blk_dev * 3 // 4
    choices = [
        (2 * max(f + t, f + r) + r, pad(f, t), r, few)
        for f in range(half, few + 1)
        for t in range(half, few + 1)
        for r in (half // 2, half)
        if abs(f - t) < 2 or t == half
    ]
    choices = sorted(choices) + [(0, (blk_dev,) * (planes - 1), blk_dev, blk_dev)]
    return [limits for _, *limits in choices]


def pack(blocks, packs, level, count, blk_dev, first_id, choices):
    def run(number, *limits):
        return lambda *args: settled(count, first_id + number, *limits, blk_dev, *args)

    runs = [run(n, *limits) for n, limits in enumerate(choices)]
    return lax.switch(level, runs, packs, blocks)


CHUNK = 8


def near_far_kernel(
    blk_dev, keep_ref, live_ref, where_ref, used_ref,
    q_ref, k_ref, v_ref, hk_ref, hv_ref, gk_ref, gv_ref, rand_hbm, out_ref, rand_ref, sems,
):
    scale = 1.0 / math.sqrt(DH)
    head = pl.program_id(0)
    chunks = rand_hbm.shape[0] // CHUNK

    @pl.when(head == 0)
    def _():
        def copy(c):
            rows = pl.ds(c * CHUNK, CHUNK)
            return pltpu.make_async_copy(rand_hbm.at[rows], rand_ref.at[rows], sems.at[c])

        for c in range(chunks):
            pl.when(c * CHUNK < used_ref[0, 1])(lambda c=c: copy(c).start())
        for c in range(chunks):
            pl.when(c * CHUNK < used_ref[0, 1])(lambda c=c: copy(c).wait())

    def tile(ref, halo_ref, i):
        if i < 0:
            return halo_ref[0, :B]
        if i >= blk_dev:
            return halo_ref[0, B:]
        return ref[i * B : (i + 1) * B]

    def one(i):
        q = q_ref[i * B : (i + 1) * B]
        near = range(i - 1, i + 2)
        picks = [where_ref[head, i * R + r] for r in range(R)]
        k_parts = [
            jnp.concatenate([tile(k_ref, hk_ref, n) for n in near], axis=0),
            gk_ref[0],
            jnp.concatenate([rand_ref[p, :B] for p in picks], axis=0),
        ]
        v_parts = [
            jnp.concatenate([tile(v_ref, hv_ref, n) for n in near], axis=0),
            gv_ref[0],
            jnp.concatenate([rand_ref[p, B:] for p in picks], axis=0),
        ]
        scores = [
            lax.dot_general(
                q, k, (((1,), (1,)), ((), ())), preferred_element_type=jnp.float32
            )
            * scale
            for k in k_parts
        ]
        lanes = lax.broadcasted_iota(jnp.int32, scores[0].shape, 1)
        if i == 0:
            dead = jnp.logical_and(lanes < B, live_ref[0] == 0)
            scores[0] = jnp.where(dead, neg_big, scores[0])
        if i == blk_dev - 1:
            dead = jnp.logical_and(lanes >= 2 * B, live_ref[1] == 0)
            scores[0] = jnp.where(dead, neg_big, scores[0])
        peak = functools.reduce(
            jnp.maximum, [jnp.max(s, axis=-1, keepdims=True) for s in scores]
        )
        numer = jnp.zeros((B, DH), jnp.float32)
        denom = jnp.zeros((B, 1), jnp.float32)
        for s, v in zip(scores, v_parts):
            w = jnp.exp(s - peak).astype(jnp.bfloat16)
            denom = denom + jnp.sum(w.astype(jnp.float32), axis=-1, keepdims=True)
            numer = numer + jnp.dot(w, v, preferred_element_type=jnp.float32)
        out_ref[i * B : (i + 1) * B, :] = (numer / denom).astype(out_ref.dtype)

    for i in range(blk_dev):
        pl.when(keep_ref[i] > 0)(functools.partial(one, i))


def near_far(keep, live, where, used, q, k, v, halo_kv, glob, rand):
    tok_dev, width_dev = q.shape
    blk_dev, head_dev = tok_dev // B, width_dev // DH

    def column(rows):
        return pl.BlockSpec((rows, DH), lambda h, *_: (0, h))

    def part(rows, which):
        return pl.BlockSpec((1, rows, DH), lambda h, *_: (which, 0, h))

    return pl.pallas_call(
        functools.partial(near_far_kernel, blk_dev),
        out_shape=jax.ShapeDtypeStruct(q.shape, q.dtype),
        grid_spec=pltpu.PrefetchScalarGridSpec(
            num_scalar_prefetch=4,
            grid=(head_dev,),
            in_specs=[column(tok_dev)] * 3
            + [part(2 * B, 0), part(2 * B, 1), part(G * B, 0), part(G * B, 1)]
            + [pl.BlockSpec(memory_space=pl.ANY)],
            out_specs=column(tok_dev),
            scratch_shapes=[
                pltpu.VMEM(rand.shape, rand.dtype),
                pltpu.SemaphoreType.DMA((rand.shape[0] // CHUNK,)),
            ],
        ),
        compiler_params=ANYWHERE,
    )(keep, live, where, used, q, k, v, halo_kv, halo_kv, glob, glob, rand)


def quotient(x, n):
    return jnp.floor((x.astype(jnp.float32) + 0.5) * (1.0 / n)).astype(jnp.int32)


def plan_kernel(
    count, head_count, blk_dev, most, caps, choices, note_ref, tab_ref, where_ref, misc_ref, pack_ref,
    need_ref, want_ref, slot_ref, both_ref, both_slot_ref,
):
    i32, f32, bf16 = jnp.int32, jnp.float32, jnp.bfloat16
    planes = count // 2
    me, group = lax.axis_index("seq"), lax.axis_index("head")
    plane, side = me // 2, me % 2
    mate = me + 1 - 2 * side
    rows, lanes = note_ref.shape[0], tab_ref.shape[1]
    head_dev = rows // (count * head_count)
    count_req = blk_dev * R
    blocks = count * blk_dev

    def iota(shape, axis):
        return lax.broadcasted_iota(i32, shape, axis)

    def dot(a, b):
        return jnp.dot(a.astype(bf16), b.astype(bf16), preferred_element_type=f32)

    def flag(x):
        return x.astype(f32)

    notes = note_ref[...]
    lane = iota((rows, lanes), 1)
    need = jnp.zeros((rows, lanes), f32)
    for e in range(count_req):
        need = jnp.where(notes[:, e : e + 1] == lane, 1.0, need)
    need_ref[...] = need

    wide_r, wide_c = iota((lanes, lanes), 0), iota((lanes, lanes), 1)
    own_r, own_c = quotient(wide_r, blk_dev), quotient(wide_c, blk_dev)
    same = flag(own_r == own_c)
    inside = flag((own_r == own_c) & (wide_r < wide_c))

    def by_head(x):
        return jnp.sum(x.reshape(-1, head_dev, lanes), axis=1)

    most_x = jnp.max(dot(by_head(need), same))
    span = head_count * head_dev
    pairs = need.reshape(planes, 2, span, lanes)
    union = jnp.maximum(pairs[:, 0], pairs[:, 1]).reshape(planes * span, lanes)
    union_count = dot(by_head(union), same)
    holder_plane = quotient(quotient(iota(union_count.shape, 1), blk_dev), 2)
    goal_plane = quotient(iota(union_count.shape, 0), head_count)
    most_z = jnp.max(jnp.where(holder_plane != goal_plane, union_count, 0.0))
    level = jnp.int32(0)
    cz, cx = jnp.int32(caps[0][0]), jnp.int32(caps[0][1])
    for n in range(1, len(caps)):
        over = (most_z > caps[n - 1][0]) | (most_x > caps[n - 1][1])
        level = jnp.where(over, n, level)
        cz = jnp.where(over, caps[n][0], cz)
        cx = jnp.where(over, caps[n][1], cx)

    for d in range(count):
        start = pl.multiple_of((d * head_count + group) * head_dev, head_dev)
        want_ref[d * head_dev : (d + 1) * head_dev, :] = need_ref[pl.ds(start, head_dev), :]
    want = want_ref[...]
    both = jnp.maximum(
        *[want.reshape(planes, 2, head_dev, lanes)[:, i] for i in range(2)]
    ).reshape(planes * head_dev, lanes)
    both_ref[...] = both

    def slots(x):
        tall = x.shape[0]
        r, c = iota((tall, tall), 0), iota((tall, tall), 1)
        above = flag((quotient(r, head_dev) == quotient(c, head_dev)) & (c < r))
        return dot(x, inside) + dot(above, dot(x, same))

    slot_ref[...] = slots(want)
    both_slot_ref[...] = slots(both)

    def head_rows(ref, i):
        return ref[pl.ds(pl.multiple_of(i * head_dev, head_dev), head_dev), :]

    def shifted(x, holder):
        return pltpu.roll(x, lax.rem(lanes - holder * blk_dev, lanes), 1)

    short = iota((head_dev, lanes), 1)
    first = iota((head_dev, 1), 0)

    def listed(flags, places, holder, worth):
        key = jnp.where(shifted(flags, holder) > 0, shifted(places, holder), -1.0).astype(i32)
        total = jnp.zeros((head_dev, lanes), f32)
        if worth is not None:
            worth = shifted(worth, holder)
        for b in range(blk_dev):
            value = (first * blk_dev + b).astype(f32) if worth is None else worth[:, b : b + 1]
            total = total + jnp.where(key[:, b : b + 1] == short, value, 0.0)
        return jnp.sum(total, axis=0, keepdims=True).astype(i32)

    tables = []
    for d in range(1, planes):
        goal = lax.rem(plane + d, planes)
        tables.append(listed(head_rows(both_ref, goal), head_rows(both_slot_ref, goal), me, None))
    here = head_rows(both_slot_ref, plane)
    for d in range(planes):
        source = lax.rem(plane - d + planes, planes) * 2 + side
        tables.append(
            listed(head_rows(want_ref, mate), head_rows(slot_ref, mate), source, here if d else None)
        )
    tables.append(listed(head_rows(want_ref, me), head_rows(slot_ref, me), me, None))
    tab_ref[...] = jnp.zeros(tab_ref.shape, i32)
    for n, row in enumerate(tables):
        tab_ref[n : n + 1, :] = row

    holder = quotient(short, blk_dev)
    h_plane = quotient(holder, 2)
    h_side = holder - 2 * h_plane
    gap = plane - h_plane
    gap = jnp.where(gap < 0, gap + planes, gap)
    x_base = (planes - 1) * cz
    by_z = (h_side == side) & (holder != me)
    start = jnp.where(
        by_z, (gap - 1) * cz, jnp.where(holder == me, x_base + planes * cx, x_base + gap * cx)
    )
    spot = start.astype(f32) + jnp.where(by_z, here, head_rows(slot_ref, me))
    mine = pl.multiple_of((me * head_count + group) * head_dev, head_dev)
    picks = note_ref[pl.ds(mine, head_dev), :]
    found = jnp.zeros((head_dev, lanes), f32)
    for e in range(count_req):
        value = jnp.sum(jnp.where(picks[:, e : e + 1] == short, spot, 0.0), axis=1, keepdims=True)
        found = jnp.where(short == e, value, found)
    where_ref[...] = found.astype(i32)

    grid_keep = note_ref[...].astype(f32)
    picked = jnp.zeros((count, grid_keep.shape[1]), f32)
    tall_r, tall_c = iota((count, rows), 0), iota((count, rows), 1)
    stride = head_count * head_dev
    picked = dot(flag(tall_c == tall_r * stride), jnp.clip(grid_keep, 0.0, 1.0))
    spread_r, spread_c = iota((picked.shape[1], lanes), 0), iota((picked.shape[1], lanes), 1)
    spread = flag(spread_r == count_req + spread_c - quotient(spread_c, blk_dev) * blk_dev)
    table = dot(picked, spread)
    row8, lane8 = iota((count, lanes), 0), iota((count, lanes), 1)
    kept_r = jnp.sum(jnp.where(quotient(lane8, blk_dev) == row8, table, 0.0), axis=0, keepdims=True)
    kept8 = jnp.broadcast_to(kept_r, (8, lanes))
    rank_r = dot(kept8, flag(wide_r < wide_c))[:1]

    sub, across = iota((blocks, lanes), 0), iota((blocks, lanes), 1)
    turn = sub == across

    def column(row):
        return jnp.sum(jnp.where(turn, row, 0.0), axis=1, keepdims=True)

    def facts(kept, rank, index):
        rank = rank.astype(i32)
        source, goal = quotient(index, blk_dev), quotient(rank, blk_dev)
        s_plane, g_plane = quotient(source, 2), quotient(goal, 2)
        gate = planes // 2 - 1
        relayed = (kept > 0) & (s_plane == gate + 1) & (g_plane < gate)
        far = jnp.where(relayed, 1, s_plane - g_plane)
        s_side, g_side = source - 2 * s_plane, goal - 2 * g_plane
        return kept > 0, rank, source, goal, g_plane, s_side, g_side, relayed, far

    index_r = iota((1, lanes), 1)
    index_c = iota((blocks, 1), 0)
    kr, _, sr, gr, pr, xr, yr, rr, fr = facts(kept_r, rank_r, index_r)
    kc, rank, sc, gc, pc, xc, yc, rc, fc = facts(column(kept_r), column(rank_r), index_c)
    earlier = across < sub

    def tally(hit):
        return jnp.sum(jnp.where(earlier & hit, 1.0, 0.0), axis=1, keepdims=True).astype(i32)

    by_z = tally((sc == sr) & (fc == fr) & kr)
    flow = (pc == pr) & (xc == xr)
    by_r = tally(flow & rr)
    by_x = tally(flow & kr & (xr != yr))
    crosses = kc & (xc != yc)
    gate = planes // 2 - 1

    def largest(hit, value):
        return jnp.max(jnp.where(hit, value + 1, 0).astype(f32))

    tops = [largest(kc & (fc == d), by_z) for d in range(1, planes)]
    top_r, top_x = largest(rc, by_r), largest(crosses, by_x)
    last = len(choices) - 1
    pick = jnp.int32(last)
    own = [jnp.int32(c) for c in choices[last][0]]
    for n in range(last - 1, -1, -1):
        limits, limit_r, limit_x = choices[n]
        ok = (top_r <= limit_r) & (top_x <= limit_x)
        for top, limit in zip(tops, limits):
            ok = ok & (top <= limit)
        pick = jnp.where(ok, n, pick)
        own = [jnp.where(ok, c, o) for c, o in zip(limits, own)]
    local = index_c - sc * blk_dev
    held = local
    base = jnp.int32(blk_dev)
    for d in range(1, planes):
        held = jnp.where(fc == d, base + by_z, held)
        base = base + own[d - 1]
    ahead = held
    held = jnp.where(rc, base + by_r, held)

    def rows_of(hit, places, worth):
        value = jnp.where(hit & (places == across), worth, 0).astype(f32)
        return jnp.sum(value, axis=0, keepdims=True).astype(i32)

    packs = [rows_of(kc & (fc == d) & (sc == me), by_z, local) for d in range(1, planes)]
    for d in range(1, max(gate, 1) + 1):
        packs.append(rows_of(rc & (xc == side) & (plane == gate) & (pc == gate - d), by_r, ahead))
    packs.append(rows_of(crosses & (pc == plane) & (xc == side), by_x, held))
    lands = kc & (gc == me)
    place = rank - gc * blk_dev
    straight = xc == side
    packs.append(rows_of(lands, place, jnp.where(straight, 1, 2)))
    packs.append(rows_of(lands & straight, place, held))
    packs.append(rows_of(lands & jnp.logical_not(straight), place, by_x))
    pack_ref[...] = jnp.zeros(pack_ref.shape, i32)
    for n, row in enumerate(packs):
        pack_ref[n : n + 1, :] = row

    used = x_base + (planes + 1) * cx
    spot8 = iota(misc_ref.shape, 1)
    misc_ref[...] = jnp.where(
        spot8 == 0, level, jnp.where(spot8 == 1, used, jnp.where(spot8 == 2, pick, 0))
    )


def plan(note, count, head_count, blk_dev, most, caps, choices):
    rows = note.shape[0]
    planes = count // 2
    head_dev = rows // (count * head_count)
    lanes = max(128, count * blk_dev)
    i32, f32 = jnp.int32, jnp.float32
    tabs = -(-2 * planes // 8) * 8
    packs = -(-(planes + max(planes // 2 - 1, 1) + 3) // 8) * 8
    shape = jax.ShapeDtypeStruct
    return pl.pallas_call(
        functools.partial(plan_kernel, count, head_count, blk_dev, most, caps, choices),
        out_shape=(
            shape((tabs, lanes), i32), shape((head_dev, lanes), i32),
            shape((8, lanes), i32), shape((packs, lanes), i32),
        ),
        scratch_shapes=[
            pltpu.VMEM((rows, lanes), f32),
            pltpu.VMEM((count * head_dev, lanes), f32), pltpu.VMEM((count * head_dev, lanes), f32),
            pltpu.VMEM((planes * head_dev, lanes), f32), pltpu.VMEM((planes * head_dev, lanes), f32),
        ],
        compiler_params=SMALL,
    )(note)


def levels(tiles, most):
    caps = []
    for part in (22, 24, 26, 28, 29, 30, 32, 36):
        cz = min(tiles, tiles * part // 64)
        caps.append((cz, min(most, max(1, most * min(24, part // 2 + 7) // 24))))
    caps.append((tiles, most))
    return sorted(set(caps))


def body(queries, keys, values, random_holder, random_offset, keep):
    tok_dev, width_dev = queries.shape
    blk_dev = tok_dev // B
    head_dev = width_dev // DH
    count = lax.axis_size("seq")
    head_count = lax.axis_size("head")
    count_req = blk_dev * R
    total = head_dev * count_req
    tiles = head_dev * blk_dev
    most = min(tiles, head_dev * max(2, (count_req + count - 1) // count))
    planes = count // 2
    if count % 2 or planes % 2 or not fits(planes, tiles, most):
        return plain_body(queries, keys, values, random_holder, random_offset, keep)
    me = lax.axis_index("seq")
    plane, side = me // 2, me % 2
    mate = me + 1 - 2 * side
    i32 = jnp.int32
    code = random_holder * blk_dev + random_offset
    code = jnp.where((keep > 0)[None, :, None], code, -1).reshape(head_dev, count_req)
    note = jnp.concatenate([code, jnp.broadcast_to(keep[None], (head_dev, blk_dev))], axis=1)
    note = jnp.broadcast_to(note, (count * head_count,) + note.shape)
    table = lax.all_to_all(note, ("seq", "head"), split_axis=0, concat_axis=0, tiled=True)
    table = table.reshape(count * head_count * head_dev, count_req + blk_dev)
    caps, choices = levels(tiles, most), settle_levels(planes, blk_dev)
    tab, where, misc, packs = plan(table, count, head_count, blk_dev, most, caps, choices)

    slots_all = -(-max((planes - 1) * c[0] + (planes + 1) * c[1] for c in caps) // CHUNK) * CHUNK
    def exchanged(number, caps):
        def run(tab, k, v):
            return exchange(count, number, *caps, slots_all, blk_dev, tab, k, v)

        return run

    rand, halo_kv, glob = lax.switch(
        misc[0, 0], [exchanged(n, c) for n, c in enumerate(caps)], tab, keys, values
    )

    live = jnp.stack([me > 0, me < count - 1]).astype(i32)
    blocks = near_far(
        keep, live, where, misc, queries, keys, values, halo_kv, glob, rand
    )
    return pack(blocks, packs, misc[0, 2], count, blk_dev, len(caps), choices)


def solution(mesh):
    in_specs = (
        P("seq", "head"),
        P("seq", "head"),
        P("seq", "head"),
        P("head", "seq", None),
        P("head", "seq", None),
        P("seq"),
    )
    out_specs = P("seq", "head")
    return jax.shard_map(body, mesh=mesh, in_specs=in_specs, out_specs=out_specs, check_vma=False)
```

```python
import functools
import math

import jax
import jax.numpy as jnp
from jax import lax
from jax.experimental import pallas as pl
from jax.experimental.pallas import tpu as pltpu
from jax.sharding import PartitionSpec as P

DH = 128
B = 128
G = 2
R = 3

neg_big = -1e30
ANYWHERE = pltpu.CompilerParams(
    dimension_semantics=("arbitrary",), vmem_limit_bytes=60 * 1024 * 1024
)


def halo(block, axis, width):
    count = lax.axis_size(axis)
    forward = [(i, i + 1) for i in range(count - 1)]
    backward = [(target, source) for source, target in forward]
    low = lax.ppermute(block[-width:], axis, forward)
    high = lax.ppermute(block[:width], axis, backward)
    return jnp.concatenate([low, high], axis=0)


def broadcast(block, axis, source):
    block = jnp.where(lax.axis_index(axis) == source, block, jnp.zeros_like(block))
    return lax.psum(block, axis)


def pick_kernel(cap, head_ref, block_ref, k_ref, v_ref, out_ref):
    dest = pl.program_id(0)

    @pl.loop(0, cap)
    def _(j):
        rows = pl.ds(pl.multiple_of(block_ref[dest, j] * B, B), B)
        cols = pl.ds(pl.multiple_of(head_ref[dest, j] * DH, DH), DH)
        out_ref[j, 0] = k_ref[rows, cols]
        out_ref[j, 1] = v_ref[rows, cols]


def pick(keys, values, heads, blocks, seq_count, cap):
    whole = pl.BlockSpec(keys.shape, lambda d, *_: (0, 0))
    return pl.pallas_call(
        functools.partial(pick_kernel, cap),
        out_shape=jax.ShapeDtypeStruct((seq_count * cap, 2, B, DH), keys.dtype),
        grid_spec=pltpu.PrefetchScalarGridSpec(
            num_scalar_prefetch=2,
            grid=(seq_count,),
            in_specs=[whole, whole],
            out_specs=pl.BlockSpec((cap, 2, B, DH), lambda d, *_: (d, 0, 0, 0)),
        ),
        compiler_params=ANYWHERE,
    )(heads, blocks, keys, values)


def attend_kernel(
    blk_dev,
    keep_ref,
    slot_ref,
    live_ref,
    where_ref,
    q_ref,
    k_ref,
    v_ref,
    hk_ref,
    hv_ref,
    gk_ref,
    gv_ref,
    rand_ref,
    out_ref,
):
    scale = 1.0 / math.sqrt(DH)
    head = pl.program_id(0)
    out_ref[...] = jnp.zeros_like(out_ref)

    def tile(ref, halo_ref, i):
        if i < 0:
            return halo_ref[:B]
        if i >= blk_dev:
            return halo_ref[B:]
        return ref[i * B : (i + 1) * B]

    def one(i):
        q = q_ref[i * B : (i + 1) * B]
        near = range(i - 1, i + 2)
        picks = [where_ref[(head * blk_dev + i) * R + r] for r in range(R)]
        k_parts = [
            jnp.concatenate([tile(k_ref, hk_ref, n) for n in near], axis=0),
            gk_ref[...],
            jnp.concatenate([rand_ref[p, 0] for p in picks], axis=0),
        ]
        v_parts = [
            jnp.concatenate([tile(v_ref, hv_ref, n) for n in near], axis=0),
            gv_ref[...],
            jnp.concatenate([rand_ref[p, 1] for p in picks], axis=0),
        ]
        scores = [
            lax.dot_general(
                q, k, (((1,), (1,)), ((), ())), preferred_element_type=jnp.float32
            )
            * scale
            for k in k_parts
        ]
        lanes = lax.broadcasted_iota(jnp.int32, scores[0].shape, 1)
        if i == 0:
            dead = jnp.logical_and(lanes < B, live_ref[0] == 0)
            scores[0] = jnp.where(dead, neg_big, scores[0])
        if i == blk_dev - 1:
            dead = jnp.logical_and(lanes >= 2 * B, live_ref[1] == 0)
            scores[0] = jnp.where(dead, neg_big, scores[0])
        peak = functools.reduce(
            jnp.maximum, [jnp.max(s, axis=-1, keepdims=True) for s in scores]
        )
        numer = jnp.zeros((B, DH), jnp.float32)
        denom = jnp.zeros((B, 1), jnp.float32)
        for s, v in zip(scores, v_parts):
            w = jnp.exp(s - peak).astype(jnp.bfloat16)
            denom = denom + jnp.sum(w.astype(jnp.float32), axis=-1, keepdims=True)
            numer = numer + jnp.dot(w, v, preferred_element_type=jnp.float32)
        rows = pl.ds(pl.multiple_of(slot_ref[i] * B, B), B)
        out_ref[rows, :] = (numer / denom).astype(out_ref.dtype)

    for i in range(blk_dev):
        pl.when(keep_ref[i] > 0)(functools.partial(one, i))


def attend(keep, slot, live, where, q, k, v, hk, hv, gk, gv, rand):
    tok_dev, width_dev = q.shape
    blk_dev, head_dev = tok_dev // B, width_dev // DH

    def column(rows):
        return pl.BlockSpec((rows, DH), lambda h, *_: (0, h))

    return pl.pallas_call(
        functools.partial(attend_kernel, blk_dev),
        out_shape=jax.ShapeDtypeStruct(q.shape, q.dtype),
        grid_spec=pltpu.PrefetchScalarGridSpec(
            num_scalar_prefetch=4,
            grid=(head_dev,),
            in_specs=[column(tok_dev)] * 3
            + [column(2 * B)] * 2
            + [column(G * B)] * 2
            + [pl.BlockSpec(rand.shape, lambda h, *_: (0, 0, 0, 0))],
            out_specs=column(tok_dev),
        ),
        compiler_params=ANYWHERE,
    )(keep, slot, live, where, q, k, v, hk, hv, gk, gv, rand)


def copy_kernel(order_ref, in_ref, out_ref):
    out_ref[...] = in_ref[...]


def take_blocks(blocks, order, cap):
    width = blocks.shape[1]
    return pl.pallas_call(
        copy_kernel,
        out_shape=jax.ShapeDtypeStruct((cap * B, width), blocks.dtype),
        grid_spec=pltpu.PrefetchScalarGridSpec(
            num_scalar_prefetch=1,
            grid=(cap,),
            in_specs=[pl.BlockSpec((B, width), lambda j, order: (order[j], 0))],
            out_specs=pl.BlockSpec((B, width), lambda j, order: (j, 0)),
        ),
        compiler_params=ANYWHERE,
    )(order, blocks)


def merge_kernel(kind_ref, from_ref, old_ref, new_ref, out_ref):
    kind = kind_ref[pl.program_id(0)]

    @pl.when(kind == 0)
    def _():
        out_ref[...] = old_ref[...]

    @pl.when(kind == 1)
    def _():
        out_ref[...] = jnp.zeros_like(out_ref)

    @pl.when(kind == 2)
    def _():
        out_ref[...] = new_ref[...]


def merge_blocks(old, new, kind, place):
    tok_dev, width = old.shape
    return pl.pallas_call(
        merge_kernel,
        out_shape=jax.ShapeDtypeStruct(old.shape, old.dtype),
        grid_spec=pltpu.PrefetchScalarGridSpec(
            num_scalar_prefetch=2,
            grid=(tok_dev // B,),
            in_specs=[
                pl.BlockSpec((B, width), lambda j, kind, place: (j, 0)),
                pl.BlockSpec((B, width), lambda j, kind, place: (place[j], 0)),
            ],
            out_specs=pl.BlockSpec((B, width), lambda j, kind, place: (j, 0)),
        ),
        compiler_params=ANYWHERE,
    )(kind, place, old, new)


def exclusive(flags, axis):
    return jnp.cumsum(flags, axis=axis) - flags


def first_at_least(caps, amount):
    return jnp.sum((amount > jnp.asarray(caps, jnp.int32)).astype(jnp.int32))


def settle(blocks, keep_all, slot, source, distance, me, count, blk_dev):
    i32 = jnp.int32
    devices = jnp.arange(count, dtype=i32)
    slots = jnp.arange(blk_dev, dtype=i32)
    sizes = sorted({0, *range(blk_dev // 2, blk_dev - 1), blk_dev})
    for bit_pos in range((count - 1).bit_length()):
        stride = 2**bit_pos
        at = source - distance % stride
        moving = (keep_all > 0) & (distance // stride % 2 > 0)
        on_slot = ((slot[:, None] == slots) & moving[:, None]).astype(i32)
        on_device = (at[:, None] == devices).astype(i32)
        leaving = jnp.sum(on_device[:, :, None] * on_slot[:, None, :], axis=0)
        needed = jnp.max(jnp.sum(leaving, axis=1))
        nth = exclusive(leaving, 1)
        mine_out, mine_nth = leaving[me], nth[me]
        send = jnp.sum(
            mine_out[:, None] * (mine_nth[:, None] == slots).astype(i32) * slots[:, None], axis=0
        )
        far = jnp.minimum(me + stride, count - 1)
        comes = jnp.where(me + stride < count, leaving[far], 0)
        kind = jnp.where(comes > 0, 2, jnp.where(mine_out > 0, 1, 0)).astype(i32)
        place = jnp.where(comes > 0, nth[far], 0)
        all_pairs = [(i, i - stride) for i in range(stride, count)]
        split = count - stride // 2
        upper = [pair for pair in all_pairs if pair[0] >= split]
        halves = 2 * stride >= count and 0 < len(upper) < len(all_pairs)

        def shifting(cap, pairs, send=send, kind=kind, place=place):
            def run(blocks):
                if cap == 0:
                    return blocks
                moved = lax.ppermute(take_blocks(blocks, send, cap), "seq", pairs)
                return merge_blocks(blocks, moved, kind, jnp.minimum(place, cap - 1))

            return run

        which = first_at_least(sizes[:-1], needed)
        runs = [shifting(cap, all_pairs) for cap in sizes]
        if halves:
            runs += [shifting(cap, upper) for cap in sizes]
            lower = jnp.sum(leaving * (devices < split)[:, None].astype(i32))
            which = which + jnp.where(lower > 0, 0, len(sizes))
        blocks = lax.switch(which, runs, blocks)
    return blocks


def plain_body(queries, keys, values, random_holder, random_offset, keep):
    tok_dev, width_dev = queries.shape
    blk_dev = tok_dev // B
    head_dev = width_dev // DH
    seq_count = lax.axis_size("seq")
    head_count = lax.axis_size("head")
    me = lax.axis_index("seq")
    count_req = blk_dev * R
    total = head_dev * count_req
    i32 = jnp.int32

    code = random_holder * blk_dev + random_offset
    code = jnp.where((keep > 0)[None, :, None], code, -1).reshape(total)
    note = jnp.concatenate([code, keep])
    note = jnp.broadcast_to(note, (seq_count * head_count,) + note.shape)
    table = lax.all_to_all(note, ("seq", "head"), split_axis=0, concat_axis=0, tiled=True)
    table = table.reshape(seq_count, head_count, total + blk_dev)
    keep_all = table[:, 0, total:].reshape(seq_count * blk_dev)
    codes = table[:, :, :total]
    devices = jnp.arange(seq_count, dtype=i32)

    halo_k, halo_v = halo(keys, "seq", B), halo(values, "seq", B)

    named = jnp.where(codes >= 0, codes // blk_dev, -1)
    counts = jnp.sum((named[..., None] == devices).astype(i32), axis=2)
    most = jnp.max(counts)
    onehot = (named[me, lax.axis_index("head")][:, None] == devices).astype(i32)
    mine = exclusive(onehot, 0)
    my_slot = jnp.sum(mine * onehot, axis=1)
    my_holder = jnp.sum(onehot * devices, axis=1)

    group = codes[:, lax.axis_index("head")]
    asks = (named[:, lax.axis_index("head")] == me).astype(i32)
    order = exclusive(asks, 1)
    full = min(total, head_dev * max(2, (count_req + seq_count - 1) // seq_count))
    chosen = asks[..., None] * (order[..., None] == jnp.arange(full, dtype=i32)).astype(i32)
    ask_head = jnp.arange(total, dtype=i32) // count_req
    ask = jnp.where(group >= 0, group % blk_dev, 0) + ask_head[None] * blk_dev
    ask = jnp.sum(chosen * ask[..., None], axis=1)
    pick_head, pick_block = ask // blk_dev, ask % blk_dev

    rank = exclusive(keep_all, 0)
    slot = rank % blk_dev
    source = jnp.arange(seq_count * blk_dev, dtype=i32) // blk_dev
    distance = jnp.where(keep_all > 0, source - rank // blk_dev, 0)
    my_slots = lax.dynamic_slice_in_dim(slot, me * blk_dev, blk_dev)
    live = jnp.stack([me > 0, me < seq_count - 1]).astype(i32)

    caps = sorted({max(1, full * part // 12) for part in range(8, 13)})

    def gathered(cap):
        def run(q, k, v, hk, hv):
            gk, gv = broadcast(jnp.stack((k[: G * B], v[: G * B])), "seq", 0)
            picked = pick(k, v, pick_head, pick_block, seq_count, cap)
            replies = lax.all_to_all(picked, "seq", split_axis=0, concat_axis=0, tiled=True)
            where = jnp.minimum(my_holder * cap + my_slot, seq_count * cap - 1)
            return attend(keep, my_slots, live, where, q, k, v, hk, hv, gk, gv, replies)

        return run

    blocks = lax.switch(
        first_at_least(caps[:-1], most),
        [gathered(cap) for cap in caps],
        queries, keys, values, halo_k, halo_v,
    )

    return settle(blocks, keep_all, slot, source, distance, me, seq_count, blk_dev)


TILE = (2 * B, DH)
SMALL = pltpu.CompilerParams(vmem_limit_bytes=60 * 1024 * 1024)


def fits(planes, tiles, most):
    slots = 2 * (planes - 1) * tiles + 2 * planes * most + most
    return slots * 2 * B * DH * 2 <= 44 * 1024 * 1024


def exchange_kernel(
    count, cz, cx, blk_dev, tab, k_ref, v_ref,
    rand_ref, home, zs, zr, xs, own,
    z_send, z_recv, x_send, x_recv, l_sem,
):
    planes = count // 2
    me = lax.axis_index("seq")
    plane, side = me // 2, me % 2
    mate = plane * 2 + 1 - side
    head_dev = k_ref.shape[1] // DH
    barrier = pltpu.get_barrier_semaphore()
    for step in range(1, count):
        peer = lax.rem(me + step, count)
        pl.semaphore_signal(
            barrier, inc=1, device_id={"seq": peer}, device_id_type=pl.DeviceIdType.MESH
        )
    pl.semaphore_wait(barrier, count - 1)

    def remote(src, dst, send, recv, peer):
        return pltpu.make_async_remote_copy(
            src_ref=src, dst_ref=dst, send_sem=send, recv_sem=recv,
            device_id={"seq": peer}, device_id_type=pl.DeviceIdType.MESH,
        )

    low, high = pl.ds(0, B), pl.ds(B, B)

    def load_home(block, carry):
        rows = pl.ds(pl.multiple_of(block * B, B), B)
        for h in range(head_dev):
            cols = slice(h * DH, (h + 1) * DH)
            home[h * blk_dev + block, low, :] = k_ref[rows, cols]
            home[h * blk_dev + block, high, :] = v_ref[rows, cols]
        return carry

    lax.fori_loop(0, blk_dev, load_home, 0)

    def from_slots(dst, src, table, row, cap):
        def one(j, carry):
            dst[j] = src[table[row, j]]
            return carry

        lax.fori_loop(0, cap, one, 0)

    deltas = range(1, planes)

    def goals(q):
        return sorted(deltas, key=lambda d: (abs((q + d) % planes - q), d))

    def arrival(q, d):
        source, half = (q - d) % planes, planes // 2
        if (source < half) == (q < half):
            return (0, abs(source - q))
        edges = (half - 1, half)
        return (1 if source in edges and q in edges else 2 if source not in edges else 3, d)

    def sources(q):
        return sorted(deltas, key=lambda d: arrival(q, d))

    x_base = (planes - 1) * cz
    z_copies = {
        d: remote(
            zs[d - 1], zr[d - 1], z_send.at[d - 1], z_recv.at[d - 1],
            lax.rem(plane + d, planes) * 2 + side,
        )
        for d in deltas
    }
    x_copies = [
        remote(
            xs[d], rand_ref.at[pl.ds(x_base + d * cx, cx)],
            x_send.at[d], x_recv.at[d], mate,
        )
        for d in range(planes)
    ]
    for d in deltas:
        from_slots(zs[d - 1], home, tab, d - 1, cz)
    from_slots(xs[0], home, tab, planes - 1, cx)
    for q in range(planes):
        @pl.when(plane == q)
        def _(q=q):
            order = goals(q)
            for d in order:
                z_copies[d].start()

    x_copies[0].start()
    from_slots(own, home, tab, 2 * planes - 1, cx)
    keep_own = pltpu.make_async_copy(
        own, rand_ref.at[pl.ds(x_base + planes * cx, cx)], l_sem.at[2]
    )
    keep_own.start()
    outs = {
        d: pltpu.make_async_copy(
            zr[d - 1], rand_ref.at[pl.ds((d - 1) * cz, cz)], l_sem.at[2 + d]
        )
        for d in deltas
    }

    def forward(d):
        z_copies[d].wait_recv()
        outs[d].start()
        from_slots(xs[d], zr[d - 1], tab, planes - 1 + d, cx)
        x_copies[d].start()

    for q in range(planes):
        @pl.when(plane == q)
        def _(q=q):
            for d in sources(q):
                forward(d)

    keep_own.wait()
    for d in deltas:
        outs[d].wait()
        z_copies[d].wait_send()
    for c in x_copies:
        c.wait()


def exchange(count, level, cz, cx, slots, blk_dev, tab, keys, values):
    planes = count // 2
    tok, width = keys.shape
    smem = pl.BlockSpec(memory_space=pltpu.SMEM)
    vmem = pl.BlockSpec(memory_space=pltpu.VMEM)
    dtype = keys.dtype
    dma = pltpu.SemaphoreType.DMA
    return pl.pallas_call(
        functools.partial(exchange_kernel, count, cz, cx, blk_dev),
        out_shape=jax.ShapeDtypeStruct((slots, *TILE), dtype),
        in_specs=[smem, vmem, vmem],
        out_specs=pl.BlockSpec(memory_space=pl.ANY),
        scratch_shapes=[
            pltpu.VMEM((tok // B * (width // DH), *TILE), dtype),
            [pltpu.VMEM((cz, *TILE), dtype) for _ in range(planes - 1)],
            [pltpu.VMEM((cz, *TILE), dtype) for _ in range(planes - 1)],
            [pltpu.VMEM((cx, *TILE), dtype) for _ in range(planes)],
            pltpu.VMEM((cx, *TILE), dtype),
            dma((planes - 1,)), dma((planes - 1,)),
            dma((planes,)), dma((planes,)),
            dma((2 + planes,)),
        ],
        compiler_params=pltpu.CompilerParams(
            collective_id=level, has_side_effects=True,
            vmem_limit_bytes=60 * 1024 * 1024,
        ),
    )(tab, keys, values)


PIECES = 4


def settle_kernel(
    count, caps, cr, cx, blk_dev, table, in_ref, out_ref,
    mine, zs, pool, rs, xs, xr, z_send, z_recv, r_send, r_recv, x_send, x_recv,
):
    planes = count // 2
    me = lax.axis_index("seq")
    plane, side = me // 2, me % 2
    mate = plane * 2 + 1 - side
    wide = in_ref.shape[1] // PIECES
    barrier = pltpu.get_barrier_semaphore()
    for step in range(1, count):
        peer = lax.rem(me + step, count)
        pl.semaphore_signal(
            barrier, inc=1, device_id={"seq": peer}, device_id_type=pl.DeviceIdType.MESH
        )
    pl.semaphore_wait(barrier, count - 1)

    def remote(src, dst, send, recv, peer):
        return pltpu.make_async_remote_copy(
            src_ref=src, dst_ref=dst, send_sem=send, recv_sem=recv,
            device_id={"seq": peer}, device_id_type=pl.DeviceIdType.MESH,
        )

    used = [d for d in range(1, planes) if caps[d - 1] > 0]
    used.sort(reverse=True)
    base = {d: blk_dev + sum(caps[: d - 1]) for d in used}
    gate = planes // 2 - 1
    beyond = range(1, gate + 1)
    r_base = blk_dev + sum(caps)
    x_row = planes - 1 + max(gate, 1)

    def sends(d):
        return jnp.logical_and(plane >= d, jnp.logical_or(plane != gate + 1, d == 1))

    def gets(d):
        return jnp.logical_and(plane + d < planes, jnp.logical_or(plane + d != gate + 1, d == 1))

    def fill(dst, src, table, row, cap):
        def one(j, carry):
            dst[j] = src[table[row, j]]
            return carry

        lax.fori_loop(0, cap, one, 0)

    def own_part(piece):
        def one(j, carry):
            rows = pl.ds(pl.multiple_of(j * B, B), B)
            block = in_ref[rows, piece * wide : (piece + 1) * wide]
            mine[piece][j] = block
            pool[piece][j] = block
            return carry

        lax.fori_loop(0, blk_dev, one, 0)

    z_copies, x_copies = {}, []
    for piece in range(PIECES):
        for n, d in enumerate(used):
            z_copies[piece, d] = remote(
                zs[piece][n], pool[piece].at[pl.ds(base[d], caps[d - 1])],
                z_send.at[piece, n], z_recv.at[piece, n],
                jnp.maximum(me - 2 * d, 0),
            )
        for d in beyond:
            z_copies[piece, -d] = remote(
                rs[piece][d - 1], pool[piece].at[pl.ds(r_base, cr)],
                r_send.at[piece, d - 1], r_recv.at[piece],
                jnp.maximum(me - 2 * d, 0),
            )
        x_copies.append(remote(xs[piece], xr[piece], x_send.at[piece], x_recv.at[piece], mate))
    def start_z(piece):
        for d in used:
            @pl.when(sends(d))
            def _(d=d):
                z_copies[piece, d].start()

    for piece in range(PIECES):
        own_part(piece)
        for n, d in enumerate(used):
            fill(zs[piece][n], mine[piece], table, d - 1, caps[d - 1])
        if piece > 0:
            start_z(piece - 1)
    start_z(PIECES - 1)

    def finish(piece):
        x_copies[piece].wait_recv()

        def one(j, carry):
            rows = pl.ds(pl.multiple_of(j * B, B), B)
            kind = table[x_row + 1, j]
            near, far = pool[piece][table[x_row + 2, j]], xr[piece][table[x_row + 3, j]]
            block = jnp.where(kind == 1, near, jnp.where(kind == 2, far, jnp.zeros_like(far)))
            out_ref[rows, piece * wide : (piece + 1) * wide] = block
            return carry

        lax.fori_loop(0, blk_dev, one, 0)

    for piece in range(PIECES):
        for d in used:
            @pl.when(gets(d))
            def _(d=d, piece=piece):
                z_copies[piece, d].wait_recv()

        @pl.when(plane == gate)
        def _(piece=piece):
            for d in beyond:
                fill(rs[piece][d - 1], pool[piece], table, planes - 2 + d, cr)
                z_copies[piece, -d].start()

        @pl.when(plane < gate)
        def _(piece=piece):
            if gate > 0:
                z_copies[piece, -1].wait_recv()

        fill(xs[piece], pool[piece], table, x_row, cx)
        x_copies[piece].start()
        if piece > 0:
            finish(piece - 1)
    finish(PIECES - 1)
    for piece in range(PIECES):
        x_copies[piece].wait_send()
        for d in used:
            @pl.when(sends(d))
            def _(d=d, piece=piece):
                z_copies[piece, d].wait_send()

        @pl.when(plane == gate)
        def _(piece=piece):
            for d in beyond:
                z_copies[piece, -d].wait_send()


def settled(count, number, caps, cr, cx, blk_dev, packs, blocks):
    tok, width = blocks.shape
    planes, wide = count // 2, width // PIECES
    smem = pl.BlockSpec(memory_space=pltpu.SMEM)
    vmem = pl.BlockSpec(memory_space=pltpu.VMEM)
    dma, dtype = pltpu.SemaphoreType.DMA, blocks.dtype
    sent = [caps[d - 1] for d in range(planes - 1, 0, -1) if caps[d - 1] > 0]

    def each(rows):
        return [pltpu.VMEM((rows, B, wide), dtype) for _ in range(PIECES)]

    return pl.pallas_call(
        functools.partial(settle_kernel, count, caps, cr, cx, blk_dev),
        out_shape=jax.ShapeDtypeStruct(blocks.shape, dtype),
        in_specs=[smem, vmem],
        out_specs=vmem,
        scratch_shapes=[
            each(blk_dev),
            [[pltpu.VMEM((c, B, wide), dtype) for c in sent] for _ in range(PIECES)],
            each(blk_dev + sum(caps) + cr),
            [[pltpu.VMEM((cr, B, wide), dtype) for _ in range(planes // 2 - 1)] for _ in range(PIECES)],
            each(cx),
            each(cx),
            dma((PIECES, len(sent))), dma((PIECES, len(sent))),
            dma((PIECES, planes // 2)), dma((PIECES,)), dma((PIECES,)), dma((PIECES,)),
        ],
        compiler_params=pltpu.CompilerParams(
            collective_id=number, has_side_effects=True,
            vmem_limit_bytes=60 * 1024 * 1024,
        ),
    )(packs, blocks)


def settle_levels(planes, blk_dev):
    def pad(first, second):
        return ((first, second) + (0,) * planes)[: planes - 1]

    half, few = blk_dev // 2, blk_dev * 3 // 4
    choices = [
        (2 * max(f + t, f + r) + r, pad(f, t), r, few)
        for f in range(half, few + 1)
        for t in range(half, few + 1)
        for r in (half // 2, half)
        if abs(f - t) < 2 or t == half
    ]
    choices = sorted(choices) + [
        (0, pad(half + 1, half + 1), few, few + 1),
        (0, pad(few + 1, half + 1), half // 2, few + 1),
        (0, ((few + 1, few) + (1,) * planes)[: planes - 1], few, few + 1),
        (0, (blk_dev,) * (planes - 1), blk_dev, blk_dev),
    ]
    return [limits for _, *limits in choices]


def pack(blocks, packs, level, count, blk_dev, first_id, choices):
    def run(number, *limits):
        return lambda *args: settled(count, first_id + number, *limits, blk_dev, *args)

    runs = [run(n, *limits) for n, limits in enumerate(choices)]
    return lax.switch(level, runs, packs, blocks)


CHUNK = 8


def near_far_kernel(
    blk_dev, keep_ref, live_ref, where_ref, used_ref,
    q_ref, k_ref, v_ref, hk_ref, hv_ref, gk_ref, gv_ref, rand_hbm, out_ref, rand_ref, sems,
):
    scale = 1.0 / math.sqrt(DH)
    head = pl.program_id(0)
    chunks = rand_hbm.shape[0] // CHUNK

    @pl.when(head == 0)
    def _():
        def copy(c):
            rows = pl.ds(c * CHUNK, CHUNK)
            return pltpu.make_async_copy(rand_hbm.at[rows], rand_ref.at[rows], sems.at[c])

        for c in range(chunks):
            pl.when(c * CHUNK < used_ref[0, 1])(lambda c=c: copy(c).start())
        for c in range(chunks):
            pl.when(c * CHUNK < used_ref[0, 1])(lambda c=c: copy(c).wait())

    def tile(ref, halo_ref, i):
        if i < 0:
            return halo_ref[0, :B]
        if i >= blk_dev:
            return halo_ref[0, B:]
        return ref[i * B : (i + 1) * B]

    def one(i):
        q = q_ref[i * B : (i + 1) * B]
        near = range(i - 1, i + 2)
        picks = [where_ref[head, i * R + r] for r in range(R)]
        k_parts = [
            jnp.concatenate([tile(k_ref, hk_ref, n) for n in near], axis=0),
            gk_ref[0],
            jnp.concatenate([rand_ref[p, :B] for p in picks], axis=0),
        ]
        v_parts = [
            jnp.concatenate([tile(v_ref, hv_ref, n) for n in near], axis=0),
            gv_ref[0],
            jnp.concatenate([rand_ref[p, B:] for p in picks], axis=0),
        ]
        scores = [
            lax.dot_general(
                q, k, (((1,), (1,)), ((), ())), preferred_element_type=jnp.float32
            )
            * scale
            for k in k_parts
        ]
        lanes = lax.broadcasted_iota(jnp.int32, scores[0].shape, 1)
        if i == 0:
            dead = jnp.logical_and(lanes < B, live_ref[0] == 0)
            scores[0] = jnp.where(dead, neg_big, scores[0])
        if i == blk_dev - 1:
            dead = jnp.logical_and(lanes >= 2 * B, live_ref[1] == 0)
            scores[0] = jnp.where(dead, neg_big, scores[0])
        peak = functools.reduce(
            jnp.maximum, [jnp.max(s, axis=-1, keepdims=True) for s in scores]
        )
        numer = jnp.zeros((B, DH), jnp.float32)
        denom = jnp.zeros((B, 1), jnp.float32)
        for s, v in zip(scores, v_parts):
            w = jnp.exp(s - peak).astype(jnp.bfloat16)
            denom = denom + jnp.sum(w.astype(jnp.float32), axis=-1, keepdims=True)
            numer = numer + jnp.dot(w, v, preferred_element_type=jnp.float32)
        out_ref[i * B : (i + 1) * B, :] = (numer / denom).astype(out_ref.dtype)

    for i in range(blk_dev):
        pl.when(keep_ref[i] > 0)(functools.partial(one, i))


def near_far(keep, live, where, used, q, k, v, halo_kv, glob, rand):
    tok_dev, width_dev = q.shape
    blk_dev, head_dev = tok_dev // B, width_dev // DH

    def column(rows):
        return pl.BlockSpec((rows, DH), lambda h, *_: (0, h))

    def part(rows, which):
        return pl.BlockSpec((1, rows, DH), lambda h, *_: (which, 0, h))

    return pl.pallas_call(
        functools.partial(near_far_kernel, blk_dev),
        out_shape=jax.ShapeDtypeStruct(q.shape, q.dtype),
        grid_spec=pltpu.PrefetchScalarGridSpec(
            num_scalar_prefetch=4,
            grid=(head_dev,),
            in_specs=[column(tok_dev)] * 3
            + [part(2 * B, 0), part(2 * B, 1), part(G * B, 0), part(G * B, 1)]
            + [pl.BlockSpec(memory_space=pl.ANY)],
            out_specs=column(tok_dev),
            scratch_shapes=[
                pltpu.VMEM(rand.shape, rand.dtype),
                pltpu.SemaphoreType.DMA((rand.shape[0] // CHUNK,)),
            ],
        ),
        compiler_params=ANYWHERE,
    )(keep, live, where, used, q, k, v, halo_kv, halo_kv, glob, glob, rand)


def quotient(x, n):
    return jnp.floor((x.astype(jnp.float32) + 0.5) * (1.0 / n)).astype(jnp.int32)


def plan_kernel(
    count, head_count, blk_dev, caps, choices, own_ref, k_ref, v_ref,
    tab_ref, where_ref, misc_ref, pack_ref, halo_ref, glob_ref,
    note_ref, need_ref, want_ref, slot_ref, both_ref, both_slot_ref,
    n_send, n_recv, h_send, h_recv, g_send, g_recv, s_send, s_recv, e_send, l_sem,
):
    i32, f32, bf16 = jnp.int32, jnp.float32, jnp.bfloat16
    planes = count // 2
    me, group = lax.axis_index("seq"), lax.axis_index("head")
    plane, side = me // 2, me % 2
    mate = me + 1 - 2 * side
    tall = own_ref.shape[0]
    everyone = count * head_count
    here_id = me * head_count + group
    barrier = pltpu.get_barrier_semaphore()

    def device(step):
        other = lax.rem(here_id + step, everyone)
        return {"seq": other // head_count, "head": lax.rem(other, head_count)}

    for step in range(1, everyone):
        pl.semaphore_signal(
            barrier, inc=1, device_id=device(step), device_id_type=pl.DeviceIdType.MESH
        )
    pl.semaphore_wait(barrier, everyone - 1)

    def remote(src, dst, send, recv, peer):
        return pltpu.make_async_remote_copy(
            src_ref=src, dst_ref=dst, send_sem=send, recv_sem=recv,
            device_id=peer, device_id_type=pl.DeviceIdType.MESH,
        )

    slot_rows = pl.ds(pl.multiple_of(here_id * tall, tall), tall)
    notices = [
        remote(
            own_ref, note_ref.at[slot_rows], n_send.at[step - 1], n_recv.at[step - 1], device(step)
        )
        for step in range(1, everyone)
    ]
    for c in notices:
        c.start()
    note_ref[slot_rows, :] = own_ref[...]

    tables = (k_ref, v_ref)
    low, high = pl.ds(0, B), pl.ds(B, B)
    tok, width = k_ref.shape
    after, before = jnp.minimum(me + 1, count - 1), jnp.maximum(me - 1, 0)
    ups = [
        remote(
            tables[i].at[pl.ds(tok - B, B)], halo_ref.at[i, low],
            h_send.at[i], h_recv.at[i], {"seq": after},
        )
        for i in range(2)
    ]
    downs = [
        remote(
            tables[i].at[pl.ds(0, B)], halo_ref.at[i, high],
            h_send.at[2 + i], h_recv.at[2 + i], {"seq": before},
        )
        for i in range(2)
    ]
    local = [
        pltpu.make_async_copy(tables[i].at[pl.ds(0, G * B)], glob_ref.at[i], l_sem.at[i])
        for i in range(2)
    ]
    onto = {"seq": jnp.minimum(me + 2, count - 1)}
    chain, swap, extra = [], [], []
    for n in range(PIECES):
        part = pl.ds(n * (width // PIECES), width // PIECES)
        item, other = glob_ref.at[side, :, part], glob_ref.at[1, :, part]
        chain.append(remote(item, item, g_send.at[n], g_recv.at[n], onto))
        swap.append(remote(item, item, s_send.at[n], s_recv.at[n], {"seq": mate}))
        extra.append(remote(other, other, e_send.at[n], g_recv.at[n], {"seq": mate}))

    @pl.when(me == 0)
    def _():
        for c in local:
            c.start()
        for c in local:
            c.wait()
        for n in range(PIECES):
            chain[n].start()
            extra[n].start()
        for c in swap:
            c.start()

    @pl.when(me < count - 1)
    def _():
        for c in ups:
            c.start()

    @pl.when(me > 0)
    def _():
        for c in downs:
            c.start()

    @pl.when(me == 0)
    def _():
        halo_ref[:, low, :] = jnp.zeros((2, B, width), k_ref.dtype)

    @pl.when(me == count - 1)
    def _():
        halo_ref[:, high, :] = jnp.zeros((2, B, width), k_ref.dtype)

    def pass_on():
        for n in range(PIECES):
            chain[n].wait_recv()

            @pl.when(plane < planes - 1)
            def _(n=n):
                chain[n].start()

            @pl.when(me > 1)
            def _(n=n):
                swap[n].start()

    for c in notices:
        c.wait_recv()

    @pl.when(jnp.logical_and(me > 0, plane <= 1))
    def _():
        pass_on()

    rows, lanes = note_ref.shape[0], tab_ref.shape[1]
    head_dev = rows // (count * head_count)
    count_req = blk_dev * R
    blocks = count * blk_dev

    def iota(shape, axis):
        return lax.broadcasted_iota(i32, shape, axis)

    def dot(a, b):
        return jnp.dot(a.astype(bf16), b.astype(bf16), preferred_element_type=f32)

    def flag(x):
        return x.astype(f32)

    notes = note_ref[...]
    lane = iota((rows, lanes), 1)
    need = jnp.zeros((rows, lanes), f32)
    for e in range(count_req):
        need = jnp.where(notes[:, e : e + 1] == lane, 1.0, need)
    need_ref[...] = need

    wide_r, wide_c = iota((lanes, lanes), 0), iota((lanes, lanes), 1)
    own_r, own_c = quotient(wide_r, blk_dev), quotient(wide_c, blk_dev)
    same = flag(own_r == own_c)
    inside = flag((own_r == own_c) & (wide_r < wide_c))

    def by_head(x):
        return jnp.sum(x.reshape(-1, head_dev, lanes), axis=1)

    most_x = jnp.max(dot(by_head(need), same))
    span = head_count * head_dev
    pairs = need.reshape(planes, 2, span, lanes)
    union = jnp.maximum(pairs[:, 0], pairs[:, 1]).reshape(planes * span, lanes)
    union_count = dot(by_head(union), same)
    holder_plane = quotient(quotient(iota(union_count.shape, 1), blk_dev), 2)
    goal_plane = quotient(iota(union_count.shape, 0), head_count)
    most_z = jnp.max(jnp.where(holder_plane != goal_plane, union_count, 0.0))
    level = jnp.int32(0)
    cz, cx = jnp.int32(caps[0][0]), jnp.int32(caps[0][1])
    for n in range(1, len(caps)):
        over = (most_z > caps[n - 1][0]) | (most_x > caps[n - 1][1])
        level = jnp.where(over, n, level)
        cz = jnp.where(over, caps[n][0], cz)
        cx = jnp.where(over, caps[n][1], cx)

    for d in range(count):
        start = pl.multiple_of((d * head_count + group) * head_dev, head_dev)
        want_ref[d * head_dev : (d + 1) * head_dev, :] = need_ref[pl.ds(start, head_dev), :]
    want = want_ref[...]
    both = jnp.maximum(
        *[want.reshape(planes, 2, head_dev, lanes)[:, i] for i in range(2)]
    ).reshape(planes * head_dev, lanes)
    both_ref[...] = both

    def slots(x):
        tall = x.shape[0]
        r, c = iota((tall, tall), 0), iota((tall, tall), 1)
        above = flag((quotient(r, head_dev) == quotient(c, head_dev)) & (c < r))
        return dot(x, inside) + dot(above, dot(x, same))

    slot_ref[...] = slots(want)
    both_slot_ref[...] = slots(both)

    def head_rows(ref, i):
        return ref[pl.ds(pl.multiple_of(i * head_dev, head_dev), head_dev), :]

    def shifted(x, holder):
        return pltpu.roll(x, lax.rem(lanes - holder * blk_dev, lanes), 1)

    short = iota((head_dev, lanes), 1)
    first = iota((head_dev, 1), 0)

    def listed(flags, places, holder, worth):
        key = jnp.where(shifted(flags, holder) > 0, shifted(places, holder), -1.0).astype(i32)
        total = jnp.zeros((head_dev, lanes), f32)
        if worth is not None:
            worth = shifted(worth, holder)
        for b in range(blk_dev):
            value = (first * blk_dev + b).astype(f32) if worth is None else worth[:, b : b + 1]
            total = total + jnp.where(key[:, b : b + 1] == short, value, 0.0)
        return jnp.sum(total, axis=0, keepdims=True).astype(i32)

    tables = []
    for d in range(1, planes):
        goal = lax.rem(plane + d, planes)
        tables.append(listed(head_rows(both_ref, goal), head_rows(both_slot_ref, goal), me, None))
    here = head_rows(both_slot_ref, plane)
    for d in range(planes):
        source = lax.rem(plane - d + planes, planes) * 2 + side
        tables.append(
            listed(head_rows(want_ref, mate), head_rows(slot_ref, mate), source, here if d else None)
        )
    tables.append(listed(head_rows(want_ref, me), head_rows(slot_ref, me), me, None))
    tab_ref[...] = jnp.zeros(tab_ref.shape, i32)
    for n, row in enumerate(tables):
        tab_ref[n : n + 1, :] = row

    holder = quotient(short, blk_dev)
    h_plane = quotient(holder, 2)
    h_side = holder - 2 * h_plane
    gap = plane - h_plane
    gap = jnp.where(gap < 0, gap + planes, gap)
    x_base = (planes - 1) * cz
    by_z = (h_side == side) & (holder != me)
    start = jnp.where(
        by_z, (gap - 1) * cz, jnp.where(holder == me, x_base + planes * cx, x_base + gap * cx)
    )
    spot = start.astype(f32) + jnp.where(by_z, here, head_rows(slot_ref, me))
    mine = pl.multiple_of((me * head_count + group) * head_dev, head_dev)
    picks = note_ref[pl.ds(mine, head_dev), :]
    found = jnp.zeros((head_dev, lanes), f32)
    for e in range(count_req):
        value = jnp.sum(jnp.where(picks[:, e : e + 1] == short, spot, 0.0), axis=1, keepdims=True)
        found = jnp.where(short == e, value, found)
    where_ref[...] = found.astype(i32)

    grid_keep = note_ref[...].astype(f32)
    picked = jnp.zeros((count, grid_keep.shape[1]), f32)
    tall_r, tall_c = iota((count, rows), 0), iota((count, rows), 1)
    stride = head_count * head_dev
    picked = dot(flag(tall_c == tall_r * stride), jnp.clip(grid_keep, 0.0, 1.0))
    spread_r, spread_c = iota((picked.shape[1], lanes), 0), iota((picked.shape[1], lanes), 1)
    spread = flag(spread_r == count_req + spread_c - quotient(spread_c, blk_dev) * blk_dev)
    table = dot(picked, spread)
    row8, lane8 = iota((count, lanes), 0), iota((count, lanes), 1)
    kept_r = jnp.sum(jnp.where(quotient(lane8, blk_dev) == row8, table, 0.0), axis=0, keepdims=True)
    kept8 = jnp.broadcast_to(kept_r, (8, lanes))
    rank_r = dot(kept8, flag(wide_r < wide_c))[:1]

    sub, across = iota((blocks, lanes), 0), iota((blocks, lanes), 1)
    turn = sub == across

    def column(row):
        return jnp.sum(jnp.where(turn, row, 0.0), axis=1, keepdims=True)

    def facts(kept, rank, index):
        rank = rank.astype(i32)
        source, goal = quotient(index, blk_dev), quotient(rank, blk_dev)
        s_plane, g_plane = quotient(source, 2), quotient(goal, 2)
        gate = planes // 2 - 1
        relayed = (kept > 0) & (s_plane == gate + 1) & (g_plane < gate)
        far = jnp.where(relayed, 1, s_plane - g_plane)
        s_side, g_side = source - 2 * s_plane, goal - 2 * g_plane
        return kept > 0, rank, source, goal, g_plane, s_side, g_side, relayed, far

    index_r = iota((1, lanes), 1)
    index_c = iota((blocks, 1), 0)
    kr, _, sr, gr, pr, xr, yr, rr, fr = facts(kept_r, rank_r, index_r)
    kc, rank, sc, gc, pc, xc, yc, rc, fc = facts(column(kept_r), column(rank_r), index_c)
    earlier = across < sub

    def tally(hit):
        return jnp.sum(jnp.where(earlier & hit, 1.0, 0.0), axis=1, keepdims=True).astype(i32)

    by_z = tally((sc == sr) & (fc == fr) & kr)
    flow = (pc == pr) & (xc == xr)
    by_r = tally(flow & rr)
    by_x = tally(flow & kr & (xr != yr))
    crosses = kc & (xc != yc)
    gate = planes // 2 - 1

    def largest(hit, value):
        return jnp.max(jnp.where(hit, value + 1, 0).astype(f32))

    tops = [largest(kc & (fc == d), by_z) for d in range(1, planes)]
    top_r, top_x = largest(rc, by_r), largest(crosses, by_x)
    last = len(choices) - 1
    pick = jnp.int32(last)
    own = [jnp.int32(c) for c in choices[last][0]]
    for n in range(last - 1, -1, -1):
        limits, limit_r, limit_x = choices[n]
        ok = (top_r <= limit_r) & (top_x <= limit_x)
        for top, limit in zip(tops, limits):
            ok = ok & (top <= limit)
        pick = jnp.where(ok, n, pick)
        own = [jnp.where(ok, c, o) for c, o in zip(limits, own)]
    local = index_c - sc * blk_dev
    held = local
    base = jnp.int32(blk_dev)
    for d in range(1, planes):
        held = jnp.where(fc == d, base + by_z, held)
        base = base + own[d - 1]
    ahead = held
    held = jnp.where(rc, base + by_r, held)

    def rows_of(hit, places, worth):
        value = jnp.where(hit & (places == across), worth, 0).astype(f32)
        return jnp.sum(value, axis=0, keepdims=True).astype(i32)

    packs = [rows_of(kc & (fc == d) & (sc == me), by_z, local) for d in range(1, planes)]
    for d in range(1, max(gate, 1) + 1):
        packs.append(rows_of(rc & (xc == side) & (plane == gate) & (pc == gate - d), by_r, ahead))
    packs.append(rows_of(crosses & (pc == plane) & (xc == side), by_x, held))
    lands = kc & (gc == me)
    place = rank - gc * blk_dev
    straight = xc == side
    packs.append(rows_of(lands, place, jnp.where(straight, 1, 2)))
    packs.append(rows_of(lands & straight, place, held))
    packs.append(rows_of(lands & jnp.logical_not(straight), place, by_x))
    pack_ref[...] = jnp.zeros(pack_ref.shape, i32)
    for n, row in enumerate(packs):
        pack_ref[n : n + 1, :] = row

    used = x_base + (planes + 1) * cx
    spot8 = iota(misc_ref.shape, 1)
    misc_ref[...] = jnp.where(
        spot8 == 0, level, jnp.where(spot8 == 1, used, jnp.where(spot8 == 2, pick, 0))
    )

    @pl.when(plane > 1)
    def _():
        pass_on()

    @pl.when(me > 0)
    def _():
        for c in swap:
            c.wait_recv()

    @pl.when(plane < planes - 1)
    def _():
        for c in chain:
            c.wait_send()

    @pl.when(me == 0)
    def _():
        for c in extra:
            c.wait_send()

    @pl.when(me != 1)
    def _():
        for c in swap:
            c.wait_send()

    @pl.when(me < count - 1)
    def _():
        for c in ups:
            c.wait_send()
        for c in downs:
            c.wait_recv()

    @pl.when(me > 0)
    def _():
        for c in downs:
            c.wait_send()
        for c in ups:
            c.wait_recv()

    for c in notices:
        c.wait_send()


def plan(note, keys, values, count, head_count, blk_dev, caps, choices, number):
    head_dev, width = note.shape[0], keys.shape[1]
    everyone = count * head_count
    rows = everyone * head_dev
    planes = count // 2
    lanes = max(128, count * blk_dev)
    i32, f32 = jnp.int32, jnp.float32
    tabs = -(-2 * planes // 8) * 8
    packs = -(-(planes + max(planes // 2 - 1, 1) + 3) // 8) * 8
    shape, dma = jax.ShapeDtypeStruct, pltpu.SemaphoreType.DMA
    vmem, anywhere = pl.BlockSpec(memory_space=pltpu.VMEM), pl.BlockSpec(memory_space=pl.ANY)
    return pl.pallas_call(
        functools.partial(plan_kernel, count, head_count, blk_dev, caps, choices),
        out_shape=(
            shape((tabs, lanes), i32), shape((head_dev, lanes), i32),
            shape((8, lanes), i32), shape((packs, lanes), i32),
            shape((2, 2 * B, width), keys.dtype), shape((2, G * B, width), keys.dtype),
        ),
        in_specs=[vmem, anywhere, anywhere],
        out_specs=(vmem,) * 6,
        scratch_shapes=[
            pltpu.VMEM((rows, note.shape[1]), i32),
            pltpu.VMEM((rows, lanes), f32),
            pltpu.VMEM((count * head_dev, lanes), f32), pltpu.VMEM((count * head_dev, lanes), f32),
            pltpu.VMEM((planes * head_dev, lanes), f32), pltpu.VMEM((planes * head_dev, lanes), f32),
            dma((everyone - 1,)), dma((everyone - 1,)), dma((4,)), dma((4,)),
            dma((PIECES,)), dma((PIECES,)), dma((PIECES,)), dma((PIECES,)), dma((PIECES,)), dma((2,)),
        ],
        compiler_params=pltpu.CompilerParams(
            collective_id=number, has_side_effects=True,
            vmem_limit_bytes=60 * 1024 * 1024,
        ),
    )(note, keys, values)


def levels(tiles, most):
    caps = []
    for part in (22, 24, 26, 28, 29, 30, 32, 36):
        cz = min(tiles, tiles * part // 64)
        caps.append((cz, min(most, max(1, most * min(24, part // 2 + 7) // 24))))
    caps.append((tiles, most))
    return sorted(set(caps))


def body(queries, keys, values, random_holder, random_offset, keep):
    tok_dev, width_dev = queries.shape
    blk_dev = tok_dev // B
    head_dev = width_dev // DH
    count = lax.axis_size("seq")
    head_count = lax.axis_size("head")
    count_req = blk_dev * R
    total = head_dev * count_req
    tiles = head_dev * blk_dev
    most = min(tiles, head_dev * max(2, (count_req + count - 1) // count))
    planes = count // 2
    if count % 2 or planes % 2 or not fits(planes, tiles, most):
        return plain_body(queries, keys, values, random_holder, random_offset, keep)
    me = lax.axis_index("seq")
    plane, side = me // 2, me % 2
    mate = me + 1 - 2 * side
    i32 = jnp.int32
    code = random_holder * blk_dev + random_offset
    code = jnp.where((keep > 0)[None, :, None], code, -1).reshape(head_dev, count_req)
    wide = -(-(count_req + blk_dev) // 128) * 128
    note = jnp.concatenate([code, jnp.broadcast_to(keep[None], (head_dev, blk_dev))], axis=1)
    note = jnp.pad(note, ((0, 0), (0, wide - count_req - blk_dev)), constant_values=-1)
    caps, choices = levels(tiles, most), settle_levels(planes, blk_dev)
    tab, where, misc, packs, halo_kv, glob = plan(
        note, keys, values, count, head_count, blk_dev, caps, choices, len(caps) + len(choices)
    )

    slots_all = -(-max((planes - 1) * c[0] + (planes + 1) * c[1] for c in caps) // CHUNK) * CHUNK
    def exchanged(number, caps):
        def run(tab, k, v):
            return exchange(count, number, *caps, slots_all, blk_dev, tab, k, v)

        return run

    rand = lax.switch(
        misc[0, 0], [exchanged(n, c) for n, c in enumerate(caps)], tab, keys, values
    )

    live = jnp.stack([me > 0, me < count - 1]).astype(i32)
    blocks = near_far(
        keep, live, where, misc, queries, keys, values, halo_kv, glob, rand
    )
    return pack(blocks, packs, misc[0, 2], count, blk_dev, len(caps), choices)


def solution(mesh):
    in_specs = (
        P("seq", "head"),
        P("seq", "head"),
        P("seq", "head"),
        P("head", "seq", None),
        P("head", "seq", None),
        P("seq"),
    )
    out_specs = P("seq", "head")
    return jax.shard_map(body, mesh=mesh, in_specs=in_specs, out_specs=out_specs, check_vma=False)
```

```python
import functools
import math

import jax
import jax.numpy as jnp
from jax import lax
from jax.experimental import pallas as pl
from jax.experimental.pallas import tpu as pltpu
from jax.sharding import PartitionSpec as P

DH = 128
B = 128
G = 2
R = 3

neg_big = -1e30
ANYWHERE = pltpu.CompilerParams(
    dimension_semantics=("arbitrary",), vmem_limit_bytes=60 * 1024 * 1024
)


def halo(block, axis, width):
    count = lax.axis_size(axis)
    forward = [(i, i + 1) for i in range(count - 1)]
    backward = [(target, source) for source, target in forward]
    low = lax.ppermute(block[-width:], axis, forward)
    high = lax.ppermute(block[:width], axis, backward)
    return jnp.concatenate([low, high], axis=0)


def broadcast(block, axis, source):
    block = jnp.where(lax.axis_index(axis) == source, block, jnp.zeros_like(block))
    return lax.psum(block, axis)


def pick_kernel(cap, head_ref, block_ref, k_ref, v_ref, out_ref):
    dest = pl.program_id(0)

    @pl.loop(0, cap)
    def _(j):
        rows = pl.ds(pl.multiple_of(block_ref[dest, j] * B, B), B)
        cols = pl.ds(pl.multiple_of(head_ref[dest, j] * DH, DH), DH)
        out_ref[j, 0] = k_ref[rows, cols]
        out_ref[j, 1] = v_ref[rows, cols]


def pick(keys, values, heads, blocks, seq_count, cap):
    whole = pl.BlockSpec(keys.shape, lambda d, *_: (0, 0))
    return pl.pallas_call(
        functools.partial(pick_kernel, cap),
        out_shape=jax.ShapeDtypeStruct((seq_count * cap, 2, B, DH), keys.dtype),
        grid_spec=pltpu.PrefetchScalarGridSpec(
            num_scalar_prefetch=2,
            grid=(seq_count,),
            in_specs=[whole, whole],
            out_specs=pl.BlockSpec((cap, 2, B, DH), lambda d, *_: (d, 0, 0, 0)),
        ),
        compiler_params=ANYWHERE,
    )(heads, blocks, keys, values)


def attend_kernel(
    blk_dev,
    keep_ref,
    slot_ref,
    live_ref,
    where_ref,
    q_ref,
    k_ref,
    v_ref,
    hk_ref,
    hv_ref,
    gk_ref,
    gv_ref,
    rand_ref,
    out_ref,
):
    scale = 1.0 / math.sqrt(DH)
    head = pl.program_id(0)
    out_ref[...] = jnp.zeros_like(out_ref)

    def tile(ref, halo_ref, i):
        if i < 0:
            return halo_ref[:B]
        if i >= blk_dev:
            return halo_ref[B:]
        return ref[i * B : (i + 1) * B]

    def one(i):
        q = q_ref[i * B : (i + 1) * B]
        near = range(i - 1, i + 2)
        picks = [where_ref[(head * blk_dev + i) * R + r] for r in range(R)]
        k_parts = [
            jnp.concatenate([tile(k_ref, hk_ref, n) for n in near], axis=0),
            gk_ref[...],
            jnp.concatenate([rand_ref[p, 0] for p in picks], axis=0),
        ]
        v_parts = [
            jnp.concatenate([tile(v_ref, hv_ref, n) for n in near], axis=0),
            gv_ref[...],
            jnp.concatenate([rand_ref[p, 1] for p in picks], axis=0),
        ]
        scores = [
            lax.dot_general(
                q, k, (((1,), (1,)), ((), ())), preferred_element_type=jnp.float32
            )
            * scale
            for k in k_parts
        ]
        lanes = lax.broadcasted_iota(jnp.int32, scores[0].shape, 1)
        if i == 0:
            dead = jnp.logical_and(lanes < B, live_ref[0] == 0)
            scores[0] = jnp.where(dead, neg_big, scores[0])
        if i == blk_dev - 1:
            dead = jnp.logical_and(lanes >= 2 * B, live_ref[1] == 0)
            scores[0] = jnp.where(dead, neg_big, scores[0])
        peak = functools.reduce(
            jnp.maximum, [jnp.max(s, axis=-1, keepdims=True) for s in scores]
        )
        numer = jnp.zeros((B, DH), jnp.float32)
        denom = jnp.zeros((B, 1), jnp.float32)
        for s, v in zip(scores, v_parts):
            w = jnp.exp(s - peak).astype(jnp.bfloat16)
            denom = denom + jnp.sum(w.astype(jnp.float32), axis=-1, keepdims=True)
            numer = numer + jnp.dot(w, v, preferred_element_type=jnp.float32)
        rows = pl.ds(pl.multiple_of(slot_ref[i] * B, B), B)
        out_ref[rows, :] = (numer / denom).astype(out_ref.dtype)

    for i in range(blk_dev):
        pl.when(keep_ref[i] > 0)(functools.partial(one, i))


def attend(keep, slot, live, where, q, k, v, hk, hv, gk, gv, rand):
    tok_dev, width_dev = q.shape
    blk_dev, head_dev = tok_dev // B, width_dev // DH

    def column(rows):
        return pl.BlockSpec((rows, DH), lambda h, *_: (0, h))

    return pl.pallas_call(
        functools.partial(attend_kernel, blk_dev),
        out_shape=jax.ShapeDtypeStruct(q.shape, q.dtype),
        grid_spec=pltpu.PrefetchScalarGridSpec(
            num_scalar_prefetch=4,
            grid=(head_dev,),
            in_specs=[column(tok_dev)] * 3
            + [column(2 * B)] * 2
            + [column(G * B)] * 2
            + [pl.BlockSpec(rand.shape, lambda h, *_: (0, 0, 0, 0))],
            out_specs=column(tok_dev),
        ),
        compiler_params=ANYWHERE,
    )(keep, slot, live, where, q, k, v, hk, hv, gk, gv, rand)


def copy_kernel(order_ref, in_ref, out_ref):
    out_ref[...] = in_ref[...]


def take_blocks(blocks, order, cap):
    width = blocks.shape[1]
    return pl.pallas_call(
        copy_kernel,
        out_shape=jax.ShapeDtypeStruct((cap * B, width), blocks.dtype),
        grid_spec=pltpu.PrefetchScalarGridSpec(
            num_scalar_prefetch=1,
            grid=(cap,),
            in_specs=[pl.BlockSpec((B, width), lambda j, order: (order[j], 0))],
            out_specs=pl.BlockSpec((B, width), lambda j, order: (j, 0)),
        ),
        compiler_params=ANYWHERE,
    )(order, blocks)


def merge_kernel(kind_ref, from_ref, old_ref, new_ref, out_ref):
    kind = kind_ref[pl.program_id(0)]

    @pl.when(kind == 0)
    def _():
        out_ref[...] = old_ref[...]

    @pl.when(kind == 1)
    def _():
        out_ref[...] = jnp.zeros_like(out_ref)

    @pl.when(kind == 2)
    def _():
        out_ref[...] = new_ref[...]


def merge_blocks(old, new, kind, place):
    tok_dev, width = old.shape
    return pl.pallas_call(
        merge_kernel,
        out_shape=jax.ShapeDtypeStruct(old.shape, old.dtype),
        grid_spec=pltpu.PrefetchScalarGridSpec(
            num_scalar_prefetch=2,
            grid=(tok_dev // B,),
            in_specs=[
                pl.BlockSpec((B, width), lambda j, kind, place: (j, 0)),
                pl.BlockSpec((B, width), lambda j, kind, place: (place[j], 0)),
            ],
            out_specs=pl.BlockSpec((B, width), lambda j, kind, place: (j, 0)),
        ),
        compiler_params=ANYWHERE,
    )(kind, place, old, new)


def exclusive(flags, axis):
    return jnp.cumsum(flags, axis=axis) - flags


def first_at_least(caps, amount):
    return jnp.sum((amount > jnp.asarray(caps, jnp.int32)).astype(jnp.int32))


def settle(blocks, keep_all, slot, source, distance, me, count, blk_dev):
    i32 = jnp.int32
    devices = jnp.arange(count, dtype=i32)
    slots = jnp.arange(blk_dev, dtype=i32)
    sizes = sorted({0, *range(blk_dev // 2, blk_dev - 1), blk_dev})
    for bit_pos in range((count - 1).bit_length()):
        stride = 2**bit_pos
        at = source - distance % stride
        moving = (keep_all > 0) & (distance // stride % 2 > 0)
        on_slot = ((slot[:, None] == slots) & moving[:, None]).astype(i32)
        on_device = (at[:, None] == devices).astype(i32)
        leaving = jnp.sum(on_device[:, :, None] * on_slot[:, None, :], axis=0)
        needed = jnp.max(jnp.sum(leaving, axis=1))
        nth = exclusive(leaving, 1)
        mine_out, mine_nth = leaving[me], nth[me]
        send = jnp.sum(
            mine_out[:, None] * (mine_nth[:, None] == slots).astype(i32) * slots[:, None], axis=0
        )
        far = jnp.minimum(me + stride, count - 1)
        comes = jnp.where(me + stride < count, leaving[far], 0)
        kind = jnp.where(comes > 0, 2, jnp.where(mine_out > 0, 1, 0)).astype(i32)
        place = jnp.where(comes > 0, nth[far], 0)
        all_pairs = [(i, i - stride) for i in range(stride, count)]
        split = count - stride // 2
        upper = [pair for pair in all_pairs if pair[0] >= split]
        halves = 2 * stride >= count and 0 < len(upper) < len(all_pairs)

        def shifting(cap, pairs, send=send, kind=kind, place=place):
            def run(blocks):
                if cap == 0:
                    return blocks
                moved = lax.ppermute(take_blocks(blocks, send, cap), "seq", pairs)
                return merge_blocks(blocks, moved, kind, jnp.minimum(place, cap - 1))

            return run

        which = first_at_least(sizes[:-1], needed)
        runs = [shifting(cap, all_pairs) for cap in sizes]
        if halves:
            runs += [shifting(cap, upper) for cap in sizes]
            lower = jnp.sum(leaving * (devices < split)[:, None].astype(i32))
            which = which + jnp.where(lower > 0, 0, len(sizes))
        blocks = lax.switch(which, runs, blocks)
    return blocks


def plain_body(queries, keys, values, random_holder, random_offset, keep):
    tok_dev, width_dev = queries.shape
    blk_dev = tok_dev // B
    head_dev = width_dev // DH
    seq_count = lax.axis_size("seq")
    head_count = lax.axis_size("head")
    me = lax.axis_index("seq")
    count_req = blk_dev * R
    total = head_dev * count_req
    i32 = jnp.int32

    code = random_holder * blk_dev + random_offset
    code = jnp.where((keep > 0)[None, :, None], code, -1).reshape(total)
    note = jnp.concatenate([code, keep])
    note = jnp.broadcast_to(note, (seq_count * head_count,) + note.shape)
    table = lax.all_to_all(note, ("seq", "head"), split_axis=0, concat_axis=0, tiled=True)
    table = table.reshape(seq_count, head_count, total + blk_dev)
    keep_all = table[:, 0, total:].reshape(seq_count * blk_dev)
    codes = table[:, :, :total]
    devices = jnp.arange(seq_count, dtype=i32)

    halo_k, halo_v = halo(keys, "seq", B), halo(values, "seq", B)

    named = jnp.where(codes >= 0, codes // blk_dev, -1)
    counts = jnp.sum((named[..., None] == devices).astype(i32), axis=2)
    most = jnp.max(counts)
    onehot = (named[me, lax.axis_index("head")][:, None] == devices).astype(i32)
    mine = exclusive(onehot, 0)
    my_slot = jnp.sum(mine * onehot, axis=1)
    my_holder = jnp.sum(onehot * devices, axis=1)

    group = codes[:, lax.axis_index("head")]
    asks = (named[:, lax.axis_index("head")] == me).astype(i32)
    order = exclusive(asks, 1)
    full = min(total, head_dev * max(2, (count_req + seq_count - 1) // seq_count))
    chosen = asks[..., None] * (order[..., None] == jnp.arange(full, dtype=i32)).astype(i32)
    ask_head = jnp.arange(total, dtype=i32) // count_req
    ask = jnp.where(group >= 0, group % blk_dev, 0) + ask_head[None] * blk_dev
    ask = jnp.sum(chosen * ask[..., None], axis=1)
    pick_head, pick_block = ask // blk_dev, ask % blk_dev

    rank = exclusive(keep_all, 0)
    slot = rank % blk_dev
    source = jnp.arange(seq_count * blk_dev, dtype=i32) // blk_dev
    distance = jnp.where(keep_all > 0, source - rank // blk_dev, 0)
    my_slots = lax.dynamic_slice_in_dim(slot, me * blk_dev, blk_dev)
    live = jnp.stack([me > 0, me < seq_count - 1]).astype(i32)

    caps = sorted({max(1, full * part // 12) for part in range(8, 13)})

    def gathered(cap):
        def run(q, k, v, hk, hv):
            gk, gv = broadcast(jnp.stack((k[: G * B], v[: G * B])), "seq", 0)
            picked = pick(k, v, pick_head, pick_block, seq_count, cap)
            replies = lax.all_to_all(picked, "seq", split_axis=0, concat_axis=0, tiled=True)
            where = jnp.minimum(my_holder * cap + my_slot, seq_count * cap - 1)
            return attend(keep, my_slots, live, where, q, k, v, hk, hv, gk, gv, replies)

        return run

    blocks = lax.switch(
        first_at_least(caps[:-1], most),
        [gathered(cap) for cap in caps],
        queries, keys, values, halo_k, halo_v,
    )

    return settle(blocks, keep_all, slot, source, distance, me, seq_count, blk_dev)


TILE = (2 * B, DH)
SMALL = pltpu.CompilerParams(vmem_limit_bytes=60 * 1024 * 1024)


def fits(planes, tiles, most):
    slots = 2 * (planes - 1) * tiles + 2 * planes * most + most
    return slots * 2 * B * DH * 2 <= 44 * 1024 * 1024


def exchange_kernel(
    count, cz, cx, blk_dev, tab, k_ref, v_ref,
    rand_ref, halo_ref, glob_ref, home, zs, zr, xs, own,
    z_send, z_recv, x_send, x_recv, h_send, h_recv, g_send, g_recv, l_sem,
):
    planes = count // 2
    me = lax.axis_index("seq")
    plane, side = me // 2, me % 2
    mate = plane * 2 + 1 - side
    tok = k_ref.shape[0]
    head_dev = k_ref.shape[1] // DH
    barrier = pltpu.get_barrier_semaphore()
    for step in range(1, count):
        peer = lax.rem(me + step, count)
        pl.semaphore_signal(
            barrier, inc=1, device_id={"seq": peer}, device_id_type=pl.DeviceIdType.MESH
        )
    pl.semaphore_wait(barrier, count - 1)

    def remote(src, dst, send, recv, peer):
        return pltpu.make_async_remote_copy(
            src_ref=src, dst_ref=dst, send_sem=send, recv_sem=recv,
            device_id={"seq": peer}, device_id_type=pl.DeviceIdType.MESH,
        )

    tables = (k_ref, v_ref)
    low, high = pl.ds(0, B), pl.ds(B, B)
    first, last = pl.ds(0, B), pl.ds(tok - B, B)
    after = jnp.minimum(me + 1, count - 1)
    before = jnp.maximum(me - 1, 0)
    ups = [
        remote(tables[i].at[last], halo_ref.at[i, low], h_send.at[i], h_recv.at[i], after)
        for i in range(2)
    ]
    downs = [
        remote(tables[i].at[first], halo_ref.at[i, high], h_send.at[2 + i], h_recv.at[2 + i], before)
        for i in range(2)
    ]
    local = [
        pltpu.make_async_copy(tables[i].at[pl.ds(0, G * B)], glob_ref.at[i], l_sem.at[i])
        for i in range(2)
    ]
    item = glob_ref.at[side]
    chain = remote(item, item, g_send.at[0], g_recv.at[0], jnp.minimum(me + 2, count - 1))
    swap = remote(item, item, g_send.at[1], g_recv.at[1], mate)
    extra = remote(glob_ref.at[1], glob_ref.at[1], g_send.at[2], g_recv.at[0], mate)

    @pl.when(me == 0)
    def _():
        for c in local:
            c.start()
        for c in local:
            c.wait()
        chain.start()
        extra.start()
        swap.start()

    def pass_on():
        @pl.when(me > 0)
        def _():
            chain.wait_recv()

            @pl.when(plane < planes - 1)
            def _():
                chain.start()

            @pl.when(me > 1)
            def _():
                swap.start()

    @pl.when(me < count - 1)
    def _():
        for c in ups:
            c.start()

    @pl.when(me > 0)
    def _():
        for c in downs:
            c.start()

    @pl.when(me == 0)
    def _():
        halo_ref[:, low, :] = jnp.zeros((2, B, k_ref.shape[1]), k_ref.dtype)

    @pl.when(me == count - 1)
    def _():
        halo_ref[:, high, :] = jnp.zeros((2, B, k_ref.shape[1]), k_ref.dtype)

    def load_home(block, carry):
        rows = pl.ds(pl.multiple_of(block * B, B), B)
        for h in range(head_dev):
            cols = slice(h * DH, (h + 1) * DH)
            home[h * blk_dev + block, low, :] = k_ref[rows, cols]
            home[h * blk_dev + block, high, :] = v_ref[rows, cols]
        return carry

    lax.fori_loop(0, blk_dev, load_home, 0)

    def from_slots(dst, src, table, row, cap):
        def one(j, carry):
            dst[j] = src[table[row, j]]
            return carry

        lax.fori_loop(0, cap, one, 0)

    deltas = range(1, planes)

    def goals(q):
        return sorted(deltas, key=lambda d: (abs((q + d) % planes - q), d))

    def arrival(q, d):
        source, half = (q - d) % planes, planes // 2
        if (source < half) == (q < half):
            return (0, abs(source - q))
        edges = (half - 1, half)
        return (1 if source in edges and q in edges else 2 if source not in edges else 3, d)

    def sources(q):
        return sorted(deltas, key=lambda d: arrival(q, d))

    x_base = (planes - 1) * cz
    z_copies = {
        d: remote(
            zs[d - 1], zr[d - 1], z_send.at[d - 1], z_recv.at[d - 1],
            lax.rem(plane + d, planes) * 2 + side,
        )
        for d in deltas
    }
    x_copies = [
        remote(
            xs[d], rand_ref.at[pl.ds(x_base + d * cx, cx)],
            x_send.at[d], x_recv.at[d], mate,
        )
        for d in range(planes)
    ]
    for d in deltas:
        from_slots(zs[d - 1], home, tab, d - 1, cz)
    from_slots(xs[0], home, tab, planes - 1, cx)
    for q in range(planes):
        @pl.when(plane == q)
        def _(q=q):
            order = goals(q)
            for n, d in enumerate(order):
                z_copies[d].start()
                if n == 0 and q == 0:
                    pass_on()

    x_copies[0].start()
    from_slots(own, home, tab, 2 * planes - 1, cx)
    keep_own = pltpu.make_async_copy(
        own, rand_ref.at[pl.ds(x_base + planes * cx, cx)], l_sem.at[2]
    )
    keep_own.start()
    outs = {
        d: pltpu.make_async_copy(
            zr[d - 1], rand_ref.at[pl.ds((d - 1) * cz, cz)], l_sem.at[2 + d]
        )
        for d in deltas
    }

    def forward(d):
        z_copies[d].wait_recv()
        outs[d].start()
        from_slots(xs[d], zr[d - 1], tab, planes - 1 + d, cx)
        x_copies[d].start()

    for q in range(planes):
        @pl.when(plane == q)
        def _(q=q):
            for n, d in enumerate(sources(q)):
                forward(d)
                if n == 0 and 0 < q < planes // 2:
                    pass_on()
            if q >= planes // 2:
                pass_on()

    @pl.when(me > 0)
    def _():
        swap.wait_recv()

    @pl.when(plane < planes - 1)
    def _():
        chain.wait_send()

    @pl.when(me == 0)
    def _():
        extra.wait_send()

    @pl.when(me != 1)
    def _():
        swap.wait_send()

    @pl.when(me < count - 1)
    def _():
        for c in ups:
            c.wait_send()
        for c in downs:
            c.wait_recv()

    @pl.when(me > 0)
    def _():
        for c in downs:
            c.wait_send()
        for c in ups:
            c.wait_recv()

    keep_own.wait()
    for d in deltas:
        outs[d].wait()
        z_copies[d].wait_send()
    for c in x_copies:
        c.wait()


def exchange(count, level, cz, cx, slots, blk_dev, tab, keys, values):
    planes = count // 2
    tok, width = keys.shape
    smem = pl.BlockSpec(memory_space=pltpu.SMEM)
    vmem = pl.BlockSpec(memory_space=pltpu.VMEM)
    dtype = keys.dtype
    dma = pltpu.SemaphoreType.DMA
    return pl.pallas_call(
        functools.partial(exchange_kernel, count, cz, cx, blk_dev),
        out_shape=(
            jax.ShapeDtypeStruct((slots, *TILE), dtype),
            jax.ShapeDtypeStruct((2, 2 * B, width), dtype),
            jax.ShapeDtypeStruct((2, G * B, width), dtype),
        ),
        in_specs=[smem, vmem, vmem],
        out_specs=(pl.BlockSpec(memory_space=pl.ANY), vmem, vmem),
        scratch_shapes=[
            pltpu.VMEM((tok // B * (width // DH), *TILE), dtype),
            [pltpu.VMEM((cz, *TILE), dtype) for _ in range(planes - 1)],
            [pltpu.VMEM((cz, *TILE), dtype) for _ in range(planes - 1)],
            [pltpu.VMEM((cx, *TILE), dtype) for _ in range(planes)],
            pltpu.VMEM((cx, *TILE), dtype),
            dma((planes - 1,)), dma((planes - 1,)),
            dma((planes,)), dma((planes,)),
            dma((4,)), dma((4,)), dma((3,)), dma((2,)), dma((2 + planes,)),
        ],
        compiler_params=pltpu.CompilerParams(
            collective_id=level, has_side_effects=True,
            vmem_limit_bytes=60 * 1024 * 1024,
        ),
    )(tab, keys, values)


PIECES = 4


def settle_kernel(
    count, caps, cr, cx, blk_dev, table, in_ref, out_ref,
    mine, zs, pool, rs, xs, xr, z_send, z_recv, r_send, r_recv, x_send, x_recv,
):
    planes = count // 2
    me = lax.axis_index("seq")
    plane, side = me // 2, me % 2
    mate = plane * 2 + 1 - side
    wide = in_ref.shape[1] // PIECES
    barrier = pltpu.get_barrier_semaphore()
    for step in range(1, count):
        peer = lax.rem(me + step, count)
        pl.semaphore_signal(
            barrier, inc=1, device_id={"seq": peer}, device_id_type=pl.DeviceIdType.MESH
        )
    pl.semaphore_wait(barrier, count - 1)

    def remote(src, dst, send, recv, peer):
        return pltpu.make_async_remote_copy(
            src_ref=src, dst_ref=dst, send_sem=send, recv_sem=recv,
            device_id={"seq": peer}, device_id_type=pl.DeviceIdType.MESH,
        )

    used = [d for d in range(1, planes) if caps[d - 1] > 0]
    used.sort(reverse=True)
    base = {d: blk_dev + sum(caps[: d - 1]) for d in used}
    gate = planes // 2 - 1
    beyond = range(1, gate + 1)
    r_base = blk_dev + sum(caps)
    x_row = planes - 1 + max(gate, 1)

    def sends(d):
        return jnp.logical_and(plane >= d, jnp.logical_or(plane != gate + 1, d == 1))

    def gets(d):
        return jnp.logical_and(plane + d < planes, jnp.logical_or(plane + d != gate + 1, d == 1))

    def fill(dst, src, table, row, cap):
        def one(j, carry):
            dst[j] = src[table[row, j]]
            return carry

        lax.fori_loop(0, cap, one, 0)

    def own_part(piece):
        def one(j, carry):
            rows = pl.ds(pl.multiple_of(j * B, B), B)
            block = in_ref[rows, piece * wide : (piece + 1) * wide]
            mine[piece][j] = block
            pool[piece][j] = block
            return carry

        lax.fori_loop(0, blk_dev, one, 0)

    z_copies, x_copies = {}, []
    for piece in range(PIECES):
        for n, d in enumerate(used):
            z_copies[piece, d] = remote(
                zs[piece][n], pool[piece].at[pl.ds(base[d], caps[d - 1])],
                z_send.at[piece, n], z_recv.at[piece, n],
                jnp.maximum(me - 2 * d, 0),
            )
        for d in beyond:
            z_copies[piece, -d] = remote(
                rs[piece][d - 1], pool[piece].at[pl.ds(r_base, cr)],
                r_send.at[piece, d - 1], r_recv.at[piece],
                jnp.maximum(me - 2 * d, 0),
            )
        x_copies.append(remote(xs[piece], xr[piece], x_send.at[piece], x_recv.at[piece], mate))
    def start_z(piece):
        for d in used:
            @pl.when(sends(d))
            def _(d=d):
                z_copies[piece, d].start()

    for piece in range(PIECES):
        own_part(piece)
        for n, d in enumerate(used):
            fill(zs[piece][n], mine[piece], table, d - 1, caps[d - 1])
        if piece > 0:
            start_z(piece - 1)
    start_z(PIECES - 1)

    def finish(piece):
        x_copies[piece].wait_recv()

        def one(j, carry):
            rows = pl.ds(pl.multiple_of(j * B, B), B)
            kind = table[x_row + 1, j]
            near, far = pool[piece][table[x_row + 2, j]], xr[piece][table[x_row + 3, j]]
            block = jnp.where(kind == 1, near, jnp.where(kind == 2, far, jnp.zeros_like(far)))
            out_ref[rows, piece * wide : (piece + 1) * wide] = block
            return carry

        lax.fori_loop(0, blk_dev, one, 0)

    for piece in range(PIECES):
        for d in used:
            @pl.when(gets(d))
            def _(d=d, piece=piece):
                z_copies[piece, d].wait_recv()

        @pl.when(plane == gate)
        def _(piece=piece):
            for d in beyond:
                fill(rs[piece][d - 1], pool[piece], table, planes - 2 + d, cr)
                z_copies[piece, -d].start()

        @pl.when(plane < gate)
        def _(piece=piece):
            if gate > 0:
                z_copies[piece, -1].wait_recv()

        fill(xs[piece], pool[piece], table, x_row, cx)
        x_copies[piece].start()
        if piece > 0:
            finish(piece - 1)
    finish(PIECES - 1)
    for piece in range(PIECES):
        x_copies[piece].wait_send()
        for d in used:
            @pl.when(sends(d))
            def _(d=d, piece=piece):
                z_copies[piece, d].wait_send()

        @pl.when(plane == gate)
        def _(piece=piece):
            for d in beyond:
                z_copies[piece, -d].wait_send()


def settled(count, number, caps, cr, cx, blk_dev, packs, blocks):
    tok, width = blocks.shape
    planes, wide = count // 2, width // PIECES
    smem = pl.BlockSpec(memory_space=pltpu.SMEM)
    vmem = pl.BlockSpec(memory_space=pltpu.VMEM)
    dma, dtype = pltpu.SemaphoreType.DMA, blocks.dtype
    sent = [caps[d - 1] for d in range(planes - 1, 0, -1) if caps[d - 1] > 0]

    def each(rows):
        return [pltpu.VMEM((rows, B, wide), dtype) for _ in range(PIECES)]

    return pl.pallas_call(
        functools.partial(settle_kernel, count, caps, cr, cx, blk_dev),
        out_shape=jax.ShapeDtypeStruct(blocks.shape, dtype),
        in_specs=[smem, vmem],
        out_specs=vmem,
        scratch_shapes=[
            each(blk_dev),
            [[pltpu.VMEM((c, B, wide), dtype) for c in sent] for _ in range(PIECES)],
            each(blk_dev + sum(caps) + cr),
            [[pltpu.VMEM((cr, B, wide), dtype) for _ in range(planes // 2 - 1)] for _ in range(PIECES)],
            each(cx),
            each(cx),
            dma((PIECES, len(sent))), dma((PIECES, len(sent))),
            dma((PIECES, planes // 2)), dma((PIECES,)), dma((PIECES,)), dma((PIECES,)),
        ],
        compiler_params=pltpu.CompilerParams(
            collective_id=number, has_side_effects=True,
            vmem_limit_bytes=60 * 1024 * 1024,
        ),
    )(packs, blocks)


def settle_levels(planes, blk_dev):
    def pad(first, second):
        return ((first, second) + (0,) * planes)[: planes - 1]

    half, few = blk_dev // 2, blk_dev * 3 // 4
    choices = [
        (2 * max(f + t, f + r) + r, pad(f, t), r, few)
        for f in range(half, few + 1)
        for t in range(half, few + 1)
        for r in (half // 2, half)
        if abs(f - t) < 2 or t == half
    ]
    choices = sorted(choices) + [
        (0, pad(half + 1, half + 1), few, few + 1),
        (0, pad(few + 1, half + 1), half // 2, few + 1),
        (0, ((few + 1, few) + (1,) * planes)[: planes - 1], few, few + 1),
        (0, (blk_dev,) * (planes - 1), blk_dev, blk_dev),
    ]
    return [limits for _, *limits in choices]


def pack(blocks, packs, level, count, blk_dev, first_id, choices):
    def run(number, *limits):
        return lambda *args: settled(count, first_id + number, *limits, blk_dev, *args)

    runs = [run(n, *limits) for n, limits in enumerate(choices)]
    return lax.switch(level, runs, packs, blocks)


CHUNK = 8


def near_far_kernel(
    blk_dev, keep_ref, live_ref, where_ref, used_ref,
    q_ref, k_ref, v_ref, hk_ref, hv_ref, gk_ref, gv_ref, rand_hbm, out_ref, rand_ref, sems,
):
    scale = 1.0 / math.sqrt(DH)
    head = pl.program_id(0)
    chunks = rand_hbm.shape[0] // CHUNK

    @pl.when(head == 0)
    def _():
        def copy(c):
            rows = pl.ds(c * CHUNK, CHUNK)
            return pltpu.make_async_copy(rand_hbm.at[rows], rand_ref.at[rows], sems.at[c])

        for c in range(chunks):
            pl.when(c * CHUNK < used_ref[0, 1])(lambda c=c: copy(c).start())
        for c in range(chunks):
            pl.when(c * CHUNK < used_ref[0, 1])(lambda c=c: copy(c).wait())

    def tile(ref, halo_ref, i):
        if i < 0:
            return halo_ref[0, :B]
        if i >= blk_dev:
            return halo_ref[0, B:]
        return ref[i * B : (i + 1) * B]

    def one(i):
        q = q_ref[i * B : (i + 1) * B]
        near = range(i - 1, i + 2)
        picks = [where_ref[head, i * R + r] for r in range(R)]
        k_parts = [
            jnp.concatenate([tile(k_ref, hk_ref, n) for n in near], axis=0),
            gk_ref[0],
            jnp.concatenate([rand_ref[p, :B] for p in picks], axis=0),
        ]
        v_parts = [
            jnp.concatenate([tile(v_ref, hv_ref, n) for n in near], axis=0),
            gv_ref[0],
            jnp.concatenate([rand_ref[p, B:] for p in picks], axis=0),
        ]
        scores = [
            lax.dot_general(
                q, k, (((1,), (1,)), ((), ())), preferred_element_type=jnp.float32
            )
            * scale
            for k in k_parts
        ]
        lanes = lax.broadcasted_iota(jnp.int32, scores[0].shape, 1)
        if i == 0:
            dead = jnp.logical_and(lanes < B, live_ref[0] == 0)
            scores[0] = jnp.where(dead, neg_big, scores[0])
        if i == blk_dev - 1:
            dead = jnp.logical_and(lanes >= 2 * B, live_ref[1] == 0)
            scores[0] = jnp.where(dead, neg_big, scores[0])
        peak = functools.reduce(
            jnp.maximum, [jnp.max(s, axis=-1, keepdims=True) for s in scores]
        )
        numer = jnp.zeros((B, DH), jnp.float32)
        denom = jnp.zeros((B, 1), jnp.float32)
        for s, v in zip(scores, v_parts):
            w = jnp.exp(s - peak).astype(jnp.bfloat16)
            denom = denom + jnp.sum(w.astype(jnp.float32), axis=-1, keepdims=True)
            numer = numer + jnp.dot(w, v, preferred_element_type=jnp.float32)
        out_ref[i * B : (i + 1) * B, :] = (numer / denom).astype(out_ref.dtype)

    for i in range(blk_dev):
        pl.when(keep_ref[i] > 0)(functools.partial(one, i))


def near_far(keep, live, where, used, q, k, v, halo_kv, glob, rand):
    tok_dev, width_dev = q.shape
    blk_dev, head_dev = tok_dev // B, width_dev // DH

    def column(rows):
        return pl.BlockSpec((rows, DH), lambda h, *_: (0, h))

    def part(rows, which):
        return pl.BlockSpec((1, rows, DH), lambda h, *_: (which, 0, h))

    return pl.pallas_call(
        functools.partial(near_far_kernel, blk_dev),
        out_shape=jax.ShapeDtypeStruct(q.shape, q.dtype),
        grid_spec=pltpu.PrefetchScalarGridSpec(
            num_scalar_prefetch=4,
            grid=(head_dev,),
            in_specs=[column(tok_dev)] * 3
            + [part(2 * B, 0), part(2 * B, 1), part(G * B, 0), part(G * B, 1)]
            + [pl.BlockSpec(memory_space=pl.ANY)],
            out_specs=column(tok_dev),
            scratch_shapes=[
                pltpu.VMEM(rand.shape, rand.dtype),
                pltpu.SemaphoreType.DMA((rand.shape[0] // CHUNK,)),
            ],
        ),
        compiler_params=ANYWHERE,
    )(keep, live, where, used, q, k, v, halo_kv, halo_kv, glob, glob, rand)


def quotient(x, n):
    return jnp.floor((x.astype(jnp.float32) + 0.5) * (1.0 / n)).astype(jnp.int32)


def plan_kernel(
    count, head_count, blk_dev, caps, choices, own_ref,
    tab_ref, where_ref, misc_ref, pack_ref,
    note_ref, need_ref, want_ref, slot_ref, both_ref, both_slot_ref,
    n_send, n_recv,
):
    i32, f32, bf16 = jnp.int32, jnp.float32, jnp.bfloat16
    planes = count // 2
    me, group = lax.axis_index("seq"), lax.axis_index("head")
    plane, side = me // 2, me % 2
    mate = me + 1 - 2 * side
    tall = own_ref.shape[0]
    everyone = count * head_count
    here_id = me * head_count + group
    barrier = pltpu.get_barrier_semaphore()

    def device(step):
        other = lax.rem(here_id + step, everyone)
        return {"seq": other // head_count, "head": lax.rem(other, head_count)}

    for step in range(1, everyone):
        pl.semaphore_signal(
            barrier, inc=1, device_id=device(step), device_id_type=pl.DeviceIdType.MESH
        )
    pl.semaphore_wait(barrier, everyone - 1)

    def remote(src, dst, send, recv, peer):
        return pltpu.make_async_remote_copy(
            src_ref=src, dst_ref=dst, send_sem=send, recv_sem=recv,
            device_id=peer, device_id_type=pl.DeviceIdType.MESH,
        )

    slot_rows = pl.ds(pl.multiple_of(here_id * tall, tall), tall)
    notices = [
        remote(
            own_ref, note_ref.at[slot_rows], n_send.at[step - 1], n_recv.at[step - 1], device(step)
        )
        for step in range(1, everyone)
    ]
    for c in notices:
        c.start()
    note_ref[slot_rows, :] = own_ref[...]

    for c in notices:
        c.wait_recv()

    rows, lanes = note_ref.shape[0], tab_ref.shape[1]
    head_dev = rows // (count * head_count)
    count_req = blk_dev * R
    blocks = count * blk_dev

    def iota(shape, axis):
        return lax.broadcasted_iota(i32, shape, axis)

    def dot(a, b):
        return jnp.dot(a.astype(bf16), b.astype(bf16), preferred_element_type=f32)

    def flag(x):
        return x.astype(f32)

    notes = note_ref[...]
    lane = iota((rows, lanes), 1)
    need = jnp.zeros((rows, lanes), f32)
    for e in range(count_req):
        need = jnp.where(notes[:, e : e + 1] == lane, 1.0, need)
    need_ref[...] = need

    wide_r, wide_c = iota((lanes, lanes), 0), iota((lanes, lanes), 1)
    own_r, own_c = quotient(wide_r, blk_dev), quotient(wide_c, blk_dev)
    same = flag(own_r == own_c)
    inside = flag((own_r == own_c) & (wide_r < wide_c))

    def by_head(x):
        return jnp.sum(x.reshape(-1, head_dev, lanes), axis=1)

    most_x = jnp.max(dot(by_head(need), same))
    span = head_count * head_dev
    pairs = need.reshape(planes, 2, span, lanes)
    union = jnp.maximum(pairs[:, 0], pairs[:, 1]).reshape(planes * span, lanes)
    union_count = dot(by_head(union), same)
    holder_plane = quotient(quotient(iota(union_count.shape, 1), blk_dev), 2)
    goal_plane = quotient(iota(union_count.shape, 0), head_count)
    most_z = jnp.max(jnp.where(holder_plane != goal_plane, union_count, 0.0))
    level = jnp.int32(0)
    cz, cx = jnp.int32(caps[0][0]), jnp.int32(caps[0][1])
    for n in range(1, len(caps)):
        over = (most_z > caps[n - 1][0]) | (most_x > caps[n - 1][1])
        level = jnp.where(over, n, level)
        cz = jnp.where(over, caps[n][0], cz)
        cx = jnp.where(over, caps[n][1], cx)

    for d in range(count):
        start = pl.multiple_of((d * head_count + group) * head_dev, head_dev)
        want_ref[d * head_dev : (d + 1) * head_dev, :] = need_ref[pl.ds(start, head_dev), :]
    want = want_ref[...]
    both = jnp.maximum(
        *[want.reshape(planes, 2, head_dev, lanes)[:, i] for i in range(2)]
    ).reshape(planes * head_dev, lanes)
    both_ref[...] = both

    def slots(x):
        tall = x.shape[0]
        r, c = iota((tall, tall), 0), iota((tall, tall), 1)
        above = flag((quotient(r, head_dev) == quotient(c, head_dev)) & (c < r))
        return dot(x, inside) + dot(above, dot(x, same))

    slot_ref[...] = slots(want)
    both_slot_ref[...] = slots(both)

    def head_rows(ref, i):
        return ref[pl.ds(pl.multiple_of(i * head_dev, head_dev), head_dev), :]

    def shifted(x, holder):
        return pltpu.roll(x, lax.rem(lanes - holder * blk_dev, lanes), 1)

    short = iota((head_dev, lanes), 1)
    first = iota((head_dev, 1), 0)

    def listed(flags, places, holder, worth):
        key = jnp.where(shifted(flags, holder) > 0, shifted(places, holder), -1.0).astype(i32)
        total = jnp.zeros((head_dev, lanes), f32)
        if worth is not None:
            worth = shifted(worth, holder)
        for b in range(blk_dev):
            value = (first * blk_dev + b).astype(f32) if worth is None else worth[:, b : b + 1]
            total = total + jnp.where(key[:, b : b + 1] == short, value, 0.0)
        return jnp.sum(total, axis=0, keepdims=True).astype(i32)

    tables = []
    for d in range(1, planes):
        goal = lax.rem(plane + d, planes)
        tables.append(listed(head_rows(both_ref, goal), head_rows(both_slot_ref, goal), me, None))
    here = head_rows(both_slot_ref, plane)
    for d in range(planes):
        source = lax.rem(plane - d + planes, planes) * 2 + side
        tables.append(
            listed(head_rows(want_ref, mate), head_rows(slot_ref, mate), source, here if d else None)
        )
    tables.append(listed(head_rows(want_ref, me), head_rows(slot_ref, me), me, None))
    tab_ref[...] = jnp.zeros(tab_ref.shape, i32)
    for n, row in enumerate(tables):
        tab_ref[n : n + 1, :] = row

    holder = quotient(short, blk_dev)
    h_plane = quotient(holder, 2)
    h_side = holder - 2 * h_plane
    gap = plane - h_plane
    gap = jnp.where(gap < 0, gap + planes, gap)
    x_base = (planes - 1) * cz
    by_z = (h_side == side) & (holder != me)
    start = jnp.where(
        by_z, (gap - 1) * cz, jnp.where(holder == me, x_base + planes * cx, x_base + gap * cx)
    )
    spot = start.astype(f32) + jnp.where(by_z, here, head_rows(slot_ref, me))
    mine = pl.multiple_of((me * head_count + group) * head_dev, head_dev)
    picks = note_ref[pl.ds(mine, head_dev), :]
    found = jnp.zeros((head_dev, lanes), f32)
    for e in range(count_req):
        value = jnp.sum(jnp.where(picks[:, e : e + 1] == short, spot, 0.0), axis=1, keepdims=True)
        found = jnp.where(short == e, value, found)
    where_ref[...] = found.astype(i32)

    grid_keep = note_ref[...].astype(f32)
    picked = jnp.zeros((count, grid_keep.shape[1]), f32)
    tall_r, tall_c = iota((count, rows), 0), iota((count, rows), 1)
    stride = head_count * head_dev
    picked = dot(flag(tall_c == tall_r * stride), jnp.clip(grid_keep, 0.0, 1.0))
    spread_r, spread_c = iota((picked.shape[1], lanes), 0), iota((picked.shape[1], lanes), 1)
    spread = flag(spread_r == count_req + spread_c - quotient(spread_c, blk_dev) * blk_dev)
    table = dot(picked, spread)
    row8, lane8 = iota((count, lanes), 0), iota((count, lanes), 1)
    kept_r = jnp.sum(jnp.where(quotient(lane8, blk_dev) == row8, table, 0.0), axis=0, keepdims=True)
    kept8 = jnp.broadcast_to(kept_r, (8, lanes))
    rank_r = dot(kept8, flag(wide_r < wide_c))[:1]

    sub, across = iota((blocks, lanes), 0), iota((blocks, lanes), 1)
    turn = sub == across

    def column(row):
        return jnp.sum(jnp.where(turn, row, 0.0), axis=1, keepdims=True)

    def facts(kept, rank, index):
        rank = rank.astype(i32)
        source, goal = quotient(index, blk_dev), quotient(rank, blk_dev)
        s_plane, g_plane = quotient(source, 2), quotient(goal, 2)
        gate = planes // 2 - 1
        relayed = (kept > 0) & (s_plane == gate + 1) & (g_plane < gate)
        far = jnp.where(relayed, 1, s_plane - g_plane)
        s_side, g_side = source - 2 * s_plane, goal - 2 * g_plane
        return kept > 0, rank, source, goal, g_plane, s_side, g_side, relayed, far

    index_r = iota((1, lanes), 1)
    index_c = iota((blocks, 1), 0)
    kr, _, sr, gr, pr, xr, yr, rr, fr = facts(kept_r, rank_r, index_r)
    kc, rank, sc, gc, pc, xc, yc, rc, fc = facts(column(kept_r), column(rank_r), index_c)
    earlier = across < sub

    def tally(hit):
        return jnp.sum(jnp.where(earlier & hit, 1.0, 0.0), axis=1, keepdims=True).astype(i32)

    by_z = tally((sc == sr) & (fc == fr) & kr)
    flow = (pc == pr) & (xc == xr)
    by_r = tally(flow & rr)
    by_x = tally(flow & kr & (xr != yr))
    crosses = kc & (xc != yc)
    gate = planes // 2 - 1

    def largest(hit, value):
        return jnp.max(jnp.where(hit, value + 1, 0).astype(f32))

    tops = [largest(kc & (fc == d), by_z) for d in range(1, planes)]
    top_r, top_x = largest(rc, by_r), largest(crosses, by_x)
    last = len(choices) - 1
    pick = jnp.int32(last)
    own = [jnp.int32(c) for c in choices[last][0]]
    for n in range(last - 1, -1, -1):
        limits, limit_r, limit_x = choices[n]
        ok = (top_r <= limit_r) & (top_x <= limit_x)
        for top, limit in zip(tops, limits):
            ok = ok & (top <= limit)
        pick = jnp.where(ok, n, pick)
        own = [jnp.where(ok, c, o) for c, o in zip(limits, own)]
    local = index_c - sc * blk_dev
    held = local
    base = jnp.int32(blk_dev)
    for d in range(1, planes):
        held = jnp.where(fc == d, base + by_z, held)
        base = base + own[d - 1]
    ahead = held
    held = jnp.where(rc, base + by_r, held)

    def rows_of(hit, places, worth):
        value = jnp.where(hit & (places == across), worth, 0).astype(f32)
        return jnp.sum(value, axis=0, keepdims=True).astype(i32)

    packs = [rows_of(kc & (fc == d) & (sc == me), by_z, local) for d in range(1, planes)]
    for d in range(1, max(gate, 1) + 1):
        packs.append(rows_of(rc & (xc == side) & (plane == gate) & (pc == gate - d), by_r, ahead))
    packs.append(rows_of(crosses & (pc == plane) & (xc == side), by_x, held))
    lands = kc & (gc == me)
    place = rank - gc * blk_dev
    straight = xc == side
    packs.append(rows_of(lands, place, jnp.where(straight, 1, 2)))
    packs.append(rows_of(lands & straight, place, held))
    packs.append(rows_of(lands & jnp.logical_not(straight), place, by_x))
    pack_ref[...] = jnp.zeros(pack_ref.shape, i32)
    for n, row in enumerate(packs):
        pack_ref[n : n + 1, :] = row

    used = x_base + (planes + 1) * cx
    spot8 = iota(misc_ref.shape, 1)
    misc_ref[...] = jnp.where(
        spot8 == 0, level, jnp.where(spot8 == 1, used, jnp.where(spot8 == 2, pick, 0))
    )

    for c in notices:
        c.wait_send()


def plan(note, count, head_count, blk_dev, caps, choices, number):
    head_dev = note.shape[0]
    everyone = count * head_count
    rows = everyone * head_dev
    planes = count // 2
    lanes = max(128, count * blk_dev)
    i32, f32 = jnp.int32, jnp.float32
    tabs = -(-2 * planes // 8) * 8
    packs = -(-(planes + max(planes // 2 - 1, 1) + 3) // 8) * 8
    shape, dma = jax.ShapeDtypeStruct, pltpu.SemaphoreType.DMA
    vmem = pl.BlockSpec(memory_space=pltpu.VMEM)
    return pl.pallas_call(
        functools.partial(plan_kernel, count, head_count, blk_dev, caps, choices),
        out_shape=(
            shape((tabs, lanes), i32), shape((head_dev, lanes), i32),
            shape((8, lanes), i32), shape((packs, lanes), i32),
        ),
        in_specs=[vmem],
        out_specs=(vmem,) * 4,
        scratch_shapes=[
            pltpu.VMEM((rows, note.shape[1]), i32),
            pltpu.VMEM((rows, lanes), f32),
            pltpu.VMEM((count * head_dev, lanes), f32), pltpu.VMEM((count * head_dev, lanes), f32),
            pltpu.VMEM((planes * head_dev, lanes), f32), pltpu.VMEM((planes * head_dev, lanes), f32),
            dma((everyone - 1,)), dma((everyone - 1,)),
        ],
        compiler_params=pltpu.CompilerParams(
            collective_id=number, has_side_effects=True,
            vmem_limit_bytes=60 * 1024 * 1024,
        ),
    )(note)


def levels(tiles, most):
    caps = []
    for part in (22, 24, 26, 28, 29, 30, 32, 36):
        cz = min(tiles, tiles * part // 64)
        caps.append((cz, min(most, max(1, most * min(24, part // 2 + 7) // 24))))
    caps.append((tiles, most))
    return sorted(set(caps))


def body(queries, keys, values, random_holder, random_offset, keep):
    tok_dev, width_dev = queries.shape
    blk_dev = tok_dev // B
    head_dev = width_dev // DH
    count = lax.axis_size("seq")
    head_count = lax.axis_size("head")
    count_req = blk_dev * R
    total = head_dev * count_req
    tiles = head_dev * blk_dev
    most = min(tiles, head_dev * max(2, (count_req + count - 1) // count))
    planes = count // 2
    if count % 2 or planes % 2 or not fits(planes, tiles, most):
        return plain_body(queries, keys, values, random_holder, random_offset, keep)
    me = lax.axis_index("seq")
    plane, side = me // 2, me % 2
    mate = me + 1 - 2 * side
    i32 = jnp.int32
    code = random_holder * blk_dev + random_offset
    code = jnp.where((keep > 0)[None, :, None], code, -1).reshape(head_dev, count_req)
    wide = -(-(count_req + blk_dev) // 128) * 128
    note = jnp.concatenate([code, jnp.broadcast_to(keep[None], (head_dev, blk_dev))], axis=1)
    note = jnp.pad(note, ((0, 0), (0, wide - count_req - blk_dev)), constant_values=-1)
    caps, choices = levels(tiles, most), settle_levels(planes, blk_dev)
    tab, where, misc, packs = plan(
        note, count, head_count, blk_dev, caps, choices, len(caps) + len(choices)
    )

    slots_all = -(-max((planes - 1) * c[0] + (planes + 1) * c[1] for c in caps) // CHUNK) * CHUNK
    def exchanged(number, caps):
        def run(tab, k, v):
            return exchange(count, number, *caps, slots_all, blk_dev, tab, k, v)

        return run

    rand, halo_kv, glob = lax.switch(
        misc[0, 0], [exchanged(n, c) for n, c in enumerate(caps)], tab, keys, values
    )

    live = jnp.stack([me > 0, me < count - 1]).astype(i32)
    blocks = near_far(
        keep, live, where, misc, queries, keys, values, halo_kv, glob, rand
    )
    return pack(blocks, packs, misc[0, 2], count, blk_dev, len(caps), choices)


def solution(mesh):
    in_specs = (
        P("seq", "head"),
        P("seq", "head"),
        P("seq", "head"),
        P("head", "seq", None),
        P("head", "seq", None),
        P("seq"),
    )
    out_specs = P("seq", "head")
    return jax.shard_map(body, mesh=mesh, in_specs=in_specs, out_specs=out_specs, check_vma=False)
```

```python
import functools
import math

import jax
import jax.numpy as jnp
from jax import lax
from jax.experimental import pallas as pl
from jax.experimental.pallas import tpu as pltpu
from jax.sharding import PartitionSpec as P

DH = 128
B = 128
G = 2
R = 3

neg_big = -1e30
ANYWHERE = pltpu.CompilerParams(
    dimension_semantics=("arbitrary",), vmem_limit_bytes=60 * 1024 * 1024
)


def halo(block, axis, width):
    count = lax.axis_size(axis)
    forward = [(i, i + 1) for i in range(count - 1)]
    backward = [(target, source) for source, target in forward]
    low = lax.ppermute(block[-width:], axis, forward)
    high = lax.ppermute(block[:width], axis, backward)
    return jnp.concatenate([low, high], axis=0)


def broadcast(block, axis, source):
    block = jnp.where(lax.axis_index(axis) == source, block, jnp.zeros_like(block))
    return lax.psum(block, axis)


def pick_kernel(cap, head_ref, block_ref, k_ref, v_ref, out_ref):
    dest = pl.program_id(0)

    @pl.loop(0, cap)
    def _(j):
        rows = pl.ds(pl.multiple_of(block_ref[dest, j] * B, B), B)
        cols = pl.ds(pl.multiple_of(head_ref[dest, j] * DH, DH), DH)
        out_ref[j, 0] = k_ref[rows, cols]
        out_ref[j, 1] = v_ref[rows, cols]


def pick(keys, values, heads, blocks, seq_count, cap):
    whole = pl.BlockSpec(keys.shape, lambda d, *_: (0, 0))
    return pl.pallas_call(
        functools.partial(pick_kernel, cap),
        out_shape=jax.ShapeDtypeStruct((seq_count * cap, 2, B, DH), keys.dtype),
        grid_spec=pltpu.PrefetchScalarGridSpec(
            num_scalar_prefetch=2,
            grid=(seq_count,),
            in_specs=[whole, whole],
            out_specs=pl.BlockSpec((cap, 2, B, DH), lambda d, *_: (d, 0, 0, 0)),
        ),
        compiler_params=ANYWHERE,
    )(heads, blocks, keys, values)


def attend_kernel(
    blk_dev,
    keep_ref,
    slot_ref,
    live_ref,
    where_ref,
    q_ref,
    k_ref,
    v_ref,
    hk_ref,
    hv_ref,
    gk_ref,
    gv_ref,
    rand_ref,
    out_ref,
):
    scale = 1.0 / math.sqrt(DH)
    head = pl.program_id(0)
    out_ref[...] = jnp.zeros_like(out_ref)

    def tile(ref, halo_ref, i):
        if i < 0:
            return halo_ref[:B]
        if i >= blk_dev:
            return halo_ref[B:]
        return ref[i * B : (i + 1) * B]

    def one(i):
        q = q_ref[i * B : (i + 1) * B]
        near = range(i - 1, i + 2)
        picks = [where_ref[(head * blk_dev + i) * R + r] for r in range(R)]
        k_parts = [
            jnp.concatenate([tile(k_ref, hk_ref, n) for n in near], axis=0),
            gk_ref[...],
            jnp.concatenate([rand_ref[p, 0] for p in picks], axis=0),
        ]
        v_parts = [
            jnp.concatenate([tile(v_ref, hv_ref, n) for n in near], axis=0),
            gv_ref[...],
            jnp.concatenate([rand_ref[p, 1] for p in picks], axis=0),
        ]
        scores = [
            lax.dot_general(
                q, k, (((1,), (1,)), ((), ())), preferred_element_type=jnp.float32
            )
            * scale
            for k in k_parts
        ]
        lanes = lax.broadcasted_iota(jnp.int32, scores[0].shape, 1)
        if i == 0:
            dead = jnp.logical_and(lanes < B, live_ref[0] == 0)
            scores[0] = jnp.where(dead, neg_big, scores[0])
        if i == blk_dev - 1:
            dead = jnp.logical_and(lanes >= 2 * B, live_ref[1] == 0)
            scores[0] = jnp.where(dead, neg_big, scores[0])
        peak = functools.reduce(
            jnp.maximum, [jnp.max(s, axis=-1, keepdims=True) for s in scores]
        )
        numer = jnp.zeros((B, DH), jnp.float32)
        denom = jnp.zeros((B, 1), jnp.float32)
        for s, v in zip(scores, v_parts):
            w = jnp.exp(s - peak).astype(jnp.bfloat16)
            denom = denom + jnp.sum(w.astype(jnp.float32), axis=-1, keepdims=True)
            numer = numer + jnp.dot(w, v, preferred_element_type=jnp.float32)
        rows = pl.ds(pl.multiple_of(slot_ref[i] * B, B), B)
        out_ref[rows, :] = (numer / denom).astype(out_ref.dtype)

    for i in range(blk_dev):
        pl.when(keep_ref[i] > 0)(functools.partial(one, i))


def attend(keep, slot, live, where, q, k, v, hk, hv, gk, gv, rand):
    tok_dev, width_dev = q.shape
    blk_dev, head_dev = tok_dev // B, width_dev // DH

    def column(rows):
        return pl.BlockSpec((rows, DH), lambda h, *_: (0, h))

    return pl.pallas_call(
        functools.partial(attend_kernel, blk_dev),
        out_shape=jax.ShapeDtypeStruct(q.shape, q.dtype),
        grid_spec=pltpu.PrefetchScalarGridSpec(
            num_scalar_prefetch=4,
            grid=(head_dev,),
            in_specs=[column(tok_dev)] * 3
            + [column(2 * B)] * 2
            + [column(G * B)] * 2
            + [pl.BlockSpec(rand.shape, lambda h, *_: (0, 0, 0, 0))],
            out_specs=column(tok_dev),
        ),
        compiler_params=ANYWHERE,
    )(keep, slot, live, where, q, k, v, hk, hv, gk, gv, rand)


def copy_kernel(order_ref, in_ref, out_ref):
    out_ref[...] = in_ref[...]


def take_blocks(blocks, order, cap):
    width = blocks.shape[1]
    return pl.pallas_call(
        copy_kernel,
        out_shape=jax.ShapeDtypeStruct((cap * B, width), blocks.dtype),
        grid_spec=pltpu.PrefetchScalarGridSpec(
            num_scalar_prefetch=1,
            grid=(cap,),
            in_specs=[pl.BlockSpec((B, width), lambda j, order: (order[j], 0))],
            out_specs=pl.BlockSpec((B, width), lambda j, order: (j, 0)),
        ),
        compiler_params=ANYWHERE,
    )(order, blocks)


def merge_kernel(kind_ref, from_ref, old_ref, new_ref, out_ref):
    kind = kind_ref[pl.program_id(0)]

    @pl.when(kind == 0)
    def _():
        out_ref[...] = old_ref[...]

    @pl.when(kind == 1)
    def _():
        out_ref[...] = jnp.zeros_like(out_ref)

    @pl.when(kind == 2)
    def _():
        out_ref[...] = new_ref[...]


def merge_blocks(old, new, kind, place):
    tok_dev, width = old.shape
    return pl.pallas_call(
        merge_kernel,
        out_shape=jax.ShapeDtypeStruct(old.shape, old.dtype),
        grid_spec=pltpu.PrefetchScalarGridSpec(
            num_scalar_prefetch=2,
            grid=(tok_dev // B,),
            in_specs=[
                pl.BlockSpec((B, width), lambda j, kind, place: (j, 0)),
                pl.BlockSpec((B, width), lambda j, kind, place: (place[j], 0)),
            ],
            out_specs=pl.BlockSpec((B, width), lambda j, kind, place: (j, 0)),
        ),
        compiler_params=ANYWHERE,
    )(kind, place, old, new)


def exclusive(flags, axis):
    return jnp.cumsum(flags, axis=axis) - flags


def first_at_least(caps, amount):
    return jnp.sum((amount > jnp.asarray(caps, jnp.int32)).astype(jnp.int32))


def settle(blocks, keep_all, slot, source, distance, me, count, blk_dev):
    i32 = jnp.int32
    devices = jnp.arange(count, dtype=i32)
    slots = jnp.arange(blk_dev, dtype=i32)
    sizes = sorted({0, *range(blk_dev // 2, blk_dev - 1), blk_dev})
    for bit_pos in range((count - 1).bit_length()):
        stride = 2**bit_pos
        at = source - distance % stride
        moving = (keep_all > 0) & (distance // stride % 2 > 0)
        on_slot = ((slot[:, None] == slots) & moving[:, None]).astype(i32)
        on_device = (at[:, None] == devices).astype(i32)
        leaving = jnp.sum(on_device[:, :, None] * on_slot[:, None, :], axis=0)
        needed = jnp.max(jnp.sum(leaving, axis=1))
        nth = exclusive(leaving, 1)
        mine_out, mine_nth = leaving[me], nth[me]
        send = jnp.sum(
            mine_out[:, None] * (mine_nth[:, None] == slots).astype(i32) * slots[:, None], axis=0
        )
        far = jnp.minimum(me + stride, count - 1)
        comes = jnp.where(me + stride < count, leaving[far], 0)
        kind = jnp.where(comes > 0, 2, jnp.where(mine_out > 0, 1, 0)).astype(i32)
        place = jnp.where(comes > 0, nth[far], 0)
        all_pairs = [(i, i - stride) for i in range(stride, count)]
        split = count - stride // 2
        upper = [pair for pair in all_pairs if pair[0] >= split]
        halves = 2 * stride >= count and 0 < len(upper) < len(all_pairs)

        def shifting(cap, pairs, send=send, kind=kind, place=place):
            def run(blocks):
                if cap == 0:
                    return blocks
                moved = lax.ppermute(take_blocks(blocks, send, cap), "seq", pairs)
                return merge_blocks(blocks, moved, kind, jnp.minimum(place, cap - 1))

            return run

        which = first_at_least(sizes[:-1], needed)
        runs = [shifting(cap, all_pairs) for cap in sizes]
        if halves:
            runs += [shifting(cap, upper) for cap in sizes]
            lower = jnp.sum(leaving * (devices < split)[:, None].astype(i32))
            which = which + jnp.where(lower > 0, 0, len(sizes))
        blocks = lax.switch(which, runs, blocks)
    return blocks


def plain_body(queries, keys, values, random_holder, random_offset, keep):
    tok_dev, width_dev = queries.shape
    blk_dev = tok_dev // B
    head_dev = width_dev // DH
    seq_count = lax.axis_size("seq")
    head_count = lax.axis_size("head")
    me = lax.axis_index("seq")
    count_req = blk_dev * R
    total = head_dev * count_req
    i32 = jnp.int32

    code = random_holder * blk_dev + random_offset
    code = jnp.where((keep > 0)[None, :, None], code, -1).reshape(total)
    note = jnp.concatenate([code, keep])
    note = jnp.broadcast_to(note, (seq_count * head_count,) + note.shape)
    table = lax.all_to_all(note, ("seq", "head"), split_axis=0, concat_axis=0, tiled=True)
    table = table.reshape(seq_count, head_count, total + blk_dev)
    keep_all = table[:, 0, total:].reshape(seq_count * blk_dev)
    codes = table[:, :, :total]
    devices = jnp.arange(seq_count, dtype=i32)

    halo_k, halo_v = halo(keys, "seq", B), halo(values, "seq", B)

    named = jnp.where(codes >= 0, codes // blk_dev, -1)
    counts = jnp.sum((named[..., None] == devices).astype(i32), axis=2)
    most = jnp.max(counts)
    onehot = (named[me, lax.axis_index("head")][:, None] == devices).astype(i32)
    mine = exclusive(onehot, 0)
    my_slot = jnp.sum(mine * onehot, axis=1)
    my_holder = jnp.sum(onehot * devices, axis=1)

    group = codes[:, lax.axis_index("head")]
    asks = (named[:, lax.axis_index("head")] == me).astype(i32)
    order = exclusive(asks, 1)
    full = min(total, head_dev * max(2, (count_req + seq_count - 1) // seq_count))
    chosen = asks[..., None] * (order[..., None] == jnp.arange(full, dtype=i32)).astype(i32)
    ask_head = jnp.arange(total, dtype=i32) // count_req
    ask = jnp.where(group >= 0, group % blk_dev, 0) + ask_head[None] * blk_dev
    ask = jnp.sum(chosen * ask[..., None], axis=1)
    pick_head, pick_block = ask // blk_dev, ask % blk_dev

    rank = exclusive(keep_all, 0)
    slot = rank % blk_dev
    source = jnp.arange(seq_count * blk_dev, dtype=i32) // blk_dev
    distance = jnp.where(keep_all > 0, source - rank // blk_dev, 0)
    my_slots = lax.dynamic_slice_in_dim(slot, me * blk_dev, blk_dev)
    live = jnp.stack([me > 0, me < seq_count - 1]).astype(i32)

    caps = sorted({max(1, full * part // 12) for part in range(8, 13)})

    def gathered(cap):
        def run(q, k, v, hk, hv):
            gk, gv = broadcast(jnp.stack((k[: G * B], v[: G * B])), "seq", 0)
            picked = pick(k, v, pick_head, pick_block, seq_count, cap)
            replies = lax.all_to_all(picked, "seq", split_axis=0, concat_axis=0, tiled=True)
            where = jnp.minimum(my_holder * cap + my_slot, seq_count * cap - 1)
            return attend(keep, my_slots, live, where, q, k, v, hk, hv, gk, gv, replies)

        return run

    blocks = lax.switch(
        first_at_least(caps[:-1], most),
        [gathered(cap) for cap in caps],
        queries, keys, values, halo_k, halo_v,
    )

    return settle(blocks, keep_all, slot, source, distance, me, seq_count, blk_dev)


TILE = (2 * B, DH)
SMALL = pltpu.CompilerParams(vmem_limit_bytes=60 * 1024 * 1024)


def fits(planes, tiles, most):
    slots = 2 * (planes - 1) * tiles + 2 * planes * most + most
    return slots * 2 * B * DH * 2 <= 44 * 1024 * 1024


def exchange_kernel(
    count, cz, cx, blk_dev, tab, k_ref, v_ref,
    rand_ref, halo_ref, glob_ref, home, zs, zr, xs, own,
    z_send, z_recv, x_send, x_recv, h_send, h_recv, g_send, g_recv, l_sem,
):
    planes = count // 2
    me = lax.axis_index("seq")
    plane, side = me // 2, me % 2
    mate = plane * 2 + 1 - side
    tok = k_ref.shape[0]
    head_dev = k_ref.shape[1] // DH
    barrier = pltpu.get_barrier_semaphore()
    for step in range(1, count):
        peer = lax.rem(me + step, count)
        pl.semaphore_signal(
            barrier, inc=1, device_id={"seq": peer}, device_id_type=pl.DeviceIdType.MESH
        )
    pl.semaphore_wait(barrier, count - 1)

    def remote(src, dst, send, recv, peer):
        return pltpu.make_async_remote_copy(
            src_ref=src, dst_ref=dst, send_sem=send, recv_sem=recv,
            device_id={"seq": peer}, device_id_type=pl.DeviceIdType.MESH,
        )

    tables = (k_ref, v_ref)
    low, high = pl.ds(0, B), pl.ds(B, B)
    first, last = pl.ds(0, B), pl.ds(tok - B, B)
    after = jnp.minimum(me + 1, count - 1)
    before = jnp.maximum(me - 1, 0)
    ups = [
        remote(tables[i].at[last], halo_ref.at[i, low], h_send.at[i], h_recv.at[i], after)
        for i in range(2)
    ]
    downs = [
        remote(tables[i].at[first], halo_ref.at[i, high], h_send.at[2 + i], h_recv.at[2 + i], before)
        for i in range(2)
    ]
    local = [
        pltpu.make_async_copy(tables[i].at[pl.ds(0, G * B)], glob_ref.at[i], l_sem.at[i])
        for i in range(2)
    ]
    item = glob_ref.at[side]
    chain = remote(item, item, g_send.at[0], g_recv.at[0], jnp.minimum(me + 2, count - 1))
    swap = remote(item, item, g_send.at[1], g_recv.at[1], mate)
    extra = remote(glob_ref.at[1], glob_ref.at[1], g_send.at[2], g_recv.at[0], mate)

    @pl.when(me == 0)
    def _():
        for c in local:
            c.start()
        for c in local:
            c.wait()
        chain.start()
        extra.start()
        swap.start()

    def pass_on():
        @pl.when(me > 0)
        def _():
            chain.wait_recv()

            @pl.when(plane < planes - 1)
            def _():
                chain.start()

            @pl.when(me > 1)
            def _():
                swap.start()

    @pl.when(me < count - 1)
    def _():
        for c in ups:
            c.start()

    @pl.when(me > 0)
    def _():
        for c in downs:
            c.start()

    @pl.when(me == 0)
    def _():
        halo_ref[:, low, :] = jnp.zeros((2, B, k_ref.shape[1]), k_ref.dtype)

    @pl.when(me == count - 1)
    def _():
        halo_ref[:, high, :] = jnp.zeros((2, B, k_ref.shape[1]), k_ref.dtype)

    def load_home(block, carry):
        rows = pl.ds(pl.multiple_of(block * B, B), B)
        for h in range(head_dev):
            cols = slice(h * DH, (h + 1) * DH)
            home[h * blk_dev + block, low, :] = k_ref[rows, cols]
            home[h * blk_dev + block, high, :] = v_ref[rows, cols]
        return carry

    lax.fori_loop(0, blk_dev, load_home, 0)

    def from_slots(dst, src, table, row, cap):
        def one(j, carry):
            dst[j] = src[table[row, j]]
            return carry

        lax.fori_loop(0, cap, one, 0)

    deltas = range(1, planes)

    core = lax.axis_index("head") % 2
    half = planes // 2
    edges = (half - 1, half)

    def goals(q, c):
        way = -1 if c and q in edges else 1
        return sorted(deltas, key=lambda d: (way * abs((q + d) % planes - q), d))

    def arrival(q, d, c):
        source = (q - d) % planes
        if (source < half) == (q < half):
            return (0, abs(source - q))
        early = source in edges and (q in edges) != bool(c)
        return (1 if early else 2 if source not in edges else 3, d)

    def sources(q, c):
        return sorted(deltas, key=lambda d: arrival(q, d, c))

    x_base = (planes - 1) * cz
    z_copies = {
        d: remote(
            zs[d - 1], zr[d - 1], z_send.at[d - 1], z_recv.at[d - 1],
            lax.rem(plane + d, planes) * 2 + side,
        )
        for d in deltas
    }
    x_copies = [
        remote(
            xs[d], rand_ref.at[pl.ds(x_base + d * cx, cx)],
            x_send.at[d], x_recv.at[d], mate,
        )
        for d in range(planes)
    ]
    for d in deltas:
        from_slots(zs[d - 1], home, tab, d - 1, cz)
    from_slots(xs[0], home, tab, planes - 1, cx)
    turns = [(q, c) for q in range(planes) for c in range(2)]
    for q, c in turns:
        @pl.when(jnp.logical_and(plane == q, core == c))
        def _(q=q, c=c):
            order = goals(q, c)
            for n, d in enumerate(order):
                z_copies[d].start()
                if n == 0 and q == 0:
                    pass_on()

    x_copies[0].start()
    from_slots(own, home, tab, 2 * planes - 1, cx)
    keep_own = pltpu.make_async_copy(
        own, rand_ref.at[pl.ds(x_base + planes * cx, cx)], l_sem.at[2]
    )
    keep_own.start()
    outs = {
        d: pltpu.make_async_copy(
            zr[d - 1], rand_ref.at[pl.ds((d - 1) * cz, cz)], l_sem.at[2 + d]
        )
        for d in deltas
    }

    def forward(d):
        z_copies[d].wait_recv()
        outs[d].start()
        from_slots(xs[d], zr[d - 1], tab, planes - 1 + d, cx)
        x_copies[d].start()

    for q, c in turns:
        @pl.when(jnp.logical_and(plane == q, core == c))
        def _(q=q, c=c):
            for n, d in enumerate(sources(q, c)):
                forward(d)
                if n == 0 and 0 < q < planes // 2:
                    pass_on()
            if q >= planes // 2:
                pass_on()

    @pl.when(me > 0)
    def _():
        swap.wait_recv()

    @pl.when(plane < planes - 1)
    def _():
        chain.wait_send()

    @pl.when(me == 0)
    def _():
        extra.wait_send()

    @pl.when(me != 1)
    def _():
        swap.wait_send()

    @pl.when(me < count - 1)
    def _():
        for c in ups:
            c.wait_send()
        for c in downs:
            c.wait_recv()

    @pl.when(me > 0)
    def _():
        for c in downs:
            c.wait_send()
        for c in ups:
            c.wait_recv()

    keep_own.wait()
    for d in deltas:
        outs[d].wait()
        z_copies[d].wait_send()
    for c in x_copies:
        c.wait()


def exchange(count, level, cz, cx, slots, blk_dev, tab, keys, values):
    planes = count // 2
    tok, width = keys.shape
    smem = pl.BlockSpec(memory_space=pltpu.SMEM)
    vmem = pl.BlockSpec(memory_space=pltpu.VMEM)
    dtype = keys.dtype
    dma = pltpu.SemaphoreType.DMA
    return pl.pallas_call(
        functools.partial(exchange_kernel, count, cz, cx, blk_dev),
        out_shape=(
            jax.ShapeDtypeStruct((slots, *TILE), dtype),
            jax.ShapeDtypeStruct((2, 2 * B, width), dtype),
            jax.ShapeDtypeStruct((2, G * B, width), dtype),
        ),
        in_specs=[smem, vmem, vmem],
        out_specs=(pl.BlockSpec(memory_space=pl.ANY), vmem, vmem),
        scratch_shapes=[
            pltpu.VMEM((tok // B * (width // DH), *TILE), dtype),
            [pltpu.VMEM((cz, *TILE), dtype) for _ in range(planes - 1)],
            [pltpu.VMEM((cz, *TILE), dtype) for _ in range(planes - 1)],
            [pltpu.VMEM((cx, *TILE), dtype) for _ in range(planes)],
            pltpu.VMEM((cx, *TILE), dtype),
            dma((planes - 1,)), dma((planes - 1,)),
            dma((planes,)), dma((planes,)),
            dma((4,)), dma((4,)), dma((3,)), dma((2,)), dma((2 + planes,)),
        ],
        compiler_params=pltpu.CompilerParams(
            collective_id=level, has_side_effects=True,
            vmem_limit_bytes=60 * 1024 * 1024,
        ),
    )(tab, keys, values)


PIECES = 8


def settle_kernel(
    count, caps, cr, cx, blk_dev, table, in_ref, out_ref,
    mine, zs, pool, rs, xs, xr, z_send, z_recv, r_send, r_recv, x_send, x_recv,
):
    planes = count // 2
    me = lax.axis_index("seq")
    plane, side = me // 2, me % 2
    mate = plane * 2 + 1 - side
    wide = in_ref.shape[1] // PIECES
    barrier = pltpu.get_barrier_semaphore()
    for step in range(1, count):
        peer = lax.rem(me + step, count)
        pl.semaphore_signal(
            barrier, inc=1, device_id={"seq": peer}, device_id_type=pl.DeviceIdType.MESH
        )
    pl.semaphore_wait(barrier, count - 1)

    def remote(src, dst, send, recv, peer):
        return pltpu.make_async_remote_copy(
            src_ref=src, dst_ref=dst, send_sem=send, recv_sem=recv,
            device_id={"seq": peer}, device_id_type=pl.DeviceIdType.MESH,
        )

    used = [d for d in range(1, planes) if caps[d - 1] > 0]
    used.sort(reverse=True)
    base = {d: blk_dev + sum(caps[: d - 1]) for d in used}
    gate = planes // 2 - 1
    beyond = range(1, gate + 1)
    r_base = blk_dev + sum(caps)
    x_row = planes - 1 + max(gate, 1)

    def sends(d):
        return jnp.logical_and(plane >= d, jnp.logical_or(plane != gate + 1, d == 1))

    def gets(d):
        return jnp.logical_and(plane + d < planes, jnp.logical_or(plane + d != gate + 1, d == 1))

    def fill(dst, src, table, row, cap):
        def one(j, carry):
            dst[j] = src[table[row, j]]
            return carry

        lax.fori_loop(0, cap, one, 0)

    def own_part(piece):
        def one(j, carry):
            rows = pl.ds(pl.multiple_of(j * B, B), B)
            block = in_ref[rows, piece * wide : (piece + 1) * wide]
            mine[piece][j] = block
            pool[piece][j] = block
            return carry

        lax.fori_loop(0, blk_dev, one, 0)

    z_copies, x_copies = {}, []
    for piece in range(PIECES):
        for n, d in enumerate(used):
            z_copies[piece, d] = remote(
                zs[piece][n], pool[piece].at[pl.ds(base[d], caps[d - 1])],
                z_send.at[piece, n], z_recv.at[piece, n],
                jnp.maximum(me - 2 * d, 0),
            )
        for d in beyond:
            z_copies[piece, -d] = remote(
                rs[piece][d - 1], pool[piece].at[pl.ds(r_base, cr)],
                r_send.at[piece, d - 1], r_recv.at[piece],
                jnp.maximum(me - 2 * d, 0),
            )
        x_copies.append(remote(xs[piece], xr[piece], x_send.at[piece], x_recv.at[piece], mate))
    def start_z(piece):
        for d in used:
            @pl.when(sends(d))
            def _(d=d):
                z_copies[piece, d].start()

    for piece in range(PIECES):
        own_part(piece)
        for n, d in enumerate(used):
            fill(zs[piece][n], mine[piece], table, d - 1, caps[d - 1])
        start_z(piece)

    def finish(piece):
        x_copies[piece].wait_recv()

        def one(j, carry):
            rows = pl.ds(pl.multiple_of(j * B, B), B)
            kind = table[x_row + 1, j]
            near, far = pool[piece][table[x_row + 2, j]], xr[piece][table[x_row + 3, j]]
            block = jnp.where(kind == 1, near, jnp.where(kind == 2, far, jnp.zeros_like(far)))
            out_ref[rows, piece * wide : (piece + 1) * wide] = block
            return carry

        lax.fori_loop(0, blk_dev, one, 0)

    for piece in range(PIECES):
        for d in used:
            @pl.when(gets(d))
            def _(d=d, piece=piece):
                z_copies[piece, d].wait_recv()

        @pl.when(plane == gate)
        def _(piece=piece):
            for d in beyond:
                fill(rs[piece][d - 1], pool[piece], table, planes - 2 + d, cr)
                z_copies[piece, -d].start()

        @pl.when(plane < gate)
        def _(piece=piece):
            if gate > 0:
                z_copies[piece, -1].wait_recv()

        fill(xs[piece], pool[piece], table, x_row, cx)
        x_copies[piece].start()
        if piece > 0:
            finish(piece - 1)
    finish(PIECES - 1)
    for piece in range(PIECES):
        x_copies[piece].wait_send()
        for d in used:
            @pl.when(sends(d))
            def _(d=d, piece=piece):
                z_copies[piece, d].wait_send()

        @pl.when(plane == gate)
        def _(piece=piece):
            for d in beyond:
                z_copies[piece, -d].wait_send()


def settled(count, number, caps, cr, cx, blk_dev, packs, blocks):
    tok, width = blocks.shape
    planes, wide = count // 2, width // PIECES
    smem = pl.BlockSpec(memory_space=pltpu.SMEM)
    vmem = pl.BlockSpec(memory_space=pltpu.VMEM)
    dma, dtype = pltpu.SemaphoreType.DMA, blocks.dtype
    sent = [caps[d - 1] for d in range(planes - 1, 0, -1) if caps[d - 1] > 0]

    def each(rows):
        return [pltpu.VMEM((rows, B, wide), dtype) for _ in range(PIECES)]

    return pl.pallas_call(
        functools.partial(settle_kernel, count, caps, cr, cx, blk_dev),
        out_shape=jax.ShapeDtypeStruct(blocks.shape, dtype),
        in_specs=[smem, vmem],
        out_specs=vmem,
        scratch_shapes=[
            each(blk_dev),
            [[pltpu.VMEM((c, B, wide), dtype) for c in sent] for _ in range(PIECES)],
            each(blk_dev + sum(caps) + cr),
            [[pltpu.VMEM((cr, B, wide), dtype) for _ in range(planes // 2 - 1)] for _ in range(PIECES)],
            each(cx),
            each(cx),
            dma((PIECES, len(sent))), dma((PIECES, len(sent))),
            dma((PIECES, planes // 2)), dma((PIECES,)), dma((PIECES,)), dma((PIECES,)),
        ],
        compiler_params=pltpu.CompilerParams(
            collective_id=number, has_side_effects=True,
            vmem_limit_bytes=60 * 1024 * 1024,
        ),
    )(packs, blocks)


def settle_levels(planes, blk_dev):
    def pad(first, second):
        return ((first, second) + (0,) * planes)[: planes - 1]

    half, few = blk_dev // 2, blk_dev * 3 // 4
    choices = [
        (pad(half, half), half, few),
        (pad(half + 1, half), half // 2, few),
        (pad(half, half + 1), half, few),
        (pad(half + 1, half + 1), half, few),
        (pad(few, half), half // 2, few),
        (pad(few, few), half, few),
        (pad(half + 1, half + 1), few, few + 1),
        (pad(few + 1, half + 1), half // 2, few + 1),
        (((few + 1, few) + (1,) * planes)[: planes - 1], few, few + 1),
    ]
    return choices + [((blk_dev,) * (planes - 1), blk_dev, blk_dev)]


def pack(blocks, packs, level, count, blk_dev, first_id, choices):
    def run(number, *limits):
        return lambda *args: settled(count, first_id + number, *limits, blk_dev, *args)

    runs = [run(n, *limits) for n, limits in enumerate(choices)]
    return lax.switch(level, runs, packs, blocks)


CHUNK = 8


def near_far_kernel(
    blk_dev, keep_ref, live_ref, where_ref, used_ref,
    q_ref, k_ref, v_ref, hk_ref, hv_ref, gk_ref, gv_ref, rand_hbm, out_ref, rand_ref, sems,
):
    scale = 1.0 / math.sqrt(DH)
    head = pl.program_id(0)
    chunks = rand_hbm.shape[0] // CHUNK

    @pl.when(head == 0)
    def _():
        def copy(c):
            rows = pl.ds(c * CHUNK, CHUNK)
            return pltpu.make_async_copy(rand_hbm.at[rows], rand_ref.at[rows], sems.at[c])

        for c in range(chunks):
            pl.when(c * CHUNK < used_ref[0, 1])(lambda c=c: copy(c).start())
        for c in range(chunks):
            pl.when(c * CHUNK < used_ref[0, 1])(lambda c=c: copy(c).wait())

    def tile(ref, halo_ref, i):
        if i < 0:
            return halo_ref[0, :B]
        if i >= blk_dev:
            return halo_ref[0, B:]
        return ref[i * B : (i + 1) * B]

    def one(i):
        q = q_ref[i * B : (i + 1) * B]
        near = range(i - 1, i + 2)
        picks = [where_ref[head, i * R + r] for r in range(R)]
        k_parts = [
            jnp.concatenate([tile(k_ref, hk_ref, n) for n in near], axis=0),
            gk_ref[0],
            jnp.concatenate([rand_ref[p, :B] for p in picks], axis=0),
        ]
        v_parts = [
            jnp.concatenate([tile(v_ref, hv_ref, n) for n in near], axis=0),
            gv_ref[0],
            jnp.concatenate([rand_ref[p, B:] for p in picks], axis=0),
        ]
        scores = [
            lax.dot_general(
                q, k, (((1,), (1,)), ((), ())), preferred_element_type=jnp.float32
            )
            * scale
            for k in k_parts
        ]
        lanes = lax.broadcasted_iota(jnp.int32, scores[0].shape, 1)
        if i == 0:
            dead = jnp.logical_and(lanes < B, live_ref[0] == 0)
            scores[0] = jnp.where(dead, neg_big, scores[0])
        if i == blk_dev - 1:
            dead = jnp.logical_and(lanes >= 2 * B, live_ref[1] == 0)
            scores[0] = jnp.where(dead, neg_big, scores[0])
        peak = functools.reduce(
            jnp.maximum, [jnp.max(s, axis=-1, keepdims=True) for s in scores]
        )
        numer = jnp.zeros((B, DH), jnp.float32)
        denom = jnp.zeros((B, 1), jnp.float32)
        for s, v in zip(scores, v_parts):
            w = jnp.exp(s - peak).astype(jnp.bfloat16)
            denom = denom + jnp.sum(w.astype(jnp.float32), axis=-1, keepdims=True)
            numer = numer + jnp.dot(w, v, preferred_element_type=jnp.float32)
        out_ref[i * B : (i + 1) * B, :] = (numer / denom).astype(out_ref.dtype)

    for i in range(blk_dev):
        pl.when(keep_ref[i] > 0)(functools.partial(one, i))


def near_far(keep, live, where, used, q, k, v, halo_kv, glob, rand):
    tok_dev, width_dev = q.shape
    blk_dev, head_dev = tok_dev // B, width_dev // DH

    def column(rows):
        return pl.BlockSpec((rows, DH), lambda h, *_: (0, h))

    def part(rows, which):
        return pl.BlockSpec((1, rows, DH), lambda h, *_: (which, 0, h))

    return pl.pallas_call(
        functools.partial(near_far_kernel, blk_dev),
        out_shape=jax.ShapeDtypeStruct(q.shape, q.dtype),
        grid_spec=pltpu.PrefetchScalarGridSpec(
            num_scalar_prefetch=4,
            grid=(head_dev,),
            in_specs=[column(tok_dev)] * 3
            + [part(2 * B, 0), part(2 * B, 1), part(G * B, 0), part(G * B, 1)]
            + [pl.BlockSpec(memory_space=pl.ANY)],
            out_specs=column(tok_dev),
            scratch_shapes=[
                pltpu.VMEM(rand.shape, rand.dtype),
                pltpu.SemaphoreType.DMA((rand.shape[0] // CHUNK,)),
            ],
        ),
        compiler_params=ANYWHERE,
    )(keep, live, where, used, q, k, v, halo_kv, halo_kv, glob, glob, rand)


def quotient(x, n):
    return jnp.floor((x.astype(jnp.float32) + 0.5) * (1.0 / n)).astype(jnp.int32)


def plan_kernel(
    count, head_count, blk_dev, caps, choices, own_ref,
    tab_ref, where_ref, misc_ref, pack_ref,
    note_ref, need_ref, want_ref, slot_ref, both_ref, both_slot_ref,
    n_send, n_recv,
):
    i32, f32, bf16 = jnp.int32, jnp.float32, jnp.bfloat16
    planes = count // 2
    me, group = lax.axis_index("seq"), lax.axis_index("head")
    plane, side = me // 2, me % 2
    mate = me + 1 - 2 * side
    tall = own_ref.shape[0]
    everyone = count * head_count
    here_id = me * head_count + group
    barrier = pltpu.get_barrier_semaphore()

    def device(step):
        other = lax.rem(here_id + step, everyone)
        return {"seq": other // head_count, "head": lax.rem(other, head_count)}

    for step in range(1, everyone):
        pl.semaphore_signal(
            barrier, inc=1, device_id=device(step), device_id_type=pl.DeviceIdType.MESH
        )
    pl.semaphore_wait(barrier, everyone - 1)

    def remote(src, dst, send, recv, peer):
        return pltpu.make_async_remote_copy(
            src_ref=src, dst_ref=dst, send_sem=send, recv_sem=recv,
            device_id=peer, device_id_type=pl.DeviceIdType.MESH,
        )

    slot_rows = pl.ds(pl.multiple_of(here_id * tall, tall), tall)
    notices = [
        remote(
            own_ref, note_ref.at[slot_rows], n_send.at[step - 1], n_recv.at[step - 1], device(step)
        )
        for step in range(1, everyone)
    ]
    for c in notices:
        c.start()
    note_ref[slot_rows, :] = own_ref[...]

    for c in notices:
        c.wait_recv()

    rows, lanes = note_ref.shape[0], tab_ref.shape[1]
    head_dev = rows // (count * head_count)
    count_req = blk_dev * R
    blocks = count * blk_dev

    def iota(shape, axis):
        return lax.broadcasted_iota(i32, shape, axis)

    def dot(a, b):
        return jnp.dot(a.astype(bf16), b.astype(bf16), preferred_element_type=f32)

    def flag(x):
        return x.astype(f32)

    notes = note_ref[...]
    lane = iota((rows, lanes), 1)
    need = jnp.zeros((rows, lanes), f32)
    for e in range(count_req):
        need = jnp.where(notes[:, e : e + 1] == lane, 1.0, need)
    need_ref[...] = need

    wide_r, wide_c = iota((lanes, lanes), 0), iota((lanes, lanes), 1)
    own_r, own_c = quotient(wide_r, blk_dev), quotient(wide_c, blk_dev)
    same = flag(own_r == own_c)
    inside = flag((own_r == own_c) & (wide_r < wide_c))

    def by_head(x):
        return jnp.sum(x.reshape(-1, head_dev, lanes), axis=1)

    most_x = jnp.max(dot(by_head(need), same))
    span = head_count * head_dev
    pairs = need.reshape(planes, 2, span, lanes)
    union = jnp.maximum(pairs[:, 0], pairs[:, 1]).reshape(planes * span, lanes)
    union_count = dot(by_head(union), same)
    holder_plane = quotient(quotient(iota(union_count.shape, 1), blk_dev), 2)
    goal_plane = quotient(iota(union_count.shape, 0), head_count)
    most_z = jnp.max(jnp.where(holder_plane != goal_plane, union_count, 0.0))
    level = jnp.int32(0)
    cz, cx = jnp.int32(caps[0][0]), jnp.int32(caps[0][1])
    for n in range(1, len(caps)):
        over = (most_z > caps[n - 1][0]) | (most_x > caps[n - 1][1])
        level = jnp.where(over, n, level)
        cz = jnp.where(over, caps[n][0], cz)
        cx = jnp.where(over, caps[n][1], cx)

    for d in range(count):
        start = pl.multiple_of((d * head_count + group) * head_dev, head_dev)
        want_ref[d * head_dev : (d + 1) * head_dev, :] = need_ref[pl.ds(start, head_dev), :]
    want = want_ref[...]
    both = jnp.maximum(
        *[want.reshape(planes, 2, head_dev, lanes)[:, i] for i in range(2)]
    ).reshape(planes * head_dev, lanes)
    both_ref[...] = both

    def slots(x):
        tall = x.shape[0]
        r, c = iota((tall, tall), 0), iota((tall, tall), 1)
        above = flag((quotient(r, head_dev) == quotient(c, head_dev)) & (c < r))
        return dot(x, inside) + dot(above, dot(x, same))

    slot_ref[...] = slots(want)
    both_slot_ref[...] = slots(both)

    def head_rows(ref, i):
        return ref[pl.ds(pl.multiple_of(i * head_dev, head_dev), head_dev), :]

    def shifted(x, holder):
        return pltpu.roll(x, lax.rem(lanes - holder * blk_dev, lanes), 1)

    short = iota((head_dev, lanes), 1)
    first = iota((head_dev, 1), 0)

    def listed(flags, places, holder, worth):
        key = jnp.where(shifted(flags, holder) > 0, shifted(places, holder), -1.0).astype(i32)
        total = jnp.zeros((head_dev, lanes), f32)
        if worth is not None:
            worth = shifted(worth, holder)
        for b in range(blk_dev):
            value = (first * blk_dev + b).astype(f32) if worth is None else worth[:, b : b + 1]
            total = total + jnp.where(key[:, b : b + 1] == short, value, 0.0)
        return jnp.sum(total, axis=0, keepdims=True).astype(i32)

    tables = []
    for d in range(1, planes):
        goal = lax.rem(plane + d, planes)
        tables.append(listed(head_rows(both_ref, goal), head_rows(both_slot_ref, goal), me, None))
    here = head_rows(both_slot_ref, plane)
    for d in range(planes):
        source = lax.rem(plane - d + planes, planes) * 2 + side
        tables.append(
            listed(head_rows(want_ref, mate), head_rows(slot_ref, mate), source, here if d else None)
        )
    tables.append(listed(head_rows(want_ref, me), head_rows(slot_ref, me), me, None))
    tab_ref[...] = jnp.zeros(tab_ref.shape, i32)
    for n, row in enumerate(tables):
        tab_ref[n : n + 1, :] = row

    holder = quotient(short, blk_dev)
    h_plane = quotient(holder, 2)
    h_side = holder - 2 * h_plane
    gap = plane - h_plane
    gap = jnp.where(gap < 0, gap + planes, gap)
    x_base = (planes - 1) * cz
    by_z = (h_side == side) & (holder != me)
    start = jnp.where(
        by_z, (gap - 1) * cz, jnp.where(holder == me, x_base + planes * cx, x_base + gap * cx)
    )
    spot = start.astype(f32) + jnp.where(by_z, here, head_rows(slot_ref, me))
    mine = pl.multiple_of((me * head_count + group) * head_dev, head_dev)
    picks = note_ref[pl.ds(mine, head_dev), :]
    found = jnp.zeros((head_dev, lanes), f32)
    for e in range(count_req):
        value = jnp.sum(jnp.where(picks[:, e : e + 1] == short, spot, 0.0), axis=1, keepdims=True)
        found = jnp.where(short == e, value, found)
    where_ref[...] = found.astype(i32)

    grid_keep = note_ref[...].astype(f32)
    picked = jnp.zeros((count, grid_keep.shape[1]), f32)
    tall_r, tall_c = iota((count, rows), 0), iota((count, rows), 1)
    stride = head_count * head_dev
    picked = dot(flag(tall_c == tall_r * stride), jnp.clip(grid_keep, 0.0, 1.0))
    spread_r, spread_c = iota((picked.shape[1], lanes), 0), iota((picked.shape[1], lanes), 1)
    spread = flag(spread_r == count_req + spread_c - quotient(spread_c, blk_dev) * blk_dev)
    table = dot(picked, spread)
    row8, lane8 = iota((count, lanes), 0), iota((count, lanes), 1)
    kept_r = jnp.sum(jnp.where(quotient(lane8, blk_dev) == row8, table, 0.0), axis=0, keepdims=True)
    kept8 = jnp.broadcast_to(kept_r, (8, lanes))
    rank_r = dot(kept8, flag(wide_r < wide_c))[:1]

    sub, across = iota((blocks, lanes), 0), iota((blocks, lanes), 1)
    turn = sub == across

    def column(row):
        return jnp.sum(jnp.where(turn, row, 0.0), axis=1, keepdims=True)

    def facts(kept, rank, index):
        rank = rank.astype(i32)
        source, goal = quotient(index, blk_dev), quotient(rank, blk_dev)
        s_plane, g_plane = quotient(source, 2), quotient(goal, 2)
        gate = planes // 2 - 1
        relayed = (kept > 0) & (s_plane == gate + 1) & (g_plane < gate)
        far = jnp.where(relayed, 1, s_plane - g_plane)
        s_side, g_side = source - 2 * s_plane, goal - 2 * g_plane
        return kept > 0, rank, source, goal, g_plane, s_side, g_side, relayed, far

    index_r = iota((1, lanes), 1)
    index_c = iota((blocks, 1), 0)
    kr, _, sr, gr, pr, xr, yr, rr, fr = facts(kept_r, rank_r, index_r)
    kc, rank, sc, gc, pc, xc, yc, rc, fc = facts(column(kept_r), column(rank_r), index_c)
    earlier = across < sub

    def tally(hit):
        return jnp.sum(jnp.where(earlier & hit, 1.0, 0.0), axis=1, keepdims=True).astype(i32)

    by_z = tally((sc == sr) & (fc == fr) & kr)
    flow = (pc == pr) & (xc == xr)
    by_r = tally(flow & rr)
    by_x = tally(flow & kr & (xr != yr))
    crosses = kc & (xc != yc)
    gate = planes // 2 - 1

    def largest(hit, value):
        return jnp.max(jnp.where(hit, value + 1, 0).astype(f32))

    tops = [largest(kc & (fc == d), by_z) for d in range(1, planes)]
    top_r, top_x = largest(rc, by_r), largest(crosses, by_x)
    last = len(choices) - 1
    pick = jnp.int32(last)
    own = [jnp.int32(c) for c in choices[last][0]]
    for n in range(last - 1, -1, -1):
        limits, limit_r, limit_x = choices[n]
        ok = (top_r <= limit_r) & (top_x <= limit_x)
        for top, limit in zip(tops, limits):
            ok = ok & (top <= limit)
        pick = jnp.where(ok, n, pick)
        own = [jnp.where(ok, c, o) for c, o in zip(limits, own)]
    local = index_c - sc * blk_dev
    held = local
    base = jnp.int32(blk_dev)
    for d in range(1, planes):
        held = jnp.where(fc == d, base + by_z, held)
        base = base + own[d - 1]
    ahead = held
    held = jnp.where(rc, base + by_r, held)

    def rows_of(hit, places, worth):
        value = jnp.where(hit & (places == across), worth, 0).astype(f32)
        return jnp.sum(value, axis=0, keepdims=True).astype(i32)

    packs = [rows_of(kc & (fc == d) & (sc == me), by_z, local) for d in range(1, planes)]
    for d in range(1, max(gate, 1) + 1):
        packs.append(rows_of(rc & (xc == side) & (plane == gate) & (pc == gate - d), by_r, ahead))
    packs.append(rows_of(crosses & (pc == plane) & (xc == side), by_x, held))
    lands = kc & (gc == me)
    place = rank - gc * blk_dev
    straight = xc == side
    packs.append(rows_of(lands, place, jnp.where(straight, 1, 2)))
    packs.append(rows_of(lands & straight, place, held))
    packs.append(rows_of(lands & jnp.logical_not(straight), place, by_x))
    pack_ref[...] = jnp.zeros(pack_ref.shape, i32)
    for n, row in enumerate(packs):
        pack_ref[n : n + 1, :] = row

    used = x_base + (planes + 1) * cx
    spot8 = iota(misc_ref.shape, 1)
    misc_ref[...] = jnp.where(
        spot8 == 0, level, jnp.where(spot8 == 1, used, jnp.where(spot8 == 2, pick, 0))
    )

    for c in notices:
        c.wait_send()


def plan(note, count, head_count, blk_dev, caps, choices, number):
    head_dev = note.shape[0]
    everyone = count * head_count
    rows = everyone * head_dev
    planes = count // 2
    lanes = max(128, count * blk_dev)
    i32, f32 = jnp.int32, jnp.float32
    tabs = -(-2 * planes // 8) * 8
    packs = -(-(planes + max(planes // 2 - 1, 1) + 3) // 8) * 8
    shape, dma = jax.ShapeDtypeStruct, pltpu.SemaphoreType.DMA
    vmem = pl.BlockSpec(memory_space=pltpu.VMEM)
    return pl.pallas_call(
        functools.partial(plan_kernel, count, head_count, blk_dev, caps, choices),
        out_shape=(
            shape((tabs, lanes), i32), shape((head_dev, lanes), i32),
            shape((8, lanes), i32), shape((packs, lanes), i32),
        ),
        in_specs=[vmem],
        out_specs=(vmem,) * 4,
        scratch_shapes=[
            pltpu.VMEM((rows, note.shape[1]), i32),
            pltpu.VMEM((rows, lanes), f32),
            pltpu.VMEM((count * head_dev, lanes), f32), pltpu.VMEM((count * head_dev, lanes), f32),
            pltpu.VMEM((planes * head_dev, lanes), f32), pltpu.VMEM((planes * head_dev, lanes), f32),
            dma((everyone - 1,)), dma((everyone - 1,)),
        ],
        compiler_params=pltpu.CompilerParams(
            collective_id=number, has_side_effects=True,
            vmem_limit_bytes=60 * 1024 * 1024,
        ),
    )(note)


def levels(tiles, most):
    caps = []
    for part in (22, 24, 26, 28, 29, 30, 32, 36):
        cz = min(tiles, tiles * part // 64)
        caps.append((cz, min(most, max(1, most * min(24, part // 2 + 7) // 24))))
    caps.append((tiles, most))
    return sorted(set(caps))


def body(queries, keys, values, random_holder, random_offset, keep):
    tok_dev, width_dev = queries.shape
    blk_dev = tok_dev // B
    head_dev = width_dev // DH
    count = lax.axis_size("seq")
    head_count = lax.axis_size("head")
    count_req = blk_dev * R
    total = head_dev * count_req
    tiles = head_dev * blk_dev
    most = min(tiles, head_dev * max(2, (count_req + count - 1) // count))
    planes = count // 2
    if count % 2 or planes % 2 or not fits(planes, tiles, most):
        return plain_body(queries, keys, values, random_holder, random_offset, keep)
    me = lax.axis_index("seq")
    plane, side = me // 2, me % 2
    mate = me + 1 - 2 * side
    i32 = jnp.int32
    code = random_holder * blk_dev + random_offset
    code = jnp.where((keep > 0)[None, :, None], code, -1).reshape(head_dev, count_req)
    wide = -(-(count_req + blk_dev) // 128) * 128
    note = jnp.concatenate([code, jnp.broadcast_to(keep[None], (head_dev, blk_dev))], axis=1)
    note = jnp.pad(note, ((0, 0), (0, wide - count_req - blk_dev)), constant_values=-1)
    caps, choices = levels(tiles, most), settle_levels(planes, blk_dev)
    tab, where, misc, packs = plan(
        note, count, head_count, blk_dev, caps, choices, len(caps) + len(choices)
    )

    slots_all = -(-max((planes - 1) * c[0] + (planes + 1) * c[1] for c in caps) // CHUNK) * CHUNK
    def exchanged(number, caps):
        def run(tab, k, v):
            return exchange(count, number, *caps, slots_all, blk_dev, tab, k, v)

        return run

    rand, halo_kv, glob = lax.switch(
        misc[0, 0], [exchanged(n, c) for n, c in enumerate(caps)], tab, keys, values
    )

    live = jnp.stack([me > 0, me < count - 1]).astype(i32)
    blocks = near_far(
        keep, live, where, misc, queries, keys, values, halo_kv, glob, rand
    )
    return pack(blocks, packs, misc[0, 2], count, blk_dev, len(caps), choices)


def solution(mesh):
    in_specs = (
        P("seq", "head"),
        P("seq", "head"),
        P("seq", "head"),
        P("head", "seq", None),
        P("head", "seq", None),
        P("seq"),
    )
    out_specs = P("seq", "head")
    return jax.shard_map(body, mesh=mesh, in_specs=in_specs, out_specs=out_specs, check_vma=False)
```

```python
import functools
import math

import jax
import jax.numpy as jnp
from jax import lax
from jax.experimental import pallas as pl
from jax.experimental.pallas import tpu as pltpu
from jax.sharding import PartitionSpec as P

DH = 128
B = 128
G = 2
R = 3

neg_big = -1e30
ANYWHERE = pltpu.CompilerParams(
    dimension_semantics=("arbitrary",), vmem_limit_bytes=60 * 1024 * 1024
)


def halo(block, axis, width):
    count = lax.axis_size(axis)
    forward = [(i, i + 1) for i in range(count - 1)]
    backward = [(target, source) for source, target in forward]
    low = lax.ppermute(block[-width:], axis, forward)
    high = lax.ppermute(block[:width], axis, backward)
    return jnp.concatenate([low, high], axis=0)


def broadcast(block, axis, source):
    block = jnp.where(lax.axis_index(axis) == source, block, jnp.zeros_like(block))
    return lax.psum(block, axis)


def pick_kernel(cap, head_ref, block_ref, k_ref, v_ref, out_ref):
    dest = pl.program_id(0)

    @pl.loop(0, cap)
    def _(j):
        rows = pl.ds(pl.multiple_of(block_ref[dest, j] * B, B), B)
        cols = pl.ds(pl.multiple_of(head_ref[dest, j] * DH, DH), DH)
        out_ref[j, 0] = k_ref[rows, cols]
        out_ref[j, 1] = v_ref[rows, cols]


def pick(keys, values, heads, blocks, seq_count, cap):
    whole = pl.BlockSpec(keys.shape, lambda d, *_: (0, 0))
    return pl.pallas_call(
        functools.partial(pick_kernel, cap),
        out_shape=jax.ShapeDtypeStruct((seq_count * cap, 2, B, DH), keys.dtype),
        grid_spec=pltpu.PrefetchScalarGridSpec(
            num_scalar_prefetch=2,
            grid=(seq_count,),
            in_specs=[whole, whole],
            out_specs=pl.BlockSpec((cap, 2, B, DH), lambda d, *_: (d, 0, 0, 0)),
        ),
        compiler_params=ANYWHERE,
    )(heads, blocks, keys, values)


def attend_kernel(
    blk_dev,
    keep_ref,
    slot_ref,
    live_ref,
    where_ref,
    q_ref,
    k_ref,
    v_ref,
    hk_ref,
    hv_ref,
    gk_ref,
    gv_ref,
    rand_ref,
    out_ref,
):
    scale = 1.0 / math.sqrt(DH)
    head = pl.program_id(0)
    out_ref[...] = jnp.zeros_like(out_ref)

    def tile(ref, halo_ref, i):
        if i < 0:
            return halo_ref[:B]
        if i >= blk_dev:
            return halo_ref[B:]
        return ref[i * B : (i + 1) * B]

    def one(i):
        q = q_ref[i * B : (i + 1) * B]
        near = range(i - 1, i + 2)
        picks = [where_ref[(head * blk_dev + i) * R + r] for r in range(R)]
        k_parts = [
            jnp.concatenate([tile(k_ref, hk_ref, n) for n in near], axis=0),
            gk_ref[...],
            jnp.concatenate([rand_ref[p, 0] for p in picks], axis=0),
        ]
        v_parts = [
            jnp.concatenate([tile(v_ref, hv_ref, n) for n in near], axis=0),
            gv_ref[...],
            jnp.concatenate([rand_ref[p, 1] for p in picks], axis=0),
        ]
        scores = [
            lax.dot_general(
                q, k, (((1,), (1,)), ((), ())), preferred_element_type=jnp.float32
            )
            * scale
            for k in k_parts
        ]
        lanes = lax.broadcasted_iota(jnp.int32, scores[0].shape, 1)
        if i == 0:
            dead = jnp.logical_and(lanes < B, live_ref[0] == 0)
            scores[0] = jnp.where(dead, neg_big, scores[0])
        if i == blk_dev - 1:
            dead = jnp.logical_and(lanes >= 2 * B, live_ref[1] == 0)
            scores[0] = jnp.where(dead, neg_big, scores[0])
        peak = functools.reduce(
            jnp.maximum, [jnp.max(s, axis=-1, keepdims=True) for s in scores]
        )
        numer = jnp.zeros((B, DH), jnp.float32)
        denom = jnp.zeros((B, 1), jnp.float32)
        for s, v in zip(scores, v_parts):
            w = jnp.exp(s - peak).astype(jnp.bfloat16)
            denom = denom + jnp.sum(w.astype(jnp.float32), axis=-1, keepdims=True)
            numer = numer + jnp.dot(w, v, preferred_element_type=jnp.float32)
        rows = pl.ds(pl.multiple_of(slot_ref[i] * B, B), B)
        out_ref[rows, :] = (numer / denom).astype(out_ref.dtype)

    for i in range(blk_dev):
        pl.when(keep_ref[i] > 0)(functools.partial(one, i))


def attend(keep, slot, live, where, q, k, v, hk, hv, gk, gv, rand):
    tok_dev, width_dev = q.shape
    blk_dev, head_dev = tok_dev // B, width_dev // DH

    def column(rows):
        return pl.BlockSpec((rows, DH), lambda h, *_: (0, h))

    return pl.pallas_call(
        functools.partial(attend_kernel, blk_dev),
        out_shape=jax.ShapeDtypeStruct(q.shape, q.dtype),
        grid_spec=pltpu.PrefetchScalarGridSpec(
            num_scalar_prefetch=4,
            grid=(head_dev,),
            in_specs=[column(tok_dev)] * 3
            + [column(2 * B)] * 2
            + [column(G * B)] * 2
            + [pl.BlockSpec(rand.shape, lambda h, *_: (0, 0, 0, 0))],
            out_specs=column(tok_dev),
        ),
        compiler_params=ANYWHERE,
    )(keep, slot, live, where, q, k, v, hk, hv, gk, gv, rand)


def copy_kernel(order_ref, in_ref, out_ref):
    out_ref[...] = in_ref[...]


def take_blocks(blocks, order, cap):
    width = blocks.shape[1]
    return pl.pallas_call(
        copy_kernel,
        out_shape=jax.ShapeDtypeStruct((cap * B, width), blocks.dtype),
        grid_spec=pltpu.PrefetchScalarGridSpec(
            num_scalar_prefetch=1,
            grid=(cap,),
            in_specs=[pl.BlockSpec((B, width), lambda j, order: (order[j], 0))],
            out_specs=pl.BlockSpec((B, width), lambda j, order: (j, 0)),
        ),
        compiler_params=ANYWHERE,
    )(order, blocks)


def merge_kernel(kind_ref, from_ref, old_ref, new_ref, out_ref):
    kind = kind_ref[pl.program_id(0)]

    @pl.when(kind == 0)
    def _():
        out_ref[...] = old_ref[...]

    @pl.when(kind == 1)
    def _():
        out_ref[...] = jnp.zeros_like(out_ref)

    @pl.when(kind == 2)
    def _():
        out_ref[...] = new_ref[...]


def merge_blocks(old, new, kind, place):
    tok_dev, width = old.shape
    return pl.pallas_call(
        merge_kernel,
        out_shape=jax.ShapeDtypeStruct(old.shape, old.dtype),
        grid_spec=pltpu.PrefetchScalarGridSpec(
            num_scalar_prefetch=2,
            grid=(tok_dev // B,),
            in_specs=[
                pl.BlockSpec((B, width), lambda j, kind, place: (j, 0)),
                pl.BlockSpec((B, width), lambda j, kind, place: (place[j], 0)),
            ],
            out_specs=pl.BlockSpec((B, width), lambda j, kind, place: (j, 0)),
        ),
        compiler_params=ANYWHERE,
    )(kind, place, old, new)


def exclusive(flags, axis):
    return jnp.cumsum(flags, axis=axis) - flags


def first_at_least(caps, amount):
    return jnp.sum((amount > jnp.asarray(caps, jnp.int32)).astype(jnp.int32))


def settle(blocks, keep_all, slot, source, distance, me, count, blk_dev):
    i32 = jnp.int32
    devices = jnp.arange(count, dtype=i32)
    slots = jnp.arange(blk_dev, dtype=i32)
    sizes = sorted({0, *range(blk_dev // 2, blk_dev - 1), blk_dev})
    for bit_pos in range((count - 1).bit_length()):
        stride = 2**bit_pos
        at = source - distance % stride
        moving = (keep_all > 0) & (distance // stride % 2 > 0)
        on_slot = ((slot[:, None] == slots) & moving[:, None]).astype(i32)
        on_device = (at[:, None] == devices).astype(i32)
        leaving = jnp.sum(on_device[:, :, None] * on_slot[:, None, :], axis=0)
        needed = jnp.max(jnp.sum(leaving, axis=1))
        nth = exclusive(leaving, 1)
        mine_out, mine_nth = leaving[me], nth[me]
        send = jnp.sum(
            mine_out[:, None] * (mine_nth[:, None] == slots).astype(i32) * slots[:, None], axis=0
        )
        far = jnp.minimum(me + stride, count - 1)
        comes = jnp.where(me + stride < count, leaving[far], 0)
        kind = jnp.where(comes > 0, 2, jnp.where(mine_out > 0, 1, 0)).astype(i32)
        place = jnp.where(comes > 0, nth[far], 0)
        all_pairs = [(i, i - stride) for i in range(stride, count)]
        split = count - stride // 2
        upper = [pair for pair in all_pairs if pair[0] >= split]
        halves = 2 * stride >= count and 0 < len(upper) < len(all_pairs)

        def shifting(cap, pairs, send=send, kind=kind, place=place):
            def run(blocks):
                if cap == 0:
                    return blocks
                moved = lax.ppermute(take_blocks(blocks, send, cap), "seq", pairs)
                return merge_blocks(blocks, moved, kind, jnp.minimum(place, cap - 1))

            return run

        which = first_at_least(sizes[:-1], needed)
        runs = [shifting(cap, all_pairs) for cap in sizes]
        if halves:
            runs += [shifting(cap, upper) for cap in sizes]
            lower = jnp.sum(leaving * (devices < split)[:, None].astype(i32))
            which = which + jnp.where(lower > 0, 0, len(sizes))
        blocks = lax.switch(which, runs, blocks)
    return blocks


def plain_body(queries, keys, values, random_holder, random_offset, keep):
    tok_dev, width_dev = queries.shape
    blk_dev = tok_dev // B
    head_dev = width_dev // DH
    seq_count = lax.axis_size("seq")
    head_count = lax.axis_size("head")
    me = lax.axis_index("seq")
    count_req = blk_dev * R
    total = head_dev * count_req
    i32 = jnp.int32

    code = random_holder * blk_dev + random_offset
    code = jnp.where((keep > 0)[None, :, None], code, -1).reshape(total)
    note = jnp.concatenate([code, keep])
    note = jnp.broadcast_to(note, (seq_count * head_count,) + note.shape)
    table = lax.all_to_all(note, ("seq", "head"), split_axis=0, concat_axis=0, tiled=True)
    table = table.reshape(seq_count, head_count, total + blk_dev)
    keep_all = table[:, 0, total:].reshape(seq_count * blk_dev)
    codes = table[:, :, :total]
    devices = jnp.arange(seq_count, dtype=i32)

    halo_k, halo_v = halo(keys, "seq", B), halo(values, "seq", B)

    named = jnp.where(codes >= 0, codes // blk_dev, -1)
    counts = jnp.sum((named[..., None] == devices).astype(i32), axis=2)
    most = jnp.max(counts)
    onehot = (named[me, lax.axis_index("head")][:, None] == devices).astype(i32)
    mine = exclusive(onehot, 0)
    my_slot = jnp.sum(mine * onehot, axis=1)
    my_holder = jnp.sum(onehot * devices, axis=1)

    group = codes[:, lax.axis_index("head")]
    asks = (named[:, lax.axis_index("head")] == me).astype(i32)
    order = exclusive(asks, 1)
    full = min(total, head_dev * max(2, (count_req + seq_count - 1) // seq_count))
    chosen = asks[..., None] * (order[..., None] == jnp.arange(full, dtype=i32)).astype(i32)
    ask_head = jnp.arange(total, dtype=i32) // count_req
    ask = jnp.where(group >= 0, group % blk_dev, 0) + ask_head[None] * blk_dev
    ask = jnp.sum(chosen * ask[..., None], axis=1)
    pick_head, pick_block = ask // blk_dev, ask % blk_dev

    rank = exclusive(keep_all, 0)
    slot = rank % blk_dev
    source = jnp.arange(seq_count * blk_dev, dtype=i32) // blk_dev
    distance = jnp.where(keep_all > 0, source - rank // blk_dev, 0)
    my_slots = lax.dynamic_slice_in_dim(slot, me * blk_dev, blk_dev)
    live = jnp.stack([me > 0, me < seq_count - 1]).astype(i32)

    caps = sorted({max(1, full * part // 12) for part in range(8, 13)})

    def gathered(cap):
        def run(q, k, v, hk, hv):
            gk, gv = broadcast(jnp.stack((k[: G * B], v[: G * B])), "seq", 0)
            picked = pick(k, v, pick_head, pick_block, seq_count, cap)
            replies = lax.all_to_all(picked, "seq", split_axis=0, concat_axis=0, tiled=True)
            where = jnp.minimum(my_holder * cap + my_slot, seq_count * cap - 1)
            return attend(keep, my_slots, live, where, q, k, v, hk, hv, gk, gv, replies)

        return run

    blocks = lax.switch(
        first_at_least(caps[:-1], most),
        [gathered(cap) for cap in caps],
        queries, keys, values, halo_k, halo_v,
    )

    return settle(blocks, keep_all, slot, source, distance, me, seq_count, blk_dev)


TILE = (2 * B, DH)
SMALL = pltpu.CompilerParams(vmem_limit_bytes=60 * 1024 * 1024)


def fits(planes, tiles, most):
    slots = 2 * (planes - 1) * tiles + 2 * planes * most + most
    return slots * 2 * B * DH * 2 <= 44 * 1024 * 1024


def exchange_kernel(
    count, cz, cx, blk_dev, tab, k_ref, v_ref,
    rand_ref, halo_ref, glob_ref, home, zs, zr, xs, own,
    z_send, z_recv, x_send, x_recv, h_send, h_recv, g_send, g_recv, l_sem,
):
    planes = count // 2
    me = lax.axis_index("seq")
    plane, side = me // 2, me % 2
    mate = plane * 2 + 1 - side
    tok = k_ref.shape[0]
    head_dev = k_ref.shape[1] // DH
    barrier = pltpu.get_barrier_semaphore()
    for step in range(1, count):
        peer = lax.rem(me + step, count)
        pl.semaphore_signal(
            barrier, inc=1, device_id={"seq": peer}, device_id_type=pl.DeviceIdType.MESH
        )
    pl.semaphore_wait(barrier, count - 1)

    def remote(src, dst, send, recv, peer):
        return pltpu.make_async_remote_copy(
            src_ref=src, dst_ref=dst, send_sem=send, recv_sem=recv,
            device_id={"seq": peer}, device_id_type=pl.DeviceIdType.MESH,
        )

    tables = (k_ref, v_ref)
    low, high = pl.ds(0, B), pl.ds(B, B)
    first, last = pl.ds(0, B), pl.ds(tok - B, B)
    after = jnp.minimum(me + 1, count - 1)
    before = jnp.maximum(me - 1, 0)
    ups = [
        remote(tables[i].at[last], halo_ref.at[i, low], h_send.at[i], h_recv.at[i], after)
        for i in range(2)
    ]
    downs = [
        remote(tables[i].at[first], halo_ref.at[i, high], h_send.at[2 + i], h_recv.at[2 + i], before)
        for i in range(2)
    ]
    local = [
        pltpu.make_async_copy(tables[i].at[pl.ds(0, G * B)], glob_ref.at[i], l_sem.at[i])
        for i in range(2)
    ]
    item = glob_ref.at[side]
    chain = remote(item, item, g_send.at[0], g_recv.at[0], jnp.minimum(me + 2, count - 1))
    swap = remote(item, item, g_send.at[1], g_recv.at[1], mate)
    extra = remote(glob_ref.at[1], glob_ref.at[1], g_send.at[2], g_recv.at[0], mate)

    @pl.when(me == 0)
    def _():
        for c in local:
            c.start()
        for c in local:
            c.wait()
        chain.start()
        extra.start()
        swap.start()

    def pass_on():
        @pl.when(me > 0)
        def _():
            chain.wait_recv()

            @pl.when(plane < planes - 1)
            def _():
                chain.start()

            @pl.when(me > 1)
            def _():
                swap.start()

    @pl.when(me < count - 1)
    def _():
        for c in ups:
            c.start()

    @pl.when(me > 0)
    def _():
        for c in downs:
            c.start()

    @pl.when(me == 0)
    def _():
        halo_ref[:, low, :] = jnp.zeros((2, B, k_ref.shape[1]), k_ref.dtype)

    @pl.when(me == count - 1)
    def _():
        halo_ref[:, high, :] = jnp.zeros((2, B, k_ref.shape[1]), k_ref.dtype)

    def load_home(block, carry):
        rows = pl.ds(pl.multiple_of(block * B, B), B)
        for h in range(head_dev):
            cols = slice(h * DH, (h + 1) * DH)
            home[h * blk_dev + block, low, :] = k_ref[rows, cols]
            home[h * blk_dev + block, high, :] = v_ref[rows, cols]
        return carry

    lax.fori_loop(0, blk_dev, load_home, 0)

    def from_slots(dst, src, table, row, cap):
        def one(j, carry):
            dst[j] = src[table[row, j]]
            return carry

        lax.fori_loop(0, cap, one, 0)

    deltas = range(1, planes)

    core = lax.axis_index("head") % 2
    half = planes // 2
    edges = (half - 1, half)

    def goals(q, c):
        way = -1 if c and q in edges else 1
        return sorted(deltas, key=lambda d: (way * abs((q + d) % planes - q), d))

    def arrival(q, d, c):
        source = (q - d) % planes
        if (source < half) == (q < half):
            return (0, abs(source - q))
        early = source in edges and (q in edges) != bool(c)
        return (1 if early else 2 if source not in edges else 3, d)

    def sources(q, c):
        return sorted(deltas, key=lambda d: arrival(q, d, c))

    x_base = (planes - 1) * cz
    z_copies = {
        d: remote(
            zs[d - 1], zr[d - 1], z_send.at[d - 1], z_recv.at[d - 1],
            lax.rem(plane + d, planes) * 2 + side,
        )
        for d in deltas
    }
    x_copies = [
        remote(
            xs[d], rand_ref.at[pl.ds(x_base + d * cx, cx)],
            x_send.at[d], x_recv.at[d], mate,
        )
        for d in range(planes)
    ]
    turns = [(q, c) for q in range(planes) for c in range(2)]
    for q, c in turns:
        @pl.when(jnp.logical_and(plane == q, core == c))
        def _(q=q, c=c):
            order = goals(q, c)
            for n, d in enumerate(order):
                from_slots(zs[d - 1], home, tab, d - 1, cz)
                if n == 1:
                    z_copies[order[0]].start()
                    if q == 0:
                        pass_on()
                if n > 1:
                    z_copies[order[n - 1]].start()
            from_slots(xs[0], home, tab, planes - 1, cx)
            z_copies[order[-1]].start()

    x_copies[0].start()
    from_slots(own, home, tab, 2 * planes - 1, cx)
    keep_own = pltpu.make_async_copy(
        own, rand_ref.at[pl.ds(x_base + planes * cx, cx)], l_sem.at[2]
    )
    keep_own.start()
    outs = {
        d: pltpu.make_async_copy(
            zr[d - 1], rand_ref.at[pl.ds((d - 1) * cz, cz)], l_sem.at[2 + d]
        )
        for d in deltas
    }

    def forward(d):
        z_copies[d].wait_recv()
        outs[d].start()
        from_slots(xs[d], zr[d - 1], tab, planes - 1 + d, cx)
        x_copies[d].start()

    for q, c in turns:
        @pl.when(jnp.logical_and(plane == q, core == c))
        def _(q=q, c=c):
            for n, d in enumerate(sources(q, c)):
                forward(d)
                if n == 0 and 0 < q < planes // 2:
                    pass_on()
            if q >= planes // 2:
                pass_on()

    @pl.when(me > 0)
    def _():
        swap.wait_recv()

    @pl.when(plane < planes - 1)
    def _():
        chain.wait_send()

    @pl.when(me == 0)
    def _():
        extra.wait_send()

    @pl.when(me != 1)
    def _():
        swap.wait_send()

    @pl.when(me < count - 1)
    def _():
        for c in ups:
            c.wait_send()
        for c in downs:
            c.wait_recv()

    @pl.when(me > 0)
    def _():
        for c in downs:
            c.wait_send()
        for c in ups:
            c.wait_recv()

    keep_own.wait()
    for d in deltas:
        outs[d].wait()
        z_copies[d].wait_send()
    for c in x_copies:
        c.wait()


def exchange(count, level, cz, cx, slots, blk_dev, tab, keys, values):
    planes = count // 2
    tok, width = keys.shape
    smem = pl.BlockSpec(memory_space=pltpu.SMEM)
    vmem = pl.BlockSpec(memory_space=pltpu.VMEM)
    dtype = keys.dtype
    dma = pltpu.SemaphoreType.DMA
    return pl.pallas_call(
        functools.partial(exchange_kernel, count, cz, cx, blk_dev),
        out_shape=(
            jax.ShapeDtypeStruct((slots, *TILE), dtype),
            jax.ShapeDtypeStruct((2, 2 * B, width), dtype),
            jax.ShapeDtypeStruct((2, G * B, width), dtype),
        ),
        in_specs=[smem, vmem, vmem],
        out_specs=(pl.BlockSpec(memory_space=pl.ANY), vmem, vmem),
        scratch_shapes=[
            pltpu.VMEM((tok // B * (width // DH), *TILE), dtype),
            [pltpu.VMEM((cz, *TILE), dtype) for _ in range(planes - 1)],
            [pltpu.VMEM((cz, *TILE), dtype) for _ in range(planes - 1)],
            [pltpu.VMEM((cx, *TILE), dtype) for _ in range(planes)],
            pltpu.VMEM((cx, *TILE), dtype),
            dma((planes - 1,)), dma((planes - 1,)),
            dma((planes,)), dma((planes,)),
            dma((4,)), dma((4,)), dma((3,)), dma((2,)), dma((2 + planes,)),
        ],
        compiler_params=pltpu.CompilerParams(
            collective_id=level, has_side_effects=True,
            vmem_limit_bytes=60 * 1024 * 1024,
        ),
    )(tab, keys, values)


PIECES = 8


def settle_kernel(
    count, caps, cr, cx, blk_dev, table, in_ref, out_ref,
    mine, zs, pool, rs, xs, xr, z_send, z_recv, r_send, r_recv, x_send, x_recv,
):
    planes = count // 2
    me = lax.axis_index("seq")
    plane, side = me // 2, me % 2
    mate = plane * 2 + 1 - side
    wide = in_ref.shape[1] // PIECES
    barrier = pltpu.get_barrier_semaphore()
    for step in range(1, count):
        peer = lax.rem(me + step, count)
        pl.semaphore_signal(
            barrier, inc=1, device_id={"seq": peer}, device_id_type=pl.DeviceIdType.MESH
        )
    pl.semaphore_wait(barrier, count - 1)

    def remote(src, dst, send, recv, peer):
        return pltpu.make_async_remote_copy(
            src_ref=src, dst_ref=dst, send_sem=send, recv_sem=recv,
            device_id={"seq": peer}, device_id_type=pl.DeviceIdType.MESH,
        )

    used = [d for d in range(1, planes) if caps[d - 1] > 0]
    used.sort(reverse=True)
    base = {d: blk_dev + sum(caps[: d - 1]) for d in used}
    gate = planes // 2 - 1
    beyond = range(1, gate + 1)
    r_base = blk_dev + sum(caps)
    x_row = planes - 1 + max(gate, 1)

    def sends(d):
        return jnp.logical_and(plane >= d, jnp.logical_or(plane != gate + 1, d == 1))

    def gets(d):
        return jnp.logical_and(plane + d < planes, jnp.logical_or(plane + d != gate + 1, d == 1))

    def fill(dst, src, table, row, cap):
        def one(j, carry):
            dst[j] = src[table[row, j]]
            return carry

        lax.fori_loop(0, cap, one, 0)

    def own_part(piece):
        def one(j, carry):
            rows = pl.ds(pl.multiple_of(j * B, B), B)
            block = in_ref[rows, piece * wide : (piece + 1) * wide]
            mine[piece][j] = block
            pool[piece][j] = block
            return carry

        lax.fori_loop(0, blk_dev, one, 0)

    z_copies, x_copies = {}, []
    for piece in range(PIECES):
        for n, d in enumerate(used):
            z_copies[piece, d] = remote(
                zs[piece][n], pool[piece].at[pl.ds(base[d], caps[d - 1])],
                z_send.at[piece, n], z_recv.at[piece, n],
                jnp.maximum(me - 2 * d, 0),
            )
        for d in beyond:
            z_copies[piece, -d] = remote(
                rs[piece][d - 1], pool[piece].at[pl.ds(r_base, cr)],
                r_send.at[piece, d - 1], r_recv.at[piece],
                jnp.maximum(me - 2 * d, 0),
            )
        x_copies.append(remote(xs[piece], xr[piece], x_send.at[piece], x_recv.at[piece], mate))
    def start_z(piece):
        for d in used:
            @pl.when(sends(d))
            def _(d=d):
                z_copies[piece, d].start()

    for piece in range(PIECES):
        own_part(piece)
        for n, d in enumerate(used):
            fill(zs[piece][n], mine[piece], table, d - 1, caps[d - 1])
        start_z(piece)

    def finish(piece):
        x_copies[piece].wait_recv()

        def one(j, carry):
            rows = pl.ds(pl.multiple_of(j * B, B), B)
            kind = table[x_row + 1, j]
            near, far = pool[piece][table[x_row + 2, j]], xr[piece][table[x_row + 3, j]]
            block = jnp.where(kind == 1, near, jnp.where(kind == 2, far, jnp.zeros_like(far)))
            out_ref[rows, piece * wide : (piece + 1) * wide] = block
            return carry

        lax.fori_loop(0, blk_dev, one, 0)

    for piece in range(PIECES):
        for d in used:
            @pl.when(gets(d))
            def _(d=d, piece=piece):
                z_copies[piece, d].wait_recv()

        @pl.when(plane == gate)
        def _(piece=piece):
            for d in beyond:
                fill(rs[piece][d - 1], pool[piece], table, planes - 2 + d, cr)
                z_copies[piece, -d].start()

        @pl.when(plane < gate)
        def _(piece=piece):
            if gate > 0:
                z_copies[piece, -1].wait_recv()

        fill(xs[piece], pool[piece], table, x_row, cx)
        x_copies[piece].start()
        if piece > 0:
            finish(piece - 1)
    finish(PIECES - 1)
    for piece in range(PIECES):
        x_copies[piece].wait_send()
        for d in used:
            @pl.when(sends(d))
            def _(d=d, piece=piece):
                z_copies[piece, d].wait_send()

        @pl.when(plane == gate)
        def _(piece=piece):
            for d in beyond:
                z_copies[piece, -d].wait_send()


def settled(count, number, caps, cr, cx, blk_dev, packs, blocks):
    tok, width = blocks.shape
    planes, wide = count // 2, width // PIECES
    smem = pl.BlockSpec(memory_space=pltpu.SMEM)
    vmem = pl.BlockSpec(memory_space=pltpu.VMEM)
    dma, dtype = pltpu.SemaphoreType.DMA, blocks.dtype
    sent = [caps[d - 1] for d in range(planes - 1, 0, -1) if caps[d - 1] > 0]

    def each(rows):
        return [pltpu.VMEM((rows, B, wide), dtype) for _ in range(PIECES)]

    return pl.pallas_call(
        functools.partial(settle_kernel, count, caps, cr, cx, blk_dev),
        out_shape=jax.ShapeDtypeStruct(blocks.shape, dtype),
        in_specs=[smem, vmem],
        out_specs=vmem,
        scratch_shapes=[
            each(blk_dev),
            [[pltpu.VMEM((c, B, wide), dtype) for c in sent] for _ in range(PIECES)],
            each(blk_dev + sum(caps) + cr),
            [[pltpu.VMEM((cr, B, wide), dtype) for _ in range(planes // 2 - 1)] for _ in range(PIECES)],
            each(cx),
            each(cx),
            dma((PIECES, len(sent))), dma((PIECES, len(sent))),
            dma((PIECES, planes // 2)), dma((PIECES,)), dma((PIECES,)), dma((PIECES,)),
        ],
        compiler_params=pltpu.CompilerParams(
            collective_id=number, has_side_effects=True,
            vmem_limit_bytes=60 * 1024 * 1024,
        ),
    )(packs, blocks)


def settle_levels(planes, blk_dev):
    def pad(first, second):
        return ((first, second) + (0,) * planes)[: planes - 1]

    half, few = blk_dev // 2, blk_dev * 3 // 4
    choices = [
        (pad(half, half), half, few),
        (pad(half + 1, half), half // 2, few),
        (pad(half, half + 1), half, few),
        (pad(half + 1, half + 1), half, few),
        (pad(few, half), half // 2, few),
        (pad(few, few), half, few),
        (pad(half + 1, half + 1), few, few + 1),
        (pad(few + 1, half + 1), half // 2, few + 1),
        (((few + 1, few) + (1,) * planes)[: planes - 1], few, few + 1),
    ]
    return choices + [((blk_dev,) * (planes - 1), blk_dev, blk_dev)]


def pack(blocks, packs, level, count, blk_dev, first_id, choices):
    def run(number, *limits):
        return lambda *args: settled(count, first_id + number, *limits, blk_dev, *args)

    runs = [run(n, *limits) for n, limits in enumerate(choices)]
    return lax.switch(level, runs, packs, blocks)


CHUNK = 8


def near_far_kernel(
    blk_dev, keep_ref, live_ref, where_ref,
    q_ref, k_ref, v_ref, hk_ref, hv_ref, gk_ref, gv_ref, rand_hbm, out_ref, held_ref, sems,
):
    scale = math.log2(math.e) / math.sqrt(DH)
    head = pl.program_id(0)
    now = lax.rem(head, 2)

    def fetches(which, half, i):
        return [
            pltpu.make_async_copy(
                rand_hbm.at[where_ref[which, i * R + r]],
                held_ref.at[half, i * R + r],
                sems.at[half, i * R + r],
            )
            for r in range(R)
        ]

    def ask(which, half):
        for i in range(blk_dev):
            @pl.when(keep_ref[i] > 0)
            def _(i=i):
                for c in fetches(which, half, i):
                    c.start()

    @pl.when(head == 0)
    def _():
        ask(head, now)

    @pl.when(head + 1 < pl.num_programs(0))
    def _():
        ask(head + 1, 1 - now)

    def tile(ref, halo_ref, i):
        if i < 0:
            return halo_ref[0, :B]
        if i >= blk_dev:
            return halo_ref[0, B:]
        return ref[i * B : (i + 1) * B]

    def one(i):
        q = q_ref[i * B : (i + 1) * B]
        near = range(i - 1, i + 2)
        for c in fetches(head, now, i):
            c.wait()
        picks = [i * R + r for r in range(R)]
        k_parts = [
            jnp.concatenate([tile(k_ref, hk_ref, n) for n in near], axis=0),
            gk_ref[0],
            jnp.concatenate([held_ref[now, p, :B] for p in picks], axis=0),
        ]
        v_parts = [
            jnp.concatenate([tile(v_ref, hv_ref, n) for n in near], axis=0),
            gv_ref[0],
            jnp.concatenate([held_ref[now, p, B:] for p in picks], axis=0),
        ]
        scores = [
            lax.dot_general(
                q, k, (((1,), (1,)), ((), ())), preferred_element_type=jnp.float32
            )
            for k in k_parts
        ]
        lanes = lax.broadcasted_iota(jnp.int32, scores[0].shape, 1)
        if i == 0:
            dead = jnp.logical_and(lanes < B, live_ref[0] == 0)
            scores[0] = jnp.where(dead, neg_big, scores[0])
        if i == blk_dev - 1:
            dead = jnp.logical_and(lanes >= 2 * B, live_ref[1] == 0)
            scores[0] = jnp.where(dead, neg_big, scores[0])
        peak = functools.reduce(
            jnp.maximum, [jnp.max(s, axis=-1, keepdims=True) for s in scores]
        )
        numer = jnp.zeros((B, DH), jnp.float32)
        denom = jnp.zeros((B, 1), jnp.float32)
        for s, v in zip(scores, v_parts):
            w = jnp.exp2((s - peak) * scale).astype(jnp.bfloat16)
            denom = denom + jnp.sum(w.astype(jnp.float32), axis=-1, keepdims=True)
            numer = numer + jnp.dot(w, v, preferred_element_type=jnp.float32)
        out_ref[i * B : (i + 1) * B, :] = (numer / denom).astype(out_ref.dtype)

    for i in range(blk_dev):
        pl.when(keep_ref[i] > 0)(functools.partial(one, i))


def near_far(keep, live, where, q, k, v, halo_kv, glob, rand):
    tok_dev, width_dev = q.shape
    blk_dev, head_dev = tok_dev // B, width_dev // DH

    def column(rows):
        return pl.BlockSpec((rows, DH), lambda h, *_: (0, h))

    def part(rows, which):
        return pl.BlockSpec((1, rows, DH), lambda h, *_: (which, 0, h))

    return pl.pallas_call(
        functools.partial(near_far_kernel, blk_dev),
        out_shape=jax.ShapeDtypeStruct(q.shape, q.dtype),
        grid_spec=pltpu.PrefetchScalarGridSpec(
            num_scalar_prefetch=3,
            grid=(head_dev,),
            in_specs=[column(tok_dev)] * 3
            + [part(2 * B, 0), part(2 * B, 1), part(G * B, 0), part(G * B, 1)]
            + [pl.BlockSpec(memory_space=pl.ANY)],
            out_specs=column(tok_dev),
            scratch_shapes=[
                pltpu.VMEM((2, blk_dev * R, *TILE), rand.dtype),
                pltpu.SemaphoreType.DMA((2, blk_dev * R)),
            ],
        ),
        compiler_params=ANYWHERE,
    )(keep, live, where, q, k, v, halo_kv, halo_kv, glob, glob, rand)


def quotient(x, n):
    return jnp.floor((x.astype(jnp.float32) + 0.5) * (1.0 / n)).astype(jnp.int32)


def plan_kernel(
    count, head_count, blk_dev, caps, choices, own_ref,
    tab_ref, where_ref, misc_ref, pack_ref,
    note_ref, need_ref, want_ref, slot_ref, both_ref, both_slot_ref,
    n_send, n_recv,
):
    i32, f32, bf16 = jnp.int32, jnp.float32, jnp.bfloat16
    planes = count // 2
    me, group = lax.axis_index("seq"), lax.axis_index("head")
    plane, side = me // 2, me % 2
    mate = me + 1 - 2 * side
    tall = own_ref.shape[0]
    everyone = count * head_count
    here_id = me * head_count + group
    barrier = pltpu.get_barrier_semaphore()

    def device(step):
        other = lax.rem(here_id + step, everyone)
        return {"seq": other // head_count, "head": lax.rem(other, head_count)}

    for step in range(1, everyone):
        pl.semaphore_signal(
            barrier, inc=1, device_id=device(step), device_id_type=pl.DeviceIdType.MESH
        )
    pl.semaphore_wait(barrier, everyone - 1)

    def remote(src, dst, send, recv, peer):
        return pltpu.make_async_remote_copy(
            src_ref=src, dst_ref=dst, send_sem=send, recv_sem=recv,
            device_id=peer, device_id_type=pl.DeviceIdType.MESH,
        )

    slot_rows = pl.ds(pl.multiple_of(here_id * tall, tall), tall)
    notices = [
        remote(
            own_ref, note_ref.at[slot_rows], n_send.at[step - 1], n_recv.at[step - 1], device(step)
        )
        for step in range(1, everyone)
    ]
    for c in notices:
        c.start()
    note_ref[slot_rows, :] = own_ref[...]

    for c in notices:
        c.wait_recv()

    rows, lanes = note_ref.shape[0], tab_ref.shape[1]
    head_dev = rows // (count * head_count)
    count_req = blk_dev * R
    blocks = count * blk_dev

    def iota(shape, axis):
        return lax.broadcasted_iota(i32, shape, axis)

    def dot(a, b):
        return jnp.dot(a.astype(bf16), b.astype(bf16), preferred_element_type=f32)

    def flag(x):
        return x.astype(f32)

    notes = note_ref[...]
    lane = iota((rows, lanes), 1)
    need = jnp.zeros((rows, lanes), f32)
    for e in range(count_req):
        need = jnp.where(notes[:, e : e + 1] == lane, 1.0, need)
    need_ref[...] = need

    wide_r, wide_c = iota((lanes, lanes), 0), iota((lanes, lanes), 1)
    own_r, own_c = quotient(wide_r, blk_dev), quotient(wide_c, blk_dev)
    same = flag(own_r == own_c)
    inside = flag((own_r == own_c) & (wide_r < wide_c))

    def by_head(x):
        return jnp.sum(x.reshape(-1, head_dev, lanes), axis=1)

    most_x = jnp.max(dot(by_head(need), same))
    span = head_count * head_dev
    pairs = need.reshape(planes, 2, span, lanes)
    union = jnp.maximum(pairs[:, 0], pairs[:, 1]).reshape(planes * span, lanes)
    union_count = dot(by_head(union), same)
    holder_plane = quotient(quotient(iota(union_count.shape, 1), blk_dev), 2)
    goal_plane = quotient(iota(union_count.shape, 0), head_count)
    most_z = jnp.max(jnp.where(holder_plane != goal_plane, union_count, 0.0))
    level = jnp.int32(0)
    cz, cx = jnp.int32(caps[0][0]), jnp.int32(caps[0][1])
    for n in range(1, len(caps)):
        over = (most_z > caps[n - 1][0]) | (most_x > caps[n - 1][1])
        level = jnp.where(over, n, level)
        cz = jnp.where(over, caps[n][0], cz)
        cx = jnp.where(over, caps[n][1], cx)

    for d in range(count):
        start = pl.multiple_of((d * head_count + group) * head_dev, head_dev)
        want_ref[d * head_dev : (d + 1) * head_dev, :] = need_ref[pl.ds(start, head_dev), :]
    want = want_ref[...]
    both = jnp.maximum(
        *[want.reshape(planes, 2, head_dev, lanes)[:, i] for i in range(2)]
    ).reshape(planes * head_dev, lanes)
    both_ref[...] = both

    def slots(x):
        tall = x.shape[0]
        r, c = iota((tall, tall), 0), iota((tall, tall), 1)
        above = flag((quotient(r, head_dev) == quotient(c, head_dev)) & (c < r))
        return dot(x, inside) + dot(above, dot(x, same))

    slot_ref[...] = slots(want)
    both_slot_ref[...] = slots(both)

    def head_rows(ref, i):
        return ref[pl.ds(pl.multiple_of(i * head_dev, head_dev), head_dev), :]

    def shifted(x, holder):
        return pltpu.roll(x, lax.rem(lanes - holder * blk_dev, lanes), 1)

    short = iota((head_dev, lanes), 1)
    first = iota((head_dev, 1), 0)

    def listed(flags, places, holder, worth):
        key = jnp.where(shifted(flags, holder) > 0, shifted(places, holder), -1.0).astype(i32)
        total = jnp.zeros((head_dev, lanes), f32)
        if worth is not None:
            worth = shifted(worth, holder)
        for b in range(blk_dev):
            value = (first * blk_dev + b).astype(f32) if worth is None else worth[:, b : b + 1]
            total = total + jnp.where(key[:, b : b + 1] == short, value, 0.0)
        return jnp.sum(total, axis=0, keepdims=True).astype(i32)

    tables = []
    for d in range(1, planes):
        goal = lax.rem(plane + d, planes)
        tables.append(listed(head_rows(both_ref, goal), head_rows(both_slot_ref, goal), me, None))
    here = head_rows(both_slot_ref, plane)
    for d in range(planes):
        source = lax.rem(plane - d + planes, planes) * 2 + side
        tables.append(
            listed(head_rows(want_ref, mate), head_rows(slot_ref, mate), source, here if d else None)
        )
    tables.append(listed(head_rows(want_ref, me), head_rows(slot_ref, me), me, None))
    tab_ref[...] = jnp.zeros(tab_ref.shape, i32)
    for n, row in enumerate(tables):
        tab_ref[n : n + 1, :] = row

    holder = quotient(short, blk_dev)
    h_plane = quotient(holder, 2)
    h_side = holder - 2 * h_plane
    gap = plane - h_plane
    gap = jnp.where(gap < 0, gap + planes, gap)
    x_base = (planes - 1) * cz
    by_z = (h_side == side) & (holder != me)
    start = jnp.where(
        by_z, (gap - 1) * cz, jnp.where(holder == me, x_base + planes * cx, x_base + gap * cx)
    )
    spot = start.astype(f32) + jnp.where(by_z, here, head_rows(slot_ref, me))
    mine = pl.multiple_of((me * head_count + group) * head_dev, head_dev)
    picks = note_ref[pl.ds(mine, head_dev), :]
    found = jnp.zeros((head_dev, lanes), f32)
    for e in range(count_req):
        value = jnp.sum(jnp.where(picks[:, e : e + 1] == short, spot, 0.0), axis=1, keepdims=True)
        found = jnp.where(short == e, value, found)
    where_ref[...] = found.astype(i32)

    grid_keep = note_ref[...].astype(f32)
    picked = jnp.zeros((count, grid_keep.shape[1]), f32)
    tall_r, tall_c = iota((count, rows), 0), iota((count, rows), 1)
    stride = head_count * head_dev
    picked = dot(flag(tall_c == tall_r * stride), jnp.clip(grid_keep, 0.0, 1.0))
    spread_r, spread_c = iota((picked.shape[1], lanes), 0), iota((picked.shape[1], lanes), 1)
    spread = flag(spread_r == count_req + spread_c - quotient(spread_c, blk_dev) * blk_dev)
    table = dot(picked, spread)
    row8, lane8 = iota((count, lanes), 0), iota((count, lanes), 1)
    kept_r = jnp.sum(jnp.where(quotient(lane8, blk_dev) == row8, table, 0.0), axis=0, keepdims=True)
    kept8 = jnp.broadcast_to(kept_r, (8, lanes))
    rank_r = dot(kept8, flag(wide_r < wide_c))[:1]

    sub, across = iota((blocks, lanes), 0), iota((blocks, lanes), 1)
    turn = sub == across

    def column(row):
        return jnp.sum(jnp.where(turn, row, 0.0), axis=1, keepdims=True)

    def facts(kept, rank, index):
        rank = rank.astype(i32)
        source, goal = quotient(index, blk_dev), quotient(rank, blk_dev)
        s_plane, g_plane = quotient(source, 2), quotient(goal, 2)
        gate = planes // 2 - 1
        relayed = (kept > 0) & (s_plane == gate + 1) & (g_plane < gate)
        far = jnp.where(relayed, 1, s_plane - g_plane)
        s_side, g_side = source - 2 * s_plane, goal - 2 * g_plane
        return kept > 0, rank, source, goal, g_plane, s_side, g_side, relayed, far

    index_r = iota((1, lanes), 1)
    index_c = iota((blocks, 1), 0)
    kr, _, sr, gr, pr, xr, yr, rr, fr = facts(kept_r, rank_r, index_r)
    kc, rank, sc, gc, pc, xc, yc, rc, fc = facts(column(kept_r), column(rank_r), index_c)
    earlier = across < sub

    def tally(hit):
        return jnp.sum(jnp.where(earlier & hit, 1.0, 0.0), axis=1, keepdims=True).astype(i32)

    by_z = tally((sc == sr) & (fc == fr) & kr)
    flow = (pc == pr) & (xc == xr)
    by_r = tally(flow & rr)
    by_x = tally(flow & kr & (xr != yr))
    crosses = kc & (xc != yc)
    gate = planes // 2 - 1

    def largest(hit, value):
        return jnp.max(jnp.where(hit, value + 1, 0).astype(f32))

    tops = [largest(kc & (fc == d), by_z) for d in range(1, planes)]
    top_r, top_x = largest(rc, by_r), largest(crosses, by_x)
    last = len(choices) - 1
    pick = jnp.int32(last)
    own = [jnp.int32(c) for c in choices[last][0]]
    for n in range(last - 1, -1, -1):
        limits, limit_r, limit_x = choices[n]
        ok = (top_r <= limit_r) & (top_x <= limit_x)
        for top, limit in zip(tops, limits):
            ok = ok & (top <= limit)
        pick = jnp.where(ok, n, pick)
        own = [jnp.where(ok, c, o) for c, o in zip(limits, own)]
    local = index_c - sc * blk_dev
    held = local
    base = jnp.int32(blk_dev)
    for d in range(1, planes):
        held = jnp.where(fc == d, base + by_z, held)
        base = base + own[d - 1]
    ahead = held
    held = jnp.where(rc, base + by_r, held)

    def rows_of(hit, places, worth):
        value = jnp.where(hit & (places == across), worth, 0).astype(f32)
        return jnp.sum(value, axis=0, keepdims=True).astype(i32)

    packs = [rows_of(kc & (fc == d) & (sc == me), by_z, local) for d in range(1, planes)]
    for d in range(1, max(gate, 1) + 1):
        packs.append(rows_of(rc & (xc == side) & (plane == gate) & (pc == gate - d), by_r, ahead))
    packs.append(rows_of(crosses & (pc == plane) & (xc == side), by_x, held))
    lands = kc & (gc == me)
    place = rank - gc * blk_dev
    straight = xc == side
    packs.append(rows_of(lands, place, jnp.where(straight, 1, 2)))
    packs.append(rows_of(lands & straight, place, held))
    packs.append(rows_of(lands & jnp.logical_not(straight), place, by_x))
    pack_ref[...] = jnp.zeros(pack_ref.shape, i32)
    for n, row in enumerate(packs):
        pack_ref[n : n + 1, :] = row

    used = x_base + (planes + 1) * cx
    spot8 = iota(misc_ref.shape, 1)
    misc_ref[...] = jnp.where(
        spot8 == 0, level, jnp.where(spot8 == 1, used, jnp.where(spot8 == 2, pick, 0))
    )

    for c in notices:
        c.wait_send()


def plan(note, count, head_count, blk_dev, caps, choices, number):
    head_dev = note.shape[0]
    everyone = count * head_count
    rows = everyone * head_dev
    planes = count // 2
    lanes = max(128, count * blk_dev)
    i32, f32 = jnp.int32, jnp.float32
    tabs = -(-2 * planes // 8) * 8
    packs = -(-(planes + max(planes // 2 - 1, 1) + 3) // 8) * 8
    shape, dma = jax.ShapeDtypeStruct, pltpu.SemaphoreType.DMA
    vmem = pl.BlockSpec(memory_space=pltpu.VMEM)
    return pl.pallas_call(
        functools.partial(plan_kernel, count, head_count, blk_dev, caps, choices),
        out_shape=(
            shape((tabs, lanes), i32), shape((head_dev, lanes), i32),
            shape((8, lanes), i32), shape((packs, lanes), i32),
        ),
        in_specs=[vmem],
        out_specs=(vmem,) * 4,
        scratch_shapes=[
            pltpu.VMEM((rows, note.shape[1]), i32),
            pltpu.VMEM((rows, lanes), f32),
            pltpu.VMEM((count * head_dev, lanes), f32), pltpu.VMEM((count * head_dev, lanes), f32),
            pltpu.VMEM((planes * head_dev, lanes), f32), pltpu.VMEM((planes * head_dev, lanes), f32),
            dma((everyone - 1,)), dma((everyone - 1,)),
        ],
        compiler_params=pltpu.CompilerParams(
            collective_id=number, has_side_effects=True,
            vmem_limit_bytes=60 * 1024 * 1024,
        ),
    )(note)


def levels(tiles, most):
    caps = []
    for part in (22, 24, 26, 27, 28, 29, 30, 31, 32, 34, 37):
        cz = min(tiles, tiles * part // 64)
        caps.append((cz, min(most, max(1, most * min(24, part // 2 + 7) // 24))))
    caps.append((tiles, most))
    return sorted(set(caps))


def body(queries, keys, values, random_holder, random_offset, keep):
    tok_dev, width_dev = queries.shape
    blk_dev = tok_dev // B
    head_dev = width_dev // DH
    count = lax.axis_size("seq")
    head_count = lax.axis_size("head")
    count_req = blk_dev * R
    total = head_dev * count_req
    tiles = head_dev * blk_dev
    most = min(tiles, head_dev * max(2, (count_req + count - 1) // count))
    planes = count // 2
    if count % 2 or planes % 2 or not fits(planes, tiles, most):
        return plain_body(queries, keys, values, random_holder, random_offset, keep)
    me = lax.axis_index("seq")
    plane, side = me // 2, me % 2
    mate = me + 1 - 2 * side
    i32 = jnp.int32
    code = random_holder * blk_dev + random_offset
    code = jnp.where((keep > 0)[None, :, None], code, -1).reshape(head_dev, count_req)
    wide = -(-(count_req + blk_dev) // 128) * 128
    note = jnp.concatenate([code, jnp.broadcast_to(keep[None], (head_dev, blk_dev))], axis=1)
    note = jnp.pad(note, ((0, 0), (0, wide - count_req - blk_dev)), constant_values=-1)
    caps, choices = levels(tiles, most), settle_levels(planes, blk_dev)
    tab, where, misc, packs = plan(
        note, count, head_count, blk_dev, caps, choices, len(caps) + len(choices)
    )

    slots_all = -(-max((planes - 1) * c[0] + (planes + 1) * c[1] for c in caps) // CHUNK) * CHUNK
    def exchanged(number, caps):
        def run(tab, k, v):
            return exchange(count, number, *caps, slots_all, blk_dev, tab, k, v)

        return run

    rand, halo_kv, glob = lax.switch(
        misc[0, 0], [exchanged(n, c) for n, c in enumerate(caps)], tab, keys, values
    )

    live = jnp.stack([me > 0, me < count - 1]).astype(i32)
    blocks = near_far(
        keep, live, where, queries, keys, values, halo_kv, glob, rand
    )
    return pack(blocks, packs, misc[0, 2], count, blk_dev, len(caps), choices)


def solution(mesh):
    in_specs = (
        P("seq", "head"),
        P("seq", "head"),
        P("seq", "head"),
        P("head", "seq", None),
        P("head", "seq", None),
        P("seq"),
    )
    out_specs = P("seq", "head")
    return jax.shard_map(body, mesh=mesh, in_specs=in_specs, out_specs=out_specs, check_vma=False)
```
